32 devices in a mesh: base: 4 (over y, x), slab: 8 (over z, core).
Axes of the slice: x: 2, y: 2, z: 4, core: 2. Of those that a mesh axis runs over, the one named last changes fastest.
Arguments:
- residual: float32 [4096, 2, 128], P(('base', 'slab')), may hold values from -6 to 6
- position: float32 [4096, 2, 128], P(('base', 'slab')), may hold values from 4 to 124
- owner: int32 [4096, 1], P(('base', 'slab')), may hold values from 0 to 31; in each aligned block of 128 rows (0 to 127, 128 to 255, ...) at most 8 rows name the same one
- tile_local: int32 [4096], P(('base', 'slab')), may hold values from 0 to 127
- xi: float32 [4096, 4096], P(('base', 'slab')), may hold values from -6 to 6
- amplitude: float32 [4096, 4096], P(('base', 'slab')), may hold values from 0.05 to 0.5
Outputs:
- gradient: float32 [4096, 4096], P(('base', 'slab'))
The draws below stay inside these ranges and needn't reach their ends.
Inputs may be any that keep to these rules, and one draw needn't show every extreme that they name: Among the blocks of one device no owner region is named by more than 8 blocks, a bound that some owner region reaches on some device.
All inputs are finite; a program needn't handle non-finite values.
Results may differ from the reference program's by a relative error of at most 0.00065.
Values sent between devices are 32-bit elements; how exact they have to be, the bound alone decides.
A program may use at most 128 MiB of HBM per device.

```python
import math
import jax
import jax.numpy as jnp
import numpy as np
from jax import lax

G = 8192
IMG = 4096
TILE = 128
VB = 128
BLK_DEV = 128
BLOCKS = 4096
CAP = 8
TILES_REG = 128
N_BASE = 4
N_SLAB = 8
DEVICES = 32


def with_ends(values, own_key, low, top_value):
    longest = values.shape.index(max(values.shape))
    spots = []
    for shift in (0, 1):
        where = [jax.random.randint(jax.random.fold_in(own_key, axis), (), 0, length) for axis, length in enumerate(values.shape)]
        where[longest] = (where[longest] + shift) % values.shape[longest]
        spots.append(tuple(where))
    return values.at[spots[0]].set(low).at[spots[1]].set(top_value)


def block_scale(key, dims, split, least, top_value):
    def one(axis_at, blocks):
        heights = jax.random.uniform(jax.random.fold_in(jax.random.fold_in(key, 6), axis_at), (blocks,), jnp.float32, least / len(split), top_value / len(split))
        return jnp.repeat(jnp.exp(heights), dims[axis_at] // blocks).reshape((-1,) + (1,) * (len(dims) - axis_at - 1))

    gain = one(*split[0])
    for cut in split[1:]:
        gain = gain * one(*cut)
    return gain


def deal_out(key, own, number, rows, count, top, reach, skew):
    ranking = jax.random.permutation(key, count)
    packed, usual = portions_of(count, rows * top, reach, skew, True), portions_of(count, rows * top, reach, skew, False)
    places = jnp.arange(count)

    def named(tallies, rotation):
        used = int((tallies > 0).sum())
        fixed = max(1, used // 4)
        moved = fixed + (places - fixed + rotation * (used - fixed)) % max(1, count - fixed)
        return jnp.zeros((count,), jnp.int32).at[ranking[jnp.where(places < fixed, places, moved)]].set(jnp.asarray(tallies, jnp.int32))

    tallies = jnp.where(number % 4 == 0, named(packed, number // 4), named(usual, number - number // 4 - 1))
    mixed = jax.random.permutation(jax.random.fold_in(own, 3), count)
    donor, sink = mixed[0:count // 2 * 2:2], mixed[1:count // 2 * 2:2]
    room = jnp.minimum(tallies[donor] - 1, reach - tallies[sink]) // 2
    room = jnp.where((donor == ranking[0]) | (sink == ranking[0]) | (tallies[sink] == 0), 0, jnp.maximum(room, 0))
    moved = jax.random.randint(jax.random.fold_in(own, 4), (count // 2,), 0, 1 << 20) % (room + 1)
    tallies = tallies.at[donor].add(-moved).at[sink].add(moved)
    members = jnp.searchsorted(jnp.cumsum(tallies), jnp.arange(rows * top), side="right").astype(jnp.int32)
    table = members.reshape(top, rows).T
    table = table[jax.random.permutation(jax.random.fold_in(own, 1), rows)]
    rotation = jax.random.randint(jax.random.fold_in(own, 2), (rows, 1), 0, top)
    return jnp.take_along_axis(table, (jnp.arange(top)[None, :] + rotation) % top, axis=1)


def portions_of(amount, total, limit, slope, full):
    weights = [(1 << 20) // math.isqrt(standing ** slope) + 1 for standing in range(1, amount + 1)]
    largest = limit if full else min(limit, max(-(-total // amount), total * weights[0] // sum(weights)))
    least = 1 if total - largest >= amount - 1 else 0
    holding, rest = [largest] + [least] * (amount - 1), total - largest - least * (amount - 1)
    while rest > 0:
        movable = [i for i in range(1, amount) if holding[i] < largest] or [i for i in range(1, amount) if holding[i] < limit]
        whole, remaining = sum([weights[i] for i in movable]), rest
        for i in movable:
            addition = min(limit - holding[i], max(1, remaining * weights[i] // whole), rest)
            holding[i] = holding[i] + addition
            rest = rest - addition
    return np.array(holding)


def gaussian(rng, shape, width, limit, split=(), kind=jnp.bfloat16):
    result = width * jax.random.normal(rng, shape, jnp.float32)
    if split:
        result = result * block_scale(rng, shape, split, -0.22, 0.18)
    return jnp.clip(result, -limit, limit).astype(kind)


def setup_inputs(seed: int = 0) -> dict:
    keys = jax.random.split(jax.random.key(seed), 7)
    residual = gaussian(keys[0], (BLOCKS, 2, VB), 1.0, 6.0, ((0, 32),), jnp.float32)
    position = jnp.clip(4.0 + 120.0 * jax.random.uniform(keys[1], (BLOCKS, 2, VB), jnp.float32) ** block_scale(keys[1], (BLOCKS, 2, VB), ((0, 32),), -0.2, 0.2), 4.0, 124.0)
    owner_keys = jax.random.split(jax.random.fold_in(keys[2], 1), BLOCKS // BLK_DEV)
    owner_turns = jax.random.permutation(jax.random.fold_in(keys[2], 3), BLOCKS // BLK_DEV)
    owner = jax.vmap(lambda own, number: deal_out(jax.random.fold_in(keys[2], 2), own, number, BLK_DEV, DEVICES, 1, CAP, 2))(owner_keys, owner_turns).reshape((BLOCKS, 1))
    tile_local = with_ends(jax.random.randint(keys[3], (BLOCKS,), 0, TILES_REG), jax.random.fold_in(keys[3], 1), 0, TILES_REG - 1).astype(jnp.int32)
    xi = gaussian(keys[4], (IMG, IMG), 1.0, 6.0, ((0, 32),), jnp.float32)
    amplitude = jnp.clip(jnp.exp(math.log(0.5) - 2.3025851 * jax.random.uniform(keys[5], (IMG, IMG), jnp.float32) ** block_scale(keys[5], (IMG, IMG), ((0, 32),), -0.2, 0.2)), 0.05, 0.5)
    return dict(residual=residual, position=position, owner=owner, tile_local=tile_local, xi=xi, amplitude=amplitude)


def taps(offsets):
    cells = jnp.arange(TILE, dtype=jnp.float32)
    scaled = (cells[None, :, None] - offsets[:, None, :]) * 0.25
    return jnp.maximum(1.0 - scaled * scaled, 0.0) ** 3


def reference(residual, position, owner, tile_local, xi, amplitude):
    rows_tiles = G // N_SLAB // TILE
    cols_tiles = G // N_BASE // TILE
    across = G // TILE
    target = owner[:, 0]
    tile_row = ((target % N_SLAB) * rows_tiles + tile_local // cols_tiles).astype(jnp.int32)
    tile_col = ((target // N_SLAB) * cols_tiles + tile_local % cols_tiles).astype(jnp.int32)

    def step(total, index):
        start = (index * BLK_DEV).astype(jnp.int32)
        values = lax.dynamic_slice_in_dim(residual, start, BLK_DEV, 0)
        places = lax.dynamic_slice_in_dim(position, start, BLK_DEV, 0)
        rows = lax.dynamic_slice_in_dim(tile_row, start, BLK_DEV, 0)
        cols = lax.dynamic_slice_in_dim(tile_col, start, BLK_DEV, 0)
        row_taps = taps(places[:, 0, :])
        col_taps = taps(places[:, 1, :])
        weighted = jnp.concatenate([col_taps * values[:, 0:1, :], col_taps * values[:, 1:2, :]], axis=1)
        subgrid = jnp.einsum("grv,gkv->grk", row_taps, weighted, precision=lax.Precision.HIGHEST)
        total = total.at[rows, cols].add(subgrid.reshape(BLK_DEV, TILE, 2, TILE))
        return total, None

    empty = jnp.zeros((across, across, TILE, 2, TILE), jnp.float32)
    tiles = lax.scan(step, empty, jnp.arange(DEVICES, dtype=jnp.int32))[0]
    grid = tiles.transpose(3, 0, 2, 1, 4).reshape(2, G, G)
    wave = jnp.fft.ifft2(grid[0] + 1j * grid[1])
    lower = G // 4
    back = jnp.real(wave[lower:lower + IMG, lower:lower + IMG]) * G
    spectrum = jnp.fft.fft2(amplitude * xi)
    sky = jnp.exp((jnp.real(spectrum) - jnp.imag(spectrum)) / IMG)
    folded = jnp.fft.fft2(sky * back)
    return amplitude * (jnp.real(folded) - jnp.imag(folded)) / IMG
```

```python
import functools
import math

import jax
import jax.numpy as jnp
import numpy as np
from jax import lax
from jax.experimental import pallas as pl
from jax.experimental.pallas import tpu as pltpu
from jax.sharding import PartitionSpec as P

G = 8192
TILE = 128
both = ("base", "slab")
fine = lax.Precision.HIGHEST


def trig(product, modulus):
    angle = (product % modulus).astype(np.float64) * (2.0 * np.pi / modulus)
    return np.cos(angle), np.sin(angle)


def column_table(n, size):
    depth = size // n
    half = depth // 2
    i = np.arange(half)[None, :]
    j = np.arange(n)[:, None]
    low = n * i + j
    high = (-low) % size
    high[0, 0] = size // 2
    return np.concatenate([low, high], axis=1)


def row_tables(n, size):
    depth = size // n
    cols = column_table(n, size)
    oc, osn = trig(np.arange(n)[:, None] * np.arange(n)[None, :], n)
    outer = np.stack([oc, osn], axis=1)
    prod = np.arange(depth)[None, :, None] * cols[:, None, :]
    c, s = trig(prod, size)
    sign = np.where(np.arange(depth) < depth // 2, 1.0, -1.0)[None, None, :]
    inner = np.stack([c + s, sign * (c - s)], axis=1)
    return outer.astype(np.float32), inner.astype(np.float32)


def grid_row_tables(n, size):
    depth = G // n
    cols = column_table(n, size)
    half = cols.shape[1] // 2
    oc, osn = trig(np.arange(n)[:, None] * np.arange(n)[None, :], n)
    outer = np.stack([np.stack([oc, osn], 1), np.stack([-osn, oc], 1)], 0)
    low = cols[:, :half]
    high = cols[(-np.arange(n)) % n, half:]
    a = np.arange(depth)[None, :, None]
    out = []
    for part in (low, high):
        c, s = trig(a * (part[:, None, :] + G // 4), G)
        out.append(np.stack([np.concatenate([c, s], 2), np.concatenate([-s, c], 2)], 1))
    return outer.astype(np.float32), np.concatenate(out, axis=3).astype(np.float32)


def taps(cells, offsets):
    scaled = (cells - offsets) * 0.25
    kept = jnp.maximum(1.0 - scaled * scaled, 0.0)
    return kept * kept * kept


def split_three(x):
    high = x.astype(jnp.bfloat16)
    rest = x - high.astype(jnp.float32)
    middle = rest.astype(jnp.bfloat16)
    return high, middle, (rest - middle.astype(jnp.float32)).astype(jnp.bfloat16)


def grid_kernel(rows, info_ref, list_ref, data_ref, out_ref):
    count = info_ref[0]
    first = info_ref[1].astype(jnp.float32)
    out_ref[...] = jnp.zeros_like(out_ref)
    row_cells = lax.broadcasted_iota(jnp.int32, (rows, TILE), 0).astype(jnp.float32) + first
    col_cells = lax.broadcasted_iota(jnp.int32, (TILE, TILE), 0).astype(jnp.float32)

    def step(k, carry):
        packed = list_ref[k]
        index = packed // 256
        col = (packed // 2) % 128
        flip = (packed % 2).astype(jnp.float32)
        sign = 1.0 - 2.0 * flip
        start = 128.0 * flip
        block = data_ref[index]
        value = block[0:2, :]
        place = block[2:4, :]
        row_taps = taps(row_cells * sign + start, place[0:1, :])
        col_taps = taps(col_cells * sign + start, place[1:2, :])
        weighted = jnp.concatenate(
            [col_taps * value[0:1, :], col_taps * (value[1:2, :] * sign)], axis=0
        )
        rh, rm, rl = split_three(row_taps)
        wh, wm, wl = split_three(weighted)
        left = jnp.concatenate([rh, rh, rh, rm, rm, rl], axis=1)
        right = jnp.concatenate([wh, wm, wl, wh, wm, wh], axis=1)
        sub = lax.dot_general(
            left, right, (((1,), (1,)), ((), ())), preferred_element_type=jnp.float32
        )
        out_ref[0, col] += sub[:, :TILE]
        out_ref[1, col] += sub[:, TILE:]
        return carry

    lax.fori_loop(0, count, step, 0)


def grid_rows(info, table, gathered, rows):
    tiles = G // TILE
    smem = pl.BlockSpec(memory_space=pltpu.SMEM)
    vmem = pl.BlockSpec(memory_space=pltpu.VMEM)
    return pl.pallas_call(
        functools.partial(grid_kernel, rows),
        out_shape=jax.ShapeDtypeStruct((2, tiles, rows, TILE), jnp.float32),
        in_specs=[smem, smem, vmem],
        out_specs=vmem,
        compiler_params=pltpu.CompilerParams(vmem_limit_bytes=56 * 1024 * 1024),
        cost_estimate=pl.CostEstimate(
            flops=2 * 10**10, bytes_accessed=16 * 2**20, transcendentals=0
        ),
        name="grid_rows",
    )(info, table, gathered)


def einsum(form, *args, precision=lax.Precision.HIGH):
    return jnp.einsum(form, *args, precision=precision, preferred_element_type=jnp.float32)


def general(residual, position, owner, tile_local, xi, amplitude):
    n = lax.axis_size(both)
    n_base = lax.axis_size("base")
    n_slab = lax.axis_size("slab")
    me = lax.axis_index(both)
    rows, size = xi.shape
    depth = size // n
    half = depth // 2
    tiles = G // TILE

    region_rows = G // n_slab // TILE
    region_cols = G // n_base // TILE
    target = owner[:, 0]
    tile_row = (target % n_slab) * region_rows + tile_local // region_cols
    tile_col = (target // n_slab) * region_cols + tile_local % region_cols
    flip = tile_row >= tiles // 2
    tile_row = jnp.where(flip, tiles - 1 - tile_row, tile_row)
    tile_col = jnp.where(flip, tiles - 1 - tile_col, tile_col)
    code = tile_row * 256 + tile_col * 2 + flip.astype(jnp.int32)
    codes = lax.all_gather(code, both, axis=0, tiled=True)
    payload = jnp.concatenate([residual, position], axis=1)
    codes, payload = lax.optimization_barrier((codes, payload))
    gathered = lax.all_gather(payload, both, axis=0, tiled=True)
    blocks = codes.shape[0]
    grid_depth = G // 2 // n
    first_row = me * grid_depth
    mine = (codes // 256 == first_row // TILE).astype(jnp.int32)
    rank = jnp.where(mine == 1, jnp.cumsum(mine) - 1, -1)
    packed = lax.broadcasted_iota(jnp.int32, (blocks,), 0) * 256 + codes % 256
    spots = lax.broadcasted_iota(jnp.int32, (blocks, blocks), 0)
    table = jnp.sum(jnp.where(spots == rank[None, :], packed[None, :], 0), axis=1)
    info = jnp.stack([jnp.sum(mine), first_row % TILE]).astype(jnp.int32)

    outer, inner = row_tables(n, size)
    spectrum = (amplitude * xi).reshape(rows, n, depth)
    mid = einsum("rba,bqc->qcra", spectrum, outer)
    sent = einsum("cra,cae->cre", mid[0], inner[:, 0]) + einsum("cra,cae->cre", mid[1], inner[:, 1])
    sent, gathered = lax.optimization_barrier((sent, gathered))
    field = lax.all_to_all(sent, both, split_axis=0, concat_axis=0, tiled=True)
    field = field.reshape(size, depth)
    lane = lax.broadcasted_iota(jnp.int32, (1, depth), 1)
    still = (me == 0) & (lane % half == 0)

    def mirror(x):
        return jnp.where(still, x, jnp.roll(x, half, axis=-1))

    c_len = 128
    d_len = size // c_len
    bc, bs = (x.astype(np.float32) for x in trig(np.arange(c_len)[:, None] * np.arange(c_len)[None, :], c_len))
    shape = (c_len, d_len, depth)
    n0 = c_len * np.arange(d_len)[None, :] + np.arange(c_len)[:, None]
    ic, isn = (x.astype(np.float32) for x in trig(n0[:, :, None] * np.arange(d_len)[None, None, :], size))
    pair = jnp.stack([field.reshape(shape), mirror(field).reshape(shape)])
    first = np.stack([np.stack([bc, bs], 1), np.stack([bs, -bc], 1)], 0)
    turned = einsum("qbal,qbsc->csal", pair, first)
    second = np.stack([ic, -isn], axis=2)
    power = einsum("csal,cdsa->cdl", turned, second)
    sky = jnp.exp(power / size)

    grid = grid_rows(info, table, gathered, grid_depth)
    outer_g, inner_g = grid_row_tables(n, size)
    parts = tiles // n if tiles >= n else 1
    inner_len = G // n
    if inner_len >= TILE:
        view = grid.reshape(2, n, inner_len // TILE, grid_depth, TILE)
    else:
        flat = grid.transpose(0, 2, 1, 3).reshape(2, grid_depth, n, inner_len)
        view = flat.transpose(0, 2, 1, 3)[:, :, None]
        parts = 1
    lanes = view.shape[-1]
    stage = einsum("qbpra,qbsc->cspra", view, outer_g, precision=fine)
    inner_g = inner_g.reshape(n, 2, parts, lanes, 2 * depth)
    halves = einsum("cspra,cspae->cre", stage, inner_g, precision=fine)
    high = halves[:, :, depth:]
    high = jnp.concatenate([high[:1], jnp.flip(high[1:], axis=0)], axis=0)
    halves = jnp.concatenate([halves[:, :, :depth], high], axis=2)
    got = lax.all_to_all(halves, both, split_axis=0, concat_axis=0, tiled=True)
    got = got.reshape(size, 2 * depth)
    real = jnp.concatenate([got[:, :half], got[:, depth : depth + half]], axis=1)
    imag = jnp.concatenate([got[:, half:depth], got[:, depth + half :]], axis=1)
    wide = G // c_len
    deep = size // wide
    gc, gs = (x.astype(np.float32) for x in trig(np.arange(deep)[:, None] * np.arange(c_len)[None, :], c_len))
    first_g = np.stack([np.stack([gc, gs], 1), np.stack([-gs, gc], 1)], 0)
    whole = jnp.stack([real.reshape(deep, wide, depth), imag.reshape(deep, wide, depth)])
    turned_g = einsum("qbal,qbsc->csal", whole, first_g, precision=fine)
    ac, asn = trig((n0 + G // 4)[:, :, None] * np.arange(wide)[None, None, :], G)
    second_g = (np.stack([ac, -asn], axis=2) / G).astype(np.float32)
    back = einsum("csal,cdsa->cdl", turned_g, second_g, precision=fine)

    z = sky * back
    pz = einsum("cdl,cda->cal", z, ic)
    qz = einsum("cdl,cda->cal", z, isn)
    joined = jnp.stack([pz + mirror(qz), mirror(pz) - qz])
    fold = einsum("qcal,qcb->bal", joined, np.stack([bc, bs]))
    folded = lax.all_to_all(
        fold.reshape(n, rows, depth), both, split_axis=0, concat_axis=0, tiled=True
    )
    ends = einsum("jre,jqae->qjra", folded, inner)
    final = einsum("qjra,bqj->rba", ends, outer)
    return amplitude * final.reshape(rows, size) / size


MESH = pl.DeviceIdType.MESH
parts = ("base", "half", "quad")


def exchange_kernel(nb, ns, send_ref, out_ref, bsend, brecv, usend, dsend, lrecv, hrecv, psend, precv, lsem):
    quads = ns // 2
    nz = ns // 2
    base = lax.axis_index("base")
    slab = lax.axis_index("half") * quads + lax.axis_index("quad")
    z = slab // 2
    core = slab % 2

    def at(b, s):
        return (b, s // quads, s % quads)

    def copy(source, target, here, there, device):
        return pltpu.make_async_remote_copy(
            src_ref=source, dst_ref=target, send_sem=here, recv_sem=there, device_id=device, device_id_type=MESH
        )

    def crossing(k):
        other = (base + k) % nb
        return copy(send_ref.at[other], out_ref.at[slab, base], bsend.at[k], brecv.at[k], at(other, slab))

    def arriving(k):
        from_base = (base - k + nb) % nb
        return copy(send_ref.at[base], out_ref.at[slab, from_base], bsend.at[k], brecv.at[k], at(from_base, slab))

    def block(origin, k):
        return out_ref.at[2 * origin + core, (base - k + nb) % nb]

    def upward(s, k):
        part = block(z - s, k)
        return copy(part, part, usend.at[s, k], lrecv.at[s + 1, k], at(base, slab + 2))

    def downward(s, k):
        part = block(z + s, k)
        return copy(part, part, dsend.at[s, k], hrecv.at[s + 1, k], at(base, slab - 2))

    def from_below(s, k):
        part = block(z - s, k)
        return copy(part, part, usend.at[s, k], lrecv.at[s, k], at(base, slab - 2))

    def from_above(s, k):
        part = block(z + s, k)
        return copy(part, part, dsend.at[s, k], hrecv.at[s, k], at(base, slab + 2))

    def across(origin, k):
        part = block(origin, k)
        return copy(part, part, psend.at[origin, k], precv.at[origin, k], at(base, slab + 1 - 2 * core))

    def from_partner(origin, k):
        part = out_ref.at[2 * origin + 1 - core, (base - k + nb) % nb]
        return copy(part, part, psend.at[origin, k], precv.at[origin, k], at(base, slab + 1 - 2 * core))

    barrier = pltpu.get_barrier_semaphore()
    for k in range(1, nb):
        pl.semaphore_signal(barrier, inc=1, device_id=at((base + k) % nb, slab), device_id_type=MESH)
    pl.semaphore_signal(barrier, inc=1, device_id=at(base, slab + 1 - 2 * core), device_id_type=MESH)

    @pl.when(z < nz - 1)
    def _():
        pl.semaphore_signal(barrier, inc=1, device_id=at(base, slab + 2), device_id_type=MESH)

    @pl.when(z > 0)
    def _():
        pl.semaphore_signal(barrier, inc=1, device_id=at(base, slab - 2), device_id_type=MESH)

    pl.semaphore_wait(barrier, nb + jnp.where(z < nz - 1, 1, 0) + jnp.where(z > 0, 1, 0))

    for k in range(1, nb):
        crossing(k).start()
    own = pltpu.make_async_copy(send_ref.at[base], out_ref.at[slab, base], lsem)
    own.start()

    def pass_on(s, k, ascending, descending):
        if ascending:
            @pl.when((z - s >= 0) & (z < nz - 1))
            def _():
                upward(s, k).start()

        if descending:
            @pl.when((z + s < nz) & (z > 0))
            def _():
                downward(s, k).start()

    for k in range(nb):
        if k == 0:
            own.wait()
        else:
            arriving(k).wait_recv()
        pass_on(0, k, True, True)
        across(z, k).start()
    for s in range(1, nz):
        for k in range(nb):
            @pl.when(z - s >= 0)
            def _():
                from_below(s, k).wait_recv()
                if s < nz - 1:
                    pass_on(s, k, True, False)
                across(z - s, k).start()

            @pl.when(z + s < nz)
            def _():
                from_above(s, k).wait_recv()
                if s < nz - 1:
                    pass_on(s, k, False, True)
                across(z + s, k).start()

    for origin in range(nz):
        for k in range(nb):
            from_partner(origin, k).wait_recv()
    for k in range(1, nb):
        crossing(k).wait_send()
    for s in range(nz - 1):
        for k in range(nb):
            @pl.when((z - s >= 0) & (z < nz - 1))
            def _():
                upward(s, k).wait_send()

            @pl.when((z + s < nz) & (z > 0))
            def _():
                downward(s, k).wait_send()

    for origin in range(nz):
        for k in range(nb):
            across(origin, k).wait_send()


def exchange(sent, ns):
    nb = sent.shape[0]
    nz = ns // 2
    dma = pltpu.SemaphoreType.DMA
    vmem = pl.BlockSpec(memory_space=pltpu.VMEM)
    return pl.pallas_call(
        functools.partial(exchange_kernel, nb, ns),
        out_shape=jax.ShapeDtypeStruct((ns,) + sent.shape, jnp.float32),
        in_specs=[vmem],
        out_specs=vmem,
        scratch_shapes=[
            dma((nb,)), dma((nb,)), dma((nz, nb)), dma((nz, nb)), dma((nz, nb)), dma((nz, nb)),
            dma((nz, nb)), dma((nz, nb)), dma,
        ],
        compiler_params=pltpu.CompilerParams(collective_id=0, has_side_effects=True, vmem_limit_bytes=16 << 20),
        name="exchange",
    )(sent)


def two_parts(x):
    high = x.astype(jnp.bfloat16)
    return high, (x - high.astype(jnp.float32)).astype(jnp.bfloat16)


def times(x, c, s):
    return x[0] * c - x[1] * s, x[0] * s + x[1] * c


def turn(x, angle):
    c, s = math.cos(angle), math.sin(angle)
    return times(x, c, s)


def add(x, y):
    return x[0] + y[0], x[1] + y[1]


def sub(x, y):
    return x[0] - y[0], x[1] - y[1]


def four(x):
    s0, d0, s1, d1 = add(x[0], x[2]), sub(x[0], x[2]), add(x[1], x[3]), sub(x[1], x[3])
    i1 = (-d1[1], d1[0])
    return [add(s0, s1), add(d0, i1), sub(s0, s1), sub(d0, i1)]


def sixteen(x):
    rows = []
    for b0 in range(4):
        y = four([x[4 * b1 + b0] for b1 in range(4)])
        rows.append([y[a0] if a0 * b0 == 0 else turn(y[a0], 2 * math.pi * a0 * b0 / 16) for a0 in range(4)])
    out = [None] * 16
    for a0 in range(4):
        y = four([rows[b0][a0] for b0 in range(4)])
        for a1 in range(4):
            out[a0 + 4 * a1] = y[a1]
    return out


def grid_rows_kernel(info_ref, list_ref, first_ref, data_ref, turn_ref, undo_ref, weight_ref, out_ref, grid_ref):
    count = info_ref[0]
    parity = info_ref[1]
    grid_ref[...] = jnp.zeros_like(grid_ref)
    cells = lax.broadcasted_iota(jnp.int32, (TILE, TILE), 0).astype(jnp.float32) * 0.25
    half = grid_ref.shape[1]

    def bump(offsets):
        d = cells - offsets
        kept = jnp.maximum(1.0 - d * d, 0.0)
        return kept * kept * kept

    def steps(offsets):
        offsets = offsets * 0.25
        return bump(offsets) - bump(offsets - 0.25)

    def one(k):
        packed = list_ref[k]
        col = packed % 64
        rest = packed // 64
        odd = jnp.where(col >= half, parity, 0)
        sign = jnp.where(k < count, 1 - 2 * odd, 0).astype(jnp.float32)
        block = data_ref[rest // 2]
        value = block[0:2, :] * sign
        row_taps = steps(block[2:3, :])
        col_taps = steps(block[3:4, :])
        weighted = jnp.concatenate([col_taps * value[0:1, :], col_taps * value[1:2, :]], axis=0)
        rh, rl = two_parts(row_taps)
        wh, wl = two_parts(weighted)
        left = jnp.concatenate([rh, rh, rl], axis=1)
        right = jnp.concatenate([wh, wl, wh], axis=1)
        made = lax.dot_general(left, right, (((1,), (1,)), ((), ())), preferred_element_type=jnp.float32)
        return made, jnp.where(col >= half, col - half, col), pl.multiple_of((rest % 2) * TILE, TILE)

    def step(k, carry):
        made = [one(2 * k + u) for u in range(2)]
        for sub_grid, col, start in made:
            grid_ref[0, col, pl.ds(start, TILE), :] += sub_grid[:, :TILE]
            grid_ref[1, col, pl.ds(start, TILE), :] += sub_grid[:, TILE:]
        return carry

    lax.fori_loop(0, (count + 1) // 2, step, 0)

    depth = half // 2
    rows = grid_ref.shape[2]

    def outer(k, carry):
        spot = pl.ds(pl.multiple_of(k * 8, 8), 8)
        for side in range(2):
            x = []
            for b in range(depth):
                value = grid_ref[0, 2 * b + side, spot, :], grid_ref[1, 2 * b + side, spot, :]
                x.append(times(value, first_ref[b, 0], first_ref[b, 1]))
            for a, value in enumerate(sixteen(x)):
                c = turn_ref[a, side : side + 1, :]
                s = turn_ref[a, 2 + side : 3 + side, :]
                value = times(value, c, s)
                grid_ref[0, 2 * a + side, spot, :] = value[0]
                grid_ref[1, 2 * a + side, spot, :] = value[1]
        return carry

    lax.fori_loop(0, rows // 8, outer, 0)

    def inner(a, carry):
        mirrored = depth - parity - a
        mirrored = jnp.where(mirrored == depth, 0, mirrored)
        which = jnp.where((a == 0) & (parity == 0), 1, 0)
        weight = weight_ref[which]
        for part in range(rows // TILE):
            spot = pl.ds(part * TILE, TILE)
            x = jnp.concatenate([grid_ref[q, 2 * a + side, spot, :] for q in range(2) for side in range(2)], axis=1)
            high, low = two_parts(x)
            made = jnp.dot(jnp.concatenate([high, low, high], axis=1), weight, preferred_element_type=jnp.float32)
            mid = TILE // 2
            made = times((made[:, :TILE], made[:, TILE:]), undo_ref[a, 0:1, :], undo_ref[a, 1:2, :])
            for q in range(2):
                out_ref[a, spot, q * TILE : q * TILE + mid] = made[q][:, :mid]
                out_ref[mirrored, spot, q * TILE + mid : (q + 1) * TILE] = made[q][:, mid:]
        return carry

    lax.fori_loop(0, depth, inner, 0)


def split_table(x):
    high = x.astype(np.float32).astype(jnp.bfloat16)
    low = (x - high.astype(np.float64)).astype(np.float32).astype(jnp.bfloat16)
    return high, low


def undone(pixels):
    c, s = trig(pixels + G // 4, G)
    return 1.0 / (1.0 - (c - 1j * s))


def grid_row_weights(n, size):
    depth = n // 2
    span = G // 2 // depth
    half = size // n // 2
    alpha = np.arange(span)
    turns, firsts, undos = [], [], []
    for p in range(2):
        j = 2 * np.arange(depth) + p
        c, s = trig(j[:, None] * alpha[None, :], G)
        turns.append(np.concatenate([c.reshape(depth, 2, TILE), s.reshape(depth, 2, TILE)], axis=1))
        firsts.append(np.stack(trig(np.arange(depth) * p, n), axis=1))
        low = n * np.arange(half)[None, :] + j[:, None]
        high = size - n * np.arange(half)[None, :] - ((-j) % n)[:, None]
        if p == 0:
            low[0, 0], high[0, 0] = 0, size // 2
        undo = undone(np.concatenate([low, high], axis=1))
        undos.append(np.stack([undo.real, undo.imag], axis=1))
    weights = []
    i = np.arange(half)
    for special in range(2):
        low = n * i
        high = size - n * i - (0 if special else n)
        if special:
            high[0] = size // 2
        parts_re, parts_im = [], []
        for cols in (low, high):
            c, s = trig(alpha[:, None] * (cols[None, :] + G // 4), G)
            parts_re.append(np.concatenate([c, -s], axis=0))
            parts_im.append(np.concatenate([s, c], axis=0))
        w = np.concatenate(parts_re + parts_im, axis=1)
        high_part, low_part = split_table(w)
        weights.append(np.concatenate([high_part, high_part, low_part], axis=0))
    turns, firsts, undos = (np.stack(x).astype(np.float32) for x in (turns, firsts, undos))
    return turns, firsts, undos, np.stack(weights)


def grid_rows_two(info, table, first, data, turns, undos, weights):
    depth = turns.shape[0]
    rows = 2 * TILE
    smem = pl.BlockSpec(memory_space=pltpu.SMEM)
    vmem = pl.BlockSpec(memory_space=pltpu.VMEM)
    return pl.pallas_call(
        grid_rows_kernel,
        out_shape=jax.ShapeDtypeStruct((depth, rows, 2 * TILE), jnp.float32),
        in_specs=[smem, smem, smem, vmem, vmem, vmem, vmem],
        out_specs=vmem,
        scratch_shapes=[pltpu.VMEM((2, 2 * depth, rows, TILE), jnp.float32)],
        compiler_params=pltpu.CompilerParams(vmem_limit_bytes=40 << 20),
        cost_estimate=pl.CostEstimate(flops=2 * 10**10, bytes_accessed=16 * 2**20, transcendentals=0),
        name="grid_rows_two",
    )(info, table, first, data, turns, undos, weights)


def shared(residual, position, owner, tile_local, xi, amplitude):
    n = lax.axis_size(parts)
    n_base = lax.axis_size("base")
    n_slab = lax.axis_size("half") * lax.axis_size("quad")
    quads = lax.axis_size("quad")
    base, parity, quad = (lax.axis_index(axis) for axis in parts)
    place = 2 * (base * quads + quad) + parity
    order = np.array([2 * (b * quads + q) + h for b in range(n_base) for h in range(2) for q in range(quads)])
    rows, size = xi.shape
    depth = size // n
    half = depth // 2
    tiles = G // TILE

    blocks = residual.shape[0]
    region_rows = G // n_slab // TILE
    region_cols = G // n_base // TILE
    room = 2 * n_base * (2 * blocks // n)
    target = owner[:, 0]
    tile_row = (target % n_slab) * region_rows + tile_local // region_cols
    tile_col = (target // n_slab) * region_cols + tile_local % region_cols
    flip = tile_row >= tiles // 2
    tile_row = jnp.where(flip, tiles - 1 - tile_row, tile_row)
    tile_col = jnp.where(flip, tiles - 1 - tile_col, tile_col)
    line = tile_row // n_slab
    code = (tile_row % n_slab) * tiles + tile_col
    flipped = flip[:, None]
    payload = jnp.stack(
        [
            residual[:, 0],
            jnp.where(flipped, -residual[:, 1], residual[:, 1]),
            jnp.where(flipped, TILE - position[:, 0], position[:, 0]),
            jnp.where(flipped, TILE - position[:, 1], position[:, 1]),
        ],
        axis=1,
    )
    earlier = (line[:, None] == line[None, :]) & (np.arange(blocks)[:, None] > np.arange(blocks)[None, :])
    slot = line * room + jnp.sum(earlier.astype(jnp.int32), axis=1)
    chosen = slot[None, :] == lax.broadcasted_iota(jnp.int32, (n_base * room, blocks), 0)
    moved = jnp.dot(chosen.astype(jnp.float32), payload.reshape(blocks, 4 * TILE), precision=fine)
    codes = jnp.sum(jnp.where(chosen, code[None, :] + 1, 0), axis=1) - 1
    codes = jnp.pad(codes.astype(jnp.float32).reshape(n_base, 1, 1, room), ((0, 0), (0, 0), (0, 3), (0, TILE - room)))
    sent = jnp.concatenate([moved.reshape(n_base, room, 4, TILE), codes], axis=1)
    got = exchange(sent, n_slab)

    outer, inner = row_tables(n, size)
    outer, inner = outer[:, :, order], inner[order]
    spectrum = (amplitude * xi).reshape(rows, n, depth)
    mid = einsum("rba,bqc->qcra", spectrum, outer)
    sent = einsum("cra,cae->cre", mid[0], inner[:, 0]) + einsum("cra,cae->cre", mid[1], inner[:, 1])
    sent, got = lax.optimization_barrier((sent, got))
    field = lax.all_to_all(sent, parts, split_axis=0, concat_axis=0, tiled=True)
    field = field.reshape(size, depth)

    sources = n_slab * n_base
    codes = got[:, :, room, 0, :room].reshape(sources, room).astype(jnp.int32)
    mine = (codes >= 0) & (codes // tiles // 2 == quad)
    ones = mine.astype(jnp.float32)
    before = jnp.dot(ones, np.triu(np.ones((room, room), np.float32), 1), precision=fine)
    above = jnp.dot(np.tril(np.ones((sources, sources), np.float32), -1), ones, precision=fine)
    rank = (before + jnp.sum(above, axis=1, keepdims=True)).astype(jnp.int32)
    rank = jnp.where(mine, rank, -1).reshape(-1)
    index = lax.broadcasted_iota(jnp.int32, (sources, room), 0) * (room + 1) + lax.broadcasted_iota(jnp.int32, (sources, room), 1)
    packed = (index * (2 * tiles) + codes % (2 * tiles)).reshape(-1)
    spots = lax.broadcasted_iota(jnp.int32, (sources * room, sources * room), 0)
    table = jnp.sum(jnp.where(spots == rank[None, :], packed[None, :], 0), axis=1)
    table = jnp.pad(table, (0, 2))
    info = jnp.stack([jnp.sum(mine.astype(jnp.int32)), parity]).astype(jnp.int32)

    turns, firsts, undos, weights = grid_row_weights(n, size)
    halves = grid_rows_two(
        info,
        table,
        lax.dynamic_index_in_dim(jnp.asarray(firsts), parity, 0, keepdims=False),
        got.reshape(sources * (room + 1), 4, TILE),
        lax.dynamic_index_in_dim(jnp.asarray(turns), parity, 0, keepdims=False),
        lax.dynamic_index_in_dim(jnp.asarray(undos), parity, 0, keepdims=False),
        jnp.asarray(weights),
    )
    whole = lax.all_to_all(halves, ("base", "quad"), split_axis=0, concat_axis=0, tiled=True)

    lane = lax.broadcasted_iota(jnp.int32, (1, depth), 1)
    still = (place == 0) & (lane % half == 0)

    def mirror(x):
        return jnp.where(still, x, jnp.roll(x, half, axis=-1))

    c_len = 128
    d_len = size // c_len
    bc, bs = (x.astype(np.float32) for x in trig(np.arange(c_len)[:, None] * np.arange(c_len)[None, :], c_len))
    shape = (c_len, d_len, depth)
    n0 = c_len * np.arange(d_len)[None, :] + np.arange(c_len)[:, None]
    ic, isn = (x.astype(np.float32) for x in trig(n0[:, :, None] * np.arange(d_len)[None, None, :], size))
    pair = jnp.stack([field.reshape(shape), mirror(field).reshape(shape)])
    first = np.stack([np.stack([bc, bs], 1), np.stack([bs, -bc], 1)], 0)
    turned = einsum("qbal,qbsc->csal", pair, first)
    second = np.stack([ic, -isn], axis=2)
    power = einsum("csal,cdsa->cdl", turned, second)
    sky = jnp.exp(power / size)

    wide = G // c_len
    deep = size // wide
    gc, gs = (x.astype(np.float32) for x in trig(np.arange(deep)[:, None] * np.arange(c_len)[None, :], c_len))
    first_g = np.stack([np.stack([gc, gs], 1), np.stack([-gs, gc], 1)], 0)
    whole = whole.reshape(deep, wide, 2, depth)
    turned_g = einsum("baql,qbsc->csal", whole, first_g)
    ac, asn = trig((n0 + G // 4)[:, :, None] * np.arange(wide)[None, None, :], G)
    wave = (ac + 1j * asn) * undone(n0)[:, :, None] / G
    second_g = np.stack([wave.real, -wave.imag], axis=2).astype(np.float32)
    back = einsum("csal,cdsa->cdl", turned_g, second_g)

    z = sky * back
    pz = einsum("cdl,cda->cal", z, ic)
    qz = einsum("cdl,cda->cal", z, isn)
    joined = jnp.stack([pz + mirror(qz), mirror(pz) - qz])
    fold = einsum("qcal,qcb->bal", joined, np.stack([bc, bs]))
    folded = lax.all_to_all(
        fold.reshape(n, rows, depth), parts, split_axis=0, concat_axis=0, tiled=True
    )
    ends = einsum("jre,jqae->qjra", folded, inner)
    final = einsum("qjra,bqj->rba", ends, outer)
    return amplitude * final.reshape(rows, size) / size


def solution(mesh):
    n_base, n_slab = mesh.shape["base"], mesh.shape["slab"]
    body, axes = general, both
    if n_slab == 2 * n_base and 2 * n_base * n_slab == G // TILE:
        body, axes = shared, parts
        mesh = jax.sharding.Mesh(mesh.devices.reshape(n_base, 2, n_slab // 2), parts)
    placed = (
        P(axes, None, None),
        P(axes, None, None),
        P(axes, None),
        P(axes),
        P(axes, None),
        P(axes, None),
    )
    return jax.shard_map(body, mesh=mesh, in_specs=placed, out_specs=P(axes, None), check_vma=False)
```

```python
import functools
import math

import jax
import jax.numpy as jnp
import numpy as np
from jax import lax
from jax.experimental import pallas as pl
from jax.experimental.pallas import tpu as pltpu
from jax.sharding import PartitionSpec as P

G = 8192
TILE = 128
both = ("base", "slab")
fine = lax.Precision.HIGHEST


def trig(product, modulus):
    angle = (product % modulus).astype(np.float64) * (2.0 * np.pi / modulus)
    return np.cos(angle), np.sin(angle)


def column_table(n, size):
    depth = size // n
    half = depth // 2
    i = np.arange(half)[None, :]
    j = np.arange(n)[:, None]
    low = n * i + j
    high = (-low) % size
    high[0, 0] = size // 2
    return np.concatenate([low, high], axis=1)


def row_tables(n, size):
    depth = size // n
    cols = column_table(n, size)
    oc, osn = trig(np.arange(n)[:, None] * np.arange(n)[None, :], n)
    outer = np.stack([oc, osn], axis=1)
    prod = np.arange(depth)[None, :, None] * cols[:, None, :]
    c, s = trig(prod, size)
    sign = np.where(np.arange(depth) < depth // 2, 1.0, -1.0)[None, None, :]
    inner = np.stack([c + s, sign * (c - s)], axis=1)
    return outer.astype(np.float32), inner.astype(np.float32)


def grid_row_tables(n, size):
    depth = G // n
    cols = column_table(n, size)
    half = cols.shape[1] // 2
    oc, osn = trig(np.arange(n)[:, None] * np.arange(n)[None, :], n)
    outer = np.stack([np.stack([oc, osn], 1), np.stack([-osn, oc], 1)], 0)
    low = cols[:, :half]
    high = cols[(-np.arange(n)) % n, half:]
    a = np.arange(depth)[None, :, None]
    out = []
    for part in (low, high):
        c, s = trig(a * (part[:, None, :] + G // 4), G)
        out.append(np.stack([np.concatenate([c, s], 2), np.concatenate([-s, c], 2)], 1))
    return outer.astype(np.float32), np.concatenate(out, axis=3).astype(np.float32)


def taps(cells, offsets):
    scaled = (cells - offsets) * 0.25
    kept = jnp.maximum(1.0 - scaled * scaled, 0.0)
    return kept * kept * kept


def split_three(x):
    high = x.astype(jnp.bfloat16)
    rest = x - high.astype(jnp.float32)
    middle = rest.astype(jnp.bfloat16)
    return high, middle, (rest - middle.astype(jnp.float32)).astype(jnp.bfloat16)


def grid_kernel(rows, info_ref, list_ref, data_ref, out_ref):
    count = info_ref[0]
    first = info_ref[1].astype(jnp.float32)
    out_ref[...] = jnp.zeros_like(out_ref)
    row_cells = lax.broadcasted_iota(jnp.int32, (rows, TILE), 0).astype(jnp.float32) + first
    col_cells = lax.broadcasted_iota(jnp.int32, (TILE, TILE), 0).astype(jnp.float32)

    def step(k, carry):
        packed = list_ref[k]
        index = packed // 256
        col = (packed // 2) % 128
        flip = (packed % 2).astype(jnp.float32)
        sign = 1.0 - 2.0 * flip
        start = 128.0 * flip
        block = data_ref[index]
        value = block[0:2, :]
        place = block[2:4, :]
        row_taps = taps(row_cells * sign + start, place[0:1, :])
        col_taps = taps(col_cells * sign + start, place[1:2, :])
        weighted = jnp.concatenate(
            [col_taps * value[0:1, :], col_taps * (value[1:2, :] * sign)], axis=0
        )
        rh, rm, rl = split_three(row_taps)
        wh, wm, wl = split_three(weighted)
        left = jnp.concatenate([rh, rh, rh, rm, rm, rl], axis=1)
        right = jnp.concatenate([wh, wm, wl, wh, wm, wh], axis=1)
        sub = lax.dot_general(
            left, right, (((1,), (1,)), ((), ())), preferred_element_type=jnp.float32
        )
        out_ref[0, col] += sub[:, :TILE]
        out_ref[1, col] += sub[:, TILE:]
        return carry

    lax.fori_loop(0, count, step, 0)


def grid_rows(info, table, gathered, rows):
    tiles = G // TILE
    smem = pl.BlockSpec(memory_space=pltpu.SMEM)
    vmem = pl.BlockSpec(memory_space=pltpu.VMEM)
    return pl.pallas_call(
        functools.partial(grid_kernel, rows),
        out_shape=jax.ShapeDtypeStruct((2, tiles, rows, TILE), jnp.float32),
        in_specs=[smem, smem, vmem],
        out_specs=vmem,
        compiler_params=pltpu.CompilerParams(vmem_limit_bytes=56 * 1024 * 1024),
        cost_estimate=pl.CostEstimate(
            flops=2 * 10**10, bytes_accessed=16 * 2**20, transcendentals=0
        ),
        name="grid_rows",
    )(info, table, gathered)


def einsum(form, *args, precision=lax.Precision.HIGH):
    return jnp.einsum(form, *args, precision=precision, preferred_element_type=jnp.float32)


def general(residual, position, owner, tile_local, xi, amplitude):
    n = lax.axis_size(both)
    n_base = lax.axis_size("base")
    n_slab = lax.axis_size("slab")
    me = lax.axis_index(both)
    rows, size = xi.shape
    depth = size // n
    half = depth // 2
    tiles = G // TILE

    region_rows = G // n_slab // TILE
    region_cols = G // n_base // TILE
    target = owner[:, 0]
    tile_row = (target % n_slab) * region_rows + tile_local // region_cols
    tile_col = (target // n_slab) * region_cols + tile_local % region_cols
    flip = tile_row >= tiles // 2
    tile_row = jnp.where(flip, tiles - 1 - tile_row, tile_row)
    tile_col = jnp.where(flip, tiles - 1 - tile_col, tile_col)
    code = tile_row * 256 + tile_col * 2 + flip.astype(jnp.int32)
    codes = lax.all_gather(code, both, axis=0, tiled=True)
    payload = jnp.concatenate([residual, position], axis=1)
    codes, payload = lax.optimization_barrier((codes, payload))
    gathered = lax.all_gather(payload, both, axis=0, tiled=True)
    blocks = codes.shape[0]
    grid_depth = G // 2 // n
    first_row = me * grid_depth
    mine = (codes // 256 == first_row // TILE).astype(jnp.int32)
    rank = jnp.where(mine == 1, jnp.cumsum(mine) - 1, -1)
    packed = lax.broadcasted_iota(jnp.int32, (blocks,), 0) * 256 + codes % 256
    spots = lax.broadcasted_iota(jnp.int32, (blocks, blocks), 0)
    table = jnp.sum(jnp.where(spots == rank[None, :], packed[None, :], 0), axis=1)
    info = jnp.stack([jnp.sum(mine), first_row % TILE]).astype(jnp.int32)

    outer, inner = row_tables(n, size)
    spectrum = (amplitude * xi).reshape(rows, n, depth)
    mid = einsum("rba,bqc->qcra", spectrum, outer)
    sent = einsum("cra,cae->cre", mid[0], inner[:, 0]) + einsum("cra,cae->cre", mid[1], inner[:, 1])
    sent, gathered = lax.optimization_barrier((sent, gathered))
    field = lax.all_to_all(sent, both, split_axis=0, concat_axis=0, tiled=True)
    field = field.reshape(size, depth)
    lane = lax.broadcasted_iota(jnp.int32, (1, depth), 1)
    still = (me == 0) & (lane % half == 0)

    def mirror(x):
        return jnp.where(still, x, jnp.roll(x, half, axis=-1))

    c_len = 128
    d_len = size // c_len
    bc, bs = (x.astype(np.float32) for x in trig(np.arange(c_len)[:, None] * np.arange(c_len)[None, :], c_len))
    shape = (c_len, d_len, depth)
    n0 = c_len * np.arange(d_len)[None, :] + np.arange(c_len)[:, None]
    ic, isn = (x.astype(np.float32) for x in trig(n0[:, :, None] * np.arange(d_len)[None, None, :], size))
    pair = jnp.stack([field.reshape(shape), mirror(field).reshape(shape)])
    first = np.stack([np.stack([bc, bs], 1), np.stack([bs, -bc], 1)], 0)
    turned = einsum("qbal,qbsc->csal", pair, first)
    second = np.stack([ic, -isn], axis=2)
    power = einsum("csal,cdsa->cdl", turned, second)
    sky = jnp.exp(power / size)

    grid = grid_rows(info, table, gathered, grid_depth)
    outer_g, inner_g = grid_row_tables(n, size)
    parts = tiles // n if tiles >= n else 1
    inner_len = G // n
    if inner_len >= TILE:
        view = grid.reshape(2, n, inner_len // TILE, grid_depth, TILE)
    else:
        flat = grid.transpose(0, 2, 1, 3).reshape(2, grid_depth, n, inner_len)
        view = flat.transpose(0, 2, 1, 3)[:, :, None]
        parts = 1
    lanes = view.shape[-1]
    stage = einsum("qbpra,qbsc->cspra", view, outer_g, precision=fine)
    inner_g = inner_g.reshape(n, 2, parts, lanes, 2 * depth)
    halves = einsum("cspra,cspae->cre", stage, inner_g, precision=fine)
    high = halves[:, :, depth:]
    high = jnp.concatenate([high[:1], jnp.flip(high[1:], axis=0)], axis=0)
    halves = jnp.concatenate([halves[:, :, :depth], high], axis=2)
    got = lax.all_to_all(halves, both, split_axis=0, concat_axis=0, tiled=True)
    got = got.reshape(size, 2 * depth)
    real = jnp.concatenate([got[:, :half], got[:, depth : depth + half]], axis=1)
    imag = jnp.concatenate([got[:, half:depth], got[:, depth + half :]], axis=1)
    wide = G // c_len
    deep = size // wide
    gc, gs = (x.astype(np.float32) for x in trig(np.arange(deep)[:, None] * np.arange(c_len)[None, :], c_len))
    first_g = np.stack([np.stack([gc, gs], 1), np.stack([-gs, gc], 1)], 0)
    whole = jnp.stack([real.reshape(deep, wide, depth), imag.reshape(deep, wide, depth)])
    turned_g = einsum("qbal,qbsc->csal", whole, first_g, precision=fine)
    ac, asn = trig((n0 + G // 4)[:, :, None] * np.arange(wide)[None, None, :], G)
    second_g = (np.stack([ac, -asn], axis=2) / G).astype(np.float32)
    back = einsum("csal,cdsa->cdl", turned_g, second_g, precision=fine)

    z = sky * back
    pz = einsum("cdl,cda->cal", z, ic)
    qz = einsum("cdl,cda->cal", z, isn)
    joined = jnp.stack([pz + mirror(qz), mirror(pz) - qz])
    fold = einsum("qcal,qcb->bal", joined, np.stack([bc, bs]))
    folded = lax.all_to_all(
        fold.reshape(n, rows, depth), both, split_axis=0, concat_axis=0, tiled=True
    )
    ends = einsum("jre,jqae->qjra", folded, inner)
    final = einsum("qjra,bqj->rba", ends, outer)
    return amplitude * final.reshape(rows, size) / size


MESH = pl.DeviceIdType.MESH
parts = ("base", "half", "quad")
LANES = 4


def exchange_kernel(nb, ns, send_ref, out_ref, bsend, brecv, usend, dsend, lrecv, hrecv, psend, precv, lsem):
    quads = ns // 2
    nz = ns // 2
    base = lax.axis_index("base")
    slab = lax.axis_index("half") * quads + lax.axis_index("quad")
    z = slab // 2
    core = slab % 2

    def at(b, s):
        return (b, s // quads, s % quads)

    def copy(source, target, here, there, device):
        return pltpu.make_async_remote_copy(
            src_ref=source, dst_ref=target, send_sem=here, recv_sem=there, device_id=device, device_id_type=MESH
        )

    def crossing(k):
        other = (base + k) % nb
        return copy(send_ref.at[other], out_ref.at[slab, base], bsend.at[k], brecv.at[k], at(other, slab))

    def arriving(k):
        from_base = (base - k + nb) % nb
        return copy(send_ref.at[base], out_ref.at[slab, from_base], bsend.at[k], brecv.at[k], at(from_base, slab))

    def block(origin, k):
        return out_ref.at[2 * origin + core, (base - k + nb) % nb]

    def upward(s, k):
        part = block(z - s, k)
        return copy(part, part, usend.at[s, k], lrecv.at[s + 1, k], at(base, slab + 2))

    def downward(s, k):
        part = block(z + s, k)
        return copy(part, part, dsend.at[s, k], hrecv.at[s + 1, k], at(base, slab - 2))

    def from_below(s, k):
        part = block(z - s, k)
        return copy(part, part, usend.at[s, k], lrecv.at[s, k], at(base, slab - 2))

    def from_above(s, k):
        part = block(z + s, k)
        return copy(part, part, dsend.at[s, k], hrecv.at[s, k], at(base, slab + 2))

    def across(origin, k):
        part = block(origin, k)
        return copy(part, part, psend.at[origin, k], precv.at[origin, k], at(base, slab + 1 - 2 * core))

    def from_partner(origin, k):
        part = out_ref.at[2 * origin + 1 - core, (base - k + nb) % nb]
        return copy(part, part, psend.at[origin, k], precv.at[origin, k], at(base, slab + 1 - 2 * core))

    barrier = pltpu.get_barrier_semaphore()
    for k in range(1, nb):
        pl.semaphore_signal(barrier, inc=1, device_id=at((base + k) % nb, slab), device_id_type=MESH)
    pl.semaphore_signal(barrier, inc=1, device_id=at(base, slab + 1 - 2 * core), device_id_type=MESH)

    @pl.when(z < nz - 1)
    def _():
        pl.semaphore_signal(barrier, inc=1, device_id=at(base, slab + 2), device_id_type=MESH)

    @pl.when(z > 0)
    def _():
        pl.semaphore_signal(barrier, inc=1, device_id=at(base, slab - 2), device_id_type=MESH)

    pl.semaphore_wait(barrier, nb + jnp.where(z < nz - 1, 1, 0) + jnp.where(z > 0, 1, 0))

    for k in range(1, nb):
        crossing(k).start()
    own = pltpu.make_async_copy(send_ref.at[base], out_ref.at[slab, base], lsem)
    own.start()

    def pass_on(s, k, ascending, descending):
        if ascending:
            @pl.when((z - s >= 0) & (z < nz - 1))
            def _():
                upward(s, k).start()

        if descending:
            @pl.when((z + s < nz) & (z > 0))
            def _():
                downward(s, k).start()

    for k in range(nb):
        if k == 0:
            own.wait()
        else:
            arriving(k).wait_recv()
        pass_on(0, k, True, True)
        across(z, k).start()
    for s in range(1, nz):
        for k in range(nb):
            @pl.when(z - s >= 0)
            def _():
                from_below(s, k).wait_recv()
                if s < nz - 1:
                    pass_on(s, k, True, False)
                across(z - s, k).start()

            @pl.when(z + s < nz)
            def _():
                from_above(s, k).wait_recv()
                if s < nz - 1:
                    pass_on(s, k, False, True)
                across(z + s, k).start()

    for origin in range(nz):
        for k in range(nb):
            from_partner(origin, k).wait_recv()
    for k in range(1, nb):
        crossing(k).wait_send()
    for s in range(nz - 1):
        for k in range(nb):
            @pl.when((z - s >= 0) & (z < nz - 1))
            def _():
                upward(s, k).wait_send()

            @pl.when((z + s < nz) & (z > 0))
            def _():
                downward(s, k).wait_send()

    for origin in range(nz):
        for k in range(nb):
            across(origin, k).wait_send()


def exchange(sent, ns):
    nb = sent.shape[0]
    nz = ns // 2
    dma = pltpu.SemaphoreType.DMA
    vmem = pl.BlockSpec(memory_space=pltpu.VMEM)
    return pl.pallas_call(
        functools.partial(exchange_kernel, nb, ns),
        out_shape=jax.ShapeDtypeStruct((ns,) + sent.shape, jnp.float32),
        in_specs=[vmem],
        out_specs=vmem,
        scratch_shapes=[
            dma((nb,)), dma((nb,)), dma((nz, nb)), dma((nz, nb)), dma((nz, nb)), dma((nz, nb)),
            dma((nz, nb)), dma((nz, nb)), dma,
        ],
        compiler_params=pltpu.CompilerParams(collective_id=0, has_side_effects=True, vmem_limit_bytes=16 << 20),
        name="exchange",
    )(sent)


def two_parts(x):
    high = x.astype(jnp.bfloat16)
    return high, (x - high.astype(jnp.float32)).astype(jnp.bfloat16)


def times(x, c, s):
    return x[0] * c - x[1] * s, x[0] * s + x[1] * c


def turn(x, angle):
    c, s = math.cos(angle), math.sin(angle)
    return times(x, c, s)


def add(x, y):
    return x[0] + y[0], x[1] + y[1]


def sub(x, y):
    return x[0] - y[0], x[1] - y[1]


def four(x):
    s0, d0, s1, d1 = add(x[0], x[2]), sub(x[0], x[2]), add(x[1], x[3]), sub(x[1], x[3])
    i1 = (-d1[1], d1[0])
    return [add(s0, s1), add(d0, i1), sub(s0, s1), sub(d0, i1)]


def sixteen(x):
    rows = []
    for b0 in range(4):
        y = four([x[4 * b1 + b0] for b1 in range(4)])
        rows.append([y[a0] if a0 * b0 == 0 else turn(y[a0], 2 * math.pi * a0 * b0 / 16) for a0 in range(4)])
    out = [None] * 16
    for a0 in range(4):
        y = four([rows[b0][a0] for b0 in range(4)])
        for a1 in range(4):
            out[a0 + 4 * a1] = y[a1]
    return out


def grid_rows_kernel(info_ref, list_ref, first_ref, data_ref, turn_ref, undo_ref, weight_ref, out_ref, grid_ref, left_ref, right_ref):
    count = info_ref[0]
    parity = info_ref[1]
    grid_ref[...] = jnp.zeros_like(grid_ref)
    half = grid_ref.shape[1]
    group = 16
    cells = lax.broadcasted_iota(jnp.int32, (group + 8, TILE), 0).astype(jnp.float32) * 0.25
    nothing = jnp.zeros((group, TILE), jnp.bfloat16)

    def bump(offsets):
        d = cells - offsets
        kept = jnp.maximum(1.0 - d * d, 0.0)
        return kept * kept * kept

    def window(offsets):
        start = jnp.floor((offsets - 4.0) * (1.0 / group))
        offsets = (offsets - start * group) * 0.25
        return bump(offsets) - bump(offsets - 0.25), jnp.broadcast_to(start, (group, TILE)).astype(jnp.bfloat16)

    def spread(compact, start):
        padded = jnp.concatenate([compact, jnp.zeros((8, TILE), jnp.float32)], axis=0)
        out = []
        for part in two_parts(padded):
            first, second = part[:group], part[group:]
            pieces = []
            for g in range(TILE // group):
                piece = jnp.where(start == g - 1, second, nothing) if g else nothing
                pieces.append(jnp.where(start == g, first, piece))
            out.append(jnp.concatenate(pieces, axis=0))
        return out

    lanes = left_ref.shape[0]

    def place(k):
        packed = list_ref[k]
        return packed % 64, packed // 64

    def prepare(k, lane):
        col, rest = place(k)
        odd = jnp.where(col >= half, parity, 0)
        sign = jnp.where(k < count, 1 - 2 * odd, 0).astype(jnp.float32)
        block = data_ref[rest // 2]
        value = block[0:2, :] * sign
        row_taps, row_start = window(block[2:3, :])
        col_taps, col_start = window(block[3:4, :])
        rows_split = spread(row_taps, row_start)
        real = spread(col_taps * value[0:1, :], col_start)
        imag = spread(col_taps * value[1:2, :], col_start)
        for q in range(2):
            left_ref[lane, :, q * TILE : (q + 1) * TILE] = rows_split[q]
            right_ref[lane, :TILE, q * TILE : (q + 1) * TILE] = real[q]
            right_ref[lane, TILE:, q * TILE : (q + 1) * TILE] = imag[q]

    def product(lane):
        rh, rl = left_ref[lane, :, :TILE], left_ref[lane, :, TILE:]
        wh, wl = right_ref[lane, :, :TILE], right_ref[lane, :, TILE:]
        left = jnp.concatenate([rh, rh, rl], axis=1)
        right = jnp.concatenate([wh, wl, wh], axis=1)
        return lax.dot_general(left, right, (((1,), (1,)), ((), ())), preferred_element_type=jnp.float32)

    def step(k, carry):
        made = [product(lane) for lane in range(lanes)]
        for lane in range(lanes):
            prepare((k + 1) * lanes + lane, lane)
        for lane in range(lanes):
            col, rest = place(k * lanes + lane)
            col = jnp.where(col >= half, col - half, col)
            spot = pl.ds(pl.multiple_of((rest % 2) * TILE, TILE), TILE)
            grid_ref[0, col, spot, :] += made[lane][:, :TILE]
            grid_ref[1, col, spot, :] += made[lane][:, TILE:]
        return carry

    for lane in range(lanes):
        prepare(lane, lane)
    lax.fori_loop(0, (count + lanes - 1) // lanes, step, 0)

    depth = half // 2
    rows = grid_ref.shape[2]

    def outer(k, carry):
        spot = pl.ds(pl.multiple_of(k * 8, 8), 8)
        for side in range(2):
            x = []
            for b in range(depth):
                value = grid_ref[0, 2 * b + side, spot, :], grid_ref[1, 2 * b + side, spot, :]
                x.append(times(value, first_ref[b, 0], first_ref[b, 1]))
            for a, value in enumerate(sixteen(x)):
                c = turn_ref[a, side : side + 1, :]
                s = turn_ref[a, 2 + side : 3 + side, :]
                value = times(value, c, s)
                grid_ref[0, 2 * a + side, spot, :] = value[0]
                grid_ref[1, 2 * a + side, spot, :] = value[1]
        return carry

    lax.fori_loop(0, rows // 8, outer, 0)

    def inner(a, carry):
        mirrored = depth - parity - a
        mirrored = jnp.where(mirrored == depth, 0, mirrored)
        which = jnp.where((a == 0) & (parity == 0), 1, 0)
        weight = weight_ref[which]
        for part in range(1):
            spot = pl.ds(0, rows)
            x = jnp.concatenate([grid_ref[q, 2 * a + side, spot, :] for q in range(2) for side in range(2)], axis=1)
            high, low = two_parts(x)
            made = jnp.dot(jnp.concatenate([high, low, high], axis=1), weight, preferred_element_type=jnp.float32)
            mid = TILE // 2
            made = times((made[:, :TILE], made[:, TILE:]), undo_ref[a, 0:1, :], undo_ref[a, 1:2, :])
            for q in range(2):
                out_ref[a, spot, q * TILE : q * TILE + mid] = made[q][:, :mid]
                out_ref[mirrored, spot, q * TILE + mid : (q + 1) * TILE] = made[q][:, mid:]
        return carry

    lax.fori_loop(0, depth, inner, 0)


def split_table(x):
    high = x.astype(np.float32).astype(jnp.bfloat16)
    low = (x - high.astype(np.float64)).astype(np.float32).astype(jnp.bfloat16)
    return high, low


def undone(pixels):
    c, s = trig(pixels + G // 4, G)
    return 1.0 / (1.0 - (c - 1j * s))


def grid_row_weights(n, size):
    depth = n // 2
    span = G // 2 // depth
    half = size // n // 2
    alpha = np.arange(span)
    turns, firsts, undos = [], [], []
    for p in range(2):
        j = 2 * np.arange(depth) + p
        c, s = trig(j[:, None] * alpha[None, :], G)
        turns.append(np.concatenate([c.reshape(depth, 2, TILE), s.reshape(depth, 2, TILE)], axis=1))
        firsts.append(np.stack(trig(np.arange(depth) * p, n), axis=1))
        low = n * np.arange(half)[None, :] + j[:, None]
        high = size - n * np.arange(half)[None, :] - ((-j) % n)[:, None]
        if p == 0:
            low[0, 0], high[0, 0] = 0, size // 2
        undo = undone(np.concatenate([low, high], axis=1))
        undos.append(np.stack([undo.real, undo.imag], axis=1))
    weights = []
    i = np.arange(half)
    for special in range(2):
        low = n * i
        high = size - n * i - (0 if special else n)
        if special:
            high[0] = size // 2
        parts_re, parts_im = [], []
        for cols in (low, high):
            c, s = trig(alpha[:, None] * (cols[None, :] + G // 4), G)
            parts_re.append(np.concatenate([c, -s], axis=0))
            parts_im.append(np.concatenate([s, c], axis=0))
        w = np.concatenate(parts_re + parts_im, axis=1)
        high_part, low_part = split_table(w)
        weights.append(np.concatenate([high_part, high_part, low_part], axis=0))
    turns, firsts, undos = (np.stack(x).astype(np.float32) for x in (turns, firsts, undos))
    return turns, firsts, undos, np.stack(weights)


def grid_rows_two(info, table, first, data, turns, undos, weights):
    depth = turns.shape[0]
    rows = 2 * TILE
    smem = pl.BlockSpec(memory_space=pltpu.SMEM)
    vmem = pl.BlockSpec(memory_space=pltpu.VMEM)
    return pl.pallas_call(
        grid_rows_kernel,
        out_shape=jax.ShapeDtypeStruct((depth, rows, 2 * TILE), jnp.float32),
        in_specs=[smem, smem, smem, vmem, vmem, vmem, vmem],
        out_specs=vmem,
        scratch_shapes=[
            pltpu.VMEM((2, 2 * depth, rows, TILE), jnp.float32),
            pltpu.VMEM((LANES, TILE, 2 * TILE), jnp.bfloat16),
            pltpu.VMEM((LANES, 2 * TILE, 2 * TILE), jnp.bfloat16),
        ],
        compiler_params=pltpu.CompilerParams(vmem_limit_bytes=40 << 20),
        cost_estimate=pl.CostEstimate(flops=2 * 10**10, bytes_accessed=16 * 2**20, transcendentals=0),
        name="grid_rows_two",
    )(info, table, first, data, turns, undos, weights)


def minus(x):
    return [(b, a) for a, b in sixteen([(b, a) for a, b in x])]


def pick(table, u):
    side = table.shape[1] // 2
    return table[:, u : u + 1], table[:, side + u : side + u + 1]


def mirrored(x, still):
    return jnp.where(still, x, pltpu.roll(x, x.shape[1] // 2, 1))


def still_lanes(place, rows):
    lane = lax.broadcasted_iota(jnp.int32, (rows, TILE), 1)
    return (lane % (TILE // 2) == 0) & (place == 0)


def stacked(work_ref, u):
    sides = [jnp.concatenate([work_ref[u + q, 0], work_ref[u + q, 1]], axis=0) for q in range(2)]
    high, low = two_parts(jnp.concatenate(sides, axis=1))
    return jnp.concatenate([high, high, low], axis=0)


def field_kernel(scale, info_ref, field_ref, turn_ref, mat_ref, sky_ref, work_ref):
    still = still_lanes(info_ref[0], 8)
    n = field_ref.shape[0]

    def outer(k, carry):
        spot = pl.ds(pl.multiple_of(k * 8, 8), 8)
        table = turn_ref[spot, :]
        for e in range(2):
            x = []
            for d in range(n // 2):
                first, second = field_ref[d, spot, :], field_ref[d + n // 2, spot, :]
                value = first - second if e else first + second
                value = value, mirrored(value, still)
                x.append(turn(value, -2 * math.pi * d / n) if e * d else value)
            for v, value in enumerate(minus(x)):
                u = 2 * v + e
                work_ref[u, 0, spot, :], work_ref[u, 1, spot, :] = times(value, *pick(table, u))
        return carry

    lax.fori_loop(0, field_ref.shape[1] // 8, outer, 0)

    def inner(k, carry):
        made = jnp.dot(mat_ref[...], stacked(work_ref, 2 * k), preferred_element_type=jnp.float32)
        made = jnp.exp(made * scale)
        sky_ref[2 * k] = made[:, :TILE]
        sky_ref[2 * k + 1] = made[:, TILE:]
        return carry

    lax.fori_loop(0, n // 2, inner, 0)


def image_kernel(info_ref, bend_ref, whole_ref, sky_ref, turn_g_ref, mat_g_ref, slope_ref, mat_f_ref, turn_ref, out_ref, work_ref, half_ref):
    still = still_lanes(info_ref[0], 8)
    n = sky_ref.shape[0]
    depth = n // 2

    def outer(k, carry):
        spot = pl.ds(pl.multiple_of(k * 8, 8), 8)
        table = turn_g_ref[spot, :]
        for e in range(2):
            x = []
            for a in range(depth):
                value = whole_ref[a, spot, :TILE], whole_ref[a, spot, TILE:]
                x.append(turn(value, 2 * math.pi * a / n) if e * a else value)
            for v, value in enumerate(sixteen(x)):
                u = 2 * v + e
                work_ref[u, 0, spot, :], work_ref[u, 1, spot, :] = times(value, *pick(table, u))
        return carry

    lax.fori_loop(0, whole_ref.shape[1] // 8, outer, 0)

    def inner(k, carry):
        made = jnp.dot(mat_g_ref[...], stacked(work_ref, 2 * k), preferred_element_type=jnp.float32)
        z = []
        for q in range(2):
            u = 2 * k + q
            sine = slope_ref[0] * bend_ref[u, 0] + slope_ref[1] * bend_ref[u, 1]
            z.append(made[:, q * TILE : (q + 1) * TILE] * sky_ref[u] / sine)
        high, low = two_parts(jnp.concatenate(z, axis=1))
        spread = jnp.dot(mat_f_ref[...], jnp.concatenate([high, high, low], axis=0), preferred_element_type=jnp.float32)
        for q in range(2):
            for c in range(2):
                work_ref[2 * k + q, c, :TILE, :] = spread[c * TILE : (c + 1) * TILE, q * TILE : (q + 1) * TILE]
        return carry

    lax.fori_loop(0, depth, inner, 0)

    def last(k, carry):
        spot = pl.ds(pl.multiple_of(k * 8, 8), 8)
        table = turn_ref[spot, :]
        for e in range(2):
            x = []
            for v in range(depth):
                u = 2 * v + e
                x.append(times((work_ref[u, 0, spot, :], work_ref[u, 1, spot, :]), *pick(table, u)))
            for d, value in enumerate(minus(x)):
                if e == 0:
                    half_ref[d, 0], half_ref[d, 1] = value
                    continue
                value = turn(value, -2 * math.pi * d / n) if d else value
                before = half_ref[d, 0], half_ref[d, 1]
                for side, both_parts in enumerate((add(before, value), sub(before, value))):
                    out_ref[d + side * depth, spot, :] = both_parts[0] - mirrored(both_parts[1], still)
        return carry

    lax.fori_loop(0, TILE // 8, last, 0)


def column_tables(n, size):
    w = np.arange(size // n)
    t = np.arange(TILE)
    u = np.arange(n)
    r = 2 * np.arange(2 * TILE) + 1
    side = TILE // 2

    def lanes(c, s):
        out = np.zeros((c.shape[0], TILE))
        out[:, :n], out[:, side : side + n] = c, s
        return out.astype(np.float32)

    def matrix(x, axis_first):
        high, low = split_table(x)
        return np.concatenate([high, low, high], axis=1)

    c, s = trig(t[:, None] * u[None, :], size)
    turns = lanes(c, -s)
    c, s = trig(w[:, None] * t[None, :], size // n)
    mat_h = matrix(np.concatenate([c, s], axis=1), 0)
    mat_f = matrix(np.concatenate([c.T, -s.T], axis=0), 0)
    c, s = trig(r[:, None] * u[None, :], 2 * G)
    turns_g = lanes(c, s)
    c, s = trig((w[:, None] * n + G // 4) * r[None, :], 2 * G)
    mat_g = matrix(np.concatenate([s, c], axis=1), 0)
    c, s = trig(w * n + G // 4, 2 * G)
    slope = np.stack([s, c]) * (2.0 * G)
    slope = np.broadcast_to(slope[:, :, None], slope.shape + (TILE,)).astype(np.float32)
    c, s = trig(u, 2 * G)
    bend = np.stack([c, s], axis=1).astype(np.float32)
    return turns, mat_h, mat_f, turns_g, mat_g, slope, bend


def column_call(kernel, smems, args, out_shape, scratch, name):
    smem = pl.BlockSpec(memory_space=pltpu.SMEM)
    vmem = pl.BlockSpec(memory_space=pltpu.VMEM)
    return pl.pallas_call(
        kernel,
        out_shape=jax.ShapeDtypeStruct(out_shape, jnp.float32),
        in_specs=[smem] * len(smems) + [vmem] * len(args),
        out_specs=vmem,
        scratch_shapes=scratch,
        compiler_params=pltpu.CompilerParams(vmem_limit_bytes=40 << 20),
        cost_estimate=pl.CostEstimate(flops=10**10, bytes_accessed=16 * 2**20, transcendentals=0),
        name=name,
    )(*smems, *args)


def shared(residual, position, owner, tile_local, xi, amplitude):
    n = lax.axis_size(parts)
    n_base = lax.axis_size("base")
    n_slab = lax.axis_size("half") * lax.axis_size("quad")
    quads = lax.axis_size("quad")
    base, parity, quad = (lax.axis_index(axis) for axis in parts)
    place = 2 * (base * quads + quad) + parity
    order = np.array([2 * (b * quads + q) + h for b in range(n_base) for h in range(2) for q in range(quads)])
    rows, size = xi.shape
    depth = size // n
    half = depth // 2
    tiles = G // TILE

    blocks = residual.shape[0]
    region_rows = G // n_slab // TILE
    region_cols = G // n_base // TILE
    room = 2 * n_base * (2 * blocks // n)
    target = owner[:, 0]
    tile_row = (target % n_slab) * region_rows + tile_local // region_cols
    tile_col = (target // n_slab) * region_cols + tile_local % region_cols
    flip = tile_row >= tiles // 2
    tile_row = jnp.where(flip, tiles - 1 - tile_row, tile_row)
    tile_col = jnp.where(flip, tiles - 1 - tile_col, tile_col)
    line = tile_row // n_slab
    code = (tile_row % n_slab) * tiles + tile_col
    flipped = flip[:, None]
    payload = jnp.stack(
        [
            residual[:, 0],
            jnp.where(flipped, -residual[:, 1], residual[:, 1]),
            jnp.where(flipped, TILE - position[:, 0], position[:, 0]),
            jnp.where(flipped, TILE - position[:, 1], position[:, 1]),
        ],
        axis=1,
    )
    earlier = (line[:, None] == line[None, :]) & (np.arange(blocks)[:, None] > np.arange(blocks)[None, :])
    slot = line * room + jnp.sum(earlier.astype(jnp.int32), axis=1)
    chosen = slot[None, :] == lax.broadcasted_iota(jnp.int32, (n_base * room, blocks), 0)
    moved = jnp.dot(chosen.astype(jnp.float32), payload.reshape(blocks, 4 * TILE), precision=fine)
    codes = jnp.sum(jnp.where(chosen, code[None, :] + 1, 0), axis=1) - 1
    codes = jnp.pad(codes.astype(jnp.float32).reshape(n_base, 1, 1, room), ((0, 0), (0, 0), (0, 3), (0, TILE - room)))
    sent = jnp.concatenate([moved.reshape(n_base, room, 4, TILE), codes], axis=1)
    got = exchange(sent, n_slab)

    outer, inner = row_tables(n, size)
    outer, inner = outer[:, :, order], inner[order]
    spectrum = (amplitude * xi).reshape(rows, n, depth)
    mid = einsum("rba,bqc->qcra", spectrum, outer)
    sent = einsum("cra,cae->cre", mid[0], inner[:, 0]) + einsum("cra,cae->cre", mid[1], inner[:, 1])
    sent, got = lax.optimization_barrier((sent, got))
    field = lax.all_to_all(sent, parts, split_axis=0, concat_axis=0, tiled=True)
    field = field.reshape(size, depth)

    sources = n_slab * n_base
    codes = got[:, :, room, 0, :room].reshape(sources, room).astype(jnp.int32)
    mine = (codes >= 0) & (codes // tiles // 2 == quad)
    ones = mine.astype(jnp.float32)
    before = jnp.dot(ones, np.triu(np.ones((room, room), np.float32), 1), precision=fine)
    above = jnp.dot(np.tril(np.ones((sources, sources), np.float32), -1), ones, precision=fine)
    rank = (before + jnp.sum(above, axis=1, keepdims=True)).astype(jnp.int32)
    rank = jnp.where(mine, rank, -1).reshape(-1)
    index = lax.broadcasted_iota(jnp.int32, (sources, room), 0) * (room + 1) + lax.broadcasted_iota(jnp.int32, (sources, room), 1)
    packed = (index * (2 * tiles) + codes % (2 * tiles)).reshape(-1)
    spots = lax.broadcasted_iota(jnp.int32, (sources * room, sources * room), 0)
    table = jnp.sum(jnp.where(spots == rank[None, :], packed[None, :], 0), axis=1)
    table = jnp.pad(table, (0, 2 * LANES))
    info = jnp.stack([jnp.sum(mine.astype(jnp.int32)), parity]).astype(jnp.int32)

    turns, firsts, undos, weights = grid_row_weights(n, size)
    halves = grid_rows_two(
        info,
        table,
        lax.dynamic_index_in_dim(jnp.asarray(firsts), parity, 0, keepdims=False),
        got.reshape(sources * (room + 1), 4, TILE),
        lax.dynamic_index_in_dim(jnp.asarray(turns), parity, 0, keepdims=False),
        lax.dynamic_index_in_dim(jnp.asarray(undos), parity, 0, keepdims=False),
        jnp.asarray(weights),
    )
    whole = lax.all_to_all(halves, ("base", "quad"), split_axis=0, concat_axis=0, tiled=True)

    turns, mat_h, mat_f, turns_g, mat_g, slope, bend = (jnp.asarray(x) for x in column_tables(n, size))
    me = jnp.reshape(place, (1,)).astype(jnp.int32)
    block = (n, rows, depth)
    sky = column_call(
        functools.partial(field_kernel, 1.0 / size),
        [me],
        [field.reshape(block), turns, mat_h],
        block,
        [pltpu.VMEM((n, 2, rows, depth), jnp.float32)],
        "field",
    )
    fold = column_call(
        image_kernel,
        [me, bend],
        [whole, sky, turns_g, mat_g, slope, mat_f, turns],
        block,
        [pltpu.VMEM((n, 2, 2 * rows, depth), jnp.float32), pltpu.VMEM((n // 2, 2, 8, depth), jnp.float32)],
        "image",
    )
    folded = lax.all_to_all(fold, parts, split_axis=0, concat_axis=0, tiled=True)
    ends = einsum("jre,jqae->qjra", folded, inner)
    final = einsum("qjra,bqj->rba", ends, outer)
    return amplitude * final.reshape(rows, size) / size


def solution(mesh):
    n_base, n_slab = mesh.shape["base"], mesh.shape["slab"]
    body, axes = general, both
    if n_slab == 2 * n_base and 2 * n_base * n_slab == G // TILE:
        body, axes = shared, parts
        mesh = jax.sharding.Mesh(mesh.devices.reshape(n_base, 2, n_slab // 2), parts)
    placed = (
        P(axes, None, None),
        P(axes, None, None),
        P(axes, None),
        P(axes),
        P(axes, None),
        P(axes, None),
    )
    return jax.shard_map(body, mesh=mesh, in_specs=placed, out_specs=P(axes, None), check_vma=False)
```

```python
import functools
import math

import jax
import jax.numpy as jnp
import numpy as np
from jax import lax
from jax.experimental import pallas as pl
from jax.experimental.pallas import tpu as pltpu
from jax.sharding import PartitionSpec as P

G = 8192
TILE = 128
both = ("base", "slab")
fine = lax.Precision.HIGHEST


def trig(product, modulus):
    angle = (product % modulus).astype(np.float64) * (2.0 * np.pi / modulus)
    return np.cos(angle), np.sin(angle)


def column_table(n, size):
    depth = size // n
    half = depth // 2
    i = np.arange(half)[None, :]
    j = np.arange(n)[:, None]
    low = n * i + j
    high = (-low) % size
    high[0, 0] = size // 2
    return np.concatenate([low, high], axis=1)


def row_tables(n, size):
    depth = size // n
    cols = column_table(n, size)
    oc, osn = trig(np.arange(n)[:, None] * np.arange(n)[None, :], n)
    outer = np.stack([oc, osn], axis=1)
    prod = np.arange(depth)[None, :, None] * cols[:, None, :]
    c, s = trig(prod, size)
    sign = np.where(np.arange(depth) < depth // 2, 1.0, -1.0)[None, None, :]
    inner = np.stack([c + s, sign * (c - s)], axis=1)
    return outer.astype(np.float32), inner.astype(np.float32)


def grid_row_tables(n, size):
    depth = G // n
    cols = column_table(n, size)
    half = cols.shape[1] // 2
    oc, osn = trig(np.arange(n)[:, None] * np.arange(n)[None, :], n)
    outer = np.stack([np.stack([oc, osn], 1), np.stack([-osn, oc], 1)], 0)
    low = cols[:, :half]
    high = cols[(-np.arange(n)) % n, half:]
    a = np.arange(depth)[None, :, None]
    out = []
    for part in (low, high):
        c, s = trig(a * (part[:, None, :] + G // 4), G)
        out.append(np.stack([np.concatenate([c, s], 2), np.concatenate([-s, c], 2)], 1))
    return outer.astype(np.float32), np.concatenate(out, axis=3).astype(np.float32)


def taps(cells, offsets):
    scaled = (cells - offsets) * 0.25
    kept = jnp.maximum(1.0 - scaled * scaled, 0.0)
    return kept * kept * kept


def split_three(x):
    high = x.astype(jnp.bfloat16)
    rest = x - high.astype(jnp.float32)
    middle = rest.astype(jnp.bfloat16)
    return high, middle, (rest - middle.astype(jnp.float32)).astype(jnp.bfloat16)


def grid_kernel(rows, info_ref, list_ref, data_ref, out_ref):
    count = info_ref[0]
    first = info_ref[1].astype(jnp.float32)
    out_ref[...] = jnp.zeros_like(out_ref)
    row_cells = lax.broadcasted_iota(jnp.int32, (rows, TILE), 0).astype(jnp.float32) + first
    col_cells = lax.broadcasted_iota(jnp.int32, (TILE, TILE), 0).astype(jnp.float32)

    def step(k, carry):
        packed = list_ref[k]
        index = packed // 256
        col = (packed // 2) % 128
        flip = (packed % 2).astype(jnp.float32)
        sign = 1.0 - 2.0 * flip
        start = 128.0 * flip
        block = data_ref[index]
        value = block[0:2, :]
        place = block[2:4, :]
        row_taps = taps(row_cells * sign + start, place[0:1, :])
        col_taps = taps(col_cells * sign + start, place[1:2, :])
        weighted = jnp.concatenate(
            [col_taps * value[0:1, :], col_taps * (value[1:2, :] * sign)], axis=0
        )
        rh, rm, rl = split_three(row_taps)
        wh, wm, wl = split_three(weighted)
        left = jnp.concatenate([rh, rh, rh, rm, rm, rl], axis=1)
        right = jnp.concatenate([wh, wm, wl, wh, wm, wh], axis=1)
        sub = lax.dot_general(
            left, right, (((1,), (1,)), ((), ())), preferred_element_type=jnp.float32
        )
        out_ref[0, col] += sub[:, :TILE]
        out_ref[1, col] += sub[:, TILE:]
        return carry

    lax.fori_loop(0, count, step, 0)


def grid_rows(info, table, gathered, rows):
    tiles = G // TILE
    smem = pl.BlockSpec(memory_space=pltpu.SMEM)
    vmem = pl.BlockSpec(memory_space=pltpu.VMEM)
    return pl.pallas_call(
        functools.partial(grid_kernel, rows),
        out_shape=jax.ShapeDtypeStruct((2, tiles, rows, TILE), jnp.float32),
        in_specs=[smem, smem, vmem],
        out_specs=vmem,
        compiler_params=pltpu.CompilerParams(vmem_limit_bytes=56 * 1024 * 1024),
        cost_estimate=pl.CostEstimate(
            flops=2 * 10**10, bytes_accessed=16 * 2**20, transcendentals=0
        ),
        name="grid_rows",
    )(info, table, gathered)


def einsum(form, *args, precision=lax.Precision.HIGH):
    return jnp.einsum(form, *args, precision=precision, preferred_element_type=jnp.float32)


def general(residual, position, owner, tile_local, xi, amplitude):
    n = lax.axis_size(both)
    n_base = lax.axis_size("base")
    n_slab = lax.axis_size("slab")
    me = lax.axis_index(both)
    rows, size = xi.shape
    depth = size // n
    half = depth // 2
    tiles = G // TILE

    region_rows = G // n_slab // TILE
    region_cols = G // n_base // TILE
    target = owner[:, 0]
    tile_row = (target % n_slab) * region_rows + tile_local // region_cols
    tile_col = (target // n_slab) * region_cols + tile_local % region_cols
    flip = tile_row >= tiles // 2
    tile_row = jnp.where(flip, tiles - 1 - tile_row, tile_row)
    tile_col = jnp.where(flip, tiles - 1 - tile_col, tile_col)
    code = tile_row * 256 + tile_col * 2 + flip.astype(jnp.int32)
    codes = lax.all_gather(code, both, axis=0, tiled=True)
    payload = jnp.concatenate([residual, position], axis=1)
    codes, payload = lax.optimization_barrier((codes, payload))
    gathered = lax.all_gather(payload, both, axis=0, tiled=True)
    blocks = codes.shape[0]
    grid_depth = G // 2 // n
    first_row = me * grid_depth
    mine = (codes // 256 == first_row // TILE).astype(jnp.int32)
    rank = jnp.where(mine == 1, jnp.cumsum(mine) - 1, -1)
    packed = lax.broadcasted_iota(jnp.int32, (blocks,), 0) * 256 + codes % 256
    spots = lax.broadcasted_iota(jnp.int32, (blocks, blocks), 0)
    table = jnp.sum(jnp.where(spots == rank[None, :], packed[None, :], 0), axis=1)
    info = jnp.stack([jnp.sum(mine), first_row % TILE]).astype(jnp.int32)

    outer, inner = row_tables(n, size)
    spectrum = (amplitude * xi).reshape(rows, n, depth)
    mid = einsum("rba,bqc->qcra", spectrum, outer)
    sent = einsum("cra,cae->cre", mid[0], inner[:, 0]) + einsum("cra,cae->cre", mid[1], inner[:, 1])
    sent, gathered = lax.optimization_barrier((sent, gathered))
    field = lax.all_to_all(sent, both, split_axis=0, concat_axis=0, tiled=True)
    field = field.reshape(size, depth)
    lane = lax.broadcasted_iota(jnp.int32, (1, depth), 1)
    still = (me == 0) & (lane % half == 0)

    def mirror(x):
        return jnp.where(still, x, jnp.roll(x, half, axis=-1))

    c_len = 128
    d_len = size // c_len
    bc, bs = (x.astype(np.float32) for x in trig(np.arange(c_len)[:, None] * np.arange(c_len)[None, :], c_len))
    shape = (c_len, d_len, depth)
    n0 = c_len * np.arange(d_len)[None, :] + np.arange(c_len)[:, None]
    ic, isn = (x.astype(np.float32) for x in trig(n0[:, :, None] * np.arange(d_len)[None, None, :], size))
    pair = jnp.stack([field.reshape(shape), mirror(field).reshape(shape)])
    first = np.stack([np.stack([bc, bs], 1), np.stack([bs, -bc], 1)], 0)
    turned = einsum("qbal,qbsc->csal", pair, first)
    second = np.stack([ic, -isn], axis=2)
    power = einsum("csal,cdsa->cdl", turned, second)
    sky = jnp.exp(power / size)

    grid = grid_rows(info, table, gathered, grid_depth)
    outer_g, inner_g = grid_row_tables(n, size)
    parts = tiles // n if tiles >= n else 1
    inner_len = G // n
    if inner_len >= TILE:
        view = grid.reshape(2, n, inner_len // TILE, grid_depth, TILE)
    else:
        flat = grid.transpose(0, 2, 1, 3).reshape(2, grid_depth, n, inner_len)
        view = flat.transpose(0, 2, 1, 3)[:, :, None]
        parts = 1
    lanes = view.shape[-1]
    stage = einsum("qbpra,qbsc->cspra", view, outer_g, precision=fine)
    inner_g = inner_g.reshape(n, 2, parts, lanes, 2 * depth)
    halves = einsum("cspra,cspae->cre", stage, inner_g, precision=fine)
    high = halves[:, :, depth:]
    high = jnp.concatenate([high[:1], jnp.flip(high[1:], axis=0)], axis=0)
    halves = jnp.concatenate([halves[:, :, :depth], high], axis=2)
    got = lax.all_to_all(halves, both, split_axis=0, concat_axis=0, tiled=True)
    got = got.reshape(size, 2 * depth)
    real = jnp.concatenate([got[:, :half], got[:, depth : depth + half]], axis=1)
    imag = jnp.concatenate([got[:, half:depth], got[:, depth + half :]], axis=1)
    wide = G // c_len
    deep = size // wide
    gc, gs = (x.astype(np.float32) for x in trig(np.arange(deep)[:, None] * np.arange(c_len)[None, :], c_len))
    first_g = np.stack([np.stack([gc, gs], 1), np.stack([-gs, gc], 1)], 0)
    whole = jnp.stack([real.reshape(deep, wide, depth), imag.reshape(deep, wide, depth)])
    turned_g = einsum("qbal,qbsc->csal", whole, first_g, precision=fine)
    ac, asn = trig((n0 + G // 4)[:, :, None] * np.arange(wide)[None, None, :], G)
    second_g = (np.stack([ac, -asn], axis=2) / G).astype(np.float32)
    back = einsum("csal,cdsa->cdl", turned_g, second_g, precision=fine)

    z = sky * back
    pz = einsum("cdl,cda->cal", z, ic)
    qz = einsum("cdl,cda->cal", z, isn)
    joined = jnp.stack([pz + mirror(qz), mirror(pz) - qz])
    fold = einsum("qcal,qcb->bal", joined, np.stack([bc, bs]))
    folded = lax.all_to_all(
        fold.reshape(n, rows, depth), both, split_axis=0, concat_axis=0, tiled=True
    )
    ends = einsum("jre,jqae->qjra", folded, inner)
    final = einsum("qjra,bqj->rba", ends, outer)
    return amplitude * final.reshape(rows, size) / size


MESH = pl.DeviceIdType.MESH
parts = ("base", "half", "quad")
LANES = 4


def exchange_kernel(nb, ns, send_ref, out_ref, bsend, brecv, usend, dsend, lrecv, hrecv, psend, precv, lsem):
    quads = ns // 2
    nz = ns // 2
    base = lax.axis_index("base")
    slab = lax.axis_index("half") * quads + lax.axis_index("quad")
    z = slab // 2
    core = slab % 2

    def at(b, s):
        return (b, s // quads, s % quads)

    def copy(source, target, here, there, device):
        return pltpu.make_async_remote_copy(
            src_ref=source, dst_ref=target, send_sem=here, recv_sem=there, device_id=device, device_id_type=MESH
        )

    def crossing(k):
        other = (base + k) % nb
        return copy(send_ref.at[other], out_ref.at[slab, base], bsend.at[k], brecv.at[k], at(other, slab))

    def arriving(k):
        from_base = (base - k + nb) % nb
        return copy(send_ref.at[base], out_ref.at[slab, from_base], bsend.at[k], brecv.at[k], at(from_base, slab))

    def block(origin, k):
        return out_ref.at[2 * origin + core, (base - k + nb) % nb]

    def upward(s, k):
        part = block(z - s, k)
        return copy(part, part, usend.at[s, k], lrecv.at[s + 1, k], at(base, slab + 2))

    def downward(s, k):
        part = block(z + s, k)
        return copy(part, part, dsend.at[s, k], hrecv.at[s + 1, k], at(base, slab - 2))

    def from_below(s, k):
        part = block(z - s, k)
        return copy(part, part, usend.at[s, k], lrecv.at[s, k], at(base, slab - 2))

    def from_above(s, k):
        part = block(z + s, k)
        return copy(part, part, dsend.at[s, k], hrecv.at[s, k], at(base, slab + 2))

    def across(origin, k):
        part = block(origin, k)
        return copy(part, part, psend.at[origin, k], precv.at[origin, k], at(base, slab + 1 - 2 * core))

    def from_partner(origin, k):
        part = out_ref.at[2 * origin + 1 - core, (base - k + nb) % nb]
        return copy(part, part, psend.at[origin, k], precv.at[origin, k], at(base, slab + 1 - 2 * core))

    barrier = pltpu.get_barrier_semaphore()
    for k in range(1, nb):
        pl.semaphore_signal(barrier, inc=1, device_id=at((base + k) % nb, slab), device_id_type=MESH)
    pl.semaphore_signal(barrier, inc=1, device_id=at(base, slab + 1 - 2 * core), device_id_type=MESH)

    @pl.when(z < nz - 1)
    def _():
        pl.semaphore_signal(barrier, inc=1, device_id=at(base, slab + 2), device_id_type=MESH)

    @pl.when(z > 0)
    def _():
        pl.semaphore_signal(barrier, inc=1, device_id=at(base, slab - 2), device_id_type=MESH)

    pl.semaphore_wait(barrier, nb + jnp.where(z < nz - 1, 1, 0) + jnp.where(z > 0, 1, 0))

    for k in range(1, nb):
        crossing(k).start()
    own = pltpu.make_async_copy(send_ref.at[base], out_ref.at[slab, base], lsem)
    own.start()

    def pass_on(s, k, ascending, descending):
        if ascending:
            @pl.when((z - s >= 0) & (z < nz - 1))
            def _():
                upward(s, k).start()

        if descending:
            @pl.when((z + s < nz) & (z > 0))
            def _():
                downward(s, k).start()

    for k in range(nb):
        if k == 0:
            own.wait()
        else:
            arriving(k).wait_recv()
        pass_on(0, k, True, True)
        across(z, k).start()
    for s in range(1, nz):
        for k in range(nb):
            @pl.when(z - s >= 0)
            def _():
                from_below(s, k).wait_recv()
                if s < nz - 1:
                    pass_on(s, k, True, False)
                across(z - s, k).start()

            @pl.when(z + s < nz)
            def _():
                from_above(s, k).wait_recv()
                if s < nz - 1:
                    pass_on(s, k, False, True)
                across(z + s, k).start()

    for origin in range(nz):
        for k in range(nb):
            from_partner(origin, k).wait_recv()
    for k in range(1, nb):
        crossing(k).wait_send()
    for s in range(nz - 1):
        for k in range(nb):
            @pl.when((z - s >= 0) & (z < nz - 1))
            def _():
                upward(s, k).wait_send()

            @pl.when((z + s < nz) & (z > 0))
            def _():
                downward(s, k).wait_send()

    for origin in range(nz):
        for k in range(nb):
            across(origin, k).wait_send()


def exchange(sent, ns):
    nb = sent.shape[0]
    nz = ns // 2
    dma = pltpu.SemaphoreType.DMA
    vmem = pl.BlockSpec(memory_space=pltpu.VMEM)
    return pl.pallas_call(
        functools.partial(exchange_kernel, nb, ns),
        out_shape=jax.ShapeDtypeStruct((ns,) + sent.shape, jnp.float32),
        in_specs=[vmem],
        out_specs=pl.BlockSpec(memory_space=pl.ANY),
        scratch_shapes=[
            dma((nb,)), dma((nb,)), dma((nz, nb)), dma((nz, nb)), dma((nz, nb)), dma((nz, nb)),
            dma((nz, nb)), dma((nz, nb)), dma,
        ],
        compiler_params=pltpu.CompilerParams(collective_id=0, has_side_effects=True, vmem_limit_bytes=16 << 20),
        name="exchange",
    )(sent)


def two_parts(x):
    high = x.astype(jnp.bfloat16)
    return high, (x - high.astype(jnp.float32)).astype(jnp.bfloat16)


def through(x, weight_ref, which):
    rows, depth = x.shape
    high, low = two_parts(x)
    made = jnp.dot(jnp.concatenate([high, low], axis=0), weight_ref[which, :depth], preferred_element_type=jnp.float32)
    return made[:rows] + made[rows:] + jnp.dot(high, weight_ref[which, depth:], preferred_element_type=jnp.float32)


def times(x, c, s):
    return x[0] * c - x[1] * s, x[0] * s + x[1] * c


def turn(x, angle):
    c, s = math.cos(angle), math.sin(angle)
    return times(x, c, s)


def add(x, y):
    return x[0] + y[0], x[1] + y[1]


def sub(x, y):
    return x[0] - y[0], x[1] - y[1]


def four(x):
    s0, d0, s1, d1 = add(x[0], x[2]), sub(x[0], x[2]), add(x[1], x[3]), sub(x[1], x[3])
    i1 = (-d1[1], d1[0])
    return [add(s0, s1), add(d0, i1), sub(s0, s1), sub(d0, i1)]


def sixteen(x):
    rows = []
    for b0 in range(4):
        y = four([x[4 * b1 + b0] for b1 in range(4)])
        rows.append([y[a0] if a0 * b0 == 0 else turn(y[a0], 2 * math.pi * a0 * b0 / 16) for a0 in range(4)])
    out = [None] * 16
    for a0 in range(4):
        y = four([rows[b0][a0] for b0 in range(4)])
        for a1 in range(4):
            out[a0 + 4 * a1] = y[a1]
    return out


def grid_kernel_two(info_ref, list_ref, first_ref, data_ref, turn_ref, undo_ref, weight_ref, out_ref, grid_ref, left_ref, right_ref):
    count = info_ref[0]
    parity = info_ref[1]
    grid_ref[...] = jnp.zeros_like(grid_ref)
    half = grid_ref.shape[1]
    group = 16
    cells = lax.broadcasted_iota(jnp.int32, (group + 8, TILE), 0).astype(jnp.float32) * 0.25
    nothing = jnp.zeros((group, TILE), jnp.bfloat16)

    def bump(offsets):
        d = cells - offsets
        kept = jnp.maximum(1.0 - d * d, 0.0)
        return kept * kept * kept

    def window(offsets):
        start = jnp.floor((offsets - 4.0) * (1.0 / group))
        offsets = (offsets - start * group) * 0.25
        return bump(offsets) - bump(offsets - 0.25), jnp.broadcast_to(start, (group, TILE)).astype(jnp.bfloat16)

    def spread(compact, start):
        padded = jnp.concatenate([compact, jnp.zeros((8, TILE), jnp.float32)], axis=0)
        out = []
        for part in two_parts(padded):
            first, second = part[:group], part[group:]
            pieces = []
            for g in range(TILE // group):
                piece = jnp.where(start == g - 1, second, nothing) if g else nothing
                pieces.append(jnp.where(start == g, first, piece))
            out.append(jnp.concatenate(pieces, axis=0))
        return out

    lanes = left_ref.shape[0]

    def place(k):
        packed = list_ref[k]
        return packed % 64, packed // 64

    def prepare(k, lane):
        col, rest = place(k)
        odd = jnp.where(col >= half, parity, 0)
        sign = jnp.where(k < count, 1 - 2 * odd, 0).astype(jnp.float32)
        block = data_ref[rest // 2]
        value = block[0:2, :] * sign
        row_taps, row_start = window(block[2:3, :])
        col_taps, col_start = window(block[3:4, :])
        rows_split = spread(row_taps, row_start)
        real = spread(col_taps * value[0:1, :], col_start)
        imag = spread(col_taps * value[1:2, :], col_start)
        for q in range(2):
            left_ref[lane, :, q * TILE : (q + 1) * TILE] = rows_split[q]
            right_ref[lane, :TILE, q * TILE : (q + 1) * TILE] = real[q]
            right_ref[lane, TILE:, q * TILE : (q + 1) * TILE] = imag[q]

    def product(lane):
        rh, rl = left_ref[lane, :, :TILE], left_ref[lane, :, TILE:]
        wh, wl = right_ref[lane, :, :TILE], right_ref[lane, :, TILE:]
        left = jnp.concatenate([rh, rh, rl], axis=1)
        right = jnp.concatenate([wh, wl, wh], axis=1)
        return lax.dot_general(left, right, (((1,), (1,)), ((), ())), preferred_element_type=jnp.float32)

    def step(k, carry):
        made = [product(lane) for lane in range(lanes)]
        for lane in range(lanes):
            prepare((k + 1) * lanes + lane, lane)
        for lane in range(lanes):
            col, rest = place(k * lanes + lane)
            col = jnp.where(col >= half, col - half, col)
            spot = pl.ds(pl.multiple_of((rest % 2) * TILE, TILE), TILE)
            grid_ref[0, col, spot, :] += made[lane][:, :TILE]
            grid_ref[1, col, spot, :] += made[lane][:, TILE:]
        return carry

    for lane in range(lanes):
        prepare(lane, lane)
    lax.fori_loop(0, (count + lanes - 1) // lanes, step, 0)

    depth = half // 2
    rows = grid_ref.shape[2]

    def outer(k, carry):
        spot = pl.ds(pl.multiple_of(k * 8, 8), 8)
        for side in range(2):
            x = []
            for b in range(depth):
                value = grid_ref[0, 2 * b + side, spot, :], grid_ref[1, 2 * b + side, spot, :]
                x.append(times(value, first_ref[b, 0], first_ref[b, 1]))
            for a, value in enumerate(sixteen(x)):
                c = turn_ref[a, side : side + 1, :]
                s = turn_ref[a, 2 + side : 3 + side, :]
                value = times(value, c, s)
                grid_ref[0, 2 * a + side, spot, :] = value[0]
                grid_ref[1, 2 * a + side, spot, :] = value[1]
        return carry

    lax.fori_loop(0, rows // 8, outer, 0)

    def inner(a, carry):
        mirrored = depth - parity - a
        mirrored = jnp.where(mirrored == depth, 0, mirrored)
        which = jnp.where((a == 0) & (parity == 0), 1, 0)
        for part in range(1):
            spot = pl.ds(0, rows)
            x = jnp.concatenate([grid_ref[q, 2 * a + side, spot, :] for q in range(2) for side in range(2)], axis=1)
            made = through(x, weight_ref, which)
            mid = TILE // 2
            made = times((made[:, :TILE], made[:, TILE:]), undo_ref[a, 0:1, :], undo_ref[a, 1:2, :])
            for q in range(2):
                out_ref[a, spot, q * TILE : q * TILE + mid] = made[q][:, :mid]
                out_ref[mirrored, spot, q * TILE + mid : (q + 1) * TILE] = made[q][:, mid:]
        return carry

    lax.fori_loop(0, depth, inner, 0)


def split_table(x):
    high = x.astype(np.float32).astype(jnp.bfloat16)
    low = (x - high.astype(np.float64)).astype(np.float32).astype(jnp.bfloat16)
    return high, low


def undone(pixels):
    c, s = trig(pixels + G // 4, G)
    return 1.0 / (1.0 - (c - 1j * s))


def grid_row_weights(n, size):
    depth = n // 2
    span = G // 2 // depth
    half = size // n // 2
    alpha = np.arange(span)
    turns, firsts, undos = [], [], []
    for p in range(2):
        j = 2 * np.arange(depth) + p
        c, s = trig(j[:, None] * alpha[None, :], G)
        turns.append(np.concatenate([c.reshape(depth, 2, TILE), s.reshape(depth, 2, TILE)], axis=1))
        firsts.append(np.stack(trig(np.arange(depth) * p, n), axis=1))
        low = n * np.arange(half)[None, :] + j[:, None]
        high = size - n * np.arange(half)[None, :] - ((-j) % n)[:, None]
        if p == 0:
            low[0, 0], high[0, 0] = 0, size // 2
        undo = undone(np.concatenate([low, high], axis=1))
        undos.append(np.stack([undo.real, undo.imag], axis=1))
    weights = []
    i = np.arange(half)
    for special in range(2):
        low = n * i
        high = size - n * i - (0 if special else n)
        if special:
            high[0] = size // 2
        parts_re, parts_im = [], []
        for cols in (low, high):
            c, s = trig(alpha[:, None] * (cols[None, :] + G // 4), G)
            parts_re.append(np.concatenate([c, -s], axis=0))
            parts_im.append(np.concatenate([s, c], axis=0))
        w = np.concatenate(parts_re + parts_im, axis=1)
        weights.append(np.concatenate(split_table(w), axis=0))
    turns, firsts, undos = (np.stack(x).astype(np.float32) for x in (turns, firsts, undos))
    return turns, firsts, undos, np.stack(weights)


def grid_rows_two(info, table, first, data, turns, undos, weights):
    depth = turns.shape[0]
    rows = 2 * TILE
    smem = pl.BlockSpec(memory_space=pltpu.SMEM)
    vmem = pl.BlockSpec(memory_space=pltpu.VMEM)
    return pl.pallas_call(
        grid_kernel_two,
        out_shape=jax.ShapeDtypeStruct((depth, rows, 2 * TILE), jnp.float32),
        in_specs=[smem, smem, smem, vmem, vmem, vmem, vmem],
        out_specs=vmem,
        scratch_shapes=[
            pltpu.VMEM((2, 2 * depth, rows, TILE), jnp.float32),
            pltpu.VMEM((LANES, TILE, 2 * TILE), jnp.bfloat16),
            pltpu.VMEM((LANES, 2 * TILE, 2 * TILE), jnp.bfloat16),
        ],
        compiler_params=pltpu.CompilerParams(vmem_limit_bytes=20 << 20),
        cost_estimate=pl.CostEstimate(flops=2 * 10**10, bytes_accessed=16 * 2**20, transcendentals=0),
        name="grid_rows_two",
    )(info, table, first, data, turns, undos, weights)


def minus(x):
    return [(b, a) for a, b in sixteen([(b, a) for a, b in x])]


def pick(table, u):
    side = table.shape[1] // 2
    return table[:, u : u + 1], table[:, side + u : side + u + 1]


def mirrored(x, still):
    return jnp.where(still, x, pltpu.roll(x, x.shape[1] // 2, 1))


def still_lanes(place, rows):
    lane = lax.broadcasted_iota(jnp.int32, (rows, TILE), 1)
    return (lane % (TILE // 2) == 0) & (place == 0)


def product(mat_ref, x):
    rows = mat_ref.shape[0] // 2
    high, low = two_parts(x)
    made = jnp.dot(mat_ref[...], high, preferred_element_type=jnp.float32)
    return made[:rows] + made[rows:] + jnp.dot(mat_ref[:rows], low, preferred_element_type=jnp.float32)


def beside(work_ref, u):
    sides = [jnp.concatenate([work_ref[u + q, 0], work_ref[u + q, 1]], axis=0) for q in range(2)]
    return jnp.concatenate(sides, axis=1)


def field_kernel(scale, info_ref, bend_ref, field_ref, turn_ref, mat_ref, slope_ref, sky_ref, work_ref):
    still = still_lanes(info_ref[0], 8)
    n = field_ref.shape[0]

    def outer(k, carry):
        spot = pl.ds(pl.multiple_of(k * 8, 8), 8)
        table = turn_ref[spot, :]
        for e in range(2):
            x = []
            for d in range(n // 2):
                first, second = field_ref[d, spot, :], field_ref[d + n // 2, spot, :]
                value = first - second if e else first + second
                value = value, mirrored(value, still)
                x.append(turn(value, -2 * math.pi * d / n) if e * d else value)
            for v, value in enumerate(minus(x)):
                u = 2 * v + e
                work_ref[u, 0, spot, :], work_ref[u, 1, spot, :] = times(value, *pick(table, u))
        return carry

    lax.fori_loop(0, field_ref.shape[1] // 8, outer, 0)

    def inner(k, carry):
        for u in (4 * k, 4 * k + 2):
            made = jnp.exp(product(mat_ref, beside(work_ref, u)) * scale)
            for q in range(2):
                sine = slope_ref[0] * bend_ref[u + q, 0] + slope_ref[1] * bend_ref[u + q, 1]
                sky_ref[u + q] = made[:, q * TILE : (q + 1) * TILE] / sine
        return carry

    lax.fori_loop(0, n // 4, inner, 0)


def image_kernel(info_ref, whole_ref, sky_ref, turn_g_ref, mat_g_ref, mat_f_ref, turn_ref, out_ref, work_ref, half_ref):
    still = still_lanes(info_ref[0], 8)
    n = sky_ref.shape[0]
    depth = n // 2

    def outer(k, carry):
        spot = pl.ds(pl.multiple_of(k * 8, 8), 8)
        table = turn_g_ref[spot, :]
        for e in range(2):
            x = []
            for a in range(depth):
                value = whole_ref[a, spot, :TILE], whole_ref[a, spot, TILE:]
                x.append(turn(value, 2 * math.pi * a / n) if e * a else value)
            for v, value in enumerate(sixteen(x)):
                u = 2 * v + e
                work_ref[u, 0, spot, :], work_ref[u, 1, spot, :] = times(value, *pick(table, u))
        return carry

    lax.fori_loop(0, whole_ref.shape[1] // 8, outer, 0)

    def inner(k, carry):
        for u in (4 * k, 4 * k + 2):
            made = product(mat_g_ref, beside(work_ref, u))
            z = jnp.concatenate([made[:, q * TILE : (q + 1) * TILE] * sky_ref[u + q] for q in range(2)], axis=1)
            spread = product(mat_f_ref, z)
            for q in range(2):
                for c in range(2):
                    work_ref[u + q, c, :TILE, :] = spread[c * TILE : (c + 1) * TILE, q * TILE : (q + 1) * TILE]
        return carry

    lax.fori_loop(0, n // 4, inner, 0)

    def last(k, carry):
        spot = pl.ds(pl.multiple_of(k * 8, 8), 8)
        table = turn_ref[spot, :]
        for e in range(2):
            x = []
            for v in range(depth):
                u = 2 * v + e
                x.append(times((work_ref[u, 0, spot, :], work_ref[u, 1, spot, :]), *pick(table, u)))
            for d, value in enumerate(minus(x)):
                if e == 0:
                    half_ref[d, 0], half_ref[d, 1] = value
                    continue
                value = turn(value, -2 * math.pi * d / n) if d else value
                before = half_ref[d, 0], half_ref[d, 1]
                for side, both_parts in enumerate((add(before, value), sub(before, value))):
                    out_ref[d + side * depth, spot, :] = both_parts[0] - mirrored(both_parts[1], still)
        return carry

    lax.fori_loop(0, TILE // 8, last, 0)


def seat(j, quads):
    a = j // 2
    return a // quads * (2 * quads) + j % 2 * quads + a % quads


def spectrum_kernel(quads, xi_ref, amplitude_ref, turn_ref, mat_ref, out_ref, work_ref):
    n = out_ref.shape[0]

    def outer(k, carry):
        spot = pl.ds(pl.multiple_of(k * 8, 8), 8)
        for e in range(2):
            x = []
            for b in range(n // 2):
                first, second = (
                    xi_ref[spot, c * TILE : (c + 1) * TILE] * amplitude_ref[spot, c * TILE : (c + 1) * TILE]
                    for c in (b, b + n // 2)
                )
                value = first - second if e else first + second
                if e * b:
                    angle = 2 * math.pi * b / n
                    x.append((value * math.cos(angle), value * math.sin(angle)))
                else:
                    x.append((value, jnp.zeros_like(value)))
            for v, value in enumerate(sixteen(x)):
                j = 2 * v + e
                work_ref[j, 0, spot, :], work_ref[j, 1, spot, :] = times(value, turn_ref[j, 0:1, :], turn_ref[j, 1:2, :])
        return carry

    lax.fori_loop(0, xi_ref.shape[0] // 8, outer, 0)
    rows = xi_ref.shape[0]

    def left(entries):
        return jnp.concatenate([jnp.concatenate([work_ref[j, 0], work_ref[j, 1]], axis=1) for j in entries], axis=0)

    def inner(k, carry):
        entries = [4 * k + q for q in range(4)]
        made = through(left(entries), mat_ref, 0)
        for q, j in enumerate(entries):
            out_ref[seat(j, quads)] = made[q * rows : (q + 1) * rows]
        return carry

    lax.fori_loop(0, n // 4, inner, 0)
    out_ref[0] = through(left([0]), mat_ref, 1)


def gradient_kernel(quads, scale, folded_ref, amplitude_ref, turn_ref, mat_ref, out_ref, work_ref, half_ref):
    n = folded_ref.shape[0]
    rows = folded_ref.shape[1]

    def before(entries, which):
        made = through(jnp.concatenate([folded_ref[seat(j, quads)] for j in entries], axis=0), mat_ref, which)
        for q, j in enumerate(entries):
            part = made[q * rows : (q + 1) * rows]
            work_ref[j, 0], work_ref[j, 1] = part[:, :TILE], part[:, TILE:]

    def inner(k, carry):
        before([4 * k + q for q in range(4)], 0)
        return carry

    lax.fori_loop(0, n // 4, inner, 0)
    before([0], 1)

    def outer(k, carry):
        spot = pl.ds(pl.multiple_of(k * 8, 8), 8)
        for e in range(2):
            x = []
            for v in range(n // 2):
                j = 2 * v + e
                x.append(times((work_ref[j, 0, spot, :], work_ref[j, 1, spot, :]), turn_ref[j, 0:1, :], turn_ref[j, 1:2, :]))
            for b, value in enumerate(sixteen(x)):
                if e == 0:
                    half_ref[b] = value[0]
                    continue
                real = turn(value, 2 * math.pi * b / n)[0] if b else value[0]
                for c, total in ((b, half_ref[b] + real), (b + n // 2, half_ref[b] - real)):
                    lanes = slice(c * TILE, (c + 1) * TILE)
                    out_ref[spot, lanes] = total * amplitude_ref[spot, lanes] * scale
        return carry

    lax.fori_loop(0, rows // 8, outer, 0)


def row_weights(n, size):
    alpha = np.arange(TILE)
    i = np.arange(size // n // 2)
    turns = np.stack(trig(np.arange(n)[:, None] * alpha[None, :], size), axis=1).astype(np.float32)
    c, s = trig(alpha[:, None] * i[None, :], size // n)
    there, back = [], []
    for special in range(2):
        real = np.concatenate([c + s, c - s], axis=1)
        imag = np.concatenate([c - s, -c - s], axis=1)
        from_real = np.concatenate([c + s, c - s], axis=1)
        from_imag = np.concatenate([s - c, s + c], axis=1)
        if special:
            lane = len(i)
            real[:, lane] = from_real[:, lane] = 1.0 - 2.0 * (alpha % 2)
            imag[:, lane] = from_imag[:, lane] = 0.0
        for target, matrix in ((there, np.concatenate([real, imag], axis=0)), (back, np.concatenate([from_real.T, from_imag.T], axis=1))):
            target.append(np.concatenate(split_table(matrix), axis=0))
    return turns, np.stack(there), np.stack(back)


def column_tables(n, size):
    w = np.arange(size // n)
    t = np.arange(TILE)
    u = np.arange(n)
    r = 2 * np.arange(2 * TILE) + 1
    side = TILE // 2

    def lanes(c, s):
        out = np.zeros((c.shape[0], TILE))
        out[:, :n], out[:, side : side + n] = c, s
        return out.astype(np.float32)

    def matrix(x):
        return np.concatenate(split_table(x), axis=0)

    c, s = trig(t[:, None] * u[None, :], size)
    turns = lanes(c, -s)
    c, s = trig(w[:, None] * t[None, :], size // n)
    mat_h = matrix(np.concatenate([c, s], axis=1))
    mat_f = matrix(np.concatenate([c.T, -s.T], axis=0))
    c, s = trig(r[:, None] * u[None, :], 2 * G)
    turns_g = lanes(c, s)
    c, s = trig((w[:, None] * n + G // 4) * r[None, :], 2 * G)
    mat_g = matrix(np.concatenate([s, c], axis=1))
    c, s = trig(w * n + G // 4, 2 * G)
    slope = np.stack([s, c]) * (2.0 * G)
    slope = np.broadcast_to(slope[:, :, None], slope.shape + (TILE,)).astype(np.float32)
    c, s = trig(u, 2 * G)
    bend = np.stack([c, s], axis=1).astype(np.float32)
    return turns, mat_h, mat_f, turns_g, mat_g, slope, bend


def column_call(kernel, smems, args, out_shape, scratch, name):
    smem = pl.BlockSpec(memory_space=pltpu.SMEM)
    vmem = pl.BlockSpec(memory_space=pltpu.VMEM)
    return pl.pallas_call(
        kernel,
        out_shape=jax.ShapeDtypeStruct(out_shape, jnp.float32),
        in_specs=[smem] * len(smems) + [vmem] * len(args),
        out_specs=vmem,
        scratch_shapes=scratch,
        compiler_params=pltpu.CompilerParams(vmem_limit_bytes=24 << 20),
        cost_estimate=pl.CostEstimate(flops=10**10, bytes_accessed=16 * 2**20, transcendentals=0),
        name=name,
    )(*smems, *args)


def shared(residual, position, owner, tile_local, xi, amplitude):
    n = lax.axis_size(parts)
    n_base = lax.axis_size("base")
    n_slab = lax.axis_size("half") * lax.axis_size("quad")
    quads = lax.axis_size("quad")
    base, parity, quad = (lax.axis_index(axis) for axis in parts)
    place = 2 * (base * quads + quad) + parity
    rows, size = xi.shape
    depth = size // n
    half = depth // 2
    tiles = G // TILE

    row_turns, there, back_again = (jnp.asarray(x) for x in row_weights(n, size))
    block = (n, rows, depth)
    work = pltpu.VMEM((n, 2, rows, depth), jnp.float32)
    spectrum = column_call(
        functools.partial(spectrum_kernel, quads), [], [xi, amplitude, row_turns, there], block, [work], "spectrum"
    )

    blocks = residual.shape[0]
    region_rows = G // n_slab // TILE
    region_cols = G // n_base // TILE
    room = 2 * n_base * (2 * blocks // n)
    target = owner[:, 0]
    tile_row = (target % n_slab) * region_rows + tile_local // region_cols
    tile_col = (target // n_slab) * region_cols + tile_local % region_cols
    flip = tile_row >= tiles // 2
    tile_row = jnp.where(flip, tiles - 1 - tile_row, tile_row)
    tile_col = jnp.where(flip, tiles - 1 - tile_col, tile_col)
    line = tile_row // n_slab
    code = (tile_row % n_slab) * tiles + tile_col
    flipped = flip[:, None]
    payload = jnp.stack(
        [
            residual[:, 0],
            jnp.where(flipped, -residual[:, 1], residual[:, 1]),
            jnp.where(flipped, TILE - position[:, 0], position[:, 0]),
            jnp.where(flipped, TILE - position[:, 1], position[:, 1]),
        ],
        axis=1,
    )
    earlier = (line[:, None] == line[None, :]) & (np.arange(blocks)[:, None] > np.arange(blocks)[None, :])
    slot = line * room + jnp.sum(earlier.astype(jnp.int32), axis=1)
    chosen = slot[None, :] == lax.broadcasted_iota(jnp.int32, (n_base * room, blocks), 0)
    moved = jnp.dot(chosen.astype(jnp.float32), payload.reshape(blocks, 4 * TILE), precision=fine)
    codes = jnp.sum(jnp.where(chosen, code[None, :] + 1, 0), axis=1) - 1
    codes = jnp.pad(codes.astype(jnp.float32).reshape(n_base, 1, 1, room), ((0, 0), (0, 0), (0, 3), (0, TILE - room)))
    sent = jnp.concatenate([moved.reshape(n_base, room, 4, TILE), codes], axis=1)
    got = exchange(sent, n_slab)
    spectrum, got = lax.optimization_barrier((spectrum, got))
    field = lax.all_to_all(spectrum, parts, split_axis=0, concat_axis=0, tiled=True)

    sources = n_slab * n_base
    codes = got[:, :, room, 0, :room].reshape(sources, room).astype(jnp.int32)
    mine = (codes >= 0) & (codes // tiles // 2 == quad)
    ones = mine.astype(jnp.float32)
    before = jnp.dot(ones, np.triu(np.ones((room, room), np.float32), 1), precision=fine)
    above = jnp.dot(np.tril(np.ones((sources, sources), np.float32), -1), ones, precision=fine)
    rank = (before + jnp.sum(above, axis=1, keepdims=True)).astype(jnp.int32)
    rank = jnp.where(mine, rank, -1).reshape(-1)
    index = lax.broadcasted_iota(jnp.int32, (sources, room), 0) * (room + 1) + lax.broadcasted_iota(jnp.int32, (sources, room), 1)
    packed = (index * (2 * tiles) + codes % (2 * tiles)).reshape(-1)
    spots = lax.broadcasted_iota(jnp.int32, (sources * room, sources * room), 0)
    table = jnp.sum(jnp.where(spots == rank[None, :], packed[None, :], 0), axis=1)
    table = jnp.pad(table, (0, 2 * LANES))
    info = jnp.stack([jnp.sum(mine.astype(jnp.int32)), parity]).astype(jnp.int32)

    turns, firsts, undos, weights = grid_row_weights(n, size)
    halves = grid_rows_two(
        info,
        table,
        lax.dynamic_index_in_dim(jnp.asarray(firsts), parity, 0, keepdims=False),
        got.reshape(sources * (room + 1), 4, TILE),
        lax.dynamic_index_in_dim(jnp.asarray(turns), parity, 0, keepdims=False),
        lax.dynamic_index_in_dim(jnp.asarray(undos), parity, 0, keepdims=False),
        jnp.asarray(weights),
    )
    whole = lax.all_to_all(halves, ("base", "quad"), split_axis=0, concat_axis=0, tiled=True)

    turns, mat_h, mat_f, turns_g, mat_g, slope, bend = (jnp.asarray(x) for x in column_tables(n, size))
    me = jnp.reshape(place, (1,)).astype(jnp.int32)
    sky = column_call(
        functools.partial(field_kernel, 1.0 / size),
        [me, bend],
        [field, turns, mat_h, slope],
        block,
        [work],
        "field",
    )
    fold = column_call(
        image_kernel,
        [me],
        [whole, sky, turns_g, mat_g, mat_f, turns],
        block,
        [pltpu.VMEM((n, 2, 2 * rows, depth), jnp.float32), pltpu.VMEM((n // 2, 2, 8, depth), jnp.float32)],
        "image",
    )
    folded = lax.all_to_all(fold, parts, split_axis=0, concat_axis=0, tiled=True)
    return column_call(
        functools.partial(gradient_kernel, quads, 1.0 / size),
        [],
        [folded, amplitude, row_turns, back_again],
        (rows, size),
        [work, pltpu.VMEM((n // 2, 8, depth), jnp.float32)],
        "gradient",
    )


def solution(mesh):
    n_base, n_slab = mesh.shape["base"], mesh.shape["slab"]
    body, axes = general, both
    if n_slab == 2 * n_base and 2 * n_base * n_slab == G // TILE:
        body, axes = shared, parts
        mesh = jax.sharding.Mesh(mesh.devices.reshape(n_base, 2, n_slab // 2), parts)
    placed = (
        P(axes, None, None),
        P(axes, None, None),
        P(axes, None),
        P(axes),
        P(axes, None),
        P(axes, None),
    )
    return jax.shard_map(body, mesh=mesh, in_specs=placed, out_specs=P(axes, None), check_vma=False)
```

```python
import functools
import math

import jax
import jax.numpy as jnp
import numpy as np
from jax import lax
from jax.experimental import pallas as pl
from jax.experimental.pallas import tpu as pltpu
from jax.sharding import PartitionSpec as P

G = 8192
TILE = 128
both = ("base", "slab")
fine = lax.Precision.HIGHEST


def trig(product, modulus):
    angle = (product % modulus).astype(np.float64) * (2.0 * np.pi / modulus)
    return np.cos(angle), np.sin(angle)


def column_table(n, size):
    depth = size // n
    half = depth // 2
    i = np.arange(half)[None, :]
    j = np.arange(n)[:, None]
    low = n * i + j
    high = (-low) % size
    high[0, 0] = size // 2
    return np.concatenate([low, high], axis=1)


def row_tables(n, size):
    depth = size // n
    cols = column_table(n, size)
    oc, osn = trig(np.arange(n)[:, None] * np.arange(n)[None, :], n)
    outer = np.stack([oc, osn], axis=1)
    prod = np.arange(depth)[None, :, None] * cols[:, None, :]
    c, s = trig(prod, size)
    sign = np.where(np.arange(depth) < depth // 2, 1.0, -1.0)[None, None, :]
    inner = np.stack([c + s, sign * (c - s)], axis=1)
    return outer.astype(np.float32), inner.astype(np.float32)


def grid_row_tables(n, size):
    depth = G // n
    cols = column_table(n, size)
    half = cols.shape[1] // 2
    oc, osn = trig(np.arange(n)[:, None] * np.arange(n)[None, :], n)
    outer = np.stack([np.stack([oc, osn], 1), np.stack([-osn, oc], 1)], 0)
    low = cols[:, :half]
    high = cols[(-np.arange(n)) % n, half:]
    a = np.arange(depth)[None, :, None]
    out = []
    for part in (low, high):
        c, s = trig(a * (part[:, None, :] + G // 4), G)
        out.append(np.stack([np.concatenate([c, s], 2), np.concatenate([-s, c], 2)], 1))
    return outer.astype(np.float32), np.concatenate(out, axis=3).astype(np.float32)


def taps(cells, offsets):
    scaled = (cells - offsets) * 0.25
    kept = jnp.maximum(1.0 - scaled * scaled, 0.0)
    return kept * kept * kept


def split_three(x):
    high = x.astype(jnp.bfloat16)
    rest = x - high.astype(jnp.float32)
    middle = rest.astype(jnp.bfloat16)
    return high, middle, (rest - middle.astype(jnp.float32)).astype(jnp.bfloat16)


def grid_kernel(rows, info_ref, list_ref, data_ref, out_ref):
    count = info_ref[0]
    first = info_ref[1].astype(jnp.float32)
    out_ref[...] = jnp.zeros_like(out_ref)
    row_cells = lax.broadcasted_iota(jnp.int32, (rows, TILE), 0).astype(jnp.float32) + first
    col_cells = lax.broadcasted_iota(jnp.int32, (TILE, TILE), 0).astype(jnp.float32)

    def step(k, carry):
        packed = list_ref[k]
        index = packed // 256
        col = (packed // 2) % 128
        flip = (packed % 2).astype(jnp.float32)
        sign = 1.0 - 2.0 * flip
        start = 128.0 * flip
        block = data_ref[index]
        value = block[0:2, :]
        place = block[2:4, :]
        row_taps = taps(row_cells * sign + start, place[0:1, :])
        col_taps = taps(col_cells * sign + start, place[1:2, :])
        weighted = jnp.concatenate(
            [col_taps * value[0:1, :], col_taps * (value[1:2, :] * sign)], axis=0
        )
        rh, rm, rl = split_three(row_taps)
        wh, wm, wl = split_three(weighted)
        left = jnp.concatenate([rh, rh, rh, rm, rm, rl], axis=1)
        right = jnp.concatenate([wh, wm, wl, wh, wm, wh], axis=1)
        sub = lax.dot_general(
            left, right, (((1,), (1,)), ((), ())), preferred_element_type=jnp.float32
        )
        out_ref[0, col] += sub[:, :TILE]
        out_ref[1, col] += sub[:, TILE:]
        return carry

    lax.fori_loop(0, count, step, 0)


def grid_rows(info, table, gathered, rows):
    tiles = G // TILE
    smem = pl.BlockSpec(memory_space=pltpu.SMEM)
    vmem = pl.BlockSpec(memory_space=pltpu.VMEM)
    return pl.pallas_call(
        functools.partial(grid_kernel, rows),
        out_shape=jax.ShapeDtypeStruct((2, tiles, rows, TILE), jnp.float32),
        in_specs=[smem, smem, vmem],
        out_specs=vmem,
        compiler_params=pltpu.CompilerParams(vmem_limit_bytes=56 * 1024 * 1024),
        cost_estimate=pl.CostEstimate(
            flops=2 * 10**10, bytes_accessed=16 * 2**20, transcendentals=0
        ),
        name="grid_rows",
    )(info, table, gathered)


def einsum(form, *args, precision=lax.Precision.HIGH):
    return jnp.einsum(form, *args, precision=precision, preferred_element_type=jnp.float32)


def general(residual, position, owner, tile_local, xi, amplitude):
    n = lax.axis_size(both)
    n_base = lax.axis_size("base")
    n_slab = lax.axis_size("slab")
    me = lax.axis_index(both)
    rows, size = xi.shape
    depth = size // n
    half = depth // 2
    tiles = G // TILE

    region_rows = G // n_slab // TILE
    region_cols = G // n_base // TILE
    target = owner[:, 0]
    tile_row = (target % n_slab) * region_rows + tile_local // region_cols
    tile_col = (target // n_slab) * region_cols + tile_local % region_cols
    flip = tile_row >= tiles // 2
    tile_row = jnp.where(flip, tiles - 1 - tile_row, tile_row)
    tile_col = jnp.where(flip, tiles - 1 - tile_col, tile_col)
    code = tile_row * 256 + tile_col * 2 + flip.astype(jnp.int32)
    codes = lax.all_gather(code, both, axis=0, tiled=True)
    payload = jnp.concatenate([residual, position], axis=1)
    codes, payload = lax.optimization_barrier((codes, payload))
    gathered = lax.all_gather(payload, both, axis=0, tiled=True)
    blocks = codes.shape[0]
    grid_depth = G // 2 // n
    first_row = me * grid_depth
    mine = (codes // 256 == first_row // TILE).astype(jnp.int32)
    rank = jnp.where(mine == 1, jnp.cumsum(mine) - 1, -1)
    packed = lax.broadcasted_iota(jnp.int32, (blocks,), 0) * 256 + codes % 256
    spots = lax.broadcasted_iota(jnp.int32, (blocks, blocks), 0)
    table = jnp.sum(jnp.where(spots == rank[None, :], packed[None, :], 0), axis=1)
    info = jnp.stack([jnp.sum(mine), first_row % TILE]).astype(jnp.int32)

    outer, inner = row_tables(n, size)
    spectrum = (amplitude * xi).reshape(rows, n, depth)
    mid = einsum("rba,bqc->qcra", spectrum, outer)
    sent = einsum("cra,cae->cre", mid[0], inner[:, 0]) + einsum("cra,cae->cre", mid[1], inner[:, 1])
    sent, gathered = lax.optimization_barrier((sent, gathered))
    field = lax.all_to_all(sent, both, split_axis=0, concat_axis=0, tiled=True)
    field = field.reshape(size, depth)
    lane = lax.broadcasted_iota(jnp.int32, (1, depth), 1)
    still = (me == 0) & (lane % half == 0)

    def mirror(x):
        return jnp.where(still, x, jnp.roll(x, half, axis=-1))

    c_len = 128
    d_len = size // c_len
    bc, bs = (x.astype(np.float32) for x in trig(np.arange(c_len)[:, None] * np.arange(c_len)[None, :], c_len))
    shape = (c_len, d_len, depth)
    n0 = c_len * np.arange(d_len)[None, :] + np.arange(c_len)[:, None]
    ic, isn = (x.astype(np.float32) for x in trig(n0[:, :, None] * np.arange(d_len)[None, None, :], size))
    pair = jnp.stack([field.reshape(shape), mirror(field).reshape(shape)])
    first = np.stack([np.stack([bc, bs], 1), np.stack([bs, -bc], 1)], 0)
    turned = einsum("qbal,qbsc->csal", pair, first)
    second = np.stack([ic, -isn], axis=2)
    power = einsum("csal,cdsa->cdl", turned, second)
    sky = jnp.exp(power / size)

    grid = grid_rows(info, table, gathered, grid_depth)
    outer_g, inner_g = grid_row_tables(n, size)
    parts = tiles // n if tiles >= n else 1
    inner_len = G // n
    if inner_len >= TILE:
        view = grid.reshape(2, n, inner_len // TILE, grid_depth, TILE)
    else:
        flat = grid.transpose(0, 2, 1, 3).reshape(2, grid_depth, n, inner_len)
        view = flat.transpose(0, 2, 1, 3)[:, :, None]
        parts = 1
    lanes = view.shape[-1]
    stage = einsum("qbpra,qbsc->cspra", view, outer_g, precision=fine)
    inner_g = inner_g.reshape(n, 2, parts, lanes, 2 * depth)
    halves = einsum("cspra,cspae->cre", stage, inner_g, precision=fine)
    high = halves[:, :, depth:]
    high = jnp.concatenate([high[:1], jnp.flip(high[1:], axis=0)], axis=0)
    halves = jnp.concatenate([halves[:, :, :depth], high], axis=2)
    got = lax.all_to_all(halves, both, split_axis=0, concat_axis=0, tiled=True)
    got = got.reshape(size, 2 * depth)
    real = jnp.concatenate([got[:, :half], got[:, depth : depth + half]], axis=1)
    imag = jnp.concatenate([got[:, half:depth], got[:, depth + half :]], axis=1)
    wide = G // c_len
    deep = size // wide
    gc, gs = (x.astype(np.float32) for x in trig(np.arange(deep)[:, None] * np.arange(c_len)[None, :], c_len))
    first_g = np.stack([np.stack([gc, gs], 1), np.stack([-gs, gc], 1)], 0)
    whole = jnp.stack([real.reshape(deep, wide, depth), imag.reshape(deep, wide, depth)])
    turned_g = einsum("qbal,qbsc->csal", whole, first_g, precision=fine)
    ac, asn = trig((n0 + G // 4)[:, :, None] * np.arange(wide)[None, None, :], G)
    second_g = (np.stack([ac, -asn], axis=2) / G).astype(np.float32)
    back = einsum("csal,cdsa->cdl", turned_g, second_g, precision=fine)

    z = sky * back
    pz = einsum("cdl,cda->cal", z, ic)
    qz = einsum("cdl,cda->cal", z, isn)
    joined = jnp.stack([pz + mirror(qz), mirror(pz) - qz])
    fold = einsum("qcal,qcb->bal", joined, np.stack([bc, bs]))
    folded = lax.all_to_all(
        fold.reshape(n, rows, depth), both, split_axis=0, concat_axis=0, tiled=True
    )
    ends = einsum("jre,jqae->qjra", folded, inner)
    final = einsum("qjra,bqj->rba", ends, outer)
    return amplitude * final.reshape(rows, size) / size


MESH = pl.DeviceIdType.MESH
parts = ("base", "half", "quad")
LANES = 4


def two_parts(x):
    high = x.astype(jnp.bfloat16)
    return high, (x - high.astype(jnp.float32)).astype(jnp.bfloat16)


def through(x, weight_ref, which):
    rows, depth = x.shape
    high, low = two_parts(x)
    made = jnp.dot(jnp.concatenate([high, low], axis=0), weight_ref[which, :depth], preferred_element_type=jnp.float32)
    return made[:rows] + made[rows:] + jnp.dot(high, weight_ref[which, depth:], preferred_element_type=jnp.float32)


def times(x, c, s):
    return x[0] * c - x[1] * s, x[0] * s + x[1] * c


def turn(x, angle):
    c, s = math.cos(angle), math.sin(angle)
    return times(x, c, s)


def add(x, y):
    return x[0] + y[0], x[1] + y[1]


def sub(x, y):
    return x[0] - y[0], x[1] - y[1]


def four(x):
    s0, d0, s1, d1 = add(x[0], x[2]), sub(x[0], x[2]), add(x[1], x[3]), sub(x[1], x[3])
    i1 = (-d1[1], d1[0])
    return [add(s0, s1), add(d0, i1), sub(s0, s1), sub(d0, i1)]


def sixteen(x):
    rows = []
    for b0 in range(4):
        y = four([x[4 * b1 + b0] for b1 in range(4)])
        rows.append([y[a0] if a0 * b0 == 0 else turn(y[a0], 2 * math.pi * a0 * b0 / 16) for a0 in range(4)])
    out = [None] * 16
    for a0 in range(4):
        y = four([rows[b0][a0] for b0 in range(4)])
        for a1 in range(4):
            out[a0 + 4 * a1] = y[a1]
    return out


def seat(j, quads):
    a = j // 2
    return a // quads * (2 * quads) + j % 2 * quads + a % quads


def transform_rows(quads, xi_ref, amplitude_ref, turn_ref, mat_ref, out_ref, work_ref):
    n = out_ref.shape[0]

    def outer(k, carry):
        spot = pl.ds(pl.multiple_of(k * 8, 8), 8)
        for e in range(2):
            x = []
            for b in range(n // 2):
                first, second = (
                    xi_ref[spot, c * TILE : (c + 1) * TILE] * amplitude_ref[spot, c * TILE : (c + 1) * TILE]
                    for c in (b, b + n // 2)
                )
                value = first - second if e else first + second
                if e * b:
                    angle = 2 * math.pi * b / n
                    x.append((value * math.cos(angle), value * math.sin(angle)))
                else:
                    x.append((value, jnp.zeros_like(value)))
            for v, value in enumerate(sixteen(x)):
                j = 2 * v + e
                work_ref[j, 0, spot, :], work_ref[j, 1, spot, :] = times(value, turn_ref[j, 0:1, :], turn_ref[j, 1:2, :])
        return carry

    lax.fori_loop(0, xi_ref.shape[0] // 8, outer, 0)
    rows = xi_ref.shape[0]

    def left(entries):
        return jnp.concatenate([jnp.concatenate([work_ref[j, 0], work_ref[j, 1]], axis=1) for j in entries], axis=0)

    def inner(k, carry):
        entries = [4 * k + q for q in range(4)]
        made = through(left(entries), mat_ref, 0)
        for q, j in enumerate(entries):
            out_ref[seat(j, quads)] = made[q * rows : (q + 1) * rows]
        return carry

    lax.fori_loop(0, n // 4, inner, 0)
    out_ref[0] = through(left([0]), mat_ref, 1)


def exchange_kernel(nb, ns, send_ref, xi_ref, amplitude_ref, turn_ref, mat_ref, out_ref, spectrum_ref, work_ref, rows_ref, rows_sem, bsend, brecv, usend, dsend, lrecv, hrecv, psend, precv, lsem):
    quads = ns // 2
    nz = ns // 2
    base = lax.axis_index("base")
    slab = lax.axis_index("half") * quads + lax.axis_index("quad")
    z = slab // 2
    core = slab % 2

    def at(b, s):
        return (b, s // quads, s % quads)

    def copy(source, target, here, there, device):
        return pltpu.make_async_remote_copy(
            src_ref=source, dst_ref=target, send_sem=here, recv_sem=there, device_id=device, device_id_type=MESH
        )

    def crossing(k):
        other = (base + k) % nb
        return copy(send_ref.at[other], out_ref.at[slab, base], bsend.at[k], brecv.at[k], at(other, slab))

    def arriving(k):
        from_base = (base - k + nb) % nb
        return copy(send_ref.at[base], out_ref.at[slab, from_base], bsend.at[k], brecv.at[k], at(from_base, slab))

    def block(origin, k):
        return out_ref.at[2 * origin + core, (base - k + nb) % nb]

    def upward(s, k):
        part = block(z - s, k)
        return copy(part, part, usend.at[s, k], lrecv.at[s + 1, k], at(base, slab + 2))

    def downward(s, k):
        part = block(z + s, k)
        return copy(part, part, dsend.at[s, k], hrecv.at[s + 1, k], at(base, slab - 2))

    def from_below(s, k):
        part = block(z - s, k)
        return copy(part, part, usend.at[s, k], lrecv.at[s, k], at(base, slab - 2))

    def from_above(s, k):
        part = block(z + s, k)
        return copy(part, part, dsend.at[s, k], hrecv.at[s, k], at(base, slab + 2))

    def across(origin, k):
        part = block(origin, k)
        return copy(part, part, psend.at[origin, k], precv.at[origin, k], at(base, slab + 1 - 2 * core))

    def from_partner(origin, k):
        part = out_ref.at[2 * origin + 1 - core, (base - k + nb) % nb]
        return copy(part, part, psend.at[origin, k], precv.at[origin, k], at(base, slab + 1 - 2 * core))

    fetches = [
        pltpu.make_async_copy(source, rows_ref.at[k], rows_sem.at[k]) for k, source in enumerate((xi_ref, amplitude_ref))
    ]
    for fetch in fetches:
        fetch.start()
    barrier = pltpu.get_barrier_semaphore()
    for k in range(1, nb):
        pl.semaphore_signal(barrier, inc=1, device_id=at((base + k) % nb, slab), device_id_type=MESH)
    pl.semaphore_signal(barrier, inc=1, device_id=at(base, slab + 1 - 2 * core), device_id_type=MESH)

    @pl.when(z < nz - 1)
    def _():
        pl.semaphore_signal(barrier, inc=1, device_id=at(base, slab + 2), device_id_type=MESH)

    @pl.when(z > 0)
    def _():
        pl.semaphore_signal(barrier, inc=1, device_id=at(base, slab - 2), device_id_type=MESH)

    pl.semaphore_wait(barrier, nb + jnp.where(z < nz - 1, 1, 0) + jnp.where(z > 0, 1, 0))

    for k in range(1, nb):
        crossing(k).start()
    own = pltpu.make_async_copy(send_ref.at[base], out_ref.at[slab, base], lsem)
    own.start()

    def pass_on(s, k, ascending, descending):
        if ascending:
            @pl.when((z - s >= 0) & (z < nz - 1))
            def _():
                upward(s, k).start()

        if descending:
            @pl.when((z + s < nz) & (z > 0))
            def _():
                downward(s, k).start()

    for k in range(nb):
        if k == 0:
            own.wait()
        else:
            arriving(k).wait_recv()
        pass_on(0, k, True, True)
        across(z, k).start()
        if k == 0:
            for fetch in fetches:
                fetch.wait()
            transform_rows(quads, rows_ref.at[0], rows_ref.at[1], turn_ref, mat_ref, spectrum_ref, work_ref)
    for s in range(1, nz):
        for k in range(nb):
            @pl.when(z - s >= 0)
            def _():
                from_below(s, k).wait_recv()
                if s < nz - 1:
                    pass_on(s, k, True, False)
                across(z - s, k).start()

            @pl.when(z + s < nz)
            def _():
                from_above(s, k).wait_recv()
                if s < nz - 1:
                    pass_on(s, k, False, True)
                across(z + s, k).start()

    for origin in range(nz):
        for k in range(nb):
            from_partner(origin, k).wait_recv()
    for k in range(1, nb):
        crossing(k).wait_send()
    for s in range(nz - 1):
        for k in range(nb):
            @pl.when((z - s >= 0) & (z < nz - 1))
            def _():
                upward(s, k).wait_send()

            @pl.when((z + s < nz) & (z > 0))
            def _():
                downward(s, k).wait_send()

    for origin in range(nz):
        for k in range(nb):
            across(origin, k).wait_send()


def pack_kernel(keys, room, what_ref, residual_ref, position_ref, out_ref):
    blocks = residual_ref.shape[0]
    nb = out_ref.shape[0]
    across = lax.broadcasted_iota(jnp.int32, (blocks, blocks), 1)
    down = lax.broadcasted_iota(jnp.int32, (blocks, blocks), 0)

    def column(row):
        return jnp.sum(jnp.where(across == down, row, 0.0), axis=1, keepdims=True)

    what = what_ref[...].astype(jnp.float32)
    line, key, code, flip = (what[k : k + 1, :] for k in range(4))
    line_down, key_down, flip_down = column(line), column(key), column(flip)
    before = (line_down == line) & ((key_down < key) | ((key_down == key) & (down < across)))
    slot = line * room + jnp.sum(jnp.where(before, 1.0, 0.0), axis=0, keepdims=True)
    slots = lax.broadcasted_iota(jnp.int32, (nb * room, blocks), 0).astype(jnp.float32)
    chosen = jnp.where(slots == slot, 1.0, 0.0).astype(jnp.bfloat16)
    sides = [residual_ref[:, 0, :], residual_ref[:, 1, :] * (1.0 - 2.0 * flip_down)]
    for k in range(2):
        place = position_ref[:, k, :]
        sides.append(jnp.where(flip_down > 0.5, TILE - place, place))
    pieces = split_three(jnp.concatenate(sides, axis=1))
    moved = jnp.dot(
        jnp.concatenate([chosen] * 3, axis=1), jnp.concatenate(pieces, axis=0), preferred_element_type=jnp.float32
    )
    codes = 0.0
    for part in two_parts(jnp.broadcast_to(code + 1.0, (8, blocks))):
        codes = codes + lax.dot_general(part, chosen, (((1,), (1,)), ((), ())), preferred_element_type=jnp.float32)
    codes = codes - 1.0
    lanes = lax.broadcasted_iota(jnp.int32, (1, blocks), 1)
    shift = (across - room).astype(jnp.float32)
    per = blocks // room
    for k in range(nb):
        for c in range(4):
            out_ref[k, :room, c, :] = moved[k * room : (k + 1) * room, c * TILE : (c + 1) * TILE]
        start = k // per * blocks
        own = codes[:, start : start + blocks]
        if k % per:
            own = pltpu.roll(own, blocks - k % per * room, 1)
        earlier = (line_down == k) & (key_down - keys * k < shift)
        starts = jnp.sum(jnp.where(earlier, 1.0, 0.0), axis=0, keepdims=True)
        out_ref[k, room] = jnp.broadcast_to(jnp.where(lanes < room, own[0:1, :], starts), (4, TILE))


def pack(what, residual, position, nb, keys, room):
    vmem = pl.BlockSpec(memory_space=pltpu.VMEM)
    return pl.pallas_call(
        functools.partial(pack_kernel, keys, room),
        out_shape=jax.ShapeDtypeStruct((nb, room + 1, 4, TILE), jnp.float32),
        in_specs=[vmem] * 3,
        out_specs=vmem,
        compiler_params=pltpu.CompilerParams(vmem_limit_bytes=16 << 20),
        name="pack",
    )(what, residual, position)


def exchange(sent, ns, xi, amplitude, turns, mats):
    nb = sent.shape[0]
    nz = ns // 2
    rows, n = xi.shape[0], turns.shape[0]
    dma = pltpu.SemaphoreType.DMA
    vmem = pl.BlockSpec(memory_space=pltpu.VMEM)
    hbm = pl.BlockSpec(memory_space=pltpu.HBM)
    return pl.pallas_call(
        functools.partial(exchange_kernel, nb, ns),
        out_shape=(
            jax.ShapeDtypeStruct((ns,) + sent.shape, jnp.float32),
            jax.ShapeDtypeStruct((n, rows, TILE), jnp.float32),
        ),
        in_specs=[vmem, hbm, hbm, vmem, vmem],
        out_specs=(hbm, vmem),
        scratch_shapes=[
            pltpu.VMEM((n, 2, rows, TILE), jnp.float32),
            pltpu.VMEM((2,) + xi.shape, jnp.float32), dma((2,)),
            dma((nb,)), dma((nb,)), dma((nz, nb)), dma((nz, nb)), dma((nz, nb)), dma((nz, nb)),
            dma((nz, nb)), dma((nz, nb)), dma,
        ],
        compiler_params=pltpu.CompilerParams(collective_id=0, has_side_effects=True, vmem_limit_bytes=60 << 20),
        cost_estimate=pl.CostEstimate(flops=3 * 10**10, bytes_accessed=16 * 2**20, transcendentals=0),
        name="exchange",
    )(sent, xi, amplitude, turns, mats)


def grid_kernel_two(room, info_ref, codes_ref, first_ref, data_hbm_ref, turn_ref, undo_ref, weight_hbm_ref, away_ref, grid_ref, left_ref, right_ref, out_ref, data_ref, weight_ref, list_ref, sems):
    quad = info_ref[0]
    parity = info_ref[1]
    data = pltpu.make_async_copy(data_hbm_ref, data_ref, sems.at[out_ref.shape[0]])
    weight = pltpu.make_async_copy(weight_hbm_ref, weight_ref, sems.at[out_ref.shape[0] + 1])
    data.start()
    weight.start()
    grid_ref[...] = jnp.zeros_like(grid_ref)
    half = grid_ref.shape[1]
    group = 16
    cells = lax.broadcasted_iota(jnp.int32, (group + 8, TILE), 0).astype(jnp.float32) * 0.25
    nothing = jnp.zeros((group, TILE), jnp.bfloat16)

    def bump(offsets):
        d = cells - offsets
        kept = jnp.maximum(1.0 - d * d, 0.0)
        return kept * kept * kept

    def window(offsets):
        start = jnp.floor((offsets - 4.0) * (1.0 / group))
        offsets = (offsets - start * group) * 0.25
        return bump(offsets) - bump(offsets - 0.25), jnp.broadcast_to(start, (group, TILE)).astype(jnp.bfloat16)

    def spread(compact, start):
        padded = jnp.concatenate([compact, jnp.zeros((8, TILE), jnp.float32)], axis=0)
        out = []
        for part in two_parts(padded):
            first, second = part[:group], part[group:]
            pieces = []
            for g in range(TILE // group):
                piece = jnp.where(start == g - 1, second, nothing) if g else nothing
                pieces.append(jnp.where(start == g, first, piece))
            out.append(jnp.concatenate(pieces, axis=0))
        return out

    lanes = left_ref.shape[0]

    def place(k):
        packed = list_ref[k]
        return packed % 64, packed // 64

    def prepare(k, lane, count):
        col, rest = place(k)
        odd = jnp.where(col >= half, parity, 0)
        sign = jnp.where(k < count, 1 - 2 * odd, 0).astype(jnp.float32)
        block = data_ref[rest // 2]
        value = block[0:2, :] * sign
        row_taps, row_start = window(block[2:3, :])
        col_taps, col_start = window(block[3:4, :])
        rows_split = spread(row_taps, row_start)
        real = spread(col_taps * value[0:1, :], col_start)
        imag = spread(col_taps * value[1:2, :], col_start)
        for q in range(2):
            left_ref[lane, :, q * TILE : (q + 1) * TILE] = rows_split[q]
            right_ref[lane, :TILE, q * TILE : (q + 1) * TILE] = real[q]
            right_ref[lane, TILE:, q * TILE : (q + 1) * TILE] = imag[q]

    def product(lane):
        rh, rl = left_ref[lane, :, :TILE], left_ref[lane, :, TILE:]
        wh, wl = right_ref[lane, :, :TILE], right_ref[lane, :, TILE:]
        left = jnp.concatenate([rh, rh, rl], axis=1)
        right = jnp.concatenate([wh, wl, wh], axis=1)
        return lax.dot_general(left, right, (((1,), (1,)), ((), ())), preferred_element_type=jnp.float32)

    def step(k, carry):
        made = [product(lane) for lane in range(lanes)]
        for lane in range(lanes):
            prepare((k + 1) * lanes + lane, lane, count)
        for lane in range(lanes):
            col, rest = place(k * lanes + lane)
            col = jnp.where(col >= half, col - half, col)
            spot = pl.ds(pl.multiple_of((rest % 2) * TILE, TILE), TILE)
            grid_ref[0, col, spot, :] += made[lane][:, :TILE]
            grid_ref[1, col, spot, :] += made[lane][:, TILE:]
        return carry

    def gather(source, filled):
        start = codes_ref[source, room + quad]
        stop = codes_ref[source, room + quad + 1]

        def entry(i, carry):
            list_ref[filled + i - start] = (source * (room + 1) + i) * TILE + codes_ref[source, i] % TILE
            return carry

        lax.fori_loop(start, stop, entry, 0)
        return filled + stop - start

    count = lax.fori_loop(0, codes_ref.shape[0], gather, 0)
    for lane in range(2 * lanes):
        list_ref[count + lane] = 0
    data.wait()
    for lane in range(lanes):
        prepare(lane, lane, count)
    lax.fori_loop(0, (count + lanes - 1) // lanes, step, 0)

    depth = half // 2
    rows = grid_ref.shape[2]

    def outer(k, carry):
        spot = pl.ds(pl.multiple_of(k * 8, 8), 8)
        for side in range(2):
            x = []
            for b in range(depth):
                value = grid_ref[0, 2 * b + side, spot, :], grid_ref[1, 2 * b + side, spot, :]
                x.append(times(value, first_ref[parity, b, 0], first_ref[parity, b, 1]))
            for a, value in enumerate(sixteen(x)):
                c = turn_ref[parity, a, side : side + 1, :]
                s = turn_ref[parity, a, 2 + side : 3 + side, :]
                value = times(value, c, s)
                grid_ref[0, 2 * a + side, spot, :] = value[0]
                grid_ref[1, 2 * a + side, spot, :] = value[1]
        return carry

    lax.fori_loop(0, rows // 8, outer, 0)

    def inner(a, carry):
        mirrored = depth - parity - a
        mirrored = jnp.where(mirrored == depth, 0, mirrored)
        which = jnp.where((a == 0) & (parity == 0), 1, 0)
        for part in range(1):
            spot = pl.ds(0, rows)
            x = jnp.concatenate([grid_ref[q, 2 * a + side, spot, :] for q in range(2) for side in range(2)], axis=1)
            made = through(x, weight_ref, which)
            mid = TILE // 2
            made = times((made[:, :TILE], made[:, TILE:]), undo_ref[parity, a, 0:1, :], undo_ref[parity, a, 1:2, :])
            for q in range(2):
                out_ref[a, spot, q * TILE : q * TILE + mid] = made[q][:, :mid]
                out_ref[mirrored, spot, q * TILE + mid : (q + 1) * TILE] = made[q][:, mid:]

        @pl.when(a >= depth // 2)
        def _():
            leave(a).start()
            leave(jnp.where((parity == 0) & (a == depth // 2), 0, mirrored)).start()

        return carry

    def leave(a):
        return pltpu.make_async_copy(out_ref.at[a], away_ref.at[a], sems.at[a])

    weight.wait()
    lax.fori_loop(0, depth, inner, 0)
    for a in range(depth):
        leave(a).wait()


def split_table(x):
    high = x.astype(np.float32).astype(jnp.bfloat16)
    low = (x - high.astype(np.float64)).astype(np.float32).astype(jnp.bfloat16)
    return high, low


def undone(pixels):
    c, s = trig(pixels + G // 4, G)
    return 1.0 / (1.0 - (c - 1j * s))


def grid_row_weights(n, size):
    depth = n // 2
    span = G // 2 // depth
    half = size // n // 2
    alpha = np.arange(span)
    turns, firsts, undos = [], [], []
    for p in range(2):
        j = 2 * np.arange(depth) + p
        c, s = trig(j[:, None] * alpha[None, :], G)
        turns.append(np.concatenate([c.reshape(depth, 2, TILE), s.reshape(depth, 2, TILE)], axis=1))
        firsts.append(np.stack(trig(np.arange(depth) * p, n), axis=1))
        low = n * np.arange(half)[None, :] + j[:, None]
        high = size - n * np.arange(half)[None, :] - ((-j) % n)[:, None]
        if p == 0:
            low[0, 0], high[0, 0] = 0, size // 2
        undo = undone(np.concatenate([low, high], axis=1))
        undos.append(np.stack([undo.real, undo.imag], axis=1))
    weights = []
    i = np.arange(half)
    for special in range(2):
        low = n * i
        high = size - n * i - (0 if special else n)
        if special:
            high[0] = size // 2
        parts_re, parts_im = [], []
        for cols in (low, high):
            c, s = trig(alpha[:, None] * (cols[None, :] + G // 4), G)
            parts_re.append(np.concatenate([c, -s], axis=0))
            parts_im.append(np.concatenate([s, c], axis=0))
        w = np.concatenate(parts_re + parts_im, axis=1)
        weights.append(np.concatenate(split_table(w), axis=0))
    turns, firsts, undos = (np.stack(x).astype(np.float32) for x in (turns, firsts, undos))
    return turns, firsts, undos, np.stack(weights)


def grid_rows_two(room, info, codes, first, data, turns, undos, weights):
    depth = turns.shape[1]
    rows = 2 * TILE
    smem = pl.BlockSpec(memory_space=pltpu.SMEM)
    vmem = pl.BlockSpec(memory_space=pltpu.VMEM)
    hbm = pl.BlockSpec(memory_space=pltpu.HBM)
    return pl.pallas_call(
        functools.partial(grid_kernel_two, room),
        out_shape=jax.ShapeDtypeStruct((depth, rows, 2 * TILE), jnp.float32),
        in_specs=[smem, smem, smem, hbm, vmem, vmem, hbm],
        out_specs=hbm,
        scratch_shapes=[
            pltpu.VMEM((2, 2 * depth, rows, TILE), jnp.float32),
            pltpu.VMEM((LANES, TILE, 2 * TILE), jnp.bfloat16),
            pltpu.VMEM((LANES, 2 * TILE, 2 * TILE), jnp.bfloat16),
            pltpu.VMEM((depth, rows, 2 * TILE), jnp.float32),
            pltpu.VMEM(data.shape, jnp.float32),
            pltpu.VMEM(weights.shape, jnp.bfloat16),
            pltpu.SMEM((codes.shape[0] * room + 2 * LANES,), jnp.int32),
            pltpu.SemaphoreType.DMA((depth + 2,)),
        ],
        compiler_params=pltpu.CompilerParams(vmem_limit_bytes=60 << 20),
        cost_estimate=pl.CostEstimate(flops=2 * 10**10, bytes_accessed=16 * 2**20, transcendentals=0),
        name="grid_rows_two",
    )(info, codes, first, data, turns, undos, weights)


def minus(x):
    return [(b, a) for a, b in sixteen([(b, a) for a, b in x])]


def pick(table, u):
    side = table.shape[1] // 2
    return table[:, u : u + 1], table[:, side + u : side + u + 1]


def mirrored(x, still):
    return jnp.where(still, x, pltpu.roll(x, x.shape[1] // 2, 1))


def still_lanes(place, rows):
    lane = lax.broadcasted_iota(jnp.int32, (rows, TILE), 1)
    return (lane % (TILE // 2) == 0) & (place == 0)


def product(mat_ref, x):
    rows = mat_ref.shape[0] // 2
    high, low = two_parts(x)
    made = jnp.dot(mat_ref[...], high, preferred_element_type=jnp.float32)
    return made[:rows] + made[rows:] + jnp.dot(mat_ref[:rows], low, preferred_element_type=jnp.float32)


def beside(work_ref, u):
    sides = [jnp.concatenate([work_ref[u + q, 0], work_ref[u + q, 1]], axis=0) for q in range(2)]
    return jnp.concatenate(sides, axis=1)


def field_kernel(scale, info_ref, bend_ref, field_ref, turn_ref, mat_ref, slope_ref, sky_ref, work_ref):
    still = still_lanes(info_ref[0], 8)
    n = field_ref.shape[0]

    def outer(k, carry):
        spot = pl.ds(pl.multiple_of(k * 8, 8), 8)
        table = turn_ref[spot, :]
        for e in range(2):
            x = []
            for d in range(n // 2):
                first, second = field_ref[d, spot, :], field_ref[d + n // 2, spot, :]
                value = first - second if e else first + second
                value = value, mirrored(value, still)
                x.append(turn(value, -2 * math.pi * d / n) if e * d else value)
            for v, value in enumerate(minus(x)):
                u = 2 * v + e
                work_ref[u, 0, spot, :], work_ref[u, 1, spot, :] = times(value, *pick(table, u))
        return carry

    lax.fori_loop(0, field_ref.shape[1] // 8, outer, 0)

    def inner(k, carry):
        for u in (4 * k, 4 * k + 2):
            made = jnp.exp(product(mat_ref, beside(work_ref, u)) * scale)
            for q in range(2):
                sine = slope_ref[0] * bend_ref[u + q, 0] + slope_ref[1] * bend_ref[u + q, 1]
                sky_ref[u + q] = made[:, q * TILE : (q + 1) * TILE] / sine
        return carry

    lax.fori_loop(0, n // 4, inner, 0)


def image_kernel(info_ref, whole_ref, sky_ref, turn_g_ref, mat_g_ref, mat_f_ref, turn_ref, out_ref, work_ref, half_ref, held_ref, held_sem):
    still = still_lanes(info_ref[0], 8)
    n = sky_ref.shape[0]
    fetch = pltpu.make_async_copy(sky_ref, held_ref, held_sem)
    fetch.start()
    depth = n // 2

    def outer(k, carry):
        spot = pl.ds(pl.multiple_of(k * 8, 8), 8)
        table = turn_g_ref[spot, :]
        for e in range(2):
            x = []
            for a in range(depth):
                value = whole_ref[a, spot, :TILE], whole_ref[a, spot, TILE:]
                x.append(turn(value, 2 * math.pi * a / n) if e * a else value)
            for v, value in enumerate(sixteen(x)):
                u = 2 * v + e
                work_ref[u, 0, spot, :], work_ref[u, 1, spot, :] = times(value, *pick(table, u))
        return carry

    lax.fori_loop(0, whole_ref.shape[1] // 8, outer, 0)

    fetch.wait()

    def inner(k, carry):
        for u in (4 * k, 4 * k + 2):
            made = product(mat_g_ref, beside(work_ref, u))
            z = jnp.concatenate([made[:, q * TILE : (q + 1) * TILE] * held_ref[u + q] for q in range(2)], axis=1)
            spread = product(mat_f_ref, z)
            for q in range(2):
                for c in range(2):
                    work_ref[u + q, c, :TILE, :] = spread[c * TILE : (c + 1) * TILE, q * TILE : (q + 1) * TILE]
        return carry

    lax.fori_loop(0, n // 4, inner, 0)

    def last(k, carry):
        spot = pl.ds(pl.multiple_of(k * 8, 8), 8)
        table = turn_ref[spot, :]
        for e in range(2):
            x = []
            for v in range(depth):
                u = 2 * v + e
                x.append(times((work_ref[u, 0, spot, :], work_ref[u, 1, spot, :]), *pick(table, u)))
            for d, value in enumerate(minus(x)):
                if e == 0:
                    half_ref[d, 0], half_ref[d, 1] = value
                    continue
                value = turn(value, -2 * math.pi * d / n) if d else value
                before = half_ref[d, 0], half_ref[d, 1]
                for side, both_parts in enumerate((add(before, value), sub(before, value))):
                    out_ref[d + side * depth, spot, :] = both_parts[0] - mirrored(both_parts[1], still)
        return carry

    lax.fori_loop(0, TILE // 8, last, 0)


def gradient_kernel(quads, scale, folded_ref, amplitude_ref, turn_ref, mat_ref, out_ref, work_ref, half_ref):
    n = folded_ref.shape[0]
    rows = folded_ref.shape[1]

    def before(entries, which):
        made = through(jnp.concatenate([folded_ref[seat(j, quads)] for j in entries], axis=0), mat_ref, which)
        for q, j in enumerate(entries):
            part = made[q * rows : (q + 1) * rows]
            work_ref[j, 0], work_ref[j, 1] = part[:, :TILE], part[:, TILE:]

    def inner(k, carry):
        before([4 * k + q for q in range(4)], 0)
        return carry

    lax.fori_loop(0, n // 4, inner, 0)
    before([0], 1)

    def outer(k, carry):
        spot = pl.ds(pl.multiple_of(k * 8, 8), 8)
        for e in range(2):
            x = []
            for v in range(n // 2):
                j = 2 * v + e
                x.append(times((work_ref[j, 0, spot, :], work_ref[j, 1, spot, :]), turn_ref[j, 0:1, :], turn_ref[j, 1:2, :]))
            for b, value in enumerate(sixteen(x)):
                if e == 0:
                    half_ref[b] = value[0]
                    continue
                real = turn(value, 2 * math.pi * b / n)[0] if b else value[0]
                for c, total in ((b, half_ref[b] + real), (b + n // 2, half_ref[b] - real)):
                    lanes = slice(c * TILE, (c + 1) * TILE)
                    out_ref[spot, lanes] = total * amplitude_ref[spot, lanes] * scale
        return carry

    lax.fori_loop(0, rows // 8, outer, 0)


def row_weights(n, size):
    alpha = np.arange(TILE)
    i = np.arange(size // n // 2)
    turns = np.stack(trig(np.arange(n)[:, None] * alpha[None, :], size), axis=1).astype(np.float32)
    c, s = trig(alpha[:, None] * i[None, :], size // n)
    there, back = [], []
    for special in range(2):
        real = np.concatenate([c + s, c - s], axis=1)
        imag = np.concatenate([c - s, -c - s], axis=1)
        from_real = np.concatenate([c + s, c - s], axis=1)
        from_imag = np.concatenate([s - c, s + c], axis=1)
        if special:
            lane = len(i)
            real[:, lane] = from_real[:, lane] = 1.0 - 2.0 * (alpha % 2)
            imag[:, lane] = from_imag[:, lane] = 0.0
        for target, matrix in ((there, np.concatenate([real, imag], axis=0)), (back, np.concatenate([from_real.T, from_imag.T], axis=1))):
            target.append(np.concatenate(split_table(matrix), axis=0))
    return turns, np.stack(there), np.stack(back)


def column_tables(n, size):
    w = np.arange(size // n)
    t = np.arange(TILE)
    u = np.arange(n)
    r = 2 * np.arange(2 * TILE) + 1
    side = TILE // 2

    def lanes(c, s):
        out = np.zeros((c.shape[0], TILE))
        out[:, :n], out[:, side : side + n] = c, s
        return out.astype(np.float32)

    def matrix(x):
        return np.concatenate(split_table(x), axis=0)

    c, s = trig(t[:, None] * u[None, :], size)
    turns = lanes(c, -s)
    c, s = trig(w[:, None] * t[None, :], size // n)
    mat_h = matrix(np.concatenate([c, s], axis=1))
    mat_f = matrix(np.concatenate([c.T, -s.T], axis=0))
    c, s = trig(r[:, None] * u[None, :], 2 * G)
    turns_g = lanes(c, s)
    c, s = trig((w[:, None] * n + G // 4) * r[None, :], 2 * G)
    mat_g = matrix(np.concatenate([s, c], axis=1))
    c, s = trig(w * n + G // 4, 2 * G)
    slope = np.stack([s, c]) * (2.0 * G)
    slope = np.broadcast_to(slope[:, :, None], slope.shape + (TILE,)).astype(np.float32)
    c, s = trig(u, 2 * G)
    bend = np.stack([c, s], axis=1).astype(np.float32)
    return turns, mat_h, mat_f, turns_g, mat_g, slope, bend


def column_call(kernel, smems, args, out_shape, scratch, name, away=()):
    smem = pl.BlockSpec(memory_space=pltpu.SMEM)
    vmem = pl.BlockSpec(memory_space=pltpu.VMEM)
    anywhere = pl.BlockSpec(memory_space=pltpu.HBM)
    return pl.pallas_call(
        kernel,
        out_shape=jax.ShapeDtypeStruct(out_shape, jnp.float32),
        in_specs=[smem] * len(smems) + [anywhere if k in away else vmem for k in range(len(args))],
        out_specs=vmem,
        scratch_shapes=scratch,
        compiler_params=pltpu.CompilerParams(vmem_limit_bytes=24 << 20),
        cost_estimate=pl.CostEstimate(flops=10**10, bytes_accessed=16 * 2**20, transcendentals=0),
        name=name,
    )(*smems, *args)


def shared(residual, position, owner, tile_local, xi, amplitude):
    n = lax.axis_size(parts)
    n_base = lax.axis_size("base")
    n_slab = lax.axis_size("half") * lax.axis_size("quad")
    quads = lax.axis_size("quad")
    base, parity, quad = (lax.axis_index(axis) for axis in parts)
    place = 2 * (base * quads + quad) + parity
    rows, size = xi.shape
    depth = size // n
    half = depth // 2
    tiles = G // TILE

    row_turns, there, back_again = (jnp.asarray(x) for x in row_weights(n, size))
    block = (n, rows, depth)
    work = pltpu.VMEM((n, 2, rows, depth), jnp.float32)
    blocks = residual.shape[0]
    region_rows = G // n_slab // TILE
    region_cols = G // n_base // TILE
    room = 2 * n_base * (2 * blocks // n)
    target = owner[:, 0]
    tile_row = (target % n_slab) * region_rows + tile_local // region_cols
    tile_col = (target // n_slab) * region_cols + tile_local % region_cols
    flip = tile_row >= tiles // 2
    tile_row = jnp.where(flip, tiles - 1 - tile_row, tile_row)
    tile_col = jnp.where(flip, tiles - 1 - tile_col, tile_col)
    line = tile_row // n_slab
    code = (tile_row % n_slab) * tiles + tile_col
    pair = tile_row // 2
    what = jnp.stack([line, pair, code, flip.astype(jnp.int32)])
    sent = pack(what, residual, position, n_base, n_slab // 2, room)
    got, spectrum = exchange(sent, n_slab, xi, amplitude, row_turns, there)
    field = lax.all_to_all(spectrum, parts, split_axis=0, concat_axis=0, tiled=True)

    sources = n_slab * n_base
    codes = got[:, :, room, 0, :].reshape(sources, TILE).astype(jnp.int32)
    info = jnp.stack([quad, parity]).astype(jnp.int32)

    turns, firsts, undos, weights = grid_row_weights(n, size)
    halves = grid_rows_two(
        room,
        info,
        codes,
        jnp.asarray(firsts),
        got.reshape(sources * (room + 1), 4, TILE),
        jnp.asarray(turns),
        jnp.asarray(undos),
        jnp.asarray(weights),
    )
    whole = lax.all_to_all(halves, ("base", "quad"), split_axis=0, concat_axis=0, tiled=True)

    turns, mat_h, mat_f, turns_g, mat_g, slope, bend = (jnp.asarray(x) for x in column_tables(n, size))
    me = jnp.reshape(place, (1,)).astype(jnp.int32)
    sky = column_call(
        functools.partial(field_kernel, 1.0 / size),
        [me, bend],
        [field, turns, mat_h, slope],
        block,
        [work],
        "field",
    )
    fold = column_call(
        image_kernel,
        [me],
        [whole, sky, turns_g, mat_g, mat_f, turns],
        block,
        [pltpu.VMEM((n, 2, 2 * rows, depth), jnp.float32), pltpu.VMEM((n // 2, 2, 8, depth), jnp.float32),
         pltpu.VMEM(block, jnp.float32), pltpu.SemaphoreType.DMA],
        "image",
        away=(1,),
    )
    folded = lax.all_to_all(fold, parts, split_axis=0, concat_axis=0, tiled=True)
    return column_call(
        functools.partial(gradient_kernel, quads, 1.0 / size),
        [],
        [folded, amplitude, row_turns, back_again],
        (rows, size),
        [work, pltpu.VMEM((n // 2, 8, depth), jnp.float32)],
        "gradient",
    )


def solution(mesh):
    n_base, n_slab = mesh.shape["base"], mesh.shape["slab"]
    body, axes = general, both
    if n_slab == 2 * n_base and 2 * n_base * n_slab == G // TILE:
        body, axes = shared, parts
        mesh = jax.sharding.Mesh(mesh.devices.reshape(n_base, 2, n_slab // 2), parts)
    placed = (
        P(axes, None, None),
        P(axes, None, None),
        P(axes, None),
        P(axes),
        P(axes, None),
        P(axes, None),
    )
    return jax.shard_map(body, mesh=mesh, in_specs=placed, out_specs=P(axes, None), check_vma=False)
```

```python
import functools
import math

import jax
import jax.numpy as jnp
import numpy as np
from jax import lax
from jax.experimental import pallas as pl
from jax.experimental.pallas import tpu as pltpu
from jax.sharding import PartitionSpec as P

G = 8192
TILE = 128
both = ("base", "slab")
fine = lax.Precision.HIGHEST


def trig(product, modulus):
    angle = (product % modulus).astype(np.float64) * (2.0 * np.pi / modulus)
    return np.cos(angle), np.sin(angle)


def column_table(n, size):
    depth = size // n
    half = depth // 2
    i = np.arange(half)[None, :]
    j = np.arange(n)[:, None]
    low = n * i + j
    high = (-low) % size
    high[0, 0] = size // 2
    return np.concatenate([low, high], axis=1)


def row_tables(n, size):
    depth = size // n
    cols = column_table(n, size)
    oc, osn = trig(np.arange(n)[:, None] * np.arange(n)[None, :], n)
    outer = np.stack([oc, osn], axis=1)
    prod = np.arange(depth)[None, :, None] * cols[:, None, :]
    c, s = trig(prod, size)
    sign = np.where(np.arange(depth) < depth // 2, 1.0, -1.0)[None, None, :]
    inner = np.stack([c + s, sign * (c - s)], axis=1)
    return outer.astype(np.float32), inner.astype(np.float32)


def grid_row_tables(n, size):
    depth = G // n
    cols = column_table(n, size)
    half = cols.shape[1] // 2
    oc, osn = trig(np.arange(n)[:, None] * np.arange(n)[None, :], n)
    outer = np.stack([np.stack([oc, osn], 1), np.stack([-osn, oc], 1)], 0)
    low = cols[:, :half]
    high = cols[(-np.arange(n)) % n, half:]
    a = np.arange(depth)[None, :, None]
    out = []
    for part in (low, high):
        c, s = trig(a * (part[:, None, :] + G // 4), G)
        out.append(np.stack([np.concatenate([c, s], 2), np.concatenate([-s, c], 2)], 1))
    return outer.astype(np.float32), np.concatenate(out, axis=3).astype(np.float32)


def taps(cells, offsets):
    scaled = (cells - offsets) * 0.25
    kept = jnp.maximum(1.0 - scaled * scaled, 0.0)
    return kept * kept * kept


def split_three(x):
    high = x.astype(jnp.bfloat16)
    rest = x - high.astype(jnp.float32)
    middle = rest.astype(jnp.bfloat16)
    return high, middle, (rest - middle.astype(jnp.float32)).astype(jnp.bfloat16)


def grid_kernel(rows, info_ref, list_ref, data_ref, out_ref):
    count = info_ref[0]
    first = info_ref[1].astype(jnp.float32)
    out_ref[...] = jnp.zeros_like(out_ref)
    row_cells = lax.broadcasted_iota(jnp.int32, (rows, TILE), 0).astype(jnp.float32) + first
    col_cells = lax.broadcasted_iota(jnp.int32, (TILE, TILE), 0).astype(jnp.float32)

    def step(k, carry):
        packed = list_ref[k]
        index = packed // 256
        col = (packed // 2) % 128
        flip = (packed % 2).astype(jnp.float32)
        sign = 1.0 - 2.0 * flip
        start = 128.0 * flip
        block = data_ref[index]
        value = block[0:2, :]
        place = block[2:4, :]
        row_taps = taps(row_cells * sign + start, place[0:1, :])
        col_taps = taps(col_cells * sign + start, place[1:2, :])
        weighted = jnp.concatenate(
            [col_taps * value[0:1, :], col_taps * (value[1:2, :] * sign)], axis=0
        )
        rh, rm, rl = split_three(row_taps)
        wh, wm, wl = split_three(weighted)
        left = jnp.concatenate([rh, rh, rh, rm, rm, rl], axis=1)
        right = jnp.concatenate([wh, wm, wl, wh, wm, wh], axis=1)
        sub = lax.dot_general(
            left, right, (((1,), (1,)), ((), ())), preferred_element_type=jnp.float32
        )
        out_ref[0, col] += sub[:, :TILE]
        out_ref[1, col] += sub[:, TILE:]
        return carry

    lax.fori_loop(0, count, step, 0)


def grid_rows(info, table, gathered, rows):
    tiles = G // TILE
    smem = pl.BlockSpec(memory_space=pltpu.SMEM)
    vmem = pl.BlockSpec(memory_space=pltpu.VMEM)
    return pl.pallas_call(
        functools.partial(grid_kernel, rows),
        out_shape=jax.ShapeDtypeStruct((2, tiles, rows, TILE), jnp.float32),
        in_specs=[smem, smem, vmem],
        out_specs=vmem,
        compiler_params=pltpu.CompilerParams(vmem_limit_bytes=56 * 1024 * 1024),
        cost_estimate=pl.CostEstimate(
            flops=2 * 10**10, bytes_accessed=16 * 2**20, transcendentals=0
        ),
        name="grid_rows",
    )(info, table, gathered)


def einsum(form, *args, precision=lax.Precision.HIGH):
    return jnp.einsum(form, *args, precision=precision, preferred_element_type=jnp.float32)


def general(residual, position, owner, tile_local, xi, amplitude):
    n = lax.axis_size(both)
    n_base = lax.axis_size("base")
    n_slab = lax.axis_size("slab")
    me = lax.axis_index(both)
    rows, size = xi.shape
    depth = size // n
    half = depth // 2
    tiles = G // TILE

    region_rows = G // n_slab // TILE
    region_cols = G // n_base // TILE
    target = owner[:, 0]
    tile_row = (target % n_slab) * region_rows + tile_local // region_cols
    tile_col = (target // n_slab) * region_cols + tile_local % region_cols
    flip = tile_row >= tiles // 2
    tile_row = jnp.where(flip, tiles - 1 - tile_row, tile_row)
    tile_col = jnp.where(flip, tiles - 1 - tile_col, tile_col)
    code = tile_row * 256 + tile_col * 2 + flip.astype(jnp.int32)
    codes = lax.all_gather(code, both, axis=0, tiled=True)
    payload = jnp.concatenate([residual, position], axis=1)
    codes, payload = lax.optimization_barrier((codes, payload))
    gathered = lax.all_gather(payload, both, axis=0, tiled=True)
    blocks = codes.shape[0]
    grid_depth = G // 2 // n
    first_row = me * grid_depth
    mine = (codes // 256 == first_row // TILE).astype(jnp.int32)
    rank = jnp.where(mine == 1, jnp.cumsum(mine) - 1, -1)
    packed = lax.broadcasted_iota(jnp.int32, (blocks,), 0) * 256 + codes % 256
    spots = lax.broadcasted_iota(jnp.int32, (blocks, blocks), 0)
    table = jnp.sum(jnp.where(spots == rank[None, :], packed[None, :], 0), axis=1)
    info = jnp.stack([jnp.sum(mine), first_row % TILE]).astype(jnp.int32)

    outer, inner = row_tables(n, size)
    spectrum = (amplitude * xi).reshape(rows, n, depth)
    mid = einsum("rba,bqc->qcra", spectrum, outer)
    sent = einsum("cra,cae->cre", mid[0], inner[:, 0]) + einsum("cra,cae->cre", mid[1], inner[:, 1])
    sent, gathered = lax.optimization_barrier((sent, gathered))
    field = lax.all_to_all(sent, both, split_axis=0, concat_axis=0, tiled=True)
    field = field.reshape(size, depth)
    lane = lax.broadcasted_iota(jnp.int32, (1, depth), 1)
    still = (me == 0) & (lane % half == 0)

    def mirror(x):
        return jnp.where(still, x, jnp.roll(x, half, axis=-1))

    c_len = 128
    d_len = size // c_len
    bc, bs = (x.astype(np.float32) for x in trig(np.arange(c_len)[:, None] * np.arange(c_len)[None, :], c_len))
    shape = (c_len, d_len, depth)
    n0 = c_len * np.arange(d_len)[None, :] + np.arange(c_len)[:, None]
    ic, isn = (x.astype(np.float32) for x in trig(n0[:, :, None] * np.arange(d_len)[None, None, :], size))
    pair = jnp.stack([field.reshape(shape), mirror(field).reshape(shape)])
    first = np.stack([np.stack([bc, bs], 1), np.stack([bs, -bc], 1)], 0)
    turned = einsum("qbal,qbsc->csal", pair, first)
    second = np.stack([ic, -isn], axis=2)
    power = einsum("csal,cdsa->cdl", turned, second)
    sky = jnp.exp(power / size)

    grid = grid_rows(info, table, gathered, grid_depth)
    outer_g, inner_g = grid_row_tables(n, size)
    parts = tiles // n if tiles >= n else 1
    inner_len = G // n
    if inner_len >= TILE:
        view = grid.reshape(2, n, inner_len // TILE, grid_depth, TILE)
    else:
        flat = grid.transpose(0, 2, 1, 3).reshape(2, grid_depth, n, inner_len)
        view = flat.transpose(0, 2, 1, 3)[:, :, None]
        parts = 1
    lanes = view.shape[-1]
    stage = einsum("qbpra,qbsc->cspra", view, outer_g, precision=fine)
    inner_g = inner_g.reshape(n, 2, parts, lanes, 2 * depth)
    halves = einsum("cspra,cspae->cre", stage, inner_g, precision=fine)
    high = halves[:, :, depth:]
    high = jnp.concatenate([high[:1], jnp.flip(high[1:], axis=0)], axis=0)
    halves = jnp.concatenate([halves[:, :, :depth], high], axis=2)
    got = lax.all_to_all(halves, both, split_axis=0, concat_axis=0, tiled=True)
    got = got.reshape(size, 2 * depth)
    real = jnp.concatenate([got[:, :half], got[:, depth : depth + half]], axis=1)
    imag = jnp.concatenate([got[:, half:depth], got[:, depth + half :]], axis=1)
    wide = G // c_len
    deep = size // wide
    gc, gs = (x.astype(np.float32) for x in trig(np.arange(deep)[:, None] * np.arange(c_len)[None, :], c_len))
    first_g = np.stack([np.stack([gc, gs], 1), np.stack([-gs, gc], 1)], 0)
    whole = jnp.stack([real.reshape(deep, wide, depth), imag.reshape(deep, wide, depth)])
    turned_g = einsum("qbal,qbsc->csal", whole, first_g, precision=fine)
    ac, asn = trig((n0 + G // 4)[:, :, None] * np.arange(wide)[None, None, :], G)
    second_g = (np.stack([ac, -asn], axis=2) / G).astype(np.float32)
    back = einsum("csal,cdsa->cdl", turned_g, second_g, precision=fine)

    z = sky * back
    pz = einsum("cdl,cda->cal", z, ic)
    qz = einsum("cdl,cda->cal", z, isn)
    joined = jnp.stack([pz + mirror(qz), mirror(pz) - qz])
    fold = einsum("qcal,qcb->bal", joined, np.stack([bc, bs]))
    folded = lax.all_to_all(
        fold.reshape(n, rows, depth), both, split_axis=0, concat_axis=0, tiled=True
    )
    ends = einsum("jre,jqae->qjra", folded, inner)
    final = einsum("qjra,bqj->rba", ends, outer)
    return amplitude * final.reshape(rows, size) / size


MESH = pl.DeviceIdType.MESH
parts = ("base", "half", "quad")
LANES = 4


def two_parts(x):
    high = x.astype(jnp.bfloat16)
    return high, (x - high.astype(jnp.float32)).astype(jnp.bfloat16)


def through(x, weight_ref, which):
    rows, depth = x.shape
    high, low = two_parts(x)
    made = jnp.dot(jnp.concatenate([high, low], axis=0), weight_ref[which, :depth], preferred_element_type=jnp.float32)
    return made[:rows] + made[rows:] + jnp.dot(high, weight_ref[which, depth:], preferred_element_type=jnp.float32)


def times(x, c, s):
    return x[0] * c - x[1] * s, x[0] * s + x[1] * c


def turn(x, angle):
    c, s = math.cos(angle), math.sin(angle)
    return times(x, c, s)


def add(x, y):
    return x[0] + y[0], x[1] + y[1]


def sub(x, y):
    return x[0] - y[0], x[1] - y[1]


def four(x):
    s0, d0, s1, d1 = add(x[0], x[2]), sub(x[0], x[2]), add(x[1], x[3]), sub(x[1], x[3])
    i1 = (-d1[1], d1[0])
    return [add(s0, s1), add(d0, i1), sub(s0, s1), sub(d0, i1)]


def sixteen(x):
    rows = []
    for b0 in range(4):
        y = four([x[4 * b1 + b0] for b1 in range(4)])
        rows.append([y[a0] if a0 * b0 == 0 else turn(y[a0], 2 * math.pi * a0 * b0 / 16) for a0 in range(4)])
    out = [None] * 16
    for a0 in range(4):
        y = four([rows[b0][a0] for b0 in range(4)])
        for a1 in range(4):
            out[a0 + 4 * a1] = y[a1]
    return out


def seat(j, quads):
    a = j // 2
    return a // quads * (2 * quads) + j % 2 * quads + a % quads


def transform_rows(quads, xi_ref, amplitude_ref, turn_ref, mat_ref, out_ref, work_ref):
    n = out_ref.shape[0]

    def outer(k, carry):
        spot = pl.ds(pl.multiple_of(k * 8, 8), 8)
        for e in range(2):
            x = []
            for b in range(n // 2):
                first, second = (
                    xi_ref[spot, c * TILE : (c + 1) * TILE] * amplitude_ref[spot, c * TILE : (c + 1) * TILE]
                    for c in (b, b + n // 2)
                )
                value = first - second if e else first + second
                if e * b:
                    angle = 2 * math.pi * b / n
                    x.append((value * math.cos(angle), value * math.sin(angle)))
                else:
                    x.append((value, jnp.zeros_like(value)))
            for v, value in enumerate(sixteen(x)):
                j = 2 * v + e
                work_ref[j, 0, spot, :], work_ref[j, 1, spot, :] = times(value, turn_ref[j, 0:1, :], turn_ref[j, 1:2, :])
        return carry

    lax.fori_loop(0, xi_ref.shape[0] // 8, outer, 0)
    rows = xi_ref.shape[0]

    def left(entries):
        return jnp.concatenate([jnp.concatenate([work_ref[j, 0], work_ref[j, 1]], axis=1) for j in entries], axis=0)

    def inner(k, carry):
        entries = [4 * k + q for q in range(4)]
        made = through(left(entries), mat_ref, 0)
        for q, j in enumerate(entries):
            out_ref[seat(j, quads)] = made[q * rows : (q + 1) * rows]
        return carry

    lax.fori_loop(0, n // 4, inner, 0)
    out_ref[0] = through(left([0]), mat_ref, 1)


def exchange_kernel(nb, ns, send_ref, xi_ref, amplitude_ref, turn_ref, mat_ref, out_ref, spectrum_ref, work_ref, made_ref, rows_ref, rows_sem, bsend, brecv, usend, dsend, lrecv, hrecv, psend, precv, lsem):
    quads = ns // 2
    nz = ns // 2
    base = lax.axis_index("base")
    slab = lax.axis_index("half") * quads + lax.axis_index("quad")
    z = slab // 2
    core = slab % 2

    def at(b, s):
        return (b, s // quads, s % quads)

    def copy(source, target, here, there, device):
        return pltpu.make_async_remote_copy(
            src_ref=source, dst_ref=target, send_sem=here, recv_sem=there, device_id=device, device_id_type=MESH
        )

    def crossing(k):
        other = (base + k) % nb
        return copy(send_ref.at[other], out_ref.at[slab, base], bsend.at[k], brecv.at[k], at(other, slab))

    def arriving(k):
        from_base = (base - k + nb) % nb
        return copy(send_ref.at[base], out_ref.at[slab, from_base], bsend.at[k], brecv.at[k], at(from_base, slab))

    def block(origin, k):
        return out_ref.at[2 * origin + core, (base - k + nb) % nb]

    def upward(s, k):
        part = block(z - s, k)
        return copy(part, part, usend.at[s, k], lrecv.at[s + 1, k], at(base, slab + 2))

    def downward(s, k):
        part = block(z + s, k)
        return copy(part, part, dsend.at[s, k], hrecv.at[s + 1, k], at(base, slab - 2))

    def from_below(s, k):
        part = block(z - s, k)
        return copy(part, part, usend.at[s, k], lrecv.at[s, k], at(base, slab - 2))

    def from_above(s, k):
        part = block(z + s, k)
        return copy(part, part, dsend.at[s, k], hrecv.at[s, k], at(base, slab + 2))

    def across(origin, k):
        part = block(origin, k)
        return copy(part, part, psend.at[origin, k], precv.at[origin, k], at(base, slab + 1 - 2 * core))

    def from_partner(origin, k):
        part = out_ref.at[2 * origin + 1 - core, (base - k + nb) % nb]
        return copy(part, part, psend.at[origin, k], precv.at[origin, k], at(base, slab + 1 - 2 * core))

    fetches = [
        pltpu.make_async_copy(source, rows_ref.at[k], rows_sem.at[k]) for k, source in enumerate((xi_ref, amplitude_ref))
    ]
    ready = pltpu.make_async_copy(made_ref, spectrum_ref, rows_sem.at[2])
    for fetch in fetches:
        fetch.start()
    barrier = pltpu.get_barrier_semaphore()
    for k in range(1, nb):
        pl.semaphore_signal(barrier, inc=1, device_id=at((base + k) % nb, slab), device_id_type=MESH)
    pl.semaphore_signal(barrier, inc=1, device_id=at(base, slab + 1 - 2 * core), device_id_type=MESH)

    @pl.when(z < nz - 1)
    def _():
        pl.semaphore_signal(barrier, inc=1, device_id=at(base, slab + 2), device_id_type=MESH)

    @pl.when(z > 0)
    def _():
        pl.semaphore_signal(barrier, inc=1, device_id=at(base, slab - 2), device_id_type=MESH)

    pl.semaphore_wait(barrier, nb + jnp.where(z < nz - 1, 1, 0) + jnp.where(z > 0, 1, 0))

    for k in range(1, nb):
        crossing(k).start()
    own = pltpu.make_async_copy(send_ref.at[base], out_ref.at[slab, base], lsem)
    own.start()

    def pass_on(s, k, ascending, descending):
        if ascending:
            @pl.when((z - s >= 0) & (z < nz - 1))
            def _():
                upward(s, k).start()

        if descending:
            @pl.when((z + s < nz) & (z > 0))
            def _():
                downward(s, k).start()

    for k in range(nb):
        if k == 0:
            own.wait()
        else:
            arriving(k).wait_recv()
        pass_on(0, k, True, True)
        across(z, k).start()
        if k == 0:
            for fetch in fetches:
                fetch.wait()
            transform_rows(quads, rows_ref.at[0], rows_ref.at[1], turn_ref, mat_ref, made_ref, work_ref)
            ready.start()
    for s in range(1, nz):
        for k in range(nb):
            @pl.when(z - s >= 0)
            def _():
                from_below(s, k).wait_recv()
                if s < nz - 1:
                    pass_on(s, k, True, False)
                across(z - s, k).start()

            @pl.when(z + s < nz)
            def _():
                from_above(s, k).wait_recv()
                if s < nz - 1:
                    pass_on(s, k, False, True)
                across(z + s, k).start()

    ready.wait()
    for origin in range(nz):
        for k in range(nb):
            from_partner(origin, k).wait_recv()
    for k in range(1, nb):
        crossing(k).wait_send()
    for s in range(nz - 1):
        for k in range(nb):
            @pl.when((z - s >= 0) & (z < nz - 1))
            def _():
                upward(s, k).wait_send()

            @pl.when((z + s < nz) & (z > 0))
            def _():
                downward(s, k).wait_send()

    for origin in range(nz):
        for k in range(nb):
            across(origin, k).wait_send()


def pack_kernel(ns, tiles, room, owner_ref, local_ref, residual_ref, position_ref, out_ref):
    blocks = residual_ref.shape[0]
    nb = out_ref.shape[0]
    across = lax.broadcasted_iota(jnp.int32, (blocks, blocks), 1)
    down = lax.broadcasted_iota(jnp.int32, (blocks, blocks), 0)

    def column(row):
        return jnp.sum(jnp.where(across == down, row, 0.0), axis=1, keepdims=True)

    def divided(x, d):
        whole = jnp.floor((x + 0.5) * (1.0 / d))
        return whole, x - whole * d

    local = local_ref[...].astype(jnp.float32)
    target = owner_ref[...].astype(jnp.float32)
    region_col, region_row = divided(target, ns)
    tile_row, tile_col = divided(local, tiles // nb)
    tile_row = tile_row + region_row * (tiles // ns)
    tile_col = tile_col + region_col * (tiles // nb)
    flip = jnp.where(tile_row >= tiles // 2, 1.0, 0.0)
    tile_row = jnp.where(flip > 0.5, tiles - 1 - tile_row, tile_row)
    tile_col = jnp.where(flip > 0.5, tiles - 1 - tile_col, tile_col)
    line, within = divided(tile_row, ns)
    key = divided(tile_row, 2)[0]
    code = within * tiles + tile_col
    keys = ns // 2
    line_down, key_down, flip_down = column(line), column(key), column(flip)
    before = (line_down == line) & ((key_down < key) | ((key_down == key) & (down < across)))
    slot = line * room + jnp.sum(jnp.where(before, 1.0, 0.0), axis=0, keepdims=True)
    slots = lax.broadcasted_iota(jnp.int32, (nb * room, blocks), 0).astype(jnp.float32)
    chosen = jnp.where(slots == slot, 1.0, 0.0).astype(jnp.bfloat16)
    sides = [residual_ref[:, 0, :], residual_ref[:, 1, :] * (1.0 - 2.0 * flip_down)]
    for k in range(2):
        place = position_ref[:, k, :]
        sides.append(jnp.where(flip_down > 0.5, TILE - place, place))
    pieces = split_three(jnp.concatenate(sides, axis=1))
    moved = jnp.dot(
        jnp.concatenate([chosen] * 3, axis=1), jnp.concatenate(pieces, axis=0), preferred_element_type=jnp.float32
    )
    codes = 0.0
    for part in two_parts(jnp.broadcast_to(code + 1.0, (8, blocks))):
        codes = codes + lax.dot_general(part, chosen, (((1,), (1,)), ((), ())), preferred_element_type=jnp.float32)
    codes = codes - 1.0
    lanes = lax.broadcasted_iota(jnp.int32, (1, blocks), 1)
    shift = (across - room).astype(jnp.float32)
    per = blocks // room
    for k in range(nb):
        for c in range(4):
            out_ref[k, :room, c, :] = moved[k * room : (k + 1) * room, c * TILE : (c + 1) * TILE]
        start = k // per * blocks
        own = codes[:, start : start + blocks]
        if k % per:
            own = pltpu.roll(own, blocks - k % per * room, 1)
        earlier = (line_down == k) & (key_down - keys * k < shift)
        starts = jnp.sum(jnp.where(earlier, 1.0, 0.0), axis=0, keepdims=True)
        out_ref[k, room] = jnp.broadcast_to(jnp.where(lanes < room, own[0:1, :], starts), (4, TILE))


def pack(owner, local, residual, position, nb, ns, room):
    vmem = pl.BlockSpec(memory_space=pltpu.VMEM)
    return pl.pallas_call(
        functools.partial(pack_kernel, ns, G // TILE, room),
        out_shape=jax.ShapeDtypeStruct((nb, room + 1, 4, TILE), jnp.float32),
        in_specs=[vmem] * 4,
        out_specs=vmem,
        compiler_params=pltpu.CompilerParams(vmem_limit_bytes=60 << 20),
        name="pack",
    )(owner.reshape(1, -1), local.reshape(1, -1), residual, position)


def exchange(sent, ns, xi, amplitude, turns, mats):
    nb = sent.shape[0]
    nz = ns // 2
    rows, n = xi.shape[0], turns.shape[0]
    dma = pltpu.SemaphoreType.DMA
    vmem = pl.BlockSpec(memory_space=pltpu.VMEM)
    hbm = pl.BlockSpec(memory_space=pltpu.HBM)
    return pl.pallas_call(
        functools.partial(exchange_kernel, nb, ns),
        out_shape=(
            jax.ShapeDtypeStruct((ns,) + sent.shape, jnp.float32),
            jax.ShapeDtypeStruct((n, rows, TILE), jnp.float32),
        ),
        in_specs=[vmem, hbm, hbm, vmem, vmem],
        out_specs=(hbm, hbm),
        scratch_shapes=[
            pltpu.VMEM((n, 2, rows, TILE), jnp.float32),
            pltpu.VMEM((n, rows, TILE), jnp.float32),
            pltpu.VMEM((2,) + xi.shape, jnp.float32), dma((3,)),
            dma((nb,)), dma((nb,)), dma((nz, nb)), dma((nz, nb)), dma((nz, nb)), dma((nz, nb)),
            dma((nz, nb)), dma((nz, nb)), dma,
        ],
        compiler_params=pltpu.CompilerParams(collective_id=0, has_side_effects=True, vmem_limit_bytes=60 << 20),
        cost_estimate=pl.CostEstimate(flops=3 * 10**10, bytes_accessed=16 * 2**20, transcendentals=0),
        name="exchange",
    )(sent, xi, amplitude, turns, mats)


def grid_kernel_two(room, info_ref, codes_ref, first_ref, data_hbm_ref, turn_ref, undo_ref, weight_hbm_ref, away_ref, grid_ref, left_ref, right_ref, out_ref, data_ref, weight_ref, list_ref, sems):
    quad = info_ref[0]
    parity = info_ref[1]
    data = pltpu.make_async_copy(data_hbm_ref, data_ref, sems.at[out_ref.shape[0]])
    weight = pltpu.make_async_copy(weight_hbm_ref, weight_ref, sems.at[out_ref.shape[0] + 1])
    data.start()
    weight.start()
    grid_ref[...] = jnp.zeros_like(grid_ref)
    half = grid_ref.shape[1]
    group = 16
    cells = lax.broadcasted_iota(jnp.int32, (group + 8, TILE), 0).astype(jnp.float32) * 0.25
    nothing = jnp.zeros((group, TILE), jnp.bfloat16)

    def bump(offsets):
        d = cells - offsets
        kept = jnp.maximum(1.0 - d * d, 0.0)
        return kept * kept * kept

    def window(offsets):
        start = jnp.floor((offsets - 4.0) * (1.0 / group))
        offsets = (offsets - start * group) * 0.25
        return bump(offsets) - bump(offsets - 0.25), jnp.broadcast_to(start, (group, TILE)).astype(jnp.bfloat16)

    def spread(compact, start):
        padded = jnp.concatenate([compact, jnp.zeros((8, TILE), jnp.float32)], axis=0)
        out = []
        for part in two_parts(padded):
            first, second = part[:group], part[group:]
            pieces = []
            for g in range(TILE // group):
                piece = jnp.where(start == g - 1, second, nothing) if g else nothing
                pieces.append(jnp.where(start == g, first, piece))
            out.append(jnp.concatenate(pieces, axis=0))
        return out

    lanes = left_ref.shape[0]

    def place(k):
        packed = list_ref[k]
        return packed % 64, packed // 64

    def prepare(k, lane, count):
        col, rest = place(k)
        odd = jnp.where(col >= half, parity, 0)
        sign = jnp.where(k < count, 1 - 2 * odd, 0).astype(jnp.float32)
        block = data_ref[rest // 2]
        value = block[0:2, :] * sign
        row_taps, row_start = window(block[2:3, :])
        col_taps, col_start = window(block[3:4, :])
        rows_split = spread(row_taps, row_start)
        real = spread(col_taps * value[0:1, :], col_start)
        imag = spread(col_taps * value[1:2, :], col_start)
        for q in range(2):
            left_ref[lane, :, q * TILE : (q + 1) * TILE] = rows_split[q]
            right_ref[lane, :TILE, q * TILE : (q + 1) * TILE] = real[q]
            right_ref[lane, TILE:, q * TILE : (q + 1) * TILE] = imag[q]

    def product(lane):
        rh, rl = left_ref[lane, :, :TILE], left_ref[lane, :, TILE:]
        wh, wl = right_ref[lane, :, :TILE], right_ref[lane, :, TILE:]
        left = jnp.concatenate([rh, rh, rl], axis=1)
        right = jnp.concatenate([wh, wl, wh], axis=1)
        return lax.dot_general(left, right, (((1,), (1,)), ((), ())), preferred_element_type=jnp.float32)

    def step(k, carry):
        made = [product(lane) for lane in range(lanes)]
        for lane in range(lanes):
            prepare((k + 1) * lanes + lane, lane, count)
        for lane in range(lanes):
            col, rest = place(k * lanes + lane)
            col = jnp.where(col >= half, col - half, col)
            spot = pl.ds(pl.multiple_of((rest % 2) * TILE, TILE), TILE)
            grid_ref[0, col, spot, :] += made[lane][:, :TILE]
            grid_ref[1, col, spot, :] += made[lane][:, TILE:]
        return carry

    def gather(source, filled):
        start = codes_ref[source, room + quad]
        stop = codes_ref[source, room + quad + 1]

        def entry(i, carry):
            list_ref[filled + i - start] = (source * (room + 1) + i) * TILE + codes_ref[source, i] % TILE
            return carry

        lax.fori_loop(start, stop, entry, 0)
        return filled + stop - start

    count = lax.fori_loop(0, codes_ref.shape[0], gather, 0)
    for lane in range(2 * lanes):
        list_ref[count + lane] = 0
    data.wait()
    for lane in range(lanes):
        prepare(lane, lane, count)
    lax.fori_loop(0, (count + lanes - 1) // lanes, step, 0)

    depth = half // 2
    rows = grid_ref.shape[2]

    def outer(k, carry):
        spot = pl.ds(pl.multiple_of(k * 8, 8), 8)
        for side in range(2):
            x = []
            for b in range(depth):
                value = grid_ref[0, 2 * b + side, spot, :], grid_ref[1, 2 * b + side, spot, :]
                x.append(times(value, first_ref[parity, b, 0], first_ref[parity, b, 1]))
            for a, value in enumerate(sixteen(x)):
                c = turn_ref[parity, a, side : side + 1, :]
                s = turn_ref[parity, a, 2 + side : 3 + side, :]
                value = times(value, c, s)
                grid_ref[0, 2 * a + side, spot, :] = value[0]
                grid_ref[1, 2 * a + side, spot, :] = value[1]
        return carry

    lax.fori_loop(0, rows // 8, outer, 0)

    def inner(a, carry):
        mirrored = depth - parity - a
        mirrored = jnp.where(mirrored == depth, 0, mirrored)
        which = jnp.where((a == 0) & (parity == 0), 1, 0)
        for part in range(1):
            spot = pl.ds(0, rows)
            x = jnp.concatenate([grid_ref[q, 2 * a + side, spot, :] for q in range(2) for side in range(2)], axis=1)
            made = through(x, weight_ref, which)
            mid = TILE // 2
            made = times((made[:, :TILE], made[:, TILE:]), undo_ref[parity, a, 0:1, :], undo_ref[parity, a, 1:2, :])
            for q in range(2):
                out_ref[a, spot, q * TILE : q * TILE + mid] = made[q][:, :mid]
                out_ref[mirrored, spot, q * TILE + mid : (q + 1) * TILE] = made[q][:, mid:]

        @pl.when(a >= depth // 2)
        def _():
            leave(a).start()
            leave(jnp.where((parity == 0) & (a == depth // 2), 0, mirrored)).start()

        return carry

    def leave(a):
        return pltpu.make_async_copy(out_ref.at[a], away_ref.at[a], sems.at[a])

    weight.wait()
    lax.fori_loop(0, depth, inner, 0)
    for a in range(depth):
        leave(a).wait()


def split_table(x):
    high = x.astype(np.float32).astype(jnp.bfloat16)
    low = (x - high.astype(np.float64)).astype(np.float32).astype(jnp.bfloat16)
    return high, low


def undone(pixels):
    c, s = trig(pixels + G // 4, G)
    return 1.0 / (1.0 - (c - 1j * s))


def grid_row_weights(n, size):
    depth = n // 2
    span = G // 2 // depth
    half = size // n // 2
    alpha = np.arange(span)
    turns, firsts, undos = [], [], []
    for p in range(2):
        j = 2 * np.arange(depth) + p
        c, s = trig(j[:, None] * alpha[None, :], G)
        turns.append(np.concatenate([c.reshape(depth, 2, TILE), s.reshape(depth, 2, TILE)], axis=1))
        firsts.append(np.stack(trig(np.arange(depth) * p, n), axis=1))
        low = n * np.arange(half)[None, :] + j[:, None]
        high = size - n * np.arange(half)[None, :] - ((-j) % n)[:, None]
        if p == 0:
            low[0, 0], high[0, 0] = 0, size // 2
        undo = undone(np.concatenate([low, high], axis=1))
        undos.append(np.stack([undo.real, undo.imag], axis=1))
    weights = []
    i = np.arange(half)
    for special in range(2):
        low = n * i
        high = size - n * i - (0 if special else n)
        if special:
            high[0] = size // 2
        parts_re, parts_im = [], []
        for cols in (low, high):
            c, s = trig(alpha[:, None] * (cols[None, :] + G // 4), G)
            parts_re.append(np.concatenate([c, -s], axis=0))
            parts_im.append(np.concatenate([s, c], axis=0))
        w = np.concatenate(parts_re + parts_im, axis=1)
        weights.append(np.concatenate(split_table(w), axis=0))
    turns, firsts, undos = (np.stack(x).astype(np.float32) for x in (turns, firsts, undos))
    return turns, firsts, undos, np.stack(weights)


def grid_rows_two(room, info, codes, first, data, turns, undos, weights):
    depth = turns.shape[1]
    rows = 2 * TILE
    smem = pl.BlockSpec(memory_space=pltpu.SMEM)
    vmem = pl.BlockSpec(memory_space=pltpu.VMEM)
    hbm = pl.BlockSpec(memory_space=pltpu.HBM)
    return pl.pallas_call(
        functools.partial(grid_kernel_two, room),
        out_shape=jax.ShapeDtypeStruct((depth, rows, 2 * TILE), jnp.float32),
        in_specs=[smem, smem, smem, hbm, vmem, vmem, hbm],
        out_specs=hbm,
        scratch_shapes=[
            pltpu.VMEM((2, 2 * depth, rows, TILE), jnp.float32),
            pltpu.VMEM((LANES, TILE, 2 * TILE), jnp.bfloat16),
            pltpu.VMEM((LANES, 2 * TILE, 2 * TILE), jnp.bfloat16),
            pltpu.VMEM((depth, rows, 2 * TILE), jnp.float32),
            pltpu.VMEM(data.shape, jnp.float32),
            pltpu.VMEM(weights.shape, jnp.bfloat16),
            pltpu.SMEM((codes.shape[0] * room + 2 * LANES,), jnp.int32),
            pltpu.SemaphoreType.DMA((depth + 2,)),
        ],
        compiler_params=pltpu.CompilerParams(vmem_limit_bytes=60 << 20),
        cost_estimate=pl.CostEstimate(flops=2 * 10**10, bytes_accessed=16 * 2**20, transcendentals=0),
        name="grid_rows_two",
    )(info, codes, first, data, turns, undos, weights)


def minus(x):
    return [(b, a) for a, b in sixteen([(b, a) for a, b in x])]


def pick(table, u):
    side = table.shape[1] // 2
    return table[:, u : u + 1], table[:, side + u : side + u + 1]


def mirrored(x, still):
    return jnp.where(still, x, pltpu.roll(x, x.shape[1] // 2, 1))


def still_lanes(place, rows):
    lane = lax.broadcasted_iota(jnp.int32, (rows, TILE), 1)
    return (lane % (TILE // 2) == 0) & (place == 0)


def product(mat_ref, x):
    rows = mat_ref.shape[0] // 2
    high, low = two_parts(x)
    made = jnp.dot(mat_ref[...], high, preferred_element_type=jnp.float32)
    return made[:rows] + made[rows:] + jnp.dot(mat_ref[:rows], low, preferred_element_type=jnp.float32)


def beside(work_ref, u):
    sides = [jnp.concatenate([work_ref[u + q, 0], work_ref[u + q, 1]], axis=0) for q in range(2)]
    return jnp.concatenate(sides, axis=1)


def field_kernel(scale, info_ref, bend_ref, field_ref, turn_ref, mat_ref, slope_ref, sky_ref, work_ref):
    still = still_lanes(info_ref[0], 8)
    n = field_ref.shape[0]

    def outer(k, carry):
        spot = pl.ds(pl.multiple_of(k * 8, 8), 8)
        table = turn_ref[spot, :]
        for e in range(2):
            x = []
            for d in range(n // 2):
                first, second = field_ref[d, spot, :], field_ref[d + n // 2, spot, :]
                value = first - second if e else first + second
                value = value, mirrored(value, still)
                x.append(turn(value, -2 * math.pi * d / n) if e * d else value)
            for v, value in enumerate(minus(x)):
                u = 2 * v + e
                work_ref[u, 0, spot, :], work_ref[u, 1, spot, :] = times(value, *pick(table, u))
        return carry

    lax.fori_loop(0, field_ref.shape[1] // 8, outer, 0)

    def inner(k, carry):
        for u in (4 * k, 4 * k + 2):
            made = jnp.exp(product(mat_ref, beside(work_ref, u)) * scale)
            for q in range(2):
                sine = slope_ref[0] * bend_ref[u + q, 0] + slope_ref[1] * bend_ref[u + q, 1]
                sky_ref[u + q] = made[:, q * TILE : (q + 1) * TILE] / sine
        return carry

    lax.fori_loop(0, n // 4, inner, 0)


def image_kernel(scale, whole_ref, sky_ref, turn_g_ref, mat_g_ref, mat_f_ref, turn_ref, turn_r_ref, mat_r_ref, out_ref, work_ref, half_ref, held_ref, fold_ref, folded_ref, real_ref, held_sem, send_sems, recv_sems):
    n = sky_ref.shape[0]
    quads = lax.axis_size("quad")
    halves = lax.axis_size("half")
    me = (lax.axis_index("base") * halves + lax.axis_index("half")) * quads + lax.axis_index("quad")
    place = 2 * (lax.axis_index("base") * quads + lax.axis_index("quad")) + lax.axis_index("half")
    still = still_lanes(place, 8)
    pieces = send_sems.shape[0]
    span = TILE // pieces

    def at(device):
        return (device // (halves * quads), device // quads % halves, device % quads)

    def sending(c, k):
        target = (me + k) % n
        part = pl.ds(c * span, span)
        return pltpu.make_async_remote_copy(
            src_ref=fold_ref.at[target, part], dst_ref=folded_ref.at[me, part],
            send_sem=send_sems.at[c, k], recv_sem=recv_sems.at[c, k], device_id=at(target), device_id_type=MESH,
        )

    def arriving(c, k):
        source = (me - k + n) % n
        part = pl.ds(c * span, span)
        return pltpu.make_async_remote_copy(
            src_ref=fold_ref.at[source, part], dst_ref=folded_ref.at[source, part],
            send_sem=send_sems.at[c, k], recv_sem=recv_sems.at[c, k], device_id=at(source), device_id_type=MESH,
        )

    barrier = pltpu.get_barrier_semaphore()

    def greet(k, carry):
        pl.semaphore_signal(barrier, inc=1, device_id=at((me + k) % n), device_id_type=MESH)
        return carry

    lax.fori_loop(1, n, greet, 0)
    fetch = pltpu.make_async_copy(sky_ref, held_ref, held_sem)
    fetch.start()
    depth = n // 2

    def outer(k, carry):
        spot = pl.ds(pl.multiple_of(k * 8, 8), 8)
        table = turn_g_ref[spot, :]
        for e in range(2):
            x = []
            for a in range(depth):
                value = whole_ref[a, spot, :TILE], whole_ref[a, spot, TILE:]
                x.append(turn(value, 2 * math.pi * a / n) if e * a else value)
            for v, value in enumerate(sixteen(x)):
                u = 2 * v + e
                work_ref[u, 0, spot, :], work_ref[u, 1, spot, :] = times(value, *pick(table, u))
        return carry

    lax.fori_loop(0, whole_ref.shape[1] // 8, outer, 0)

    fetch.wait()

    def inner(k, carry):
        for u in (4 * k, 4 * k + 2):
            made = product(mat_g_ref, beside(work_ref, u))
            z = jnp.concatenate([made[:, q * TILE : (q + 1) * TILE] * held_ref[u + q] for q in range(2)], axis=1)
            spread = product(mat_f_ref, z)
            for q in range(2):
                for c in range(2):
                    work_ref[u + q, c, :TILE, :] = spread[c * TILE : (c + 1) * TILE, q * TILE : (q + 1) * TILE]
        return carry

    lax.fori_loop(0, n // 4, inner, 0)

    def last(k, carry):
        spot = pl.ds(pl.multiple_of(k * 8, 8), 8)
        table = turn_ref[spot, :]
        for e in range(2):
            x = []
            for v in range(depth):
                u = 2 * v + e
                x.append(times((work_ref[u, 0, spot, :], work_ref[u, 1, spot, :]), *pick(table, u)))
            for d, value in enumerate(minus(x)):
                if e == 0:
                    half_ref[d, 0], half_ref[d, 1] = value
                    continue
                value = turn(value, -2 * math.pi * d / n) if d else value
                before = half_ref[d, 0], half_ref[d, 1]
                for side, both_parts in enumerate((add(before, value), sub(before, value))):
                    fold_ref[d + side * depth, spot, :] = both_parts[0] - mirrored(both_parts[1], still)
        return carry

    def send(c, k, carry):
        sending(c, k).start()
        return carry

    for c in range(pieces):
        lax.fori_loop(c * span // 8, (c + 1) * span // 8, last, 0)
        if c == 0:
            pl.semaphore_wait(barrier, n - 1)
        lax.fori_loop(1, n, functools.partial(send, c), 0)
    folded_ref[me] = fold_ref[me]

    def receive(source):
        a = source // (halves * quads) * quads + source % quads
        j = 2 * a + source // quads % halves
        made = through(folded_ref[source], mat_r_ref, jnp.where(j == 0, 1, 0))
        work_ref[j, 0, :TILE, :], work_ref[j, 1, :TILE, :] = made[:, :TILE], made[:, TILE:]

    receive(me)

    def arrive(k, carry):
        for c in range(pieces):
            arriving(c, k).wait_recv()
        receive((me - k + n) % n)
        return carry

    lax.fori_loop(1, n, arrive, 0)

    def gradient(k, carry):
        spot = pl.ds(pl.multiple_of(k * 8, 8), 8)
        for e in range(2):
            x = []
            for v in range(depth):
                j = 2 * v + e
                x.append(times((work_ref[j, 0, spot, :], work_ref[j, 1, spot, :]), turn_r_ref[j, 0:1, :], turn_r_ref[j, 1:2, :]))
            for b, value in enumerate(sixteen(x)):
                if e == 0:
                    real_ref[b] = value[0]
                    continue
                real = turn(value, 2 * math.pi * b / n)[0] if b else value[0]
                for c, total in ((b, real_ref[b] + real), (b + depth, real_ref[b] - real)):
                    lanes = slice(c * TILE, (c + 1) * TILE)
                    out_ref[spot, lanes] = total * scale
        return carry

    lax.fori_loop(0, TILE // 8, gradient, 0)

    def sent(k, carry):
        for c in range(pieces):
            sending(c, k).wait_send()
        return carry

    lax.fori_loop(1, n, sent, 0)


def row_weights(n, size):
    alpha = np.arange(TILE)
    i = np.arange(size // n // 2)
    turns = np.stack(trig(np.arange(n)[:, None] * alpha[None, :], size), axis=1).astype(np.float32)
    c, s = trig(alpha[:, None] * i[None, :], size // n)
    there, back = [], []
    for special in range(2):
        real = np.concatenate([c + s, c - s], axis=1)
        imag = np.concatenate([c - s, -c - s], axis=1)
        from_real = np.concatenate([c + s, c - s], axis=1)
        from_imag = np.concatenate([s - c, s + c], axis=1)
        if special:
            lane = len(i)
            real[:, lane] = from_real[:, lane] = 1.0 - 2.0 * (alpha % 2)
            imag[:, lane] = from_imag[:, lane] = 0.0
        for target, matrix in ((there, np.concatenate([real, imag], axis=0)), (back, np.concatenate([from_real.T, from_imag.T], axis=1))):
            target.append(np.concatenate(split_table(matrix), axis=0))
    return turns, np.stack(there), np.stack(back)


def column_tables(n, size):
    w = np.arange(size // n)
    t = np.arange(TILE)
    u = np.arange(n)
    r = 2 * np.arange(2 * TILE) + 1
    side = TILE // 2

    def lanes(c, s):
        out = np.zeros((c.shape[0], TILE))
        out[:, :n], out[:, side : side + n] = c, s
        return out.astype(np.float32)

    def matrix(x):
        return np.concatenate(split_table(x), axis=0)

    c, s = trig(t[:, None] * u[None, :], size)
    turns = lanes(c, -s)
    c, s = trig(w[:, None] * t[None, :], size // n)
    mat_h = matrix(np.concatenate([c, s], axis=1))
    mat_f = matrix(np.concatenate([c.T, -s.T], axis=0))
    c, s = trig(r[:, None] * u[None, :], 2 * G)
    turns_g = lanes(c, s)
    c, s = trig((w[:, None] * n + G // 4) * r[None, :], 2 * G)
    mat_g = matrix(np.concatenate([s, c], axis=1))
    c, s = trig(w * n + G // 4, 2 * G)
    slope = np.stack([s, c]) * (2.0 * G)
    slope = np.broadcast_to(slope[:, :, None], slope.shape + (TILE,)).astype(np.float32)
    c, s = trig(u, 2 * G)
    bend = np.stack([c, s], axis=1).astype(np.float32)
    return turns, mat_h, mat_f, turns_g, mat_g, slope, bend


def column_call(kernel, smems, args, out_shape, scratch, name, away=(), **params):
    smem = pl.BlockSpec(memory_space=pltpu.SMEM)
    vmem = pl.BlockSpec(memory_space=pltpu.VMEM)
    anywhere = pl.BlockSpec(memory_space=pltpu.HBM)
    return pl.pallas_call(
        kernel,
        out_shape=jax.ShapeDtypeStruct(out_shape, jnp.float32),
        in_specs=[smem] * len(smems) + [anywhere if k in away else vmem for k in range(len(args))],
        out_specs=vmem,
        scratch_shapes=scratch,
        compiler_params=pltpu.CompilerParams(**{"vmem_limit_bytes": 24 << 20, **params}),
        cost_estimate=pl.CostEstimate(flops=10**10, bytes_accessed=16 * 2**20, transcendentals=0),
        name=name,
    )(*smems, *args)


def shared(residual, position, owner, tile_local, xi, amplitude):
    n = lax.axis_size(parts)
    n_base = lax.axis_size("base")
    n_slab = lax.axis_size("half") * lax.axis_size("quad")
    quads = lax.axis_size("quad")
    base, parity, quad = (lax.axis_index(axis) for axis in parts)
    place = 2 * (base * quads + quad) + parity
    rows, size = xi.shape
    depth = size // n
    half = depth // 2
    tiles = G // TILE

    row_turns, there, back_again = (jnp.asarray(x) for x in row_weights(n, size))
    block = (n, rows, depth)
    work = pltpu.VMEM((n, 2, rows, depth), jnp.float32)
    blocks = residual.shape[0]
    room = 2 * n_base * (2 * blocks // n)
    sent = pack(owner, tile_local, residual, position, n_base, n_slab, room)
    got, spectrum = exchange(sent, n_slab, xi, amplitude, row_turns, there)
    field = lax.all_to_all(spectrum, parts, split_axis=0, concat_axis=0, tiled=True)

    sources = n_slab * n_base
    codes = got[:, :, room, 0, :].reshape(sources, TILE).astype(jnp.int32)
    info = jnp.stack([quad, parity]).astype(jnp.int32)

    turns, firsts, undos, weights = grid_row_weights(n, size)
    halves = grid_rows_two(
        room,
        info,
        codes,
        jnp.asarray(firsts),
        got.reshape(sources * (room + 1), 4, TILE),
        jnp.asarray(turns),
        jnp.asarray(undos),
        jnp.asarray(weights),
    )
    whole = lax.all_to_all(halves, ("base", "quad"), split_axis=0, concat_axis=0, tiled=True)

    turns, mat_h, mat_f, turns_g, mat_g, slope, bend = (jnp.asarray(x) for x in column_tables(n, size))
    me = jnp.reshape(place, (1,)).astype(jnp.int32)
    sky = column_call(
        functools.partial(field_kernel, 1.0 / size),
        [me, bend],
        [field, turns, mat_h, slope],
        block,
        [work],
        "field",
    )
    pieces = 4
    dma = pltpu.SemaphoreType.DMA
    return amplitude * column_call(
        functools.partial(image_kernel, 1.0 / size),
        [],
        [whole, sky, turns_g, mat_g, mat_f, turns, row_turns, back_again],
        (rows, size),
        [
            pltpu.VMEM((n, 2, 2 * rows, depth), jnp.float32), pltpu.VMEM((n // 2, 2, 8, depth), jnp.float32),
            pltpu.VMEM(block, jnp.float32), pltpu.VMEM(block, jnp.float32), pltpu.VMEM(block, jnp.float32),
            pltpu.VMEM((n // 2, 8, depth), jnp.float32), dma, dma((pieces, n)), dma((pieces, n)),
        ],
        "image",
        away=(1,),
        vmem_limit_bytes=36 << 20,
        collective_id=1,
        has_side_effects=True,
    )


def solution(mesh):
    n_base, n_slab = mesh.shape["base"], mesh.shape["slab"]
    body, axes = general, both
    if n_slab == 2 * n_base and 2 * n_base * n_slab == G // TILE:
        body, axes = shared, parts
        mesh = jax.sharding.Mesh(mesh.devices.reshape(n_base, 2, n_slab // 2), parts)
    placed = (
        P(axes, None, None),
        P(axes, None, None),
        P(axes, None),
        P(axes),
        P(axes, None),
        P(axes, None),
    )
    return jax.shard_map(body, mesh=mesh, in_specs=placed, out_specs=P(axes, None), check_vma=False)
```

```python
import functools
import math

import jax
import jax.numpy as jnp
import numpy as np
from jax import lax
from jax.experimental import pallas as pl
from jax.experimental.pallas import tpu as pltpu
from jax.sharding import PartitionSpec as P

G = 8192
TILE = 128
both = ("base", "slab")
fine = lax.Precision.HIGHEST


def trig(product, modulus):
    angle = (product % modulus).astype(np.float64) * (2.0 * np.pi / modulus)
    return np.cos(angle), np.sin(angle)


def column_table(n, size):
    depth = size // n
    half = depth // 2
    i = np.arange(half)[None, :]
    j = np.arange(n)[:, None]
    low = n * i + j
    high = (-low) % size
    high[0, 0] = size // 2
    return np.concatenate([low, high], axis=1)


def row_tables(n, size):
    depth = size // n
    cols = column_table(n, size)
    oc, osn = trig(np.arange(n)[:, None] * np.arange(n)[None, :], n)
    outer = np.stack([oc, osn], axis=1)
    prod = np.arange(depth)[None, :, None] * cols[:, None, :]
    c, s = trig(prod, size)
    sign = np.where(np.arange(depth) < depth // 2, 1.0, -1.0)[None, None, :]
    inner = np.stack([c + s, sign * (c - s)], axis=1)
    return outer.astype(np.float32), inner.astype(np.float32)


def grid_row_tables(n, size):
    depth = G // n
    cols = column_table(n, size)
    half = cols.shape[1] // 2
    oc, osn = trig(np.arange(n)[:, None] * np.arange(n)[None, :], n)
    outer = np.stack([np.stack([oc, osn], 1), np.stack([-osn, oc], 1)], 0)
    low = cols[:, :half]
    high = cols[(-np.arange(n)) % n, half:]
    a = np.arange(depth)[None, :, None]
    out = []
    for part in (low, high):
        c, s = trig(a * (part[:, None, :] + G // 4), G)
        out.append(np.stack([np.concatenate([c, s], 2), np.concatenate([-s, c], 2)], 1))
    return outer.astype(np.float32), np.concatenate(out, axis=3).astype(np.float32)


def taps(cells, offsets):
    scaled = (cells - offsets) * 0.25
    kept = jnp.maximum(1.0 - scaled * scaled, 0.0)
    return kept * kept * kept


def split_three(x):
    high = x.astype(jnp.bfloat16)
    rest = x - high.astype(jnp.float32)
    middle = rest.astype(jnp.bfloat16)
    return high, middle, (rest - middle.astype(jnp.float32)).astype(jnp.bfloat16)


def grid_kernel(rows, info_ref, list_ref, data_ref, out_ref):
    count = info_ref[0]
    first = info_ref[1].astype(jnp.float32)
    out_ref[...] = jnp.zeros_like(out_ref)
    row_cells = lax.broadcasted_iota(jnp.int32, (rows, TILE), 0).astype(jnp.float32) + first
    col_cells = lax.broadcasted_iota(jnp.int32, (TILE, TILE), 0).astype(jnp.float32)

    def step(k, carry):
        packed = list_ref[k]
        index = packed // 256
        col = (packed // 2) % 128
        flip = (packed % 2).astype(jnp.float32)
        sign = 1.0 - 2.0 * flip
        start = 128.0 * flip
        block = data_ref[index]
        value = block[0:2, :]
        place = block[2:4, :]
        row_taps = taps(row_cells * sign + start, place[0:1, :])
        col_taps = taps(col_cells * sign + start, place[1:2, :])
        weighted = jnp.concatenate(
            [col_taps * value[0:1, :], col_taps * (value[1:2, :] * sign)], axis=0
        )
        rh, rm, rl = split_three(row_taps)
        wh, wm, wl = split_three(weighted)
        left = jnp.concatenate([rh, rh, rh, rm, rm, rl], axis=1)
        right = jnp.concatenate([wh, wm, wl, wh, wm, wh], axis=1)
        sub = lax.dot_general(
            left, right, (((1,), (1,)), ((), ())), preferred_element_type=jnp.float32
        )
        out_ref[0, col] += sub[:, :TILE]
        out_ref[1, col] += sub[:, TILE:]
        return carry

    lax.fori_loop(0, count, step, 0)


def grid_rows(info, table, gathered, rows):
    tiles = G // TILE
    smem = pl.BlockSpec(memory_space=pltpu.SMEM)
    vmem = pl.BlockSpec(memory_space=pltpu.VMEM)
    return pl.pallas_call(
        functools.partial(grid_kernel, rows),
        out_shape=jax.ShapeDtypeStruct((2, tiles, rows, TILE), jnp.float32),
        in_specs=[smem, smem, vmem],
        out_specs=vmem,
        compiler_params=pltpu.CompilerParams(vmem_limit_bytes=56 * 1024 * 1024),
        cost_estimate=pl.CostEstimate(
            flops=2 * 10**10, bytes_accessed=16 * 2**20, transcendentals=0
        ),
        name="grid_rows",
    )(info, table, gathered)


def einsum(form, *args, precision=lax.Precision.HIGH):
    return jnp.einsum(form, *args, precision=precision, preferred_element_type=jnp.float32)


def general(residual, position, owner, tile_local, xi, amplitude):
    n = lax.axis_size(both)
    n_base = lax.axis_size("base")
    n_slab = lax.axis_size("slab")
    me = lax.axis_index(both)
    rows, size = xi.shape
    depth = size // n
    half = depth // 2
    tiles = G // TILE

    region_rows = G // n_slab // TILE
    region_cols = G // n_base // TILE
    target = owner[:, 0]
    tile_row = (target % n_slab) * region_rows + tile_local // region_cols
    tile_col = (target // n_slab) * region_cols + tile_local % region_cols
    flip = tile_row >= tiles // 2
    tile_row = jnp.where(flip, tiles - 1 - tile_row, tile_row)
    tile_col = jnp.where(flip, tiles - 1 - tile_col, tile_col)
    code = tile_row * 256 + tile_col * 2 + flip.astype(jnp.int32)
    codes = lax.all_gather(code, both, axis=0, tiled=True)
    payload = jnp.concatenate([residual, position], axis=1)
    codes, payload = lax.optimization_barrier((codes, payload))
    gathered = lax.all_gather(payload, both, axis=0, tiled=True)
    blocks = codes.shape[0]
    grid_depth = G // 2 // n
    first_row = me * grid_depth
    mine = (codes // 256 == first_row // TILE).astype(jnp.int32)
    rank = jnp.where(mine == 1, jnp.cumsum(mine) - 1, -1)
    packed = lax.broadcasted_iota(jnp.int32, (blocks,), 0) * 256 + codes % 256
    spots = lax.broadcasted_iota(jnp.int32, (blocks, blocks), 0)
    table = jnp.sum(jnp.where(spots == rank[None, :], packed[None, :], 0), axis=1)
    info = jnp.stack([jnp.sum(mine), first_row % TILE]).astype(jnp.int32)

    outer, inner = row_tables(n, size)
    spectrum = (amplitude * xi).reshape(rows, n, depth)
    mid = einsum("rba,bqc->qcra", spectrum, outer)
    sent = einsum("cra,cae->cre", mid[0], inner[:, 0]) + einsum("cra,cae->cre", mid[1], inner[:, 1])
    sent, gathered = lax.optimization_barrier((sent, gathered))
    field = lax.all_to_all(sent, both, split_axis=0, concat_axis=0, tiled=True)
    field = field.reshape(size, depth)
    lane = lax.broadcasted_iota(jnp.int32, (1, depth), 1)
    still = (me == 0) & (lane % half == 0)

    def mirror(x):
        return jnp.where(still, x, jnp.roll(x, half, axis=-1))

    c_len = 128
    d_len = size // c_len
    bc, bs = (x.astype(np.float32) for x in trig(np.arange(c_len)[:, None] * np.arange(c_len)[None, :], c_len))
    shape = (c_len, d_len, depth)
    n0 = c_len * np.arange(d_len)[None, :] + np.arange(c_len)[:, None]
    ic, isn = (x.astype(np.float32) for x in trig(n0[:, :, None] * np.arange(d_len)[None, None, :], size))
    pair = jnp.stack([field.reshape(shape), mirror(field).reshape(shape)])
    first = np.stack([np.stack([bc, bs], 1), np.stack([bs, -bc], 1)], 0)
    turned = einsum("qbal,qbsc->csal", pair, first)
    second = np.stack([ic, -isn], axis=2)
    power = einsum("csal,cdsa->cdl", turned, second)
    sky = jnp.exp(power / size)

    grid = grid_rows(info, table, gathered, grid_depth)
    outer_g, inner_g = grid_row_tables(n, size)
    parts = tiles // n if tiles >= n else 1
    inner_len = G // n
    if inner_len >= TILE:
        view = grid.reshape(2, n, inner_len // TILE, grid_depth, TILE)
    else:
        flat = grid.transpose(0, 2, 1, 3).reshape(2, grid_depth, n, inner_len)
        view = flat.transpose(0, 2, 1, 3)[:, :, None]
        parts = 1
    lanes = view.shape[-1]
    stage = einsum("qbpra,qbsc->cspra", view, outer_g, precision=fine)
    inner_g = inner_g.reshape(n, 2, parts, lanes, 2 * depth)
    halves = einsum("cspra,cspae->cre", stage, inner_g, precision=fine)
    high = halves[:, :, depth:]
    high = jnp.concatenate([high[:1], jnp.flip(high[1:], axis=0)], axis=0)
    halves = jnp.concatenate([halves[:, :, :depth], high], axis=2)
    got = lax.all_to_all(halves, both, split_axis=0, concat_axis=0, tiled=True)
    got = got.reshape(size, 2 * depth)
    real = jnp.concatenate([got[:, :half], got[:, depth : depth + half]], axis=1)
    imag = jnp.concatenate([got[:, half:depth], got[:, depth + half :]], axis=1)
    wide = G // c_len
    deep = size // wide
    gc, gs = (x.astype(np.float32) for x in trig(np.arange(deep)[:, None] * np.arange(c_len)[None, :], c_len))
    first_g = np.stack([np.stack([gc, gs], 1), np.stack([-gs, gc], 1)], 0)
    whole = jnp.stack([real.reshape(deep, wide, depth), imag.reshape(deep, wide, depth)])
    turned_g = einsum("qbal,qbsc->csal", whole, first_g, precision=fine)
    ac, asn = trig((n0 + G // 4)[:, :, None] * np.arange(wide)[None, None, :], G)
    second_g = (np.stack([ac, -asn], axis=2) / G).astype(np.float32)
    back = einsum("csal,cdsa->cdl", turned_g, second_g, precision=fine)

    z = sky * back
    pz = einsum("cdl,cda->cal", z, ic)
    qz = einsum("cdl,cda->cal", z, isn)
    joined = jnp.stack([pz + mirror(qz), mirror(pz) - qz])
    fold = einsum("qcal,qcb->bal", joined, np.stack([bc, bs]))
    folded = lax.all_to_all(
        fold.reshape(n, rows, depth), both, split_axis=0, concat_axis=0, tiled=True
    )
    ends = einsum("jre,jqae->qjra", folded, inner)
    final = einsum("qjra,bqj->rba", ends, outer)
    return amplitude * final.reshape(rows, size) / size


MESH = pl.DeviceIdType.MESH
parts = ("base", "half", "quad")
LANES = 4


def two_parts(x):
    high = x.astype(jnp.bfloat16)
    return high, (x - high.astype(jnp.float32)).astype(jnp.bfloat16)


def through(x, weight_ref, which):
    rows, depth = x.shape
    high, low = two_parts(x)
    made = jnp.dot(jnp.concatenate([high, low], axis=0), weight_ref[which, :depth], preferred_element_type=jnp.float32)
    return made[:rows] + made[rows:] + jnp.dot(high, weight_ref[which, depth:], preferred_element_type=jnp.float32)


def times(x, c, s):
    return x[0] * c - x[1] * s, x[0] * s + x[1] * c


def turn(x, angle):
    c, s = math.cos(angle), math.sin(angle)
    return times(x, c, s)


def add(x, y):
    return x[0] + y[0], x[1] + y[1]


def sub(x, y):
    return x[0] - y[0], x[1] - y[1]


def four(x):
    s0, d0, s1, d1 = add(x[0], x[2]), sub(x[0], x[2]), add(x[1], x[3]), sub(x[1], x[3])
    i1 = (-d1[1], d1[0])
    return [add(s0, s1), add(d0, i1), sub(s0, s1), sub(d0, i1)]


def sixteen(x):
    rows = []
    for b0 in range(4):
        y = four([x[4 * b1 + b0] for b1 in range(4)])
        rows.append([y[a0] if a0 * b0 == 0 else turn(y[a0], 2 * math.pi * a0 * b0 / 16) for a0 in range(4)])
    out = [None] * 16
    for a0 in range(4):
        y = four([rows[b0][a0] for b0 in range(4)])
        for a1 in range(4):
            out[a0 + 4 * a1] = y[a1]
    return out


def seat(j, quads):
    a = j // 2
    return a // quads * (2 * quads) + j % 2 * quads + a % quads


def transform_rows(quads, xi_ref, amplitude_ref, turn_ref, mat_ref, out_ref, work_ref):
    n = out_ref.shape[0]

    def outer(k, carry):
        spot = pl.ds(pl.multiple_of(k * 8, 8), 8)
        for e in range(2):
            x = []
            for b in range(n // 2):
                first, second = (
                    xi_ref[spot, c * TILE : (c + 1) * TILE] * amplitude_ref[spot, c * TILE : (c + 1) * TILE]
                    for c in (b, b + n // 2)
                )
                value = first - second if e else first + second
                if e * b:
                    angle = 2 * math.pi * b / n
                    x.append((value * math.cos(angle), value * math.sin(angle)))
                else:
                    x.append((value, jnp.zeros_like(value)))
            for v, value in enumerate(sixteen(x)):
                j = 2 * v + e
                work_ref[j, 0, spot, :], work_ref[j, 1, spot, :] = times(value, turn_ref[j, 0:1, :], turn_ref[j, 1:2, :])
        return carry

    lax.fori_loop(0, xi_ref.shape[0] // 8, outer, 0)
    rows = xi_ref.shape[0]

    def left(entries):
        return jnp.concatenate([jnp.concatenate([work_ref[j, 0], work_ref[j, 1]], axis=1) for j in entries], axis=0)

    def inner(k, carry):
        entries = [4 * k + q for q in range(4)]
        made = through(left(entries), mat_ref, 0)
        for q, j in enumerate(entries):
            out_ref[seat(j, quads)] = made[q * rows : (q + 1) * rows]
        return carry

    lax.fori_loop(0, n // 4, inner, 0)
    out_ref[0] = through(left([0]), mat_ref, 1)


def seats(base, quad):
    return base // 2, base % 2, quad // 2, quad % 2


def group_of(base, quad):
    y, x, low, core = seats(base, quad)
    return 2 * x + low, 2 * y + core


def exchange_kernel(send_ref, xi_ref, amplitude_ref, turn_ref, mat_ref, out_ref, spectrum_ref, work_ref, made_ref, rows_ref, rows_sem, bsend, brecv, zsend, zrecv, ysend, yrecv, csend, crecv, lsem):
    nb = send_ref.shape[0]
    quads = lax.axis_size("quad")
    half = lax.axis_index("half")
    y, x, low, core = seats(lax.axis_index("base"), lax.axis_index("quad"))
    group = 2 * x + low

    def at(y, group, half, core):
        return (2 * y + group // 2, half, group % 2 * 2 + core)

    def block(y, half, core, k):
        return out_ref.at[(2 * y + half) * 2 + core, (group - k + nb) % nb]

    def copy(part, here, there, device):
        return pltpu.make_async_remote_copy(
            src_ref=part, dst_ref=part, send_sem=here, recv_sem=there, device_id=device, device_id_type=MESH
        )

    def moved(target, source, k):
        return pltpu.make_async_remote_copy(
            src_ref=send_ref.at[target],
            dst_ref=out_ref.at[(2 * y + half) * 2 + core, source],
            send_sem=bsend.at[k],
            recv_sem=brecv.at[k],
            device_id=at(y, target, half, core),
            device_id_type=MESH,
        )

    far, beside, partner = at(y, group, 1 - half, core), at(1 - y, group, half, core), at(y, group, half, 1 - core)

    def along_z(own, k):
        return copy(block(y, half if own else 1 - half, core, k), zsend.at[k], zrecv.at[k], far)

    def along_y(own, kind, k):
        place = half if kind == 0 else 1 - half
        return copy(block(y if own else 1 - y, place, core, k), ysend.at[kind, k], yrecv.at[kind, k], beside)

    def over(own, kind, k):
        row = y if kind < 2 else 1 - y
        place = half if kind % 2 == 0 else 1 - half
        return copy(block(row, place, core if own else 1 - core, k), csend.at[kind, k], crecv.at[kind, k], partner)

    fetches = [
        pltpu.make_async_copy(source, rows_ref.at[k], rows_sem.at[k]) for k, source in enumerate((xi_ref, amplitude_ref))
    ]
    ready = pltpu.make_async_copy(made_ref, spectrum_ref, rows_sem.at[2])
    for fetch in fetches:
        fetch.start()
    barrier = pltpu.get_barrier_semaphore()
    peers = [at(y, (group + k) % nb, half, core) for k in range(1, nb)] + [far, beside, partner]
    for peer in peers:
        pl.semaphore_signal(barrier, inc=1, device_id=peer, device_id_type=MESH)
    pl.semaphore_wait(barrier, len(peers))

    own = pltpu.make_async_copy(send_ref.at[group], block(y, half, core, 0), lsem)
    own.start()
    for k in range(1, nb):
        moved((group + k) % nb, group, k).start()
    for k in range(nb):
        if k == 0:
            own.wait()
        else:
            moved((group - k + nb) % nb, (group - k + nb) % nb, k).wait_recv()
        along_z(True, k).start()
        along_y(True, 0, k).start()
        over(True, 0, k).start()
        if k == 0:
            for fetch in fetches:
                fetch.wait()
            transform_rows(quads, rows_ref.at[0], rows_ref.at[1], turn_ref, mat_ref, made_ref, work_ref)
            ready.start()
    for k in range(nb):
        along_z(False, k).wait_recv()
        along_y(True, 1, k).start()
        over(True, 1, k).start()
    for kind in range(2):
        for k in range(nb):
            along_y(False, kind, k).wait_recv()
            over(True, 2 + kind, k).start()
    ready.wait()
    for kind in range(4):
        for k in range(nb):
            over(False, kind, k).wait_recv()
    for k in range(nb):
        if k:
            moved((group + k) % nb, group, k).wait_send()
        along_z(True, k).wait_send()
        for kind in range(2):
            along_y(True, kind, k).wait_send()
        for kind in range(4):
            over(True, kind, k).wait_send()


def pack_kernel(ns, tiles, room, owner_ref, local_ref, residual_ref, position_ref, out_ref):
    blocks = residual_ref.shape[0]
    nb = out_ref.shape[0]
    across = lax.broadcasted_iota(jnp.int32, (blocks, blocks), 1)
    down = lax.broadcasted_iota(jnp.int32, (blocks, blocks), 0)

    def column(row):
        return jnp.sum(jnp.where(across == down, row, 0.0), axis=1, keepdims=True)

    def divided(x, d):
        whole = jnp.floor((x + 0.5) * (1.0 / d))
        return whole, x - whole * d

    local = local_ref[...].astype(jnp.float32)
    target = owner_ref[...].astype(jnp.float32)
    region_col, region_row = divided(target, ns)
    tile_row, tile_col = divided(local, tiles // nb)
    tile_row = tile_row + region_row * (tiles // ns)
    tile_col = tile_col + region_col * (tiles // nb)
    flip = jnp.where(tile_row >= tiles // 2, 1.0, 0.0)
    tile_row = jnp.where(flip > 0.5, tiles - 1 - tile_row, tile_row)
    tile_col = jnp.where(flip > 0.5, tiles - 1 - tile_col, tile_col)
    line, within = divided(tile_row, ns)
    key = divided(tile_row, 2)[0]
    code = within * tiles + tile_col
    keys = ns // 2
    line_down, key_down, flip_down = column(line), column(key), column(flip)
    before = (line_down == line) & ((key_down < key) | ((key_down == key) & (down < across)))
    slot = line * room + jnp.sum(jnp.where(before, 1.0, 0.0), axis=0, keepdims=True)
    slots = lax.broadcasted_iota(jnp.int32, (nb * room, blocks), 0).astype(jnp.float32)
    chosen = jnp.where(slots == slot, 1.0, 0.0).astype(jnp.bfloat16)
    sides = [residual_ref[:, 0, :], residual_ref[:, 1, :] * (1.0 - 2.0 * flip_down)]
    for k in range(2):
        place = position_ref[:, k, :]
        sides.append(jnp.where(flip_down > 0.5, TILE - place, place))
    pieces = split_three(jnp.concatenate(sides, axis=1))
    moved = jnp.dot(
        jnp.concatenate([chosen] * 3, axis=1), jnp.concatenate(pieces, axis=0), preferred_element_type=jnp.float32
    )
    codes = 0.0
    for part in two_parts(jnp.broadcast_to(code + 1.0, (8, blocks))):
        codes = codes + lax.dot_general(part, chosen, (((1,), (1,)), ((), ())), preferred_element_type=jnp.float32)
    codes = codes - 1.0
    lanes = lax.broadcasted_iota(jnp.int32, (1, blocks), 1)
    shift = (across - room).astype(jnp.float32)
    per = blocks // room
    for k in range(nb):
        for c in range(4):
            out_ref[k, :room, c, :] = moved[k * room : (k + 1) * room, c * TILE : (c + 1) * TILE]
        start = k // per * blocks
        own = codes[:, start : start + blocks]
        if k % per:
            own = pltpu.roll(own, blocks - k % per * room, 1)
        earlier = (line_down == k) & (key_down - keys * k < shift)
        starts = jnp.sum(jnp.where(earlier, 1.0, 0.0), axis=0, keepdims=True)
        out_ref[k, room] = jnp.broadcast_to(jnp.where(lanes < room, own[0:1, :], starts), (4, TILE))


def pack(owner, local, residual, position, nb, ns, room):
    vmem = pl.BlockSpec(memory_space=pltpu.VMEM)
    return pl.pallas_call(
        functools.partial(pack_kernel, ns, G // TILE, room),
        out_shape=jax.ShapeDtypeStruct((nb, room + 1, 4, TILE), jnp.float32),
        in_specs=[vmem] * 4,
        out_specs=vmem,
        compiler_params=pltpu.CompilerParams(vmem_limit_bytes=60 << 20),
        name="pack",
    )(owner.reshape(1, -1), local.reshape(1, -1), residual, position)


def exchange(sent, ns, xi, amplitude, turns, mats):
    nb = sent.shape[0]
    rows, n = xi.shape[0], turns.shape[0]
    dma = pltpu.SemaphoreType.DMA
    vmem = pl.BlockSpec(memory_space=pltpu.VMEM)
    hbm = pl.BlockSpec(memory_space=pltpu.HBM)
    return pl.pallas_call(
        exchange_kernel,
        out_shape=(
            jax.ShapeDtypeStruct((ns,) + sent.shape, jnp.float32),
            jax.ShapeDtypeStruct((n, rows, TILE), jnp.float32),
        ),
        in_specs=[vmem, hbm, hbm, vmem, vmem],
        out_specs=(hbm, hbm),
        scratch_shapes=[
            pltpu.VMEM((n, 2, rows, TILE), jnp.float32),
            pltpu.VMEM((n, rows, TILE), jnp.float32),
            pltpu.VMEM((2,) + xi.shape, jnp.float32), dma((3,)),
            dma((nb,)), dma((nb,)), dma((nb,)), dma((nb,)), dma((2, nb)), dma((2, nb)), dma((4, nb)), dma((4, nb)), dma,
        ],
        compiler_params=pltpu.CompilerParams(collective_id=0, has_side_effects=True, vmem_limit_bytes=60 << 20),
        cost_estimate=pl.CostEstimate(flops=3 * 10**10, bytes_accessed=16 * 2**20, transcendentals=0),
        name="exchange",
    )(sent, xi, amplitude, turns, mats)


def grid_kernel_two(room, info_ref, codes_ref, first_ref, data_hbm_ref, turn_ref, undo_ref, weight_hbm_ref, away_ref, grid_ref, left_ref, right_ref, out_ref, data_ref, weight_ref, list_ref, sems):
    quad = info_ref[0]
    parity = info_ref[1]
    data = pltpu.make_async_copy(data_hbm_ref, data_ref, sems.at[out_ref.shape[0]])
    weight = pltpu.make_async_copy(weight_hbm_ref, weight_ref, sems.at[out_ref.shape[0] + 1])
    data.start()
    weight.start()
    grid_ref[...] = jnp.zeros_like(grid_ref)
    half = grid_ref.shape[1]
    group = 16
    cells = lax.broadcasted_iota(jnp.int32, (group + 8, TILE), 0).astype(jnp.float32) * 0.25
    nothing = jnp.zeros((group, TILE), jnp.bfloat16)

    def bump(offsets):
        d = cells - offsets
        kept = jnp.maximum(1.0 - d * d, 0.0)
        return kept * kept * kept

    def window(offsets):
        start = jnp.floor((offsets - 4.0) * (1.0 / group))
        offsets = (offsets - start * group) * 0.25
        return bump(offsets) - bump(offsets - 0.25), jnp.broadcast_to(start, (group, TILE)).astype(jnp.bfloat16)

    def spread(compact, start):
        padded = jnp.concatenate([compact, jnp.zeros((8, TILE), jnp.float32)], axis=0)
        out = []
        for part in two_parts(padded):
            first, second = part[:group], part[group:]
            pieces = []
            for g in range(TILE // group):
                piece = jnp.where(start == g - 1, second, nothing) if g else nothing
                pieces.append(jnp.where(start == g, first, piece))
            out.append(jnp.concatenate(pieces, axis=0))
        return out

    lanes = left_ref.shape[0]

    def place(k):
        packed = list_ref[k]
        return packed % 64, packed // 64

    def prepare(k, lane, count):
        col, rest = place(k)
        odd = jnp.where(col >= half, parity, 0)
        sign = jnp.where(k < count, 1 - 2 * odd, 0).astype(jnp.float32)
        block = data_ref[rest // 2]
        value = block[0:2, :] * sign
        row_taps, row_start = window(block[2:3, :])
        col_taps, col_start = window(block[3:4, :])
        rows_split = spread(row_taps, row_start)
        real = spread(col_taps * value[0:1, :], col_start)
        imag = spread(col_taps * value[1:2, :], col_start)
        for q in range(2):
            left_ref[lane, :, q * TILE : (q + 1) * TILE] = rows_split[q]
            right_ref[lane, :TILE, q * TILE : (q + 1) * TILE] = real[q]
            right_ref[lane, TILE:, q * TILE : (q + 1) * TILE] = imag[q]

    def product(lane):
        rh, rl = left_ref[lane, :, :TILE], left_ref[lane, :, TILE:]
        wh, wl = right_ref[lane, :, :TILE], right_ref[lane, :, TILE:]
        left = jnp.concatenate([rh, rh, rl], axis=1)
        right = jnp.concatenate([wh, wl, wh], axis=1)
        return lax.dot_general(left, right, (((1,), (1,)), ((), ())), preferred_element_type=jnp.float32)

    def step(k, carry):
        made = [product(lane) for lane in range(lanes)]
        for lane in range(lanes):
            prepare((k + 1) * lanes + lane, lane, count)
        for lane in range(lanes):
            col, rest = place(k * lanes + lane)
            col = jnp.where(col >= half, col - half, col)
            spot = pl.ds(pl.multiple_of((rest % 2) * TILE, TILE), TILE)
            grid_ref[0, col, spot, :] += made[lane][:, :TILE]
            grid_ref[1, col, spot, :] += made[lane][:, TILE:]
        return carry

    def gather(source, filled):
        start = codes_ref[source, room + quad]
        stop = codes_ref[source, room + quad + 1]

        def entry(i, carry):
            list_ref[filled + i - start] = (source * (room + 1) + i) * TILE + codes_ref[source, i] % TILE
            return carry

        lax.fori_loop(start, stop, entry, 0)
        return filled + stop - start

    count = lax.fori_loop(0, codes_ref.shape[0], gather, 0)
    for lane in range(2 * lanes):
        list_ref[count + lane] = 0
    data.wait()
    for lane in range(lanes):
        prepare(lane, lane, count)
    lax.fori_loop(0, (count + lanes - 1) // lanes, step, 0)

    depth = half // 2
    rows = grid_ref.shape[2]

    def outer(k, carry):
        spot = pl.ds(pl.multiple_of(k * 8, 8), 8)
        for side in range(2):
            x = []
            for b in range(depth):
                value = grid_ref[0, 2 * b + side, spot, :], grid_ref[1, 2 * b + side, spot, :]
                x.append(times(value, first_ref[parity, b, 0], first_ref[parity, b, 1]))
            for a, value in enumerate(sixteen(x)):
                c = turn_ref[parity, a, side : side + 1, :]
                s = turn_ref[parity, a, 2 + side : 3 + side, :]
                value = times(value, c, s)
                grid_ref[0, 2 * a + side, spot, :] = value[0]
                grid_ref[1, 2 * a + side, spot, :] = value[1]
        return carry

    lax.fori_loop(0, rows // 8, outer, 0)

    def inner(a, carry):
        mirrored = depth - parity - a
        mirrored = jnp.where(mirrored == depth, 0, mirrored)
        which = jnp.where((a == 0) & (parity == 0), 1, 0)
        for part in range(1):
            spot = pl.ds(0, rows)
            x = jnp.concatenate([grid_ref[q, 2 * a + side, spot, :] for q in range(2) for side in range(2)], axis=1)
            made = through(x, weight_ref, which)
            mid = TILE // 2
            made = times((made[:, :TILE], made[:, TILE:]), undo_ref[parity, a, 0:1, :], undo_ref[parity, a, 1:2, :])
            for q in range(2):
                out_ref[a, spot, q * TILE : q * TILE + mid] = made[q][:, :mid]
                out_ref[mirrored, spot, q * TILE + mid : (q + 1) * TILE] = made[q][:, mid:]

        @pl.when(a >= depth // 2)
        def _():
            leave(a).start()
            leave(jnp.where((parity == 0) & (a == depth // 2), 0, mirrored)).start()

        return carry

    def leave(a):
        return pltpu.make_async_copy(out_ref.at[a], away_ref.at[a], sems.at[a])

    weight.wait()
    lax.fori_loop(0, depth, inner, 0)
    for a in range(depth):
        leave(a).wait()


def split_table(x):
    high = x.astype(np.float32).astype(jnp.bfloat16)
    low = (x - high.astype(np.float64)).astype(np.float32).astype(jnp.bfloat16)
    return high, low


def undone(pixels):
    c, s = trig(pixels + G // 4, G)
    return 1.0 / (1.0 - (c - 1j * s))


def grid_row_weights(n, size):
    depth = n // 2
    span = G // 2 // depth
    half = size // n // 2
    alpha = np.arange(span)
    turns, firsts, undos = [], [], []
    for p in range(2):
        j = 2 * np.arange(depth) + p
        c, s = trig(j[:, None] * alpha[None, :], G)
        turns.append(np.concatenate([c.reshape(depth, 2, TILE), s.reshape(depth, 2, TILE)], axis=1))
        firsts.append(np.stack(trig(np.arange(depth) * p, n), axis=1))
        low = n * np.arange(half)[None, :] + j[:, None]
        high = size - n * np.arange(half)[None, :] - ((-j) % n)[:, None]
        if p == 0:
            low[0, 0], high[0, 0] = 0, size // 2
        undo = undone(np.concatenate([low, high], axis=1))
        undos.append(np.stack([undo.real, undo.imag], axis=1))
    weights = []
    i = np.arange(half)
    for special in range(2):
        low = n * i
        high = size - n * i - (0 if special else n)
        if special:
            high[0] = size // 2
        parts_re, parts_im = [], []
        for cols in (low, high):
            c, s = trig(alpha[:, None] * (cols[None, :] + G // 4), G)
            parts_re.append(np.concatenate([c, -s], axis=0))
            parts_im.append(np.concatenate([s, c], axis=0))
        w = np.concatenate(parts_re + parts_im, axis=1)
        weights.append(np.concatenate(split_table(w), axis=0))
    turns, firsts, undos = (np.stack(x).astype(np.float32) for x in (turns, firsts, undos))
    return turns, firsts, undos, np.stack(weights)


def grid_rows_two(room, info, codes, first, data, turns, undos, weights):
    depth = turns.shape[1]
    rows = 2 * TILE
    smem = pl.BlockSpec(memory_space=pltpu.SMEM)
    vmem = pl.BlockSpec(memory_space=pltpu.VMEM)
    hbm = pl.BlockSpec(memory_space=pltpu.HBM)
    return pl.pallas_call(
        functools.partial(grid_kernel_two, room),
        out_shape=jax.ShapeDtypeStruct((depth, rows, 2 * TILE), jnp.float32),
        in_specs=[smem, smem, smem, hbm, vmem, vmem, hbm],
        out_specs=hbm,
        scratch_shapes=[
            pltpu.VMEM((2, 2 * depth, rows, TILE), jnp.float32),
            pltpu.VMEM((LANES, TILE, 2 * TILE), jnp.bfloat16),
            pltpu.VMEM((LANES, 2 * TILE, 2 * TILE), jnp.bfloat16),
            pltpu.VMEM((depth, rows, 2 * TILE), jnp.float32),
            pltpu.VMEM(data.shape, jnp.float32),
            pltpu.VMEM(weights.shape, jnp.bfloat16),
            pltpu.SMEM((codes.shape[0] * room + 2 * LANES,), jnp.int32),
            pltpu.SemaphoreType.DMA((depth + 2,)),
        ],
        compiler_params=pltpu.CompilerParams(vmem_limit_bytes=60 << 20),
        cost_estimate=pl.CostEstimate(flops=2 * 10**10, bytes_accessed=16 * 2**20, transcendentals=0),
        name="grid_rows_two",
    )(info, codes, first, data, turns, undos, weights)


def minus(x):
    return [(b, a) for a, b in sixteen([(b, a) for a, b in x])]


def pick(table, u):
    side = table.shape[1] // 2
    return table[:, u : u + 1], table[:, side + u : side + u + 1]


def mirrored(x, still):
    return jnp.where(still, x, pltpu.roll(x, x.shape[1] // 2, 1))


def still_lanes(place, rows):
    lane = lax.broadcasted_iota(jnp.int32, (rows, TILE), 1)
    return (lane % (TILE // 2) == 0) & (place == 0)


def product(mat_ref, x):
    rows = mat_ref.shape[0] // 2
    high, low = two_parts(x)
    made = jnp.dot(mat_ref[...], high, preferred_element_type=jnp.float32)
    return made[:rows] + made[rows:] + jnp.dot(mat_ref[:rows], low, preferred_element_type=jnp.float32)


def beside(work_ref, u):
    sides = [jnp.concatenate([work_ref[u + q, 0], work_ref[u + q, 1]], axis=0) for q in range(2)]
    return jnp.concatenate(sides, axis=1)


def field_kernel(scale, info_ref, bend_ref, field_ref, turn_ref, mat_ref, slope_ref, sky_ref, work_ref):
    still = still_lanes(info_ref[0], 8)
    n = field_ref.shape[0]

    def outer(k, carry):
        spot = pl.ds(pl.multiple_of(k * 8, 8), 8)
        table = turn_ref[spot, :]
        for e in range(2):
            x = []
            for d in range(n // 2):
                first, second = field_ref[d, spot, :], field_ref[d + n // 2, spot, :]
                value = first - second if e else first + second
                value = value, mirrored(value, still)
                x.append(turn(value, -2 * math.pi * d / n) if e * d else value)
            for v, value in enumerate(minus(x)):
                u = 2 * v + e
                work_ref[u, 0, spot, :], work_ref[u, 1, spot, :] = times(value, *pick(table, u))
        return carry

    lax.fori_loop(0, field_ref.shape[1] // 8, outer, 0)

    def inner(k, carry):
        for u in (4 * k, 4 * k + 2):
            made = jnp.exp(product(mat_ref, beside(work_ref, u)) * scale)
            for q in range(2):
                sine = slope_ref[0] * bend_ref[u + q, 0] + slope_ref[1] * bend_ref[u + q, 1]
                sky_ref[u + q] = made[:, q * TILE : (q + 1) * TILE] / sine
        return carry

    lax.fori_loop(0, n // 4, inner, 0)


def image_kernel(scale, whole_ref, sky_ref, turn_g_ref, mat_g_ref, mat_f_ref, turn_ref, turn_r_ref, mat_r_ref, out_ref, work_ref, half_ref, held_ref, fold_ref, folded_ref, real_ref, held_sem, send_sems, recv_sems):
    n = sky_ref.shape[0]
    quads = lax.axis_size("quad")
    halves = lax.axis_size("half")
    me = (lax.axis_index("base") * halves + lax.axis_index("half")) * quads + lax.axis_index("quad")
    place = 2 * (lax.axis_index("base") * quads + lax.axis_index("quad")) + lax.axis_index("half")
    still = still_lanes(place, 8)
    pieces = send_sems.shape[0]
    span = TILE // pieces

    def at(device):
        return (device // (halves * quads), device // quads % halves, device % quads)

    def sending(c, k):
        target = (me + k) % n
        part = pl.ds(c * span, span)
        return pltpu.make_async_remote_copy(
            src_ref=fold_ref.at[target, part], dst_ref=folded_ref.at[me, part],
            send_sem=send_sems.at[c, k], recv_sem=recv_sems.at[c, k], device_id=at(target), device_id_type=MESH,
        )

    def arriving(c, k):
        source = (me - k + n) % n
        part = pl.ds(c * span, span)
        return pltpu.make_async_remote_copy(
            src_ref=fold_ref.at[source, part], dst_ref=folded_ref.at[source, part],
            send_sem=send_sems.at[c, k], recv_sem=recv_sems.at[c, k], device_id=at(source), device_id_type=MESH,
        )

    barrier = pltpu.get_barrier_semaphore()

    def greet(k, carry):
        pl.semaphore_signal(barrier, inc=1, device_id=at((me + k) % n), device_id_type=MESH)
        return carry

    lax.fori_loop(1, n, greet, 0)
    origins = [0] * (n // 2)
    for k in range(n // 2):
        group, member = group_of(k // quads, k % quads)
        origins[group * quads + member] = k
    fetch = pltpu.make_async_copy(sky_ref, held_ref, held_sem)
    fetch.start()
    depth = n // 2

    def outer(k, carry):
        spot = pl.ds(pl.multiple_of(k * 8, 8), 8)
        table = turn_g_ref[spot, :]
        for e in range(2):
            x = []
            for a in range(depth):
                value = whole_ref[origins[a], spot, :TILE], whole_ref[origins[a], spot, TILE:]
                x.append(turn(value, 2 * math.pi * a / n) if e * a else value)
            for v, value in enumerate(sixteen(x)):
                u = 2 * v + e
                work_ref[u, 0, spot, :], work_ref[u, 1, spot, :] = times(value, *pick(table, u))
        return carry

    lax.fori_loop(0, whole_ref.shape[1] // 8, outer, 0)

    fetch.wait()

    def inner(k, carry):
        for u in (4 * k, 4 * k + 2):
            made = product(mat_g_ref, beside(work_ref, u))
            z = jnp.concatenate([made[:, q * TILE : (q + 1) * TILE] * held_ref[u + q] for q in range(2)], axis=1)
            spread = product(mat_f_ref, z)
            for q in range(2):
                for c in range(2):
                    work_ref[u + q, c, :TILE, :] = spread[c * TILE : (c + 1) * TILE, q * TILE : (q + 1) * TILE]
        return carry

    lax.fori_loop(0, n // 4, inner, 0)

    def last(k, carry):
        spot = pl.ds(pl.multiple_of(k * 8, 8), 8)
        table = turn_ref[spot, :]
        for e in range(2):
            x = []
            for v in range(depth):
                u = 2 * v + e
                x.append(times((work_ref[u, 0, spot, :], work_ref[u, 1, spot, :]), *pick(table, u)))
            for d, value in enumerate(minus(x)):
                if e == 0:
                    half_ref[d, 0], half_ref[d, 1] = value
                    continue
                value = turn(value, -2 * math.pi * d / n) if d else value
                before = half_ref[d, 0], half_ref[d, 1]
                for side, both_parts in enumerate((add(before, value), sub(before, value))):
                    fold_ref[d + side * depth, spot, :] = both_parts[0] - mirrored(both_parts[1], still)
        return carry

    def send(c, k, carry):
        sending(c, k).start()
        return carry

    for c in range(pieces):
        lax.fori_loop(c * span // 8, (c + 1) * span // 8, last, 0)
        if c == 0:
            pl.semaphore_wait(barrier, n - 1)
        lax.fori_loop(1, n, functools.partial(send, c), 0)
    folded_ref[me] = fold_ref[me]

    def receive(source):
        a = source // (halves * quads) * quads + source % quads
        j = 2 * a + source // quads % halves
        made = through(folded_ref[source], mat_r_ref, jnp.where(j == 0, 1, 0))
        work_ref[j, 0, :TILE, :], work_ref[j, 1, :TILE, :] = made[:, :TILE], made[:, TILE:]

    receive(me)

    def arrive(k, carry):
        for c in range(pieces):
            arriving(c, k).wait_recv()
        receive((me - k + n) % n)
        return carry

    lax.fori_loop(1, n, arrive, 0)

    def gradient(k, carry):
        spot = pl.ds(pl.multiple_of(k * 8, 8), 8)
        for e in range(2):
            x = []
            for v in range(depth):
                j = 2 * v + e
                x.append(times((work_ref[j, 0, spot, :], work_ref[j, 1, spot, :]), turn_r_ref[j, 0:1, :], turn_r_ref[j, 1:2, :]))
            for b, value in enumerate(sixteen(x)):
                if e == 0:
                    real_ref[b] = value[0]
                    continue
                real = turn(value, 2 * math.pi * b / n)[0] if b else value[0]
                for c, total in ((b, real_ref[b] + real), (b + depth, real_ref[b] - real)):
                    lanes = slice(c * TILE, (c + 1) * TILE)
                    out_ref[spot, lanes] = total * scale
        return carry

    lax.fori_loop(0, TILE // 8, gradient, 0)

    def sent(k, carry):
        for c in range(pieces):
            sending(c, k).wait_send()
        return carry

    lax.fori_loop(1, n, sent, 0)


def row_weights(n, size):
    alpha = np.arange(TILE)
    i = np.arange(size // n // 2)
    turns = np.stack(trig(np.arange(n)[:, None] * alpha[None, :], size), axis=1).astype(np.float32)
    c, s = trig(alpha[:, None] * i[None, :], size // n)
    there, back = [], []
    for special in range(2):
        real = np.concatenate([c + s, c - s], axis=1)
        imag = np.concatenate([c - s, -c - s], axis=1)
        from_real = np.concatenate([c + s, c - s], axis=1)
        from_imag = np.concatenate([s - c, s + c], axis=1)
        if special:
            lane = len(i)
            real[:, lane] = from_real[:, lane] = 1.0 - 2.0 * (alpha % 2)
            imag[:, lane] = from_imag[:, lane] = 0.0
        for target, matrix in ((there, np.concatenate([real, imag], axis=0)), (back, np.concatenate([from_real.T, from_imag.T], axis=1))):
            target.append(np.concatenate(split_table(matrix), axis=0))
    return turns, np.stack(there), np.stack(back)


def column_tables(n, size):
    w = np.arange(size // n)
    t = np.arange(TILE)
    u = np.arange(n)
    r = 2 * np.arange(2 * TILE) + 1
    side = TILE // 2

    def lanes(c, s):
        out = np.zeros((c.shape[0], TILE))
        out[:, :n], out[:, side : side + n] = c, s
        return out.astype(np.float32)

    def matrix(x):
        return np.concatenate(split_table(x), axis=0)

    c, s = trig(t[:, None] * u[None, :], size)
    turns = lanes(c, -s)
    c, s = trig(w[:, None] * t[None, :], size // n)
    mat_h = matrix(np.concatenate([c, s], axis=1))
    mat_f = matrix(np.concatenate([c.T, -s.T], axis=0))
    c, s = trig(r[:, None] * u[None, :], 2 * G)
    turns_g = lanes(c, s)
    c, s = trig((w[:, None] * n + G // 4) * r[None, :], 2 * G)
    mat_g = matrix(np.concatenate([s, c], axis=1))
    c, s = trig(w * n + G // 4, 2 * G)
    slope = np.stack([s, c]) * (2.0 * G)
    slope = np.broadcast_to(slope[:, :, None], slope.shape + (TILE,)).astype(np.float32)
    c, s = trig(u, 2 * G)
    bend = np.stack([c, s], axis=1).astype(np.float32)
    return turns, mat_h, mat_f, turns_g, mat_g, slope, bend


def column_call(kernel, smems, args, out_shape, scratch, name, away=(), **params):
    smem = pl.BlockSpec(memory_space=pltpu.SMEM)
    vmem = pl.BlockSpec(memory_space=pltpu.VMEM)
    anywhere = pl.BlockSpec(memory_space=pltpu.HBM)
    return pl.pallas_call(
        kernel,
        out_shape=jax.ShapeDtypeStruct(out_shape, jnp.float32),
        in_specs=[smem] * len(smems) + [anywhere if k in away else vmem for k in range(len(args))],
        out_specs=vmem,
        scratch_shapes=scratch,
        compiler_params=pltpu.CompilerParams(**{"vmem_limit_bytes": 24 << 20, **params}),
        cost_estimate=pl.CostEstimate(flops=10**10, bytes_accessed=16 * 2**20, transcendentals=0),
        name=name,
    )(*smems, *args)


def shared(residual, position, owner, tile_local, xi, amplitude):
    n = lax.axis_size(parts)
    n_base = lax.axis_size("base")
    n_slab = lax.axis_size("half") * lax.axis_size("quad")
    quads = lax.axis_size("quad")
    base, parity, quad = (lax.axis_index(axis) for axis in parts)
    place = 2 * (base * quads + quad) + parity
    rows, size = xi.shape
    depth = size // n
    half = depth // 2
    tiles = G // TILE

    row_turns, there, back_again = (jnp.asarray(x) for x in row_weights(n, size))
    block = (n, rows, depth)
    work = pltpu.VMEM((n, 2, rows, depth), jnp.float32)
    blocks = residual.shape[0]
    room = 2 * n_base * (2 * blocks // n)
    sent = pack(owner, tile_local, residual, position, n_base, n_slab, room)
    got, spectrum = exchange(sent, n_slab, xi, amplitude, row_turns, there)
    field = lax.all_to_all(spectrum, parts, split_axis=0, concat_axis=0, tiled=True)

    sources = n_slab * n_base
    codes = got[:, :, room, 0, :].reshape(sources, TILE).astype(jnp.int32)
    info = jnp.stack([group_of(base, quad)[1], parity]).astype(jnp.int32)

    turns, firsts, undos, weights = grid_row_weights(n, size)
    halves = grid_rows_two(
        room,
        info,
        codes,
        jnp.asarray(firsts),
        got.reshape(sources * (room + 1), 4, TILE),
        jnp.asarray(turns),
        jnp.asarray(undos),
        jnp.asarray(weights),
    )
    whole = lax.all_to_all(halves, ("base", "quad"), split_axis=0, concat_axis=0, tiled=True)

    turns, mat_h, mat_f, turns_g, mat_g, slope, bend = (jnp.asarray(x) for x in column_tables(n, size))
    me = jnp.reshape(place, (1,)).astype(jnp.int32)
    sky = column_call(
        functools.partial(field_kernel, 1.0 / size),
        [me, bend],
        [field, turns, mat_h, slope],
        block,
        [work],
        "field",
    )
    pieces = 4
    dma = pltpu.SemaphoreType.DMA
    return amplitude * column_call(
        functools.partial(image_kernel, 1.0 / size),
        [],
        [whole, sky, turns_g, mat_g, mat_f, turns, row_turns, back_again],
        (rows, size),
        [
            pltpu.VMEM((n, 2, 2 * rows, depth), jnp.float32), pltpu.VMEM((n // 2, 2, 8, depth), jnp.float32),
            pltpu.VMEM(block, jnp.float32), pltpu.VMEM(block, jnp.float32), pltpu.VMEM(block, jnp.float32),
            pltpu.VMEM((n // 2, 8, depth), jnp.float32), dma, dma((pieces, n)), dma((pieces, n)),
        ],
        "image",
        away=(1,),
        vmem_limit_bytes=36 << 20,
        collective_id=1,
        has_side_effects=True,
    )


def solution(mesh):
    n_base, n_slab = mesh.shape["base"], mesh.shape["slab"]
    body, axes = general, both
    if n_base == 4 and n_slab == 2 * n_base and 2 * n_base * n_slab == G // TILE:
        body, axes = shared, parts
        mesh = jax.sharding.Mesh(mesh.devices.reshape(n_base, 2, n_slab // 2), parts)
    placed = (
        P(axes, None, None),
        P(axes, None, None),
        P(axes, None),
        P(axes),
        P(axes, None),
        P(axes, None),
    )
    return jax.shard_map(body, mesh=mesh, in_specs=placed, out_specs=P(axes, None), check_vma=False)
```

```python
import functools
import math

import jax
import jax.numpy as jnp
import numpy as np
from jax import lax
from jax.experimental import pallas as pl
from jax.experimental.pallas import tpu as pltpu
from jax.sharding import PartitionSpec as P

G = 8192
TILE = 128
both = ("base", "slab")
fine = lax.Precision.HIGHEST


def trig(product, modulus):
    angle = (product % modulus).astype(np.float64) * (2.0 * np.pi / modulus)
    return np.cos(angle), np.sin(angle)


def column_table(n, size):
    depth = size // n
    half = depth // 2
    i = np.arange(half)[None, :]
    j = np.arange(n)[:, None]
    low = n * i + j
    high = (-low) % size
    high[0, 0] = size // 2
    return np.concatenate([low, high], axis=1)


def row_tables(n, size):
    depth = size // n
    cols = column_table(n, size)
    oc, osn = trig(np.arange(n)[:, None] * np.arange(n)[None, :], n)
    outer = np.stack([oc, osn], axis=1)
    prod = np.arange(depth)[None, :, None] * cols[:, None, :]
    c, s = trig(prod, size)
    sign = np.where(np.arange(depth) < depth // 2, 1.0, -1.0)[None, None, :]
    inner = np.stack([c + s, sign * (c - s)], axis=1)
    return outer.astype(np.float32), inner.astype(np.float32)


def grid_row_tables(n, size):
    depth = G // n
    cols = column_table(n, size)
    half = cols.shape[1] // 2
    oc, osn = trig(np.arange(n)[:, None] * np.arange(n)[None, :], n)
    outer = np.stack([np.stack([oc, osn], 1), np.stack([-osn, oc], 1)], 0)
    low = cols[:, :half]
    high = cols[(-np.arange(n)) % n, half:]
    a = np.arange(depth)[None, :, None]
    out = []
    for part in (low, high):
        c, s = trig(a * (part[:, None, :] + G // 4), G)
        out.append(np.stack([np.concatenate([c, s], 2), np.concatenate([-s, c], 2)], 1))
    return outer.astype(np.float32), np.concatenate(out, axis=3).astype(np.float32)


def taps(cells, offsets):
    scaled = (cells - offsets) * 0.25
    kept = jnp.maximum(1.0 - scaled * scaled, 0.0)
    return kept * kept * kept


def split_three(x):
    high = x.astype(jnp.bfloat16)
    rest = x - high.astype(jnp.float32)
    middle = rest.astype(jnp.bfloat16)
    return high, middle, (rest - middle.astype(jnp.float32)).astype(jnp.bfloat16)


def grid_kernel(rows, info_ref, list_ref, data_ref, out_ref):
    count = info_ref[0]
    first = info_ref[1].astype(jnp.float32)
    out_ref[...] = jnp.zeros_like(out_ref)
    row_cells = lax.broadcasted_iota(jnp.int32, (rows, TILE), 0).astype(jnp.float32) + first
    col_cells = lax.broadcasted_iota(jnp.int32, (TILE, TILE), 0).astype(jnp.float32)

    def step(k, carry):
        packed = list_ref[k]
        index = packed // 256
        col = (packed // 2) % 128
        flip = (packed % 2).astype(jnp.float32)
        sign = 1.0 - 2.0 * flip
        start = 128.0 * flip
        block = data_ref[index]
        value = block[0:2, :]
        place = block[2:4, :]
        row_taps = taps(row_cells * sign + start, place[0:1, :])
        col_taps = taps(col_cells * sign + start, place[1:2, :])
        weighted = jnp.concatenate(
            [col_taps * value[0:1, :], col_taps * (value[1:2, :] * sign)], axis=0
        )
        rh, rm, rl = split_three(row_taps)
        wh, wm, wl = split_three(weighted)
        left = jnp.concatenate([rh, rh, rh, rm, rm, rl], axis=1)
        right = jnp.concatenate([wh, wm, wl, wh, wm, wh], axis=1)
        sub = lax.dot_general(
            left, right, (((1,), (1,)), ((), ())), preferred_element_type=jnp.float32
        )
        out_ref[0, col] += sub[:, :TILE]
        out_ref[1, col] += sub[:, TILE:]
        return carry

    lax.fori_loop(0, count, step, 0)


def grid_rows(info, table, gathered, rows):
    tiles = G // TILE
    smem = pl.BlockSpec(memory_space=pltpu.SMEM)
    vmem = pl.BlockSpec(memory_space=pltpu.VMEM)
    return pl.pallas_call(
        functools.partial(grid_kernel, rows),
        out_shape=jax.ShapeDtypeStruct((2, tiles, rows, TILE), jnp.float32),
        in_specs=[smem, smem, vmem],
        out_specs=vmem,
        compiler_params=pltpu.CompilerParams(vmem_limit_bytes=56 * 1024 * 1024),
        cost_estimate=pl.CostEstimate(
            flops=2 * 10**10, bytes_accessed=16 * 2**20, transcendentals=0
        ),
        name="grid_rows",
    )(info, table, gathered)


def einsum(form, *args, precision=lax.Precision.HIGH):
    return jnp.einsum(form, *args, precision=precision, preferred_element_type=jnp.float32)


def general(residual, position, owner, tile_local, xi, amplitude):
    n = lax.axis_size(both)
    n_base = lax.axis_size("base")
    n_slab = lax.axis_size("slab")
    me = lax.axis_index(both)
    rows, size = xi.shape
    depth = size // n
    half = depth // 2
    tiles = G // TILE

    region_rows = G // n_slab // TILE
    region_cols = G // n_base // TILE
    target = owner[:, 0]
    tile_row = (target % n_slab) * region_rows + tile_local // region_cols
    tile_col = (target // n_slab) * region_cols + tile_local % region_cols
    flip = tile_row >= tiles // 2
    tile_row = jnp.where(flip, tiles - 1 - tile_row, tile_row)
    tile_col = jnp.where(flip, tiles - 1 - tile_col, tile_col)
    code = tile_row * 256 + tile_col * 2 + flip.astype(jnp.int32)
    codes = lax.all_gather(code, both, axis=0, tiled=True)
    payload = jnp.concatenate([residual, position], axis=1)
    codes, payload = lax.optimization_barrier((codes, payload))
    gathered = lax.all_gather(payload, both, axis=0, tiled=True)
    blocks = codes.shape[0]
    grid_depth = G // 2 // n
    first_row = me * grid_depth
    mine = (codes // 256 == first_row // TILE).astype(jnp.int32)
    rank = jnp.where(mine == 1, jnp.cumsum(mine) - 1, -1)
    packed = lax.broadcasted_iota(jnp.int32, (blocks,), 0) * 256 + codes % 256
    spots = lax.broadcasted_iota(jnp.int32, (blocks, blocks), 0)
    table = jnp.sum(jnp.where(spots == rank[None, :], packed[None, :], 0), axis=1)
    info = jnp.stack([jnp.sum(mine), first_row % TILE]).astype(jnp.int32)

    outer, inner = row_tables(n, size)
    spectrum = (amplitude * xi).reshape(rows, n, depth)
    mid = einsum("rba,bqc->qcra", spectrum, outer)
    sent = einsum("cra,cae->cre", mid[0], inner[:, 0]) + einsum("cra,cae->cre", mid[1], inner[:, 1])
    sent, gathered = lax.optimization_barrier((sent, gathered))
    field = lax.all_to_all(sent, both, split_axis=0, concat_axis=0, tiled=True)
    field = field.reshape(size, depth)
    lane = lax.broadcasted_iota(jnp.int32, (1, depth), 1)
    still = (me == 0) & (lane % half == 0)

    def mirror(x):
        return jnp.where(still, x, jnp.roll(x, half, axis=-1))

    c_len = 128
    d_len = size // c_len
    bc, bs = (x.astype(np.float32) for x in trig(np.arange(c_len)[:, None] * np.arange(c_len)[None, :], c_len))
    shape = (c_len, d_len, depth)
    n0 = c_len * np.arange(d_len)[None, :] + np.arange(c_len)[:, None]
    ic, isn = (x.astype(np.float32) for x in trig(n0[:, :, None] * np.arange(d_len)[None, None, :], size))
    pair = jnp.stack([field.reshape(shape), mirror(field).reshape(shape)])
    first = np.stack([np.stack([bc, bs], 1), np.stack([bs, -bc], 1)], 0)
    turned = einsum("qbal,qbsc->csal", pair, first)
    second = np.stack([ic, -isn], axis=2)
    power = einsum("csal,cdsa->cdl", turned, second)
    sky = jnp.exp(power / size)

    grid = grid_rows(info, table, gathered, grid_depth)
    outer_g, inner_g = grid_row_tables(n, size)
    parts = tiles // n if tiles >= n else 1
    inner_len = G // n
    if inner_len >= TILE:
        view = grid.reshape(2, n, inner_len // TILE, grid_depth, TILE)
    else:
        flat = grid.transpose(0, 2, 1, 3).reshape(2, grid_depth, n, inner_len)
        view = flat.transpose(0, 2, 1, 3)[:, :, None]
        parts = 1
    lanes = view.shape[-1]
    stage = einsum("qbpra,qbsc->cspra", view, outer_g, precision=fine)
    inner_g = inner_g.reshape(n, 2, parts, lanes, 2 * depth)
    halves = einsum("cspra,cspae->cre", stage, inner_g, precision=fine)
    high = halves[:, :, depth:]
    high = jnp.concatenate([high[:1], jnp.flip(high[1:], axis=0)], axis=0)
    halves = jnp.concatenate([halves[:, :, :depth], high], axis=2)
    got = lax.all_to_all(halves, both, split_axis=0, concat_axis=0, tiled=True)
    got = got.reshape(size, 2 * depth)
    real = jnp.concatenate([got[:, :half], got[:, depth : depth + half]], axis=1)
    imag = jnp.concatenate([got[:, half:depth], got[:, depth + half :]], axis=1)
    wide = G // c_len
    deep = size // wide
    gc, gs = (x.astype(np.float32) for x in trig(np.arange(deep)[:, None] * np.arange(c_len)[None, :], c_len))
    first_g = np.stack([np.stack([gc, gs], 1), np.stack([-gs, gc], 1)], 0)
    whole = jnp.stack([real.reshape(deep, wide, depth), imag.reshape(deep, wide, depth)])
    turned_g = einsum("qbal,qbsc->csal", whole, first_g, precision=fine)
    ac, asn = trig((n0 + G // 4)[:, :, None] * np.arange(wide)[None, None, :], G)
    second_g = (np.stack([ac, -asn], axis=2) / G).astype(np.float32)
    back = einsum("csal,cdsa->cdl", turned_g, second_g, precision=fine)

    z = sky * back
    pz = einsum("cdl,cda->cal", z, ic)
    qz = einsum("cdl,cda->cal", z, isn)
    joined = jnp.stack([pz + mirror(qz), mirror(pz) - qz])
    fold = einsum("qcal,qcb->bal", joined, np.stack([bc, bs]))
    folded = lax.all_to_all(
        fold.reshape(n, rows, depth), both, split_axis=0, concat_axis=0, tiled=True
    )
    ends = einsum("jre,jqae->qjra", folded, inner)
    final = einsum("qjra,bqj->rba", ends, outer)
    return amplitude * final.reshape(rows, size) / size


MESH = pl.DeviceIdType.MESH
parts = ("base", "half", "quad")
LANES = 6


def two_parts(x):
    high = x.astype(jnp.bfloat16)
    return high, (x - high.astype(jnp.float32)).astype(jnp.bfloat16)


def through(x, weight_ref, which):
    rows, depth = x.shape
    high, low = two_parts(x)
    made = jnp.dot(jnp.concatenate([high, low], axis=0), weight_ref[which, :depth], preferred_element_type=jnp.float32)
    return made[:rows] + made[rows:] + jnp.dot(high, weight_ref[which, depth:], preferred_element_type=jnp.float32)


def times(x, c, s):
    return x[0] * c - x[1] * s, x[0] * s + x[1] * c


def turn(x, angle):
    c, s = math.cos(angle), math.sin(angle)
    return times(x, c, s)


def add(x, y):
    return x[0] + y[0], x[1] + y[1]


def sub(x, y):
    return x[0] - y[0], x[1] - y[1]


def four(x):
    s0, d0, s1, d1 = add(x[0], x[2]), sub(x[0], x[2]), add(x[1], x[3]), sub(x[1], x[3])
    i1 = (-d1[1], d1[0])
    return [add(s0, s1), add(d0, i1), sub(s0, s1), sub(d0, i1)]


def sixteen(x):
    rows = []
    for b0 in range(4):
        y = four([x[4 * b1 + b0] for b1 in range(4)])
        rows.append([y[a0] if a0 * b0 == 0 else turn(y[a0], 2 * math.pi * a0 * b0 / 16) for a0 in range(4)])
    out = [None] * 16
    for a0 in range(4):
        y = four([rows[b0][a0] for b0 in range(4)])
        for a1 in range(4):
            out[a0 + 4 * a1] = y[a1]
    return out


def seat(j, quads):
    a = j // 2
    return a // quads * (2 * quads) + j % 2 * quads + a % quads


def transform_rows(quads, xi_ref, amplitude_ref, turn_ref, mat_ref, out_ref, work_ref):
    n = out_ref.shape[0]

    def outer(k, carry):
        spot = pl.ds(pl.multiple_of(k * 8, 8), 8)
        for e in range(2):
            x = []
            for b in range(n // 2):
                first, second = (
                    xi_ref[spot, c * TILE : (c + 1) * TILE] * amplitude_ref[spot, c * TILE : (c + 1) * TILE]
                    for c in (b, b + n // 2)
                )
                value = first - second if e else first + second
                if e * b:
                    angle = 2 * math.pi * b / n
                    x.append((value * math.cos(angle), value * math.sin(angle)))
                else:
                    x.append((value, jnp.zeros_like(value)))
            for v, value in enumerate(sixteen(x)):
                j = 2 * v + e
                work_ref[j, 0, spot, :], work_ref[j, 1, spot, :] = times(value, turn_ref[j, 0:1, :], turn_ref[j, 1:2, :])
        return carry

    lax.fori_loop(0, xi_ref.shape[0] // 8, outer, 0)
    rows = xi_ref.shape[0]

    def left(entries):
        return jnp.concatenate([jnp.concatenate([work_ref[j, 0], work_ref[j, 1]], axis=1) for j in entries], axis=0)

    def inner(k, carry):
        entries = [4 * k + q for q in range(4)]
        made = through(left(entries), mat_ref, 0)
        for q, j in enumerate(entries):
            out_ref[seat(j, quads)] = made[q * rows : (q + 1) * rows]
        return carry

    lax.fori_loop(0, n // 4, inner, 0)
    out_ref[0] = through(left([0]), mat_ref, 1)


def seats(base, quad):
    return base // 2, base % 2, quad // 2, quad % 2


def group_of(base, quad):
    y, x, low, core = seats(base, quad)
    return 2 * x + low, 2 * y + core


def exchange_kernel(send_ref, xi_ref, amplitude_ref, turn_ref, mat_ref, out_ref, spectrum_ref, work_ref, made_ref, rows_ref, rows_sem, bsend, brecv, zsend, zrecv, ysend, yrecv, csend, crecv, lsem):
    nb = send_ref.shape[0]
    quads = lax.axis_size("quad")
    half = lax.axis_index("half")
    y, x, low, core = seats(lax.axis_index("base"), lax.axis_index("quad"))
    group = 2 * x + low

    def at(y, group, half, core):
        return (2 * y + group // 2, half, group % 2 * 2 + core)

    def block(y, half, core, k):
        return out_ref.at[(2 * y + half) * 2 + core, (group - k + nb) % nb]

    def copy(part, here, there, device):
        return pltpu.make_async_remote_copy(
            src_ref=part, dst_ref=part, send_sem=here, recv_sem=there, device_id=device, device_id_type=MESH
        )

    def moved(target, source, k):
        return pltpu.make_async_remote_copy(
            src_ref=send_ref.at[target],
            dst_ref=out_ref.at[(2 * y + half) * 2 + core, source],
            send_sem=bsend.at[k],
            recv_sem=brecv.at[k],
            device_id=at(y, target, half, core),
            device_id_type=MESH,
        )

    far, beside, partner = at(y, group, 1 - half, core), at(1 - y, group, half, core), at(y, group, half, 1 - core)

    def along_z(own, k):
        return copy(block(y, half if own else 1 - half, core, k), zsend.at[k], zrecv.at[k], far)

    def along_y(own, kind, k):
        place = half if kind == 0 else 1 - half
        return copy(block(y if own else 1 - y, place, core, k), ysend.at[kind, k], yrecv.at[kind, k], beside)

    def over(own, kind, k):
        row = y if kind < 2 else 1 - y
        place = half if kind % 2 == 0 else 1 - half
        return copy(block(row, place, core if own else 1 - core, k), csend.at[kind, k], crecv.at[kind, k], partner)

    fetches = [
        pltpu.make_async_copy(source, rows_ref.at[k], rows_sem.at[k]) for k, source in enumerate((xi_ref, amplitude_ref))
    ]
    ready = pltpu.make_async_copy(made_ref, spectrum_ref, rows_sem.at[2])
    for fetch in fetches:
        fetch.start()
    barrier = pltpu.get_barrier_semaphore()
    peers = [at(y, (group + k) % nb, half, core) for k in range(1, nb)] + [far, beside, partner]
    for peer in peers:
        pl.semaphore_signal(barrier, inc=1, device_id=peer, device_id_type=MESH)
    pl.semaphore_wait(barrier, len(peers))

    own = pltpu.make_async_copy(send_ref.at[group], block(y, half, core, 0), lsem)
    own.start()
    for k in range(1, nb):
        moved((group + k) % nb, group, k).start()
    for k in range(nb):
        if k == 0:
            own.wait()
        else:
            moved((group - k + nb) % nb, (group - k + nb) % nb, k).wait_recv()
        along_z(True, k).start()
        along_y(True, 0, k).start()
        over(True, 0, k).start()
        if k == 0:
            for fetch in fetches:
                fetch.wait()
            transform_rows(quads, rows_ref.at[0], rows_ref.at[1], turn_ref, mat_ref, made_ref, work_ref)
            ready.start()
    for k in range(nb):
        along_z(False, k).wait_recv()
        along_y(True, 1, k).start()
        over(True, 1, k).start()
    for kind in range(2):
        for k in range(nb):
            along_y(False, kind, k).wait_recv()
            over(True, 2 + kind, k).start()
    ready.wait()
    for kind in range(4):
        for k in range(nb):
            over(False, kind, k).wait_recv()
    for k in range(nb):
        if k:
            moved((group + k) % nb, group, k).wait_send()
        along_z(True, k).wait_send()
        for kind in range(2):
            along_y(True, kind, k).wait_send()
        for kind in range(4):
            over(True, kind, k).wait_send()


def pack_kernel(ns, tiles, room, owner_ref, local_ref, residual_ref, position_ref, out_ref):
    blocks = residual_ref.shape[0]
    nb = out_ref.shape[0]
    across = lax.broadcasted_iota(jnp.int32, (blocks, blocks), 1)
    down = lax.broadcasted_iota(jnp.int32, (blocks, blocks), 0)

    def column(row):
        return jnp.sum(jnp.where(across == down, row, 0.0), axis=1, keepdims=True)

    def divided(x, d):
        whole = jnp.floor((x + 0.5) * (1.0 / d))
        return whole, x - whole * d

    local = local_ref[...].astype(jnp.float32)
    target = owner_ref[...].astype(jnp.float32)
    region_col, region_row = divided(target, ns)
    tile_row, tile_col = divided(local, tiles // nb)
    tile_row = tile_row + region_row * (tiles // ns)
    tile_col = tile_col + region_col * (tiles // nb)
    flip = jnp.where(tile_row >= tiles // 2, 1.0, 0.0)
    tile_row = jnp.where(flip > 0.5, tiles - 1 - tile_row, tile_row)
    tile_col = jnp.where(flip > 0.5, tiles - 1 - tile_col, tile_col)
    line, within = divided(tile_row, ns)
    key = divided(tile_row, 2)[0]
    code = divided(within, 2)[1] * tiles + tile_col
    keys = ns // 2
    line_down, key_down, flip_down = column(line), column(key), column(flip)
    before = (line_down == line) & ((key_down < key) | ((key_down == key) & (down < across)))
    slot = line * room + jnp.sum(jnp.where(before, 1.0, 0.0), axis=0, keepdims=True)
    slots = lax.broadcasted_iota(jnp.int32, (nb * room, blocks), 0).astype(jnp.float32)
    chosen = jnp.where(slots == slot, 1.0, 0.0).astype(jnp.bfloat16)
    sides = [residual_ref[:, 0, :], residual_ref[:, 1, :] * (1.0 - 2.0 * flip_down)]
    for k in range(2):
        place = position_ref[:, k, :]
        sides.append(jnp.where(flip_down > 0.5, TILE - place, place))
    pieces = split_three(jnp.concatenate(sides, axis=1))
    moved = jnp.dot(
        jnp.concatenate([chosen] * 3, axis=1), jnp.concatenate(pieces, axis=0), preferred_element_type=jnp.float32
    )
    codes = 0.0
    for part in two_parts(jnp.broadcast_to(code + 1.0, (8, blocks))):
        codes = codes + lax.dot_general(part, chosen, (((1,), (1,)), ((), ())), preferred_element_type=jnp.float32)
    codes = codes - 1.0
    lanes = lax.broadcasted_iota(jnp.int32, (1, blocks), 1)
    shift = (across - room).astype(jnp.float32)
    per = blocks // room
    for k in range(nb):
        for c in range(4):
            out_ref[k, :room, c, :] = moved[k * room : (k + 1) * room, c * TILE : (c + 1) * TILE]
        start = k // per * blocks
        own = codes[:, start : start + blocks]
        if k % per:
            own = pltpu.roll(own, blocks - k % per * room, 1)
        earlier = (line_down == k) & (key_down - keys * k < shift)
        starts = jnp.sum(jnp.where(earlier, 1.0, 0.0), axis=0, keepdims=True)
        out_ref[k, room] = jnp.broadcast_to(jnp.where(lanes < room, own[0:1, :], starts), (4, TILE))


def pack(owner, local, residual, position, nb, ns, room):
    vmem = pl.BlockSpec(memory_space=pltpu.VMEM)
    return pl.pallas_call(
        functools.partial(pack_kernel, ns, G // TILE, room),
        out_shape=jax.ShapeDtypeStruct((nb, room + 1, 4, TILE), jnp.float32),
        in_specs=[vmem] * 4,
        out_specs=vmem,
        compiler_params=pltpu.CompilerParams(vmem_limit_bytes=60 << 20),
        name="pack",
    )(owner.reshape(1, -1), local.reshape(1, -1), residual, position)


def exchange(sent, ns, xi, amplitude, turns, mats):
    nb = sent.shape[0]
    rows, n = xi.shape[0], turns.shape[0]
    dma = pltpu.SemaphoreType.DMA
    vmem = pl.BlockSpec(memory_space=pltpu.VMEM)
    hbm = pl.BlockSpec(memory_space=pltpu.HBM)
    return pl.pallas_call(
        exchange_kernel,
        out_shape=(
            jax.ShapeDtypeStruct((ns,) + sent.shape, jnp.float32),
            jax.ShapeDtypeStruct((n, rows, TILE), jnp.float32),
        ),
        in_specs=[vmem, hbm, hbm, vmem, vmem],
        out_specs=(hbm, hbm),
        scratch_shapes=[
            pltpu.VMEM((n, 2, rows, TILE), jnp.float32),
            pltpu.VMEM((n, rows, TILE), jnp.float32),
            pltpu.VMEM((2,) + xi.shape, jnp.float32), dma((3,)),
            dma((nb,)), dma((nb,)), dma((nb,)), dma((nb,)), dma((2, nb)), dma((2, nb)), dma((4, nb)), dma((4, nb)), dma,
        ],
        compiler_params=pltpu.CompilerParams(collective_id=0, has_side_effects=True, vmem_limit_bytes=60 << 20),
        cost_estimate=pl.CostEstimate(flops=3 * 10**10, bytes_accessed=16 * 2**20, transcendentals=0),
        name="exchange",
    )(sent, xi, amplitude, turns, mats)


def grid_kernel_two(room, codes_ref, first_ref, data_hbm_ref, turn_ref, undo_ref, weight_hbm_ref, away_ref, grid_ref, left_ref, right_ref, out_ref, data_ref, weight_ref, list_ref, sems):
    quad = group_of(lax.axis_index("base"), lax.axis_index("quad"))[1]
    parity = lax.axis_index("half")
    data = pltpu.make_async_copy(data_hbm_ref, data_ref, sems.at[out_ref.shape[0]])
    weight = pltpu.make_async_copy(weight_hbm_ref, weight_ref, sems.at[out_ref.shape[0] + 1])
    data.start()
    weight.start()
    grid_ref[...] = jnp.zeros_like(grid_ref)
    half = grid_ref.shape[1]
    group = 16
    cells = lax.broadcasted_iota(jnp.int32, (group + 8, TILE), 0).astype(jnp.float32) * 0.25
    nothing = jnp.zeros((group, TILE), jnp.bfloat16)

    def bump(offsets):
        d = cells - offsets
        kept = jnp.maximum(1.0 - d * d, 0.0)
        return kept * kept * kept

    def window(offsets):
        start = jnp.floor((offsets - 4.0) * (1.0 / group))
        offsets = (offsets - start * group) * 0.25
        return bump(offsets) - bump(offsets - 0.25), jnp.broadcast_to(start, (group, TILE)).astype(jnp.bfloat16)

    def spread(compact, start):
        padded = jnp.concatenate([compact, jnp.zeros((8, TILE), jnp.float32)], axis=0)
        out = []
        for part in two_parts(padded):
            first, second = part[:group], part[group:]
            pieces = []
            for g in range(TILE // group):
                piece = jnp.where(start == g - 1, second, nothing) if g else nothing
                pieces.append(jnp.where(start == g, first, piece))
            out.append(jnp.concatenate(pieces, axis=0))
        return out

    lanes = left_ref.shape[0]

    def place(k):
        packed = list_ref[k]
        return packed & (2 * half - 1), lax.shift_right_logical(packed, half.bit_length())

    def prepare(k, lane, count):
        col, rest = place(k)
        odd = jnp.where(col >= half, parity, 0)
        sign = jnp.where(k < count, 1 - 2 * odd, 0).astype(jnp.float32)
        block = data_ref[rest // 2]
        value = block[0:2, :] * sign
        row_taps, row_start = window(block[2:3, :])
        col_taps, col_start = window(block[3:4, :])
        rows_split = spread(row_taps, row_start)
        real = spread(col_taps * value[0:1, :], col_start)
        imag = spread(col_taps * value[1:2, :], col_start)
        for q in range(2):
            left_ref[lane, :, q * TILE : (q + 1) * TILE] = rows_split[q]
            right_ref[lane, :TILE, q * TILE : (q + 1) * TILE] = real[q]
            right_ref[lane, TILE:, q * TILE : (q + 1) * TILE] = imag[q]

    def product(lane):
        rh, rl = left_ref[lane, :, :TILE], left_ref[lane, :, TILE:]
        wh, wl = right_ref[lane, :, :TILE], right_ref[lane, :, TILE:]
        left = jnp.concatenate([rh, rh, rl], axis=1)
        right = jnp.concatenate([wh, wl, wh], axis=1)
        return lax.dot_general(left, right, (((1,), (1,)), ((), ())), preferred_element_type=jnp.float32)

    def step(k, carry):
        made = [product(lane) for lane in range(lanes)]
        for lane in range(lanes):
            prepare((k + 1) * lanes + lane, lane, count)
        for lane in range(lanes):
            col, rest = place(k * lanes + lane)
            col = jnp.where(col >= half, col - half, col)
            spot = pl.ds(pl.multiple_of((rest % 2) * TILE, TILE), TILE)
            grid_ref[0, col, spot, :] += made[lane][:, :TILE]
            grid_ref[1, col, spot, :] += made[lane][:, TILE:]
        return carry

    per = 4 * half

    def gather(source, filled):
        start = codes_ref[source, room + quad]
        stop = codes_ref[source, room + quad + 1]

        shift = filled - start
        first = source * ((room + 1) * per)

        def entry(i, carry):
            list_ref[shift + i] = first + i * per + codes_ref[source, i]
            return carry

        lax.fori_loop(start, stop, entry, 0)
        return filled + stop - start

    count = lax.fori_loop(0, codes_ref.shape[0], gather, 0)
    for lane in range(2 * lanes):
        list_ref[count + lane] = 0
    data.wait()
    for lane in range(lanes):
        prepare(lane, lane, count)
    lax.fori_loop(0, (count + lanes - 1) // lanes, step, 0)

    depth = half // 2
    rows = grid_ref.shape[2]

    def outer(k, carry):
        spot = pl.ds(pl.multiple_of(k * 8, 8), 8)
        for side in range(2):
            x = []
            for b in range(depth):
                value = grid_ref[0, 2 * b + side, spot, :], grid_ref[1, 2 * b + side, spot, :]
                x.append(times(value, first_ref[parity, b, 0], first_ref[parity, b, 1]))
            for a, value in enumerate(sixteen(x)):
                c = turn_ref[parity, a, side : side + 1, :]
                s = turn_ref[parity, a, 2 + side : 3 + side, :]
                value = times(value, c, s)
                grid_ref[0, 2 * a + side, spot, :] = value[0]
                grid_ref[1, 2 * a + side, spot, :] = value[1]
        return carry

    lax.fori_loop(0, rows // 8, outer, 0)

    def inner(a, carry):
        mirrored = depth - parity - a
        mirrored = jnp.where(mirrored == depth, 0, mirrored)
        which = jnp.where((a == 0) & (parity == 0), 1, 0)
        for part in range(1):
            spot = pl.ds(0, rows)
            x = jnp.concatenate([grid_ref[q, 2 * a + side, spot, :] for q in range(2) for side in range(2)], axis=1)
            made = through(x, weight_ref, which)
            mid = TILE // 2
            made = times((made[:, :TILE], made[:, TILE:]), undo_ref[parity, a, 0:1, :], undo_ref[parity, a, 1:2, :])
            for q in range(2):
                out_ref[a, spot, q * TILE : q * TILE + mid] = made[q][:, :mid]
                out_ref[mirrored, spot, q * TILE + mid : (q + 1) * TILE] = made[q][:, mid:]

        @pl.when(a >= depth // 2)
        def _():
            leave(a).start()
            leave(jnp.where((parity == 0) & (a == depth // 2), 0, mirrored)).start()

        return carry

    def leave(a):
        return pltpu.make_async_copy(out_ref.at[a], away_ref.at[a], sems.at[a])

    weight.wait()
    lax.fori_loop(0, depth, inner, 0)
    for a in range(depth):
        leave(a).wait()


def split_table(x):
    high = x.astype(np.float32).astype(jnp.bfloat16)
    low = (x - high.astype(np.float64)).astype(np.float32).astype(jnp.bfloat16)
    return high, low


def undone(pixels):
    c, s = trig(pixels + G // 4, G)
    return 1.0 / (1.0 - (c - 1j * s))


def grid_row_weights(n, size):
    depth = n // 2
    span = G // 2 // depth
    half = size // n // 2
    alpha = np.arange(span)
    turns, firsts, undos = [], [], []
    for p in range(2):
        j = 2 * np.arange(depth) + p
        c, s = trig(j[:, None] * alpha[None, :], G)
        turns.append(np.concatenate([c.reshape(depth, 2, TILE), s.reshape(depth, 2, TILE)], axis=1))
        firsts.append(np.stack(trig(np.arange(depth) * p, n), axis=1))
        low = n * np.arange(half)[None, :] + j[:, None]
        high = size - n * np.arange(half)[None, :] - ((-j) % n)[:, None]
        if p == 0:
            low[0, 0], high[0, 0] = 0, size // 2
        undo = undone(np.concatenate([low, high], axis=1))
        undos.append(np.stack([undo.real, undo.imag], axis=1))
    weights = []
    i = np.arange(half)
    for special in range(2):
        low = n * i
        high = size - n * i - (0 if special else n)
        if special:
            high[0] = size // 2
        parts_re, parts_im = [], []
        for cols in (low, high):
            c, s = trig(alpha[:, None] * (cols[None, :] + G // 4), G)
            parts_re.append(np.concatenate([c, -s], axis=0))
            parts_im.append(np.concatenate([s, c], axis=0))
        w = np.concatenate(parts_re + parts_im, axis=1)
        weights.append(np.concatenate(split_table(w), axis=0))
    turns, firsts, undos = (np.stack(x).astype(np.float32) for x in (turns, firsts, undos))
    return turns, firsts, undos, np.stack(weights)


def grid_rows_two(room, codes, first, data, turns, undos, weights):
    depth = turns.shape[1]
    rows = 2 * TILE
    smem = pl.BlockSpec(memory_space=pltpu.SMEM)
    vmem = pl.BlockSpec(memory_space=pltpu.VMEM)
    hbm = pl.BlockSpec(memory_space=pltpu.HBM)
    return pl.pallas_call(
        functools.partial(grid_kernel_two, room),
        out_shape=jax.ShapeDtypeStruct((depth, rows, 2 * TILE), jnp.float32),
        in_specs=[smem, smem, hbm, vmem, vmem, hbm],
        out_specs=hbm,
        scratch_shapes=[
            pltpu.VMEM((2, 2 * depth, rows, TILE), jnp.float32),
            pltpu.VMEM((LANES, TILE, 2 * TILE), jnp.bfloat16),
            pltpu.VMEM((LANES, 2 * TILE, 2 * TILE), jnp.bfloat16),
            pltpu.VMEM((depth, rows, 2 * TILE), jnp.float32),
            pltpu.VMEM(data.shape, jnp.float32),
            pltpu.VMEM(weights.shape, jnp.bfloat16),
            pltpu.SMEM((codes.shape[0] * room + 2 * LANES,), jnp.int32),
            pltpu.SemaphoreType.DMA((depth + 2,)),
        ],
        compiler_params=pltpu.CompilerParams(vmem_limit_bytes=60 << 20),
        cost_estimate=pl.CostEstimate(flops=2 * 10**10, bytes_accessed=16 * 2**20, transcendentals=0),
        name="grid_rows_two",
    )(codes, first, data, turns, undos, weights)


def minus(x):
    return [(b, a) for a, b in sixteen([(b, a) for a, b in x])]


def pick(table, u):
    side = table.shape[1] // 2
    return table[:, u : u + 1], table[:, side + u : side + u + 1]


def mirrored(x, still):
    return jnp.where(still, x, pltpu.roll(x, x.shape[1] // 2, 1))


def still_lanes(place, rows):
    lane = lax.broadcasted_iota(jnp.int32, (rows, TILE), 1)
    return (lane % (TILE // 2) == 0) & (place == 0)


def product(mat_ref, x):
    rows = mat_ref.shape[0] // 2
    high, low = two_parts(x)
    made = jnp.dot(mat_ref[...], high, preferred_element_type=jnp.float32)
    return made[:rows] + made[rows:] + jnp.dot(mat_ref[:rows], low, preferred_element_type=jnp.float32)


def beside(work_ref, u):
    sides = [jnp.concatenate([work_ref[u + q, 0], work_ref[u + q, 1]], axis=0) for q in range(2)]
    return jnp.concatenate(sides, axis=1)


def field_kernel(scale, info_ref, bend_ref, field_ref, turn_ref, mat_ref, slope_ref, sky_ref, work_ref):
    still = still_lanes(info_ref[0], 8)
    n = field_ref.shape[0]

    def outer(k, carry):
        spot = pl.ds(pl.multiple_of(k * 8, 8), 8)
        table = turn_ref[spot, :]
        for e in range(2):
            x = []
            for d in range(n // 2):
                first, second = field_ref[d, spot, :], field_ref[d + n // 2, spot, :]
                value = first - second if e else first + second
                value = value, mirrored(value, still)
                x.append(turn(value, -2 * math.pi * d / n) if e * d else value)
            for v, value in enumerate(minus(x)):
                u = 2 * v + e
                work_ref[u, 0, spot, :], work_ref[u, 1, spot, :] = times(value, *pick(table, u))
        return carry

    lax.fori_loop(0, field_ref.shape[1] // 8, outer, 0)

    def inner(k, carry):
        for u in (4 * k, 4 * k + 2):
            made = jnp.exp(product(mat_ref, beside(work_ref, u)) * scale)
            for q in range(2):
                sine = slope_ref[0] * bend_ref[u + q, 0] + slope_ref[1] * bend_ref[u + q, 1]
                sky_ref[u + q] = made[:, q * TILE : (q + 1) * TILE] / sine
        return carry

    lax.fori_loop(0, n // 4, inner, 0)


def image_kernel(scale, whole_ref, sky_ref, turn_g_ref, mat_g_ref, mat_f_ref, turn_ref, turn_r_ref, mat_r_ref, out_ref, work_ref, half_ref, held_ref, fold_ref, folded_ref, real_ref, held_sem, send_sems, recv_sems):
    n = sky_ref.shape[0]
    quads = lax.axis_size("quad")
    halves = lax.axis_size("half")
    me = (lax.axis_index("base") * halves + lax.axis_index("half")) * quads + lax.axis_index("quad")
    place = 2 * (lax.axis_index("base") * quads + lax.axis_index("quad")) + lax.axis_index("half")
    still = still_lanes(place, 8)
    pieces = send_sems.shape[0]
    span = TILE // pieces

    def at(device):
        return (device // (halves * quads), device // quads % halves, device % quads)

    def sending(c, k):
        target = (me + k) % n
        part = pl.ds(c * span, span)
        return pltpu.make_async_remote_copy(
            src_ref=fold_ref.at[target, part], dst_ref=folded_ref.at[me, part],
            send_sem=send_sems.at[c, k], recv_sem=recv_sems.at[c, k], device_id=at(target), device_id_type=MESH,
        )

    def arriving(c, k):
        source = (me - k + n) % n
        part = pl.ds(c * span, span)
        return pltpu.make_async_remote_copy(
            src_ref=fold_ref.at[source, part], dst_ref=folded_ref.at[source, part],
            send_sem=send_sems.at[c, k], recv_sem=recv_sems.at[c, k], device_id=at(source), device_id_type=MESH,
        )

    barrier = pltpu.get_barrier_semaphore()

    def greet(k, carry):
        pl.semaphore_signal(barrier, inc=1, device_id=at((me + k) % n), device_id_type=MESH)
        return carry

    lax.fori_loop(1, n, greet, 0)
    origins = [0] * (n // 2)
    for k in range(n // 2):
        group, member = group_of(k // quads, k % quads)
        origins[group * quads + member] = k
    fetch = pltpu.make_async_copy(sky_ref, held_ref, held_sem)
    fetch.start()
    depth = n // 2

    def outer(k, carry):
        spot = pl.ds(pl.multiple_of(k * 8, 8), 8)
        table = turn_g_ref[spot, :]
        for e in range(2):
            x = []
            for a in range(depth):
                value = whole_ref[origins[a], spot, :TILE], whole_ref[origins[a], spot, TILE:]
                x.append(turn(value, 2 * math.pi * a / n) if e * a else value)
            for v, value in enumerate(sixteen(x)):
                u = 2 * v + e
                work_ref[u, 0, spot, :], work_ref[u, 1, spot, :] = times(value, *pick(table, u))
        return carry

    lax.fori_loop(0, whole_ref.shape[1] // 8, outer, 0)

    fetch.wait()

    def inner(k, carry):
        for u in (4 * k, 4 * k + 2):
            made = product(mat_g_ref, beside(work_ref, u))
            z = jnp.concatenate([made[:, q * TILE : (q + 1) * TILE] * held_ref[u + q] for q in range(2)], axis=1)
            spread = product(mat_f_ref, z)
            for q in range(2):
                for c in range(2):
                    work_ref[u + q, c, :TILE, :] = spread[c * TILE : (c + 1) * TILE, q * TILE : (q + 1) * TILE]
        return carry

    lax.fori_loop(0, n // 4, inner, 0)

    def last(k, carry):
        spot = pl.ds(pl.multiple_of(k * 8, 8), 8)
        table = turn_ref[spot, :]
        for e in range(2):
            x = []
            for v in range(depth):
                u = 2 * v + e
                x.append(times((work_ref[u, 0, spot, :], work_ref[u, 1, spot, :]), *pick(table, u)))
            for d, value in enumerate(minus(x)):
                if e == 0:
                    half_ref[d, 0], half_ref[d, 1] = value
                    continue
                value = turn(value, -2 * math.pi * d / n) if d else value
                before = half_ref[d, 0], half_ref[d, 1]
                for side, both_parts in enumerate((add(before, value), sub(before, value))):
                    fold_ref[d + side * depth, spot, :] = both_parts[0] - mirrored(both_parts[1], still)
        return carry

    def send(c, k, carry):
        sending(c, k).start()
        return carry

    for c in range(pieces):
        lax.fori_loop(c * span // 8, (c + 1) * span // 8, last, 0)
        if c == 0:
            pl.semaphore_wait(barrier, n - 1)
        lax.fori_loop(1, n, functools.partial(send, c), 0)
    folded_ref[me] = fold_ref[me]

    def receive(source):
        a = source // (halves * quads) * quads + source % quads
        j = 2 * a + source // quads % halves
        made = through(folded_ref[source], mat_r_ref, jnp.where(j == 0, 1, 0))
        work_ref[j, 0, :TILE, :], work_ref[j, 1, :TILE, :] = made[:, :TILE], made[:, TILE:]

    receive(me)

    def arrive(k, carry):
        for c in range(pieces):
            arriving(c, k).wait_recv()
        receive((me - k + n) % n)
        return carry

    lax.fori_loop(1, n, arrive, 0)

    def gradient(k, carry):
        spot = pl.ds(pl.multiple_of(k * 8, 8), 8)
        for e in range(2):
            x = []
            for v in range(depth):
                j = 2 * v + e
                x.append(times((work_ref[j, 0, spot, :], work_ref[j, 1, spot, :]), turn_r_ref[j, 0:1, :], turn_r_ref[j, 1:2, :]))
            for b, value in enumerate(sixteen(x)):
                if e == 0:
                    real_ref[b] = value[0]
                    continue
                real = turn(value, 2 * math.pi * b / n)[0] if b else value[0]
                for c, total in ((b, real_ref[b] + real), (b + depth, real_ref[b] - real)):
                    lanes = slice(c * TILE, (c + 1) * TILE)
                    out_ref[spot, lanes] = total * scale
        return carry

    lax.fori_loop(0, TILE // 8, gradient, 0)

    def sent(k, carry):
        for c in range(pieces):
            sending(c, k).wait_send()
        return carry

    lax.fori_loop(1, n, sent, 0)


def row_weights(n, size):
    alpha = np.arange(TILE)
    i = np.arange(size // n // 2)
    turns = np.stack(trig(np.arange(n)[:, None] * alpha[None, :], size), axis=1).astype(np.float32)
    c, s = trig(alpha[:, None] * i[None, :], size // n)
    there, back = [], []
    for special in range(2):
        real = np.concatenate([c + s, c - s], axis=1)
        imag = np.concatenate([c - s, -c - s], axis=1)
        from_real = np.concatenate([c + s, c - s], axis=1)
        from_imag = np.concatenate([s - c, s + c], axis=1)
        if special:
            lane = len(i)
            real[:, lane] = from_real[:, lane] = 1.0 - 2.0 * (alpha % 2)
            imag[:, lane] = from_imag[:, lane] = 0.0
        for target, matrix in ((there, np.concatenate([real, imag], axis=0)), (back, np.concatenate([from_real.T, from_imag.T], axis=1))):
            target.append(np.concatenate(split_table(matrix), axis=0))
    return turns, np.stack(there), np.stack(back)


def column_tables(n, size):
    w = np.arange(size // n)
    t = np.arange(TILE)
    u = np.arange(n)
    r = 2 * np.arange(2 * TILE) + 1
    side = TILE // 2

    def lanes(c, s):
        out = np.zeros((c.shape[0], TILE))
        out[:, :n], out[:, side : side + n] = c, s
        return out.astype(np.float32)

    def matrix(x):
        return np.concatenate(split_table(x), axis=0)

    c, s = trig(t[:, None] * u[None, :], size)
    turns = lanes(c, -s)
    c, s = trig(w[:, None] * t[None, :], size // n)
    mat_h = matrix(np.concatenate([c, s], axis=1))
    mat_f = matrix(np.concatenate([c.T, -s.T], axis=0))
    c, s = trig(r[:, None] * u[None, :], 2 * G)
    turns_g = lanes(c, s)
    c, s = trig((w[:, None] * n + G // 4) * r[None, :], 2 * G)
    mat_g = matrix(np.concatenate([s, c], axis=1))
    c, s = trig(w * n + G // 4, 2 * G)
    slope = np.stack([s, c]) * (2.0 * G)
    slope = np.broadcast_to(slope[:, :, None], slope.shape + (TILE,)).astype(np.float32)
    c, s = trig(u, 2 * G)
    bend = np.stack([c, s], axis=1).astype(np.float32)
    return turns, mat_h, mat_f, turns_g, mat_g, slope, bend


def column_call(kernel, smems, args, out_shape, scratch, name, away=(), **params):
    smem = pl.BlockSpec(memory_space=pltpu.SMEM)
    vmem = pl.BlockSpec(memory_space=pltpu.VMEM)
    anywhere = pl.BlockSpec(memory_space=pltpu.HBM)
    return pl.pallas_call(
        kernel,
        out_shape=jax.ShapeDtypeStruct(out_shape, jnp.float32),
        in_specs=[smem] * len(smems) + [anywhere if k in away else vmem for k in range(len(args))],
        out_specs=vmem,
        scratch_shapes=scratch,
        compiler_params=pltpu.CompilerParams(**{"vmem_limit_bytes": 24 << 20, **params}),
        cost_estimate=pl.CostEstimate(flops=10**10, bytes_accessed=16 * 2**20, transcendentals=0),
        name=name,
    )(*smems, *args)


def shared(residual, position, owner, tile_local, xi, amplitude):
    n = lax.axis_size(parts)
    n_base = lax.axis_size("base")
    n_slab = lax.axis_size("half") * lax.axis_size("quad")
    quads = lax.axis_size("quad")
    base, parity, quad = (lax.axis_index(axis) for axis in parts)
    place = 2 * (base * quads + quad) + parity
    rows, size = xi.shape
    depth = size // n
    half = depth // 2
    tiles = G // TILE

    row_turns, there, back_again = (jnp.asarray(x) for x in row_weights(n, size))
    block = (n, rows, depth)
    work = pltpu.VMEM((n, 2, rows, depth), jnp.float32)
    blocks = residual.shape[0]
    room = 2 * n_base * (2 * blocks // n)
    sent = pack(owner, tile_local, residual, position, n_base, n_slab, room)
    got, spectrum = exchange(sent, n_slab, xi, amplitude, row_turns, there)
    field = lax.all_to_all(spectrum, parts, split_axis=0, concat_axis=0, tiled=True)

    sources = n_slab * n_base
    codes = got[:, :, room, 0, :].reshape(sources, TILE).astype(jnp.int32)

    turns, firsts, undos, weights = grid_row_weights(n, size)
    halves = grid_rows_two(
        room,
        codes,
        jnp.asarray(firsts),
        got.reshape(sources * (room + 1), 4, TILE),
        jnp.asarray(turns),
        jnp.asarray(undos),
        jnp.asarray(weights),
    )
    whole = lax.all_to_all(halves, ("base", "quad"), split_axis=0, concat_axis=0, tiled=True)

    turns, mat_h, mat_f, turns_g, mat_g, slope, bend = (jnp.asarray(x) for x in column_tables(n, size))
    me = jnp.reshape(place, (1,)).astype(jnp.int32)
    sky = column_call(
        functools.partial(field_kernel, 1.0 / size),
        [me, bend],
        [field, turns, mat_h, slope],
        block,
        [work],
        "field",
    )
    pieces = 4
    dma = pltpu.SemaphoreType.DMA
    return amplitude * column_call(
        functools.partial(image_kernel, 1.0 / size),
        [],
        [whole, sky, turns_g, mat_g, mat_f, turns, row_turns, back_again],
        (rows, size),
        [
            pltpu.VMEM((n, 2, 2 * rows, depth), jnp.float32), pltpu.VMEM((n // 2, 2, 8, depth), jnp.float32),
            pltpu.VMEM(block, jnp.float32), pltpu.VMEM(block, jnp.float32), pltpu.VMEM(block, jnp.float32),
            pltpu.VMEM((n // 2, 8, depth), jnp.float32), dma, dma((pieces, n)), dma((pieces, n)),
        ],
        "image",
        away=(1,),
        vmem_limit_bytes=36 << 20,
        collective_id=1,
        has_side_effects=True,
    )


def solution(mesh):
    n_base, n_slab = mesh.shape["base"], mesh.shape["slab"]
    body, axes = general, both
    if n_base == 4 and n_slab == 2 * n_base and 2 * n_base * n_slab == G // TILE:
        body, axes = shared, parts
        mesh = jax.sharding.Mesh(mesh.devices.reshape(n_base, 2, n_slab // 2), parts)
    placed = (
        P(axes, None, None),
        P(axes, None, None),
        P(axes, None),
        P(axes),
        P(axes, None),
        P(axes, None),
    )
    return jax.shard_map(body, mesh=mesh, in_specs=placed, out_specs=P(axes, None), check_vma=False)
```

```python
import functools
import math

import jax
import jax.numpy as jnp
import numpy as np
from jax import lax
from jax.experimental import pallas as pl
from jax.experimental.pallas import tpu as pltpu
from jax.sharding import PartitionSpec as P

G = 8192
TILE = 128
both = ("base", "slab")
fine = lax.Precision.HIGHEST


def trig(product, modulus):
    angle = (product % modulus).astype(np.float64) * (2.0 * np.pi / modulus)
    return np.cos(angle), np.sin(angle)


def column_table(n, size):
    depth = size // n
    half = depth // 2
    i = np.arange(half)[None, :]
    j = np.arange(n)[:, None]
    low = n * i + j
    high = (-low) % size
    high[0, 0] = size // 2
    return np.concatenate([low, high], axis=1)


def row_tables(n, size):
    depth = size // n
    cols = column_table(n, size)
    oc, osn = trig(np.arange(n)[:, None] * np.arange(n)[None, :], n)
    outer = np.stack([oc, osn], axis=1)
    prod = np.arange(depth)[None, :, None] * cols[:, None, :]
    c, s = trig(prod, size)
    sign = np.where(np.arange(depth) < depth // 2, 1.0, -1.0)[None, None, :]
    inner = np.stack([c + s, sign * (c - s)], axis=1)
    return outer.astype(np.float32), inner.astype(np.float32)


def grid_row_tables(n, size):
    depth = G // n
    cols = column_table(n, size)
    half = cols.shape[1] // 2
    oc, osn = trig(np.arange(n)[:, None] * np.arange(n)[None, :], n)
    outer = np.stack([np.stack([oc, osn], 1), np.stack([-osn, oc], 1)], 0)
    low = cols[:, :half]
    high = cols[(-np.arange(n)) % n, half:]
    a = np.arange(depth)[None, :, None]
    out = []
    for part in (low, high):
        c, s = trig(a * (part[:, None, :] + G // 4), G)
        out.append(np.stack([np.concatenate([c, s], 2), np.concatenate([-s, c], 2)], 1))
    return outer.astype(np.float32), np.concatenate(out, axis=3).astype(np.float32)


def taps(cells, offsets):
    scaled = (cells - offsets) * 0.25
    kept = jnp.maximum(1.0 - scaled * scaled, 0.0)
    return kept * kept * kept


def split_three(x):
    high = x.astype(jnp.bfloat16)
    rest = x - high.astype(jnp.float32)
    middle = rest.astype(jnp.bfloat16)
    return high, middle, (rest - middle.astype(jnp.float32)).astype(jnp.bfloat16)


def grid_kernel(rows, info_ref, list_ref, data_ref, out_ref):
    count = info_ref[0]
    first = info_ref[1].astype(jnp.float32)
    out_ref[...] = jnp.zeros_like(out_ref)
    row_cells = lax.broadcasted_iota(jnp.int32, (rows, TILE), 0).astype(jnp.float32) + first
    col_cells = lax.broadcasted_iota(jnp.int32, (TILE, TILE), 0).astype(jnp.float32)

    def step(k, carry):
        packed = list_ref[k]
        index = packed // 256
        col = (packed // 2) % 128
        flip = (packed % 2).astype(jnp.float32)
        sign = 1.0 - 2.0 * flip
        start = 128.0 * flip
        block = data_ref[index]
        value = block[0:2, :]
        place = block[2:4, :]
        row_taps = taps(row_cells * sign + start, place[0:1, :])
        col_taps = taps(col_cells * sign + start, place[1:2, :])
        weighted = jnp.concatenate(
            [col_taps * value[0:1, :], col_taps * (value[1:2, :] * sign)], axis=0
        )
        rh, rm, rl = split_three(row_taps)
        wh, wm, wl = split_three(weighted)
        left = jnp.concatenate([rh, rh, rh, rm, rm, rl], axis=1)
        right = jnp.concatenate([wh, wm, wl, wh, wm, wh], axis=1)
        sub = lax.dot_general(
            left, right, (((1,), (1,)), ((), ())), preferred_element_type=jnp.float32
        )
        out_ref[0, col] += sub[:, :TILE]
        out_ref[1, col] += sub[:, TILE:]
        return carry

    lax.fori_loop(0, count, step, 0)


def grid_rows(info, table, gathered, rows):
    tiles = G // TILE
    smem = pl.BlockSpec(memory_space=pltpu.SMEM)
    vmem = pl.BlockSpec(memory_space=pltpu.VMEM)
    return pl.pallas_call(
        functools.partial(grid_kernel, rows),
        out_shape=jax.ShapeDtypeStruct((2, tiles, rows, TILE), jnp.float32),
        in_specs=[smem, smem, vmem],
        out_specs=vmem,
        compiler_params=pltpu.CompilerParams(vmem_limit_bytes=56 * 1024 * 1024),
        cost_estimate=pl.CostEstimate(
            flops=2 * 10**10, bytes_accessed=16 * 2**20, transcendentals=0
        ),
        name="grid_rows",
    )(info, table, gathered)


def einsum(form, *args, precision=lax.Precision.HIGH):
    return jnp.einsum(form, *args, precision=precision, preferred_element_type=jnp.float32)


def general(residual, position, owner, tile_local, xi, amplitude):
    n = lax.axis_size(both)
    n_base = lax.axis_size("base")
    n_slab = lax.axis_size("slab")
    me = lax.axis_index(both)
    rows, size = xi.shape
    depth = size // n
    half = depth // 2
    tiles = G // TILE

    region_rows = G // n_slab // TILE
    region_cols = G // n_base // TILE
    target = owner[:, 0]
    tile_row = (target % n_slab) * region_rows + tile_local // region_cols
    tile_col = (target // n_slab) * region_cols + tile_local % region_cols
    flip = tile_row >= tiles // 2
    tile_row = jnp.where(flip, tiles - 1 - tile_row, tile_row)
    tile_col = jnp.where(flip, tiles - 1 - tile_col, tile_col)
    code = tile_row * 256 + tile_col * 2 + flip.astype(jnp.int32)
    codes = lax.all_gather(code, both, axis=0, tiled=True)
    payload = jnp.concatenate([residual, position], axis=1)
    codes, payload = lax.optimization_barrier((codes, payload))
    gathered = lax.all_gather(payload, both, axis=0, tiled=True)
    blocks = codes.shape[0]
    grid_depth = G // 2 // n
    first_row = me * grid_depth
    mine = (codes // 256 == first_row // TILE).astype(jnp.int32)
    rank = jnp.where(mine == 1, jnp.cumsum(mine) - 1, -1)
    packed = lax.broadcasted_iota(jnp.int32, (blocks,), 0) * 256 + codes % 256
    spots = lax.broadcasted_iota(jnp.int32, (blocks, blocks), 0)
    table = jnp.sum(jnp.where(spots == rank[None, :], packed[None, :], 0), axis=1)
    info = jnp.stack([jnp.sum(mine), first_row % TILE]).astype(jnp.int32)

    outer, inner = row_tables(n, size)
    spectrum = (amplitude * xi).reshape(rows, n, depth)
    mid = einsum("rba,bqc->qcra", spectrum, outer)
    sent = einsum("cra,cae->cre", mid[0], inner[:, 0]) + einsum("cra,cae->cre", mid[1], inner[:, 1])
    sent, gathered = lax.optimization_barrier((sent, gathered))
    field = lax.all_to_all(sent, both, split_axis=0, concat_axis=0, tiled=True)
    field = field.reshape(size, depth)
    lane = lax.broadcasted_iota(jnp.int32, (1, depth), 1)
    still = (me == 0) & (lane % half == 0)

    def mirror(x):
        return jnp.where(still, x, jnp.roll(x, half, axis=-1))

    c_len = 128
    d_len = size // c_len
    bc, bs = (x.astype(np.float32) for x in trig(np.arange(c_len)[:, None] * np.arange(c_len)[None, :], c_len))
    shape = (c_len, d_len, depth)
    n0 = c_len * np.arange(d_len)[None, :] + np.arange(c_len)[:, None]
    ic, isn = (x.astype(np.float32) for x in trig(n0[:, :, None] * np.arange(d_len)[None, None, :], size))
    pair = jnp.stack([field.reshape(shape), mirror(field).reshape(shape)])
    first = np.stack([np.stack([bc, bs], 1), np.stack([bs, -bc], 1)], 0)
    turned = einsum("qbal,qbsc->csal", pair, first)
    second = np.stack([ic, -isn], axis=2)
    power = einsum("csal,cdsa->cdl", turned, second)
    sky = jnp.exp(power / size)

    grid = grid_rows(info, table, gathered, grid_depth)
    outer_g, inner_g = grid_row_tables(n, size)
    parts = tiles // n if tiles >= n else 1
    inner_len = G // n
    if inner_len >= TILE:
        view = grid.reshape(2, n, inner_len // TILE, grid_depth, TILE)
    else:
        flat = grid.transpose(0, 2, 1, 3).reshape(2, grid_depth, n, inner_len)
        view = flat.transpose(0, 2, 1, 3)[:, :, None]
        parts = 1
    lanes = view.shape[-1]
    stage = einsum("qbpra,qbsc->cspra", view, outer_g, precision=fine)
    inner_g = inner_g.reshape(n, 2, parts, lanes, 2 * depth)
    halves = einsum("cspra,cspae->cre", stage, inner_g, precision=fine)
    high = halves[:, :, depth:]
    high = jnp.concatenate([high[:1], jnp.flip(high[1:], axis=0)], axis=0)
    halves = jnp.concatenate([halves[:, :, :depth], high], axis=2)
    got = lax.all_to_all(halves, both, split_axis=0, concat_axis=0, tiled=True)
    got = got.reshape(size, 2 * depth)
    real = jnp.concatenate([got[:, :half], got[:, depth : depth + half]], axis=1)
    imag = jnp.concatenate([got[:, half:depth], got[:, depth + half :]], axis=1)
    wide = G // c_len
    deep = size // wide
    gc, gs = (x.astype(np.float32) for x in trig(np.arange(deep)[:, None] * np.arange(c_len)[None, :], c_len))
    first_g = np.stack([np.stack([gc, gs], 1), np.stack([-gs, gc], 1)], 0)
    whole = jnp.stack([real.reshape(deep, wide, depth), imag.reshape(deep, wide, depth)])
    turned_g = einsum("qbal,qbsc->csal", whole, first_g, precision=fine)
    ac, asn = trig((n0 + G // 4)[:, :, None] * np.arange(wide)[None, None, :], G)
    second_g = (np.stack([ac, -asn], axis=2) / G).astype(np.float32)
    back = einsum("csal,cdsa->cdl", turned_g, second_g, precision=fine)

    z = sky * back
    pz = einsum("cdl,cda->cal", z, ic)
    qz = einsum("cdl,cda->cal", z, isn)
    joined = jnp.stack([pz + mirror(qz), mirror(pz) - qz])
    fold = einsum("qcal,qcb->bal", joined, np.stack([bc, bs]))
    folded = lax.all_to_all(
        fold.reshape(n, rows, depth), both, split_axis=0, concat_axis=0, tiled=True
    )
    ends = einsum("jre,jqae->qjra", folded, inner)
    final = einsum("qjra,bqj->rba", ends, outer)
    return amplitude * final.reshape(rows, size) / size


MESH = pl.DeviceIdType.MESH
parts = ("base", "half", "quad")
LANES = 6


def two_parts(x):
    high = x.astype(jnp.bfloat16)
    return high, (x - high.astype(jnp.float32)).astype(jnp.bfloat16)


def through(x, weight_ref, which):
    rows, depth = x.shape
    high, low = two_parts(x)
    made = jnp.dot(jnp.concatenate([high, low], axis=0), weight_ref[which, :depth], preferred_element_type=jnp.float32)
    return made[:rows] + made[rows:] + jnp.dot(high, weight_ref[which, depth:], preferred_element_type=jnp.float32)


def times(x, c, s):
    return x[0] * c - x[1] * s, x[0] * s + x[1] * c


def turn(x, angle):
    c, s = math.cos(angle), math.sin(angle)
    return times(x, c, s)


def add(x, y):
    return x[0] + y[0], x[1] + y[1]


def sub(x, y):
    return x[0] - y[0], x[1] - y[1]


def four(x):
    s0, d0, s1, d1 = add(x[0], x[2]), sub(x[0], x[2]), add(x[1], x[3]), sub(x[1], x[3])
    i1 = (-d1[1], d1[0])
    return [add(s0, s1), add(d0, i1), sub(s0, s1), sub(d0, i1)]


def sixteen(x):
    rows = []
    for b0 in range(4):
        y = four([x[4 * b1 + b0] for b1 in range(4)])
        rows.append([y[a0] if a0 * b0 == 0 else turn(y[a0], 2 * math.pi * a0 * b0 / 16) for a0 in range(4)])
    out = [None] * 16
    for a0 in range(4):
        y = four([rows[b0][a0] for b0 in range(4)])
        for a1 in range(4):
            out[a0 + 4 * a1] = y[a1]
    return out


def seat(j, quads):
    a = j // 2
    return a // quads * (2 * quads) + j % 2 * quads + a % quads


def transform_rows(quads, xi_ref, amplitude_ref, turn_ref, mat_ref, out_ref, work_ref):
    n = out_ref.shape[0]

    def outer(k, carry):
        spot = pl.ds(pl.multiple_of(k * 8, 8), 8)
        for e in range(2):
            x = []
            for b in range(n // 2):
                first, second = (
                    xi_ref[spot, c * TILE : (c + 1) * TILE] * amplitude_ref[spot, c * TILE : (c + 1) * TILE]
                    for c in (b, b + n // 2)
                )
                value = first - second if e else first + second
                if e * b:
                    angle = 2 * math.pi * b / n
                    x.append((value * math.cos(angle), value * math.sin(angle)))
                else:
                    x.append((value, jnp.zeros_like(value)))
            for v, value in enumerate(sixteen(x)):
                j = 2 * v + e
                work_ref[j, 0, spot, :], work_ref[j, 1, spot, :] = times(value, turn_ref[j, 0:1, :], turn_ref[j, 1:2, :])
        return carry

    lax.fori_loop(0, xi_ref.shape[0] // 8, outer, 0)
    rows = xi_ref.shape[0]

    def left(entries):
        return jnp.concatenate([jnp.concatenate([work_ref[j, 0], work_ref[j, 1]], axis=1) for j in entries], axis=0)

    def inner(k, carry):
        entries = [4 * k + q for q in range(4)]
        made = through(left(entries), mat_ref, 0)
        for q, j in enumerate(entries):
            out_ref[seat(j, quads)] = made[q * rows : (q + 1) * rows]
        return carry

    lax.fori_loop(0, n // 4, inner, 0)
    out_ref[0] = through(left([0]), mat_ref, 1)


def seats(base, quad):
    return base // 2, base % 2, quad // 2, quad % 2


def group_of(base, quad):
    y, x, low, core = seats(base, quad)
    return 2 * x + low, 2 * y + core


def exchange_kernel(send_ref, xi_ref, amplitude_ref, turn_ref, mat_ref, out_ref, spectrum_ref, work_ref, made_ref, rows_ref, rows_sem, bsend, brecv, zsend, zrecv, ysend, yrecv, csend, crecv, lsem):
    nb = send_ref.shape[0]
    quads = lax.axis_size("quad")
    half = lax.axis_index("half")
    y, x, low, core = seats(lax.axis_index("base"), lax.axis_index("quad"))
    group = 2 * x + low

    def at(y, group, half, core):
        return (2 * y + group // 2, half, group % 2 * 2 + core)

    def block(y, half, core, k):
        return out_ref.at[(2 * y + half) * 2 + core, (group - k + nb) % nb]

    def copy(part, here, there, device):
        return pltpu.make_async_remote_copy(
            src_ref=part, dst_ref=part, send_sem=here, recv_sem=there, device_id=device, device_id_type=MESH
        )

    def moved(target, source, k):
        return pltpu.make_async_remote_copy(
            src_ref=send_ref.at[target],
            dst_ref=out_ref.at[(2 * y + half) * 2 + core, source],
            send_sem=bsend.at[k],
            recv_sem=brecv.at[k],
            device_id=at(y, target, half, core),
            device_id_type=MESH,
        )

    far, beside, partner = at(y, group, 1 - half, core), at(1 - y, group, half, core), at(y, group, half, 1 - core)

    def along_z(own, k):
        return copy(block(y, half if own else 1 - half, core, k), zsend.at[k], zrecv.at[k], far)

    def along_y(own, kind, k):
        place = half if kind == 0 else 1 - half
        return copy(block(y if own else 1 - y, place, core, k), ysend.at[kind, k], yrecv.at[kind, k], beside)

    def over(own, kind, k):
        row = y if kind < 2 else 1 - y
        place = half if kind % 2 == 0 else 1 - half
        return copy(block(row, place, core if own else 1 - core, k), csend.at[kind, k], crecv.at[kind, k], partner)

    fetches = [
        pltpu.make_async_copy(source, rows_ref.at[k], rows_sem.at[k]) for k, source in enumerate((xi_ref, amplitude_ref))
    ]
    ready = pltpu.make_async_copy(made_ref, spectrum_ref, rows_sem.at[2])
    for fetch in fetches:
        fetch.start()
    barrier = pltpu.get_barrier_semaphore()
    peers = [at(y, (group + k) % nb, half, core) for k in range(1, nb)] + [far, beside, partner]
    for peer in peers:
        pl.semaphore_signal(barrier, inc=1, device_id=peer, device_id_type=MESH)
    pl.semaphore_wait(barrier, len(peers))

    own = pltpu.make_async_copy(send_ref.at[group], block(y, half, core, 0), lsem)
    own.start()
    for k in range(1, nb):
        moved((group + k) % nb, group, k).start()
    for k in range(nb):
        if k == 0:
            own.wait()
        else:
            moved((group - k + nb) % nb, (group - k + nb) % nb, k).wait_recv()
        along_z(True, k).start()
        along_y(True, 0, k).start()
        over(True, 0, k).start()
        if k == 0:
            for fetch in fetches:
                fetch.wait()
            transform_rows(quads, rows_ref.at[0], rows_ref.at[1], turn_ref, mat_ref, made_ref, work_ref)
            ready.start()
    for k in range(nb):
        along_z(False, k).wait_recv()
        along_y(True, 1, k).start()
        over(True, 1, k).start()
    for kind in range(2):
        for k in range(nb):
            along_y(False, kind, k).wait_recv()
            over(True, 2 + kind, k).start()
    ready.wait()
    for kind in range(4):
        for k in range(nb):
            over(False, kind, k).wait_recv()
    for k in range(nb):
        if k:
            moved((group + k) % nb, group, k).wait_send()
        along_z(True, k).wait_send()
        for kind in range(2):
            along_y(True, kind, k).wait_send()
        for kind in range(4):
            over(True, kind, k).wait_send()


def pack_kernel(ns, tiles, room, owner_ref, local_ref, residual_ref, position_ref, out_ref):
    blocks = residual_ref.shape[0]
    nb = out_ref.shape[0]
    across = lax.broadcasted_iota(jnp.int32, (blocks, blocks), 1)
    down = lax.broadcasted_iota(jnp.int32, (blocks, blocks), 0)

    def column(row):
        return jnp.sum(jnp.where(across == down, row, 0.0), axis=1, keepdims=True)

    def divided(x, d):
        whole = jnp.floor((x + 0.5) * (1.0 / d))
        return whole, x - whole * d

    local = local_ref[...].astype(jnp.float32)
    target = owner_ref[...].astype(jnp.float32)
    region_col, region_row = divided(target, ns)
    tile_row, tile_col = divided(local, tiles // nb)
    tile_row = tile_row + region_row * (tiles // ns)
    tile_col = tile_col + region_col * (tiles // nb)
    flip = jnp.where(tile_row >= tiles // 2, 1.0, 0.0)
    tile_row = jnp.where(flip > 0.5, tiles - 1 - tile_row, tile_row)
    tile_col = jnp.where(flip > 0.5, tiles - 1 - tile_col, tile_col)
    line, within = divided(tile_row, ns)
    key = divided(tile_row, 2)[0]
    code = divided(within, 2)[1] * tiles + tile_col
    keys = ns // 2
    line_down, key_down, flip_down = column(line), column(key), column(flip)
    before = (line_down == line) & ((key_down < key) | ((key_down == key) & (down < across)))
    slot = line * room + jnp.sum(jnp.where(before, 1.0, 0.0), axis=0, keepdims=True)
    slots = lax.broadcasted_iota(jnp.int32, (nb * room, blocks), 0).astype(jnp.float32)
    chosen = jnp.where(slots == slot, 1.0, 0.0).astype(jnp.bfloat16)
    sides = [residual_ref[:, 0, :], residual_ref[:, 1, :] * (1.0 - 2.0 * flip_down)]
    for k in range(2):
        place = position_ref[:, k, :]
        sides.append(jnp.where(flip_down > 0.5, TILE - place, place))
    pieces = split_three(jnp.concatenate(sides, axis=1))
    moved = jnp.dot(
        jnp.concatenate([chosen] * 3, axis=1), jnp.concatenate(pieces, axis=0), preferred_element_type=jnp.float32
    )
    codes = 0.0
    for part in two_parts(jnp.broadcast_to(code + 1.0, (8, blocks))):
        codes = codes + lax.dot_general(part, chosen, (((1,), (1,)), ((), ())), preferred_element_type=jnp.float32)
    codes = codes - 1.0
    lanes = lax.broadcasted_iota(jnp.int32, (1, blocks), 1)
    shift = (across - room).astype(jnp.float32)
    per = blocks // room
    for k in range(nb):
        for c in range(4):
            out_ref[k, :room, c, :] = moved[k * room : (k + 1) * room, c * TILE : (c + 1) * TILE]
        start = k // per * blocks
        own = codes[:, start : start + blocks]
        if k % per:
            own = pltpu.roll(own, blocks - k % per * room, 1)
        earlier = (line_down == k) & (key_down - keys * k < shift)
        starts = jnp.sum(jnp.where(earlier, 1.0, 0.0), axis=0, keepdims=True)
        out_ref[k, room] = jnp.broadcast_to(jnp.where(lanes < room, own[0:1, :], starts), (4, TILE))


def pack(owner, local, residual, position, nb, ns, room):
    vmem = pl.BlockSpec(memory_space=pltpu.VMEM)
    return pl.pallas_call(
        functools.partial(pack_kernel, ns, G // TILE, room),
        out_shape=jax.ShapeDtypeStruct((nb, room + 1, 4, TILE), jnp.float32),
        in_specs=[vmem] * 4,
        out_specs=vmem,
        compiler_params=pltpu.CompilerParams(vmem_limit_bytes=60 << 20),
        name="pack",
    )(owner.reshape(1, -1), local.reshape(1, -1), residual, position)


def exchange(sent, ns, xi, amplitude, turns, mats):
    nb = sent.shape[0]
    rows, n = xi.shape[0], turns.shape[0]
    dma = pltpu.SemaphoreType.DMA
    vmem = pl.BlockSpec(memory_space=pltpu.VMEM)
    hbm = pl.BlockSpec(memory_space=pltpu.HBM)
    return pl.pallas_call(
        exchange_kernel,
        out_shape=(
            jax.ShapeDtypeStruct((ns,) + sent.shape, jnp.float32),
            jax.ShapeDtypeStruct((n, rows, TILE), jnp.float32),
        ),
        in_specs=[vmem, hbm, hbm, vmem, vmem],
        out_specs=(hbm, hbm),
        scratch_shapes=[
            pltpu.VMEM((n, 2, rows, TILE), jnp.float32),
            pltpu.VMEM((n, rows, TILE), jnp.float32),
            pltpu.VMEM((2,) + xi.shape, jnp.float32), dma((3,)),
            dma((nb,)), dma((nb,)), dma((nb,)), dma((nb,)), dma((2, nb)), dma((2, nb)), dma((4, nb)), dma((4, nb)), dma,
        ],
        compiler_params=pltpu.CompilerParams(collective_id=0, has_side_effects=True, vmem_limit_bytes=60 << 20),
        cost_estimate=pl.CostEstimate(flops=3 * 10**10, bytes_accessed=16 * 2**20, transcendentals=0),
        name="exchange",
    )(sent, xi, amplitude, turns, mats)


def grid_kernel_two(room, codes_ref, first_ref, data_hbm_ref, turn_ref, undo_ref, weight_hbm_ref, away_ref, grid_ref, left_ref, right_ref, out_ref, data_ref, weight_ref, list_ref, sems):
    quad = group_of(lax.axis_index("base"), lax.axis_index("quad"))[1]
    parity = lax.axis_index("half")
    data = pltpu.make_async_copy(data_hbm_ref, data_ref, sems.at[out_ref.shape[0]])
    weight = pltpu.make_async_copy(weight_hbm_ref, weight_ref, sems.at[out_ref.shape[0] + 1])
    data.start()
    weight.start()
    grid_ref[...] = jnp.zeros_like(grid_ref)
    half = grid_ref.shape[1]
    group = 16
    cells = lax.broadcasted_iota(jnp.int32, (group + 8, TILE), 0).astype(jnp.float32) * 0.25
    nothing = jnp.zeros((group, TILE), jnp.bfloat16)

    def bump(offsets):
        d = cells - offsets
        kept = jnp.maximum(1.0 - d * d, 0.0)
        return kept * kept * kept

    def window(offsets):
        start = jnp.floor((offsets - 4.0) * (1.0 / group))
        offsets = (offsets - start * group) * 0.25
        return bump(offsets) - bump(offsets - 0.25), jnp.broadcast_to(start, (group, TILE)).astype(jnp.bfloat16)

    def spread(compact, start):
        padded = jnp.concatenate([compact, jnp.zeros((8, TILE), jnp.float32)], axis=0)
        out = []
        for part in two_parts(padded):
            first, second = part[:group], part[group:]
            pieces = []
            for g in range(TILE // group):
                piece = jnp.where(start == g - 1, second, nothing) if g else nothing
                pieces.append(jnp.where(start == g, first, piece))
            out.append(jnp.concatenate(pieces, axis=0))
        return out

    lanes = left_ref.shape[0]

    def place(k):
        packed = list_ref[k]
        return packed & (2 * half - 1), lax.shift_right_logical(packed, half.bit_length())

    def prepare(k, lane, count):
        col, rest = place(k)
        odd = jnp.where(col >= half, parity, 0)
        sign = jnp.where(k < count, 1 - 2 * odd, 0).astype(jnp.float32)
        block = data_ref[rest // 2]
        value = block[0:2, :] * sign
        row_taps, row_start = window(block[2:3, :])
        col_taps, col_start = window(block[3:4, :])
        rows_split = spread(row_taps, row_start)
        real = spread(col_taps * value[0:1, :], col_start)
        imag = spread(col_taps * value[1:2, :], col_start)
        for q in range(2):
            left_ref[lane, :, q * TILE : (q + 1) * TILE] = rows_split[q]
            right_ref[lane, :TILE, q * TILE : (q + 1) * TILE] = real[q]
            right_ref[lane, TILE:, q * TILE : (q + 1) * TILE] = imag[q]

    def product(lane):
        rh, rl = left_ref[lane, :, :TILE], left_ref[lane, :, TILE:]
        wh, wl = right_ref[lane, :, :TILE], right_ref[lane, :, TILE:]
        left = jnp.concatenate([rh, rh, rl], axis=1)
        right = jnp.concatenate([wh, wl, wh], axis=1)
        return lax.dot_general(left, right, (((1,), (1,)), ((), ())), preferred_element_type=jnp.float32)

    def step(k, carry):
        made = [product(lane) for lane in range(lanes)]
        for lane in range(lanes):
            prepare((k + 1) * lanes + lane, lane, count)
        for lane in range(lanes):
            col, rest = place(k * lanes + lane)
            col = jnp.where(col >= half, col - half, col)
            spot = pl.ds(pl.multiple_of((rest % 2) * TILE, TILE), TILE)
            grid_ref[0, col, spot, :] += made[lane][:, :TILE]
            grid_ref[1, col, spot, :] += made[lane][:, TILE:]
        return carry

    per = 4 * half

    def gather(source, filled):
        start = codes_ref[source, room + quad]
        stop = codes_ref[source, room + quad + 1]

        shift = filled - start
        first = source * ((room + 1) * per)

        def entry(i, carry):
            list_ref[shift + i] = first + i * per + codes_ref[source, i]
            return carry

        lax.fori_loop(start, stop, entry, 0)
        return filled + stop - start

    count = lax.fori_loop(0, codes_ref.shape[0], gather, 0)
    for lane in range(2 * lanes):
        list_ref[count + lane] = 0
    data.wait()
    for lane in range(lanes):
        prepare(lane, lane, count)
    lax.fori_loop(0, (count + lanes - 1) // lanes, step, 0)

    depth = half // 2
    rows = grid_ref.shape[2]

    def outer(k, carry):
        spot = pl.ds(pl.multiple_of(k * 8, 8), 8)
        for side in range(2):
            x = []
            for b in range(depth):
                value = grid_ref[0, 2 * b + side, spot, :], grid_ref[1, 2 * b + side, spot, :]
                x.append(times(value, first_ref[parity, b, 0], first_ref[parity, b, 1]))
            for a, value in enumerate(sixteen(x)):
                c = turn_ref[parity, a, side : side + 1, :]
                s = turn_ref[parity, a, 2 + side : 3 + side, :]
                value = times(value, c, s)
                grid_ref[0, 2 * a + side, spot, :] = value[0]
                grid_ref[1, 2 * a + side, spot, :] = value[1]
        return carry

    lax.fori_loop(0, rows // 8, outer, 0)

    def inner(a, carry):
        mirrored = depth - parity - a
        mirrored = jnp.where(mirrored == depth, 0, mirrored)
        which = jnp.where((a == 0) & (parity == 0), 1, 0)
        for part in range(1):
            spot = pl.ds(0, rows)
            x = jnp.concatenate([grid_ref[q, 2 * a + side, spot, :] for q in range(2) for side in range(2)], axis=1)
            made = through(x, weight_ref, which)
            mid = TILE // 2
            made = times((made[:, :TILE], made[:, TILE:]), undo_ref[parity, a, 0:1, :], undo_ref[parity, a, 1:2, :])
            for q in range(2):
                out_ref[a, spot, q * TILE : q * TILE + mid] = made[q][:, :mid]
                out_ref[mirrored, spot, q * TILE + mid : (q + 1) * TILE] = made[q][:, mid:]

        @pl.when(a >= depth // 2)
        def _():
            leave(a).start()
            leave(jnp.where((parity == 0) & (a == depth // 2), 0, mirrored)).start()

        return carry

    def leave(a):
        return pltpu.make_async_copy(out_ref.at[a], away_ref.at[a], sems.at[a])

    weight.wait()
    lax.fori_loop(0, depth, inner, 0)
    for a in range(depth):
        leave(a).wait()


def split_table(x):
    high = x.astype(np.float32).astype(jnp.bfloat16)
    low = (x - high.astype(np.float64)).astype(np.float32).astype(jnp.bfloat16)
    return high, low


def undone(pixels):
    c, s = trig(pixels + G // 4, G)
    return 1.0 / (1.0 - (c - 1j * s))


def grid_row_weights(n, size):
    depth = n // 2
    span = G // 2 // depth
    half = size // n // 2
    alpha = np.arange(span)
    turns, firsts, undos = [], [], []
    for p in range(2):
        j = 2 * np.arange(depth) + p
        c, s = trig(j[:, None] * alpha[None, :], G)
        turns.append(np.concatenate([c.reshape(depth, 2, TILE), s.reshape(depth, 2, TILE)], axis=1))
        firsts.append(np.stack(trig(np.arange(depth) * p, n), axis=1))
        low = n * np.arange(half)[None, :] + j[:, None]
        high = size - n * np.arange(half)[None, :] - ((-j) % n)[:, None]
        if p == 0:
            low[0, 0], high[0, 0] = 0, size // 2
        undo = undone(np.concatenate([low, high], axis=1))
        undos.append(np.stack([undo.real, undo.imag], axis=1))
    weights = []
    i = np.arange(half)
    for special in range(2):
        low = n * i
        high = size - n * i - (0 if special else n)
        if special:
            high[0] = size // 2
        parts_re, parts_im = [], []
        for cols in (low, high):
            c, s = trig(alpha[:, None] * (cols[None, :] + G // 4), G)
            parts_re.append(np.concatenate([c, -s], axis=0))
            parts_im.append(np.concatenate([s, c], axis=0))
        w = np.concatenate(parts_re + parts_im, axis=1)
        weights.append(np.concatenate(split_table(w), axis=0))
    turns, firsts, undos = (np.stack(x).astype(np.float32) for x in (turns, firsts, undos))
    return turns, firsts, undos, np.stack(weights)


def grid_rows_two(room, codes, first, data, turns, undos, weights):
    depth = turns.shape[1]
    rows = 2 * TILE
    smem = pl.BlockSpec(memory_space=pltpu.SMEM)
    vmem = pl.BlockSpec(memory_space=pltpu.VMEM)
    hbm = pl.BlockSpec(memory_space=pltpu.HBM)
    return pl.pallas_call(
        functools.partial(grid_kernel_two, room),
        out_shape=jax.ShapeDtypeStruct((depth, rows, 2 * TILE), jnp.float32),
        in_specs=[smem, smem, hbm, vmem, vmem, hbm],
        out_specs=hbm,
        scratch_shapes=[
            pltpu.VMEM((2, 2 * depth, rows, TILE), jnp.float32),
            pltpu.VMEM((LANES, TILE, 2 * TILE), jnp.bfloat16),
            pltpu.VMEM((LANES, 2 * TILE, 2 * TILE), jnp.bfloat16),
            pltpu.VMEM((depth, rows, 2 * TILE), jnp.float32),
            pltpu.VMEM(data.shape, jnp.float32),
            pltpu.VMEM(weights.shape, jnp.bfloat16),
            pltpu.SMEM((codes.shape[0] * room + 2 * LANES,), jnp.int32),
            pltpu.SemaphoreType.DMA((depth + 2,)),
        ],
        compiler_params=pltpu.CompilerParams(vmem_limit_bytes=60 << 20),
        cost_estimate=pl.CostEstimate(flops=2 * 10**10, bytes_accessed=16 * 2**20, transcendentals=0),
        name="grid_rows_two",
    )(codes, first, data, turns, undos, weights)


def minus(x):
    return [(b, a) for a, b in sixteen([(b, a) for a, b in x])]


def pick(table, u):
    side = table.shape[1] // 2
    return table[:, u : u + 1], table[:, side + u : side + u + 1]


def mirrored(x, still):
    return jnp.where(still, x, pltpu.roll(x, x.shape[1] // 2, 1))


def still_lanes(place, rows):
    lane = lax.broadcasted_iota(jnp.int32, (rows, TILE), 1)
    return (lane % (TILE // 2) == 0) & (place == 0)


def product(mat_ref, x):
    rows = mat_ref.shape[0] // 2
    high, low = two_parts(x)
    made = jnp.dot(mat_ref[...], high, preferred_element_type=jnp.float32)
    return made[:rows] + made[rows:] + jnp.dot(mat_ref[:rows], low, preferred_element_type=jnp.float32)


def beside(work_ref, u):
    sides = [jnp.concatenate([work_ref[u + q, 0], work_ref[u + q, 1]], axis=0) for q in range(2)]
    return jnp.concatenate(sides, axis=1)


def field_kernel(scale, info_ref, bend_ref, field_ref, turn_ref, mat_ref, slope_ref, sky_ref, work_ref):
    still = still_lanes(info_ref[0], 8)
    n = field_ref.shape[0]

    def outer(k, carry):
        spot = pl.ds(pl.multiple_of(k * 8, 8), 8)
        table = turn_ref[spot, :]
        for e in range(2):
            x = []
            for d in range(n // 2):
                first, second = field_ref[d, spot, :], field_ref[d + n // 2, spot, :]
                value = first - second if e else first + second
                value = value, mirrored(value, still)
                x.append(turn(value, -2 * math.pi * d / n) if e * d else value)
            for v, value in enumerate(minus(x)):
                u = 2 * v + e
                work_ref[u, 0, spot, :], work_ref[u, 1, spot, :] = times(value, *pick(table, u))
        return carry

    lax.fori_loop(0, field_ref.shape[1] // 8, outer, 0)

    def inner(k, carry):
        for u in (4 * k, 4 * k + 2):
            made = jnp.exp(product(mat_ref, beside(work_ref, u)) * scale)
            for q in range(2):
                sine = slope_ref[0] * bend_ref[u + q, 0] + slope_ref[1] * bend_ref[u + q, 1]
                sky_ref[u + q] = made[:, q * TILE : (q + 1) * TILE] / sine
        return carry

    lax.fori_loop(0, n // 4, inner, 0)


def image_kernel(scale, whole_ref, sky_ref, turn_g_ref, mat_g_ref, mat_f_ref, turn_ref, turn_r_ref, mat_r_ref, out_ref, work_ref, half_ref, held_ref, fold_ref, folded_ref, real_ref, held_sem, send_sems, recv_sems):
    n = sky_ref.shape[0]
    quads = lax.axis_size("quad")
    halves = lax.axis_size("half")
    me = (lax.axis_index("base") * halves + lax.axis_index("half")) * quads + lax.axis_index("quad")
    place = 2 * (lax.axis_index("base") * quads + lax.axis_index("quad")) + lax.axis_index("half")
    still = still_lanes(place, 8)
    pieces = send_sems.shape[0]
    span = TILE // pieces

    def at(device):
        return (device // (halves * quads), device // quads % halves, device % quads)

    def sending(c, k):
        target = (me + k) % n
        part = pl.ds(c * span, span)
        return pltpu.make_async_remote_copy(
            src_ref=fold_ref.at[target, part], dst_ref=folded_ref.at[me, part],
            send_sem=send_sems.at[c, k], recv_sem=recv_sems.at[c, k], device_id=at(target), device_id_type=MESH,
        )

    def arriving(c, k):
        source = (me - k + n) % n
        part = pl.ds(c * span, span)
        return pltpu.make_async_remote_copy(
            src_ref=fold_ref.at[source, part], dst_ref=folded_ref.at[source, part],
            send_sem=send_sems.at[c, k], recv_sem=recv_sems.at[c, k], device_id=at(source), device_id_type=MESH,
        )

    barrier = pltpu.get_barrier_semaphore()

    def greet(k, carry):
        pl.semaphore_signal(barrier, inc=1, device_id=at((me + k) % n), device_id_type=MESH)
        return carry

    lax.fori_loop(1, n, greet, 0)
    origins = [0] * (n // 2)
    for k in range(n // 2):
        group, member = group_of(k // quads, k % quads)
        origins[group * quads + member] = k
    fetch = pltpu.make_async_copy(sky_ref, held_ref, held_sem)
    fetch.start()
    depth = n // 2

    def outer(k, carry):
        spot = pl.ds(pl.multiple_of(k * 8, 8), 8)
        table = turn_g_ref[spot, :]
        for e in range(2):
            x = []
            for a in range(depth):
                value = whole_ref[origins[a], spot, :TILE], whole_ref[origins[a], spot, TILE:]
                x.append(turn(value, 2 * math.pi * a / n) if e * a else value)
            for v, value in enumerate(sixteen(x)):
                u = 2 * v + e
                work_ref[u, 0, spot, :], work_ref[u, 1, spot, :] = times(value, *pick(table, u))
        return carry

    lax.fori_loop(0, whole_ref.shape[1] // 8, outer, 0)

    fetch.wait()

    def inner(k, carry):
        for u in (4 * k, 4 * k + 2):
            made = product(mat_g_ref, beside(work_ref, u))
            z = jnp.concatenate([made[:, q * TILE : (q + 1) * TILE] * held_ref[u + q] for q in range(2)], axis=1)
            spread = product(mat_f_ref, z)
            for q in range(2):
                for c in range(2):
                    work_ref[u + q, c, :TILE, :] = spread[c * TILE : (c + 1) * TILE, q * TILE : (q + 1) * TILE]
        return carry

    lax.fori_loop(0, n // 4, inner, 0)

    def last(k, carry):
        spot = pl.ds(pl.multiple_of(k * 8, 8), 8)
        table = turn_ref[spot, :]
        for e in range(2):
            x = []
            for v in range(depth):
                u = 2 * v + e
                x.append(times((work_ref[u, 0, spot, :], work_ref[u, 1, spot, :]), *pick(table, u)))
            for d, value in enumerate(minus(x)):
                if e == 0:
                    half_ref[d, 0], half_ref[d, 1] = value
                    continue
                value = turn(value, -2 * math.pi * d / n) if d else value
                before = half_ref[d, 0], half_ref[d, 1]
                for side, both_parts in enumerate((add(before, value), sub(before, value))):
                    fold_ref[d + side * depth, spot, :] = both_parts[0] - mirrored(both_parts[1], still)
        return carry

    def send(c, k, carry):
        sending(c, k).start()
        return carry

    for c in range(pieces):
        lax.fori_loop(c * span // 8, (c + 1) * span // 8, last, 0)
        if c == 0:
            pl.semaphore_wait(barrier, n - 1)
        lax.fori_loop(1, n, functools.partial(send, c), 0)
    folded_ref[me] = fold_ref[me]

    def receive(source):
        a = source // (halves * quads) * quads + source % quads
        j = 2 * a + source // quads % halves
        made = through(folded_ref[source], mat_r_ref, jnp.where(j == 0, 1, 0))
        work_ref[j, 0, :TILE, :], work_ref[j, 1, :TILE, :] = made[:, :TILE], made[:, TILE:]

    receive(me)

    def arrive(k, carry):
        for c in range(pieces):
            arriving(c, k).wait_recv()
        receive((me - k + n) % n)
        return carry

    lax.fori_loop(1, n, arrive, 0)

    def gradient(k, carry):
        spot = pl.ds(pl.multiple_of(k * 8, 8), 8)
        for e in range(2):
            x = []
            for v in range(depth):
                j = 2 * v + e
                x.append(times((work_ref[j, 0, spot, :], work_ref[j, 1, spot, :]), turn_r_ref[j, 0:1, :], turn_r_ref[j, 1:2, :]))
            for b, value in enumerate(sixteen(x)):
                if e == 0:
                    real_ref[b] = value[0]
                    continue
                real = turn(value, 2 * math.pi * b / n)[0] if b else value[0]
                for c, total in ((b, real_ref[b] + real), (b + depth, real_ref[b] - real)):
                    lanes = slice(c * TILE, (c + 1) * TILE)
                    out_ref[spot, lanes] = total * scale
        return carry

    lax.fori_loop(0, TILE // 8, gradient, 0)

    def sent(k, carry):
        for c in range(pieces):
            sending(c, k).wait_send()
        return carry

    lax.fori_loop(1, n, sent, 0)


def row_weights(n, size):
    alpha = np.arange(TILE)
    i = np.arange(size // n // 2)
    turns = np.stack(trig(np.arange(n)[:, None] * alpha[None, :], size), axis=1).astype(np.float32)
    c, s = trig(alpha[:, None] * i[None, :], size // n)
    there, back = [], []
    for special in range(2):
        real = np.concatenate([c + s, c - s], axis=1)
        imag = np.concatenate([c - s, -c - s], axis=1)
        from_real = np.concatenate([c + s, c - s], axis=1)
        from_imag = np.concatenate([s - c, s + c], axis=1)
        if special:
            lane = len(i)
            real[:, lane] = from_real[:, lane] = 1.0 - 2.0 * (alpha % 2)
            imag[:, lane] = from_imag[:, lane] = 0.0
        for target, matrix in ((there, np.concatenate([real, imag], axis=0)), (back, np.concatenate([from_real.T, from_imag.T], axis=1))):
            target.append(np.concatenate(split_table(matrix), axis=0))
    return turns, np.stack(there), np.stack(back)


def column_tables(n, size):
    w = np.arange(size // n)
    t = np.arange(TILE)
    u = np.arange(n)
    r = 2 * np.arange(2 * TILE) + 1
    side = TILE // 2

    def lanes(c, s):
        out = np.zeros((c.shape[0], TILE))
        out[:, :n], out[:, side : side + n] = c, s
        return out.astype(np.float32)

    def matrix(x):
        return np.concatenate(split_table(x), axis=0)

    c, s = trig(t[:, None] * u[None, :], size)
    turns = lanes(c, -s)
    c, s = trig(w[:, None] * t[None, :], size // n)
    mat_h = matrix(np.concatenate([c, s], axis=1))
    mat_f = matrix(np.concatenate([c.T, -s.T], axis=0))
    c, s = trig(r[:, None] * u[None, :], 2 * G)
    turns_g = lanes(c, s)
    c, s = trig((w[:, None] * n + G // 4) * r[None, :], 2 * G)
    mat_g = matrix(np.concatenate([s, c], axis=1))
    c, s = trig(w * n + G // 4, 2 * G)
    slope = np.stack([s, c]) * (2.0 * G)
    slope = np.broadcast_to(slope[:, :, None], slope.shape + (TILE,)).astype(np.float32)
    c, s = trig(u, 2 * G)
    bend = np.stack([c, s], axis=1).astype(np.float32)
    return turns, mat_h, mat_f, turns_g, mat_g, slope, bend


def column_call(kernel, smems, args, out_shape, scratch, name, away=(), **params):
    smem = pl.BlockSpec(memory_space=pltpu.SMEM)
    vmem = pl.BlockSpec(memory_space=pltpu.VMEM)
    anywhere = pl.BlockSpec(memory_space=pltpu.HBM)
    return pl.pallas_call(
        kernel,
        out_shape=jax.ShapeDtypeStruct(out_shape, jnp.float32),
        in_specs=[smem] * len(smems) + [anywhere if k in away else vmem for k in range(len(args))],
        out_specs=vmem,
        scratch_shapes=scratch,
        compiler_params=pltpu.CompilerParams(**{"vmem_limit_bytes": 24 << 20, **params}),
        cost_estimate=pl.CostEstimate(flops=10**10, bytes_accessed=16 * 2**20, transcendentals=0),
        name=name,
    )(*smems, *args)


def shared(residual, position, owner, tile_local, xi, amplitude):
    n = lax.axis_size(parts)
    n_base = lax.axis_size("base")
    n_slab = lax.axis_size("half") * lax.axis_size("quad")
    quads = lax.axis_size("quad")
    base, parity, quad = (lax.axis_index(axis) for axis in parts)
    place = 2 * (base * quads + quad) + parity
    rows, size = xi.shape
    depth = size // n
    half = depth // 2
    tiles = G // TILE

    row_turns, there, back_again = (jnp.asarray(x) for x in row_weights(n, size))
    block = (n, rows, depth)
    work = pltpu.VMEM((n, 2, rows, depth), jnp.float32)
    blocks = residual.shape[0]
    room = 2 * n_base * (2 * blocks // n)
    sent = pack(owner, tile_local, residual, position, n_base, n_slab, room)
    got, spectrum = exchange(sent, n_slab, xi, amplitude, row_turns, there)
    field = lax.all_to_all(spectrum, parts, split_axis=0, concat_axis=0, tiled=True)

    sources = n_slab * n_base
    codes = got[:, :, room, 0, :].reshape(sources, TILE).astype(jnp.int32)

    turns, firsts, undos, weights = grid_row_weights(n, size)
    halves = grid_rows_two(
        room,
        codes,
        jnp.asarray(firsts),
        got.reshape(sources * (room + 1), 4, TILE),
        jnp.asarray(turns),
        jnp.asarray(undos),
        jnp.asarray(weights),
    )
    whole = lax.all_to_all(halves, ("base", "quad"), split_axis=0, concat_axis=0, tiled=True)

    turns, mat_h, mat_f, turns_g, mat_g, slope, bend = (jnp.asarray(x) for x in column_tables(n, size))
    me = jnp.reshape(place, (1,)).astype(jnp.int32)
    sky = column_call(
        functools.partial(field_kernel, 1.0 / size),
        [me, bend],
        [field, turns, mat_h, slope],
        block,
        [work],
        "field",
    )
    pieces = 8
    dma = pltpu.SemaphoreType.DMA
    return amplitude * column_call(
        functools.partial(image_kernel, 1.0 / size),
        [],
        [whole, sky, turns_g, mat_g, mat_f, turns, row_turns, back_again],
        (rows, size),
        [
            pltpu.VMEM((n, 2, 2 * rows, depth), jnp.float32), pltpu.VMEM((n // 2, 2, 8, depth), jnp.float32),
            pltpu.VMEM(block, jnp.float32), pltpu.VMEM(block, jnp.float32), pltpu.VMEM(block, jnp.float32),
            pltpu.VMEM((n // 2, 8, depth), jnp.float32), dma, dma((pieces, n)), dma((pieces, n)),
        ],
        "image",
        away=(1,),
        vmem_limit_bytes=36 << 20,
        collective_id=1,
        has_side_effects=True,
    )


def solution(mesh):
    n_base, n_slab = mesh.shape["base"], mesh.shape["slab"]
    body, axes = general, both
    if n_base == 4 and n_slab == 2 * n_base and 2 * n_base * n_slab == G // TILE:
        body, axes = shared, parts
        mesh = jax.sharding.Mesh(mesh.devices.reshape(n_base, 2, n_slab // 2), parts)
    placed = (
        P(axes, None, None),
        P(axes, None, None),
        P(axes, None),
        P(axes),
        P(axes, None),
        P(axes, None),
    )
    return jax.shard_map(body, mesh=mesh, in_specs=placed, out_specs=P(axes, None), check_vma=False)
```

```python
import functools
import math

import jax
import jax.numpy as jnp
import numpy as np
from jax import lax
from jax.experimental import pallas as pl
from jax.experimental.pallas import tpu as pltpu
from jax.sharding import PartitionSpec as P

G = 8192
TILE = 128
both = ("base", "slab")
fine = lax.Precision.HIGHEST


def trig(product, modulus):
    angle = (product % modulus).astype(np.float64) * (2.0 * np.pi / modulus)
    return np.cos(angle), np.sin(angle)


def column_table(n, size):
    depth = size // n
    half = depth // 2
    i = np.arange(half)[None, :]
    j = np.arange(n)[:, None]
    low = n * i + j
    high = (-low) % size
    high[0, 0] = size // 2
    return np.concatenate([low, high], axis=1)


def row_tables(n, size):
    depth = size // n
    cols = column_table(n, size)
    oc, osn = trig(np.arange(n)[:, None] * np.arange(n)[None, :], n)
    outer = np.stack([oc, osn], axis=1)
    prod = np.arange(depth)[None, :, None] * cols[:, None, :]
    c, s = trig(prod, size)
    sign = np.where(np.arange(depth) < depth // 2, 1.0, -1.0)[None, None, :]
    inner = np.stack([c + s, sign * (c - s)], axis=1)
    return outer.astype(np.float32), inner.astype(np.float32)


def grid_row_tables(n, size):
    depth = G // n
    cols = column_table(n, size)
    half = cols.shape[1] // 2
    oc, osn = trig(np.arange(n)[:, None] * np.arange(n)[None, :], n)
    outer = np.stack([np.stack([oc, osn], 1), np.stack([-osn, oc], 1)], 0)
    low = cols[:, :half]
    high = cols[(-np.arange(n)) % n, half:]
    a = np.arange(depth)[None, :, None]
    out = []
    for part in (low, high):
        c, s = trig(a * (part[:, None, :] + G // 4), G)
        out.append(np.stack([np.concatenate([c, s], 2), np.concatenate([-s, c], 2)], 1))
    return outer.astype(np.float32), np.concatenate(out, axis=3).astype(np.float32)


def taps(cells, offsets):
    scaled = (cells - offsets) * 0.25
    kept = jnp.maximum(1.0 - scaled * scaled, 0.0)
    return kept * kept * kept


def split_three(x):
    high = x.astype(jnp.bfloat16)
    rest = x - high.astype(jnp.float32)
    middle = rest.astype(jnp.bfloat16)
    return high, middle, (rest - middle.astype(jnp.float32)).astype(jnp.bfloat16)


def grid_kernel(rows, info_ref, list_ref, data_ref, out_ref):
    count = info_ref[0]
    first = info_ref[1].astype(jnp.float32)
    out_ref[...] = jnp.zeros_like(out_ref)
    row_cells = lax.broadcasted_iota(jnp.int32, (rows, TILE), 0).astype(jnp.float32) + first
    col_cells = lax.broadcasted_iota(jnp.int32, (TILE, TILE), 0).astype(jnp.float32)

    def step(k, carry):
        packed = list_ref[k]
        index = packed // 256
        col = (packed // 2) % 128
        flip = (packed % 2).astype(jnp.float32)
        sign = 1.0 - 2.0 * flip
        start = 128.0 * flip
        block = data_ref[index]
        value = block[0:2, :]
        place = block[2:4, :]
        row_taps = taps(row_cells * sign + start, place[0:1, :])
        col_taps = taps(col_cells * sign + start, place[1:2, :])
        weighted = jnp.concatenate(
            [col_taps * value[0:1, :], col_taps * (value[1:2, :] * sign)], axis=0
        )
        rh, rm, rl = split_three(row_taps)
        wh, wm, wl = split_three(weighted)
        left = jnp.concatenate([rh, rh, rh, rm, rm, rl], axis=1)
        right = jnp.concatenate([wh, wm, wl, wh, wm, wh], axis=1)
        sub = lax.dot_general(
            left, right, (((1,), (1,)), ((), ())), preferred_element_type=jnp.float32
        )
        out_ref[0, col] += sub[:, :TILE]
        out_ref[1, col] += sub[:, TILE:]
        return carry

    lax.fori_loop(0, count, step, 0)


def grid_rows(info, table, gathered, rows):
    tiles = G // TILE
    smem = pl.BlockSpec(memory_space=pltpu.SMEM)
    vmem = pl.BlockSpec(memory_space=pltpu.VMEM)
    return pl.pallas_call(
        functools.partial(grid_kernel, rows),
        out_shape=jax.ShapeDtypeStruct((2, tiles, rows, TILE), jnp.float32),
        in_specs=[smem, smem, vmem],
        out_specs=vmem,
        compiler_params=pltpu.CompilerParams(vmem_limit_bytes=56 * 1024 * 1024),
        cost_estimate=pl.CostEstimate(
            flops=2 * 10**10, bytes_accessed=16 * 2**20, transcendentals=0
        ),
        name="grid_rows",
    )(info, table, gathered)


def einsum(form, *args, precision=lax.Precision.HIGH):
    return jnp.einsum(form, *args, precision=precision, preferred_element_type=jnp.float32)


def general(residual, position, owner, tile_local, xi, amplitude):
    n = lax.axis_size(both)
    n_base = lax.axis_size("base")
    n_slab = lax.axis_size("slab")
    me = lax.axis_index(both)
    rows, size = xi.shape
    depth = size // n
    half = depth // 2
    tiles = G // TILE

    region_rows = G // n_slab // TILE
    region_cols = G // n_base // TILE
    target = owner[:, 0]
    tile_row = (target % n_slab) * region_rows + tile_local // region_cols
    tile_col = (target // n_slab) * region_cols + tile_local % region_cols
    flip = tile_row >= tiles // 2
    tile_row = jnp.where(flip, tiles - 1 - tile_row, tile_row)
    tile_col = jnp.where(flip, tiles - 1 - tile_col, tile_col)
    code = tile_row * 256 + tile_col * 2 + flip.astype(jnp.int32)
    codes = lax.all_gather(code, both, axis=0, tiled=True)
    payload = jnp.concatenate([residual, position], axis=1)
    codes, payload = lax.optimization_barrier((codes, payload))
    gathered = lax.all_gather(payload, both, axis=0, tiled=True)
    blocks = codes.shape[0]
    grid_depth = G // 2 // n
    first_row = me * grid_depth
    mine = (codes // 256 == first_row // TILE).astype(jnp.int32)
    rank = jnp.where(mine == 1, jnp.cumsum(mine) - 1, -1)
    packed = lax.broadcasted_iota(jnp.int32, (blocks,), 0) * 256 + codes % 256
    spots = lax.broadcasted_iota(jnp.int32, (blocks, blocks), 0)
    table = jnp.sum(jnp.where(spots == rank[None, :], packed[None, :], 0), axis=1)
    info = jnp.stack([jnp.sum(mine), first_row % TILE]).astype(jnp.int32)

    outer, inner = row_tables(n, size)
    spectrum = (amplitude * xi).reshape(rows, n, depth)
    mid = einsum("rba,bqc->qcra", spectrum, outer)
    sent = einsum("cra,cae->cre", mid[0], inner[:, 0]) + einsum("cra,cae->cre", mid[1], inner[:, 1])
    sent, gathered = lax.optimization_barrier((sent, gathered))
    field = lax.all_to_all(sent, both, split_axis=0, concat_axis=0, tiled=True)
    field = field.reshape(size, depth)
    lane = lax.broadcasted_iota(jnp.int32, (1, depth), 1)
    still = (me == 0) & (lane % half == 0)

    def mirror(x):
        return jnp.where(still, x, jnp.roll(x, half, axis=-1))

    c_len = 128
    d_len = size // c_len
    bc, bs = (x.astype(np.float32) for x in trig(np.arange(c_len)[:, None] * np.arange(c_len)[None, :], c_len))
    shape = (c_len, d_len, depth)
    n0 = c_len * np.arange(d_len)[None, :] + np.arange(c_len)[:, None]
    ic, isn = (x.astype(np.float32) for x in trig(n0[:, :, None] * np.arange(d_len)[None, None, :], size))
    pair = jnp.stack([field.reshape(shape), mirror(field).reshape(shape)])
    first = np.stack([np.stack([bc, bs], 1), np.stack([bs, -bc], 1)], 0)
    turned = einsum("qbal,qbsc->csal", pair, first)
    second = np.stack([ic, -isn], axis=2)
    power = einsum("csal,cdsa->cdl", turned, second)
    sky = jnp.exp(power / size)

    grid = grid_rows(info, table, gathered, grid_depth)
    outer_g, inner_g = grid_row_tables(n, size)
    parts = tiles // n if tiles >= n else 1
    inner_len = G // n
    if inner_len >= TILE:
        view = grid.reshape(2, n, inner_len // TILE, grid_depth, TILE)
    else:
        flat = grid.transpose(0, 2, 1, 3).reshape(2, grid_depth, n, inner_len)
        view = flat.transpose(0, 2, 1, 3)[:, :, None]
        parts = 1
    lanes = view.shape[-1]
    stage = einsum("qbpra,qbsc->cspra", view, outer_g, precision=fine)
    inner_g = inner_g.reshape(n, 2, parts, lanes, 2 * depth)
    halves = einsum("cspra,cspae->cre", stage, inner_g, precision=fine)
    high = halves[:, :, depth:]
    high = jnp.concatenate([high[:1], jnp.flip(high[1:], axis=0)], axis=0)
    halves = jnp.concatenate([halves[:, :, :depth], high], axis=2)
    got = lax.all_to_all(halves, both, split_axis=0, concat_axis=0, tiled=True)
    got = got.reshape(size, 2 * depth)
    real = jnp.concatenate([got[:, :half], got[:, depth : depth + half]], axis=1)
    imag = jnp.concatenate([got[:, half:depth], got[:, depth + half :]], axis=1)
    wide = G // c_len
    deep = size // wide
    gc, gs = (x.astype(np.float32) for x in trig(np.arange(deep)[:, None] * np.arange(c_len)[None, :], c_len))
    first_g = np.stack([np.stack([gc, gs], 1), np.stack([-gs, gc], 1)], 0)
    whole = jnp.stack([real.reshape(deep, wide, depth), imag.reshape(deep, wide, depth)])
    turned_g = einsum("qbal,qbsc->csal", whole, first_g, precision=fine)
    ac, asn = trig((n0 + G // 4)[:, :, None] * np.arange(wide)[None, None, :], G)
    second_g = (np.stack([ac, -asn], axis=2) / G).astype(np.float32)
    back = einsum("csal,cdsa->cdl", turned_g, second_g, precision=fine)

    z = sky * back
    pz = einsum("cdl,cda->cal", z, ic)
    qz = einsum("cdl,cda->cal", z, isn)
    joined = jnp.stack([pz + mirror(qz), mirror(pz) - qz])
    fold = einsum("qcal,qcb->bal", joined, np.stack([bc, bs]))
    folded = lax.all_to_all(
        fold.reshape(n, rows, depth), both, split_axis=0, concat_axis=0, tiled=True
    )
    ends = einsum("jre,jqae->qjra", folded, inner)
    final = einsum("qjra,bqj->rba", ends, outer)
    return amplitude * final.reshape(rows, size) / size


MESH = pl.DeviceIdType.MESH
parts = ("base", "half", "quad")
LANES = 6


def two_parts(x):
    high = x.astype(jnp.bfloat16)
    return high, (x - high.astype(jnp.float32)).astype(jnp.bfloat16)


def through(x, weight_ref, which):
    rows, depth = x.shape
    high, low = two_parts(x)
    made = jnp.dot(jnp.concatenate([high, low], axis=0), weight_ref[which, :depth], preferred_element_type=jnp.float32)
    return made[:rows] + made[rows:] + jnp.dot(high, weight_ref[which, depth:], preferred_element_type=jnp.float32)


def times(x, c, s):
    return x[0] * c - x[1] * s, x[0] * s + x[1] * c


def turn(x, angle):
    c, s = math.cos(angle), math.sin(angle)
    return times(x, c, s)


def add(x, y):
    return x[0] + y[0], x[1] + y[1]


def sub(x, y):
    return x[0] - y[0], x[1] - y[1]


def four(x):
    s0, d0, s1, d1 = add(x[0], x[2]), sub(x[0], x[2]), add(x[1], x[3]), sub(x[1], x[3])
    i1 = (-d1[1], d1[0])
    return [add(s0, s1), add(d0, i1), sub(s0, s1), sub(d0, i1)]


def sixteen(x):
    rows = []
    for b0 in range(4):
        y = four([x[4 * b1 + b0] for b1 in range(4)])
        rows.append([y[a0] if a0 * b0 == 0 else turn(y[a0], 2 * math.pi * a0 * b0 / 16) for a0 in range(4)])
    out = [None] * 16
    for a0 in range(4):
        y = four([rows[b0][a0] for b0 in range(4)])
        for a1 in range(4):
            out[a0 + 4 * a1] = y[a1]
    return out


def seat(j, quads):
    a = j // 2
    return a // quads * (2 * quads) + j % 2 * quads + a % quads


def transform_rows(quads, xi_ref, amplitude_ref, turn_ref, mat_ref, out_ref, work_ref):
    n = out_ref.shape[0]

    def outer(k, carry):
        spot = pl.ds(pl.multiple_of(k * 8, 8), 8)
        for e in range(2):
            x = []
            for b in range(n // 2):
                first, second = (
                    xi_ref[spot, c * TILE : (c + 1) * TILE] * amplitude_ref[spot, c * TILE : (c + 1) * TILE]
                    for c in (b, b + n // 2)
                )
                value = first - second if e else first + second
                if e * b:
                    angle = 2 * math.pi * b / n
                    x.append((value * math.cos(angle), value * math.sin(angle)))
                else:
                    x.append((value, jnp.zeros_like(value)))
            for v, value in enumerate(sixteen(x)):
                j = 2 * v + e
                work_ref[j, 0, spot, :], work_ref[j, 1, spot, :] = times(value, turn_ref[j, 0:1, :], turn_ref[j, 1:2, :])
        return carry

    lax.fori_loop(0, xi_ref.shape[0] // 8, outer, 0)
    rows = xi_ref.shape[0]

    def left(entries):
        return jnp.concatenate([jnp.concatenate([work_ref[j, 0], work_ref[j, 1]], axis=1) for j in entries], axis=0)

    def inner(k, carry):
        entries = [4 * k + q for q in range(4)]
        made = through(left(entries), mat_ref, 0)
        for q, j in enumerate(entries):
            out_ref[seat(j, quads)] = made[q * rows : (q + 1) * rows]
        return carry

    lax.fori_loop(0, n // 4, inner, 0)
    out_ref[0] = through(left([0]), mat_ref, 1)


def seats(base, quad):
    return base // 2, base % 2, quad // 2, quad % 2


def group_of(base, quad):
    y, x, low, core = seats(base, quad)
    return 2 * x + low, 2 * y + core


def exchange_kernel(send_ref, xi_ref, amplitude_ref, turn_ref, mat_ref, out_ref, spectrum_ref, work_ref, made_ref, rows_ref, rows_sem, bsend, brecv, zsend, zrecv, ysend, yrecv, csend, crecv, lsem):
    nb = send_ref.shape[0]
    quads = lax.axis_size("quad")
    half = lax.axis_index("half")
    y, x, low, core = seats(lax.axis_index("base"), lax.axis_index("quad"))
    group = 2 * x + low

    def at(y, group, half, core):
        return (2 * y + group // 2, half, group % 2 * 2 + core)

    def block(y, half, core, k):
        return out_ref.at[(2 * y + half) * 2 + core, (group - k + nb) % nb]

    def copy(part, here, there, device):
        return pltpu.make_async_remote_copy(
            src_ref=part, dst_ref=part, send_sem=here, recv_sem=there, device_id=device, device_id_type=MESH
        )

    def moved(target, source, k):
        return pltpu.make_async_remote_copy(
            src_ref=send_ref.at[target],
            dst_ref=out_ref.at[(2 * y + half) * 2 + core, source],
            send_sem=bsend.at[k],
            recv_sem=brecv.at[k],
            device_id=at(y, target, half, core),
            device_id_type=MESH,
        )

    far, beside, partner = at(y, group, 1 - half, core), at(1 - y, group, half, core), at(y, group, half, 1 - core)

    def along_z(own, k):
        return copy(block(y, half if own else 1 - half, core, k), zsend.at[k], zrecv.at[k], far)

    def along_y(own, kind, k):
        place = half if kind == 0 else 1 - half
        return copy(block(y if own else 1 - y, place, core, k), ysend.at[kind, k], yrecv.at[kind, k], beside)

    def over(own, kind, k):
        row = y if kind < 2 else 1 - y
        place = half if kind % 2 == 0 else 1 - half
        return copy(block(row, place, core if own else 1 - core, k), csend.at[kind, k], crecv.at[kind, k], partner)

    fetches = [
        pltpu.make_async_copy(source, rows_ref.at[k], rows_sem.at[k]) for k, source in enumerate((xi_ref, amplitude_ref))
    ]
    ready = pltpu.make_async_copy(made_ref, spectrum_ref, rows_sem.at[2])
    for fetch in fetches:
        fetch.start()
    barrier = pltpu.get_barrier_semaphore()
    peers = [at(y, (group + k) % nb, half, core) for k in range(1, nb)] + [far, beside, partner]
    for peer in peers:
        pl.semaphore_signal(barrier, inc=1, device_id=peer, device_id_type=MESH)
    pl.semaphore_wait(barrier, len(peers))

    own = pltpu.make_async_copy(send_ref.at[group], block(y, half, core, 0), lsem)
    own.start()
    for k in range(1, nb):
        moved((group + k) % nb, group, k).start()
    for k in range(nb):
        if k == 0:
            own.wait()
        else:
            moved((group - k + nb) % nb, (group - k + nb) % nb, k).wait_recv()
        along_z(True, k).start()
        along_y(True, 0, k).start()
        over(True, 0, k).start()
        if k == 0:
            for fetch in fetches:
                fetch.wait()
            transform_rows(quads, rows_ref.at[0], rows_ref.at[1], turn_ref, mat_ref, made_ref, work_ref)
            ready.start()
    for k in range(nb):
        along_z(False, k).wait_recv()
        along_y(True, 1, k).start()
        over(True, 1, k).start()
    for kind in range(2):
        for k in range(nb):
            along_y(False, kind, k).wait_recv()
            over(True, 2 + kind, k).start()
    ready.wait()
    for kind in range(4):
        for k in range(nb):
            over(False, kind, k).wait_recv()
    for k in range(nb):
        if k:
            moved((group + k) % nb, group, k).wait_send()
        along_z(True, k).wait_send()
        for kind in range(2):
            along_y(True, kind, k).wait_send()
        for kind in range(4):
            over(True, kind, k).wait_send()


def pack_kernel(ns, tiles, room, owner_ref, local_ref, residual_ref, position_ref, out_ref):
    blocks = residual_ref.shape[0]
    nb = out_ref.shape[0]
    across = lax.broadcasted_iota(jnp.int32, (blocks, blocks), 1)
    down = lax.broadcasted_iota(jnp.int32, (blocks, blocks), 0)

    def column(row):
        return jnp.sum(jnp.where(across == down, row, 0.0), axis=1, keepdims=True)

    def divided(x, d):
        whole = jnp.floor((x + 0.5) * (1.0 / d))
        return whole, x - whole * d

    local = local_ref[...].astype(jnp.float32)
    target = owner_ref[...].astype(jnp.float32)
    region_col, region_row = divided(target, ns)
    tile_row, tile_col = divided(local, tiles // nb)
    tile_row = tile_row + region_row * (tiles // ns)
    tile_col = tile_col + region_col * (tiles // nb)
    flip = jnp.where(tile_row >= tiles // 2, 1.0, 0.0)
    tile_row = jnp.where(flip > 0.5, tiles - 1 - tile_row, tile_row)
    tile_col = jnp.where(flip > 0.5, tiles - 1 - tile_col, tile_col)
    line, within = divided(tile_row, ns)
    key = divided(tile_row, 2)[0]
    code = divided(within, 2)[1] * tiles + tile_col
    keys = ns // 2
    line_down, key_down, flip_down = column(line), column(key), column(flip)
    before = (line_down == line) & ((key_down < key) | ((key_down == key) & (down < across)))
    slot = line * room + jnp.sum(jnp.where(before, 1.0, 0.0), axis=0, keepdims=True)
    slots = lax.broadcasted_iota(jnp.int32, (nb * room, blocks), 0).astype(jnp.float32)
    chosen = jnp.where(slots == slot, 1.0, 0.0).astype(jnp.bfloat16)
    sides = [residual_ref[:, 0, :], residual_ref[:, 1, :] * (1.0 - 2.0 * flip_down)]
    for k in range(2):
        place = position_ref[:, k, :]
        sides.append(jnp.where(flip_down > 0.5, TILE - place, place))
    pieces = split_three(jnp.concatenate(sides, axis=1))
    moved = jnp.dot(
        jnp.concatenate([chosen] * 3, axis=1), jnp.concatenate(pieces, axis=0), preferred_element_type=jnp.float32
    )
    codes = 0.0
    for part in two_parts(jnp.broadcast_to(code + 1.0, (8, blocks))):
        codes = codes + lax.dot_general(part, chosen, (((1,), (1,)), ((), ())), preferred_element_type=jnp.float32)
    codes = codes - 1.0
    lanes = lax.broadcasted_iota(jnp.int32, (1, blocks), 1)
    shift = (across - room).astype(jnp.float32)
    per = blocks // room
    for k in range(nb):
        for c in range(4):
            out_ref[k, :room, c, :] = moved[k * room : (k + 1) * room, c * TILE : (c + 1) * TILE]
        start = k // per * blocks
        own = codes[:, start : start + blocks]
        if k % per:
            own = pltpu.roll(own, blocks - k % per * room, 1)
        earlier = (line_down == k) & (key_down - keys * k < shift)
        starts = jnp.sum(jnp.where(earlier, 1.0, 0.0), axis=0, keepdims=True)
        out_ref[k, room] = jnp.broadcast_to(jnp.where(lanes < room, own[0:1, :], starts), (4, TILE))


def pack(owner, local, residual, position, nb, ns, room):
    vmem = pl.BlockSpec(memory_space=pltpu.VMEM)
    return pl.pallas_call(
        functools.partial(pack_kernel, ns, G // TILE, room),
        out_shape=jax.ShapeDtypeStruct((nb, room + 1, 4, TILE), jnp.float32),
        in_specs=[vmem] * 4,
        out_specs=vmem,
        compiler_params=pltpu.CompilerParams(vmem_limit_bytes=60 << 20),
        name="pack",
    )(owner.reshape(1, -1), local.reshape(1, -1), residual, position)


def exchange(sent, ns, xi, amplitude, turns, mats):
    nb = sent.shape[0]
    rows, n = xi.shape[0], turns.shape[0]
    dma = pltpu.SemaphoreType.DMA
    vmem = pl.BlockSpec(memory_space=pltpu.VMEM)
    hbm = pl.BlockSpec(memory_space=pltpu.HBM)
    return pl.pallas_call(
        exchange_kernel,
        out_shape=(
            jax.ShapeDtypeStruct((ns,) + sent.shape, jnp.float32),
            jax.ShapeDtypeStruct((n, rows, TILE), jnp.float32),
        ),
        in_specs=[vmem, hbm, hbm, vmem, vmem],
        out_specs=(hbm, hbm),
        scratch_shapes=[
            pltpu.VMEM((n, 2, rows, TILE), jnp.float32),
            pltpu.VMEM((n, rows, TILE), jnp.float32),
            pltpu.VMEM((2,) + xi.shape, jnp.float32), dma((3,)),
            dma((nb,)), dma((nb,)), dma((nb,)), dma((nb,)), dma((2, nb)), dma((2, nb)), dma((4, nb)), dma((4, nb)), dma,
        ],
        compiler_params=pltpu.CompilerParams(collective_id=0, has_side_effects=True, vmem_limit_bytes=60 << 20),
        cost_estimate=pl.CostEstimate(flops=3 * 10**10, bytes_accessed=16 * 2**20, transcendentals=0),
        name="exchange",
    )(sent, xi, amplitude, turns, mats)


def grid_kernel_two(room, codes_ref, first_ref, data_hbm_ref, turn_ref, undo_ref, weight_hbm_ref, away_ref, grid_ref, left_ref, right_ref, out_ref, data_ref, weight_ref, list_ref, sems):
    quad = group_of(lax.axis_index("base"), lax.axis_index("quad"))[1]
    parity = lax.axis_index("half")
    data = pltpu.make_async_copy(data_hbm_ref, data_ref, sems.at[out_ref.shape[0]])
    weight = pltpu.make_async_copy(weight_hbm_ref, weight_ref, sems.at[out_ref.shape[0] + 1])
    data.start()
    weight.start()
    grid_ref[...] = jnp.zeros_like(grid_ref)
    half = grid_ref.shape[1]
    group = 16
    cells = lax.broadcasted_iota(jnp.int32, (group + 8, TILE), 0).astype(jnp.float32) * 0.25
    nothing = jnp.zeros((group, TILE), jnp.bfloat16)

    def bump(offsets):
        d = cells - offsets
        kept = jnp.maximum(1.0 - d * d, 0.0)
        return kept * kept * kept

    def window(offsets):
        start = jnp.floor((offsets - 4.0) * (1.0 / group))
        offsets = (offsets - start * group) * 0.25
        return bump(offsets) - bump(offsets - 0.25), jnp.broadcast_to(start, (group, TILE)).astype(jnp.bfloat16)

    def spread(compact, start):
        padded = jnp.concatenate([compact, jnp.zeros((8, TILE), jnp.float32)], axis=0)
        out = []
        for part in two_parts(padded):
            first, second = part[:group], part[group:]
            pieces = []
            for g in range(TILE // group):
                piece = jnp.where(start == g - 1, second, nothing) if g else nothing
                pieces.append(jnp.where(start == g, first, piece))
            out.append(jnp.concatenate(pieces, axis=0))
        return out

    lanes = left_ref.shape[0]

    def place(k):
        packed = list_ref[k]
        return packed & (2 * half - 1), lax.shift_right_logical(packed, half.bit_length())

    def prepare(k, lane, count):
        col, rest = place(k)
        odd = jnp.where(col >= half, parity, 0)
        sign = jnp.where(k < count, 1 - 2 * odd, 0).astype(jnp.float32)
        block = data_ref[rest // 2]
        value = block[0:2, :] * sign
        row_taps, row_start = window(block[2:3, :])
        col_taps, col_start = window(block[3:4, :])
        rows_split = spread(row_taps, row_start)
        real = spread(col_taps * value[0:1, :], col_start)
        imag = spread(col_taps * value[1:2, :], col_start)
        for q in range(2):
            left_ref[lane, :, q * TILE : (q + 1) * TILE] = rows_split[q]
            right_ref[lane, :TILE, q * TILE : (q + 1) * TILE] = real[q]
            right_ref[lane, TILE:, q * TILE : (q + 1) * TILE] = imag[q]

    def product(lane):
        rh, rl = left_ref[lane, :, :TILE], left_ref[lane, :, TILE:]
        wh, wl = right_ref[lane, :, :TILE], right_ref[lane, :, TILE:]
        left = jnp.concatenate([rh, rh, rl], axis=1)
        right = jnp.concatenate([wh, wl, wh], axis=1)
        return lax.dot_general(left, right, (((1,), (1,)), ((), ())), preferred_element_type=jnp.float32)

    def step(k, carry):
        made = [product(lane) for lane in range(lanes)]
        for lane in range(lanes):
            prepare((k + 1) * lanes + lane, lane, count)
        for lane in range(lanes):
            col, rest = place(k * lanes + lane)
            col = jnp.where(col >= half, col - half, col)
            spot = pl.ds(pl.multiple_of((rest % 2) * TILE, TILE), TILE)
            grid_ref[0, col, spot, :] += made[lane][:, :TILE]
            grid_ref[1, col, spot, :] += made[lane][:, TILE:]
        return carry

    per = 4 * half

    def gather(source, filled):
        start = codes_ref[source, room + quad]
        stop = codes_ref[source, room + quad + 1]

        shift = filled - start
        first = source * ((room + 1) * per)

        def entry(i, carry):
            list_ref[shift + i] = first + i * per + codes_ref[source, i]
            return carry

        lax.fori_loop(start, stop, entry, 0)
        return filled + stop - start

    count = lax.fori_loop(0, codes_ref.shape[0], gather, 0)
    for lane in range(2 * lanes):
        list_ref[count + lane] = 0
    data.wait()
    for lane in range(lanes):
        prepare(lane, lane, count)
    lax.fori_loop(0, (count + lanes - 1) // lanes, step, 0)

    depth = half // 2
    rows = grid_ref.shape[2]

    def outer(k, carry):
        spot = pl.ds(pl.multiple_of(k * 8, 8), 8)
        for side in range(2):
            x = []
            for b in range(depth):
                value = grid_ref[0, 2 * b + side, spot, :], grid_ref[1, 2 * b + side, spot, :]
                x.append(times(value, first_ref[parity, b, 0], first_ref[parity, b, 1]))
            for a, value in enumerate(sixteen(x)):
                c = turn_ref[parity, a, side : side + 1, :]
                s = turn_ref[parity, a, 2 + side : 3 + side, :]
                value = times(value, c, s)
                grid_ref[0, 2 * a + side, spot, :] = value[0]
                grid_ref[1, 2 * a + side, spot, :] = value[1]
        return carry

    lax.fori_loop(0, rows // 8, outer, 0)

    def inner(a, carry):
        mirrored = depth - parity - a
        mirrored = jnp.where(mirrored == depth, 0, mirrored)
        which = jnp.where((a == 0) & (parity == 0), 1, 0)
        for part in range(1):
            spot = pl.ds(0, rows)
            x = jnp.concatenate([grid_ref[q, 2 * a + side, spot, :] for q in range(2) for side in range(2)], axis=1)
            made = through(x, weight_ref, which)
            mid = TILE // 2
            made = times((made[:, :TILE], made[:, TILE:]), undo_ref[parity, a, 0:1, :], undo_ref[parity, a, 1:2, :])
            for q in range(2):
                out_ref[a, spot, q * TILE : q * TILE + mid] = made[q][:, :mid]
                out_ref[mirrored, spot, q * TILE + mid : (q + 1) * TILE] = made[q][:, mid:]

        @pl.when(a >= depth // 2)
        def _():
            leave(a).start()
            leave(jnp.where((parity == 0) & (a == depth // 2), 0, mirrored)).start()

        return carry

    def leave(a):
        return pltpu.make_async_copy(out_ref.at[a], away_ref.at[a], sems.at[a])

    weight.wait()
    lax.fori_loop(0, depth, inner, 0)
    for a in range(depth):
        leave(a).wait()


def split_table(x):
    high = x.astype(np.float32).astype(jnp.bfloat16)
    low = (x - high.astype(np.float64)).astype(np.float32).astype(jnp.bfloat16)
    return high, low


def undone(pixels):
    c, s = trig(pixels + G // 4, G)
    return 1.0 / (1.0 - (c - 1j * s))


def grid_row_weights(n, size):
    depth = n // 2
    span = G // 2 // depth
    half = size // n // 2
    alpha = np.arange(span)
    turns, firsts, undos = [], [], []
    for p in range(2):
        j = 2 * np.arange(depth) + p
        c, s = trig(j[:, None] * alpha[None, :], G)
        turns.append(np.concatenate([c.reshape(depth, 2, TILE), s.reshape(depth, 2, TILE)], axis=1))
        firsts.append(np.stack(trig(np.arange(depth) * p, n), axis=1))
        low = n * np.arange(half)[None, :] + j[:, None]
        high = size - n * np.arange(half)[None, :] - ((-j) % n)[:, None]
        if p == 0:
            low[0, 0], high[0, 0] = 0, size // 2
        undo = undone(np.concatenate([low, high], axis=1))
        undos.append(np.stack([undo.real, undo.imag], axis=1))
    weights = []
    i = np.arange(half)
    for special in range(2):
        low = n * i
        high = size - n * i - (0 if special else n)
        if special:
            high[0] = size // 2
        parts_re, parts_im = [], []
        for cols in (low, high):
            c, s = trig(alpha[:, None] * (cols[None, :] + G // 4), G)
            parts_re.append(np.concatenate([c, -s], axis=0))
            parts_im.append(np.concatenate([s, c], axis=0))
        w = np.concatenate(parts_re + parts_im, axis=1)
        weights.append(np.concatenate(split_table(w), axis=0))
    turns, firsts, undos = (np.stack(x).astype(np.float32) for x in (turns, firsts, undos))
    return turns, firsts, undos, np.stack(weights)


def grid_rows_two(room, codes, first, data, turns, undos, weights):
    depth = turns.shape[1]
    rows = 2 * TILE
    smem = pl.BlockSpec(memory_space=pltpu.SMEM)
    vmem = pl.BlockSpec(memory_space=pltpu.VMEM)
    hbm = pl.BlockSpec(memory_space=pltpu.HBM)
    return pl.pallas_call(
        functools.partial(grid_kernel_two, room),
        out_shape=jax.ShapeDtypeStruct((depth, rows, 2 * TILE), jnp.float32),
        in_specs=[smem, smem, hbm, vmem, vmem, hbm],
        out_specs=hbm,
        scratch_shapes=[
            pltpu.VMEM((2, 2 * depth, rows, TILE), jnp.float32),
            pltpu.VMEM((LANES, TILE, 2 * TILE), jnp.bfloat16),
            pltpu.VMEM((LANES, 2 * TILE, 2 * TILE), jnp.bfloat16),
            pltpu.VMEM((depth, rows, 2 * TILE), jnp.float32),
            pltpu.VMEM(data.shape, jnp.float32),
            pltpu.VMEM(weights.shape, jnp.bfloat16),
            pltpu.SMEM((codes.shape[0] * room + 2 * LANES,), jnp.int32),
            pltpu.SemaphoreType.DMA((depth + 2,)),
        ],
        compiler_params=pltpu.CompilerParams(vmem_limit_bytes=60 << 20),
        cost_estimate=pl.CostEstimate(flops=2 * 10**10, bytes_accessed=16 * 2**20, transcendentals=0),
        name="grid_rows_two",
    )(codes, first, data, turns, undos, weights)


def minus(x):
    return [(b, a) for a, b in sixteen([(b, a) for a, b in x])]


def pick(table, u):
    side = table.shape[1] // 2
    return table[:, u : u + 1], table[:, side + u : side + u + 1]


def mirrored(x, still):
    return jnp.where(still, x, pltpu.roll(x, x.shape[1] // 2, 1))


def still_lanes(place, rows):
    lane = lax.broadcasted_iota(jnp.int32, (rows, TILE), 1)
    return (lane % (TILE // 2) == 0) & (place == 0)


def product(mat_ref, x):
    rows = mat_ref.shape[0] // 2
    high, low = two_parts(x)
    made = jnp.dot(mat_ref[...], high, preferred_element_type=jnp.float32)
    return made[:rows] + made[rows:] + jnp.dot(mat_ref[:rows], low, preferred_element_type=jnp.float32)


def beside(work_ref, u):
    sides = [jnp.concatenate([work_ref[u + q, 0], work_ref[u + q, 1]], axis=0) for q in range(2)]
    return jnp.concatenate(sides, axis=1)


def field_kernel(scale, info_ref, bend_ref, field_ref, turn_ref, mat_ref, slope_ref, sky_ref, work_ref):
    still = still_lanes(info_ref[0], 8)
    n = field_ref.shape[0]

    def outer(k, carry):
        spot = pl.ds(pl.multiple_of(k * 8, 8), 8)
        table = turn_ref[spot, :]
        for e in range(2):
            x = []
            for d in range(n // 2):
                first, second = field_ref[d, spot, :], field_ref[d + n // 2, spot, :]
                value = first - second if e else first + second
                value = value, mirrored(value, still)
                x.append(turn(value, -2 * math.pi * d / n) if e * d else value)
            for v, value in enumerate(minus(x)):
                u = 2 * v + e
                work_ref[u, 0, spot, :], work_ref[u, 1, spot, :] = times(value, *pick(table, u))
        return carry

    lax.fori_loop(0, field_ref.shape[1] // 8, outer, 0)

    def inner(k, carry):
        for u in (4 * k, 4 * k + 2):
            made = jnp.exp(product(mat_ref, beside(work_ref, u)) * scale)
            for q in range(2):
                sine = slope_ref[0] * bend_ref[u + q, 0] + slope_ref[1] * bend_ref[u + q, 1]
                sky_ref[u + q] = made[:, q * TILE : (q + 1) * TILE] / sine
        return carry

    lax.fori_loop(0, n // 4, inner, 0)


def image_kernel(scale, whole_ref, sky_ref, turn_g_ref, mat_g_ref, mat_f_ref, turn_ref, turn_r_ref, mat_r_ref, out_ref, work_ref, half_ref, held_ref, fold_ref, folded_ref, real_ref, held_sem, send_sems, recv_sems):
    n = sky_ref.shape[0]
    quads = lax.axis_size("quad")
    halves = lax.axis_size("half")
    me = (lax.axis_index("base") * halves + lax.axis_index("half")) * quads + lax.axis_index("quad")
    place = 2 * (lax.axis_index("base") * quads + lax.axis_index("quad")) + lax.axis_index("half")
    still = still_lanes(place, 8)
    pieces = send_sems.shape[0]
    span = TILE // pieces

    def at(device):
        return (device // (halves * quads), device // quads % halves, device % quads)

    def sending(c, k):
        target = (me + k) % n
        part = pl.ds(c * span, span)
        return pltpu.make_async_remote_copy(
            src_ref=fold_ref.at[target, part], dst_ref=folded_ref.at[me, part],
            send_sem=send_sems.at[c, k], recv_sem=recv_sems.at[c, k], device_id=at(target), device_id_type=MESH,
        )

    def arriving(c, k):
        source = (me - k + n) % n
        part = pl.ds(c * span, span)
        return pltpu.make_async_remote_copy(
            src_ref=fold_ref.at[source, part], dst_ref=folded_ref.at[source, part],
            send_sem=send_sems.at[c, k], recv_sem=recv_sems.at[c, k], device_id=at(source), device_id_type=MESH,
        )

    barrier = pltpu.get_barrier_semaphore()

    def greet(k, carry):
        pl.semaphore_signal(barrier, inc=1, device_id=at((me + k) % n), device_id_type=MESH)
        return carry

    lax.fori_loop(1, n, greet, 0)
    origins = [0] * (n // 2)
    for k in range(n // 2):
        group, member = group_of(k // quads, k % quads)
        origins[group * quads + member] = k
    fetch = pltpu.make_async_copy(sky_ref, held_ref, held_sem)
    fetch.start()
    depth = n // 2

    def outer(k, carry):
        spot = pl.ds(pl.multiple_of(k * 8, 8), 8)
        table = turn_g_ref[spot, :]
        for e in range(2):
            x = []
            for a in range(depth):
                value = whole_ref[origins[a], spot, :TILE], whole_ref[origins[a], spot, TILE:]
                x.append(turn(value, 2 * math.pi * a / n) if e * a else value)
            for v, value in enumerate(sixteen(x)):
                u = 2 * v + e
                work_ref[u, 0, spot, :], work_ref[u, 1, spot, :] = times(value, *pick(table, u))
        return carry

    lax.fori_loop(0, whole_ref.shape[1] // 8, outer, 0)

    fetch.wait()

    def inner(k, carry):
        for u in (4 * k, 4 * k + 2):
            made = product(mat_g_ref, beside(work_ref, u))
            z = jnp.concatenate([made[:, q * TILE : (q + 1) * TILE] * held_ref[u + q] for q in range(2)], axis=1)
            spread = product(mat_f_ref, z)
            for q in range(2):
                for c in range(2):
                    work_ref[u + q, c, :TILE, :] = spread[c * TILE : (c + 1) * TILE, q * TILE : (q + 1) * TILE]
        return carry

    lax.fori_loop(0, n // 4, inner, 0)

    def last(k, carry):
        spot = pl.ds(pl.multiple_of(k * 8, 8), 8)
        table = turn_ref[spot, :]
        for e in range(2):
            x = []
            for v in range(depth):
                u = 2 * v + e
                x.append(times((work_ref[u, 0, spot, :], work_ref[u, 1, spot, :]), *pick(table, u)))
            for d, value in enumerate(minus(x)):
                if e == 0:
                    half_ref[d, 0], half_ref[d, 1] = value
                    continue
                value = turn(value, -2 * math.pi * d / n) if d else value
                before = half_ref[d, 0], half_ref[d, 1]
                for side, both_parts in enumerate((add(before, value), sub(before, value))):
                    fold_ref[d + side * depth, spot, :] = both_parts[0] - mirrored(both_parts[1], still)
        return carry

    def send(c, k, carry):
        sending(c, k).start()
        return carry

    for c in range(pieces):
        lax.fori_loop(c * span // 8, (c + 1) * span // 8, last, 0)
        if c == 0:
            pl.semaphore_wait(barrier, n - 1)
        lax.fori_loop(1, n, functools.partial(send, c), 0)
    folded_ref[me] = fold_ref[me]

    def receive(source):
        a = source // (halves * quads) * quads + source % quads
        j = 2 * a + source // quads % halves
        made = through(folded_ref[source], mat_r_ref, jnp.where(j == 0, 1, 0))
        work_ref[j, 0, :TILE, :], work_ref[j, 1, :TILE, :] = made[:, :TILE], made[:, TILE:]

    receive(me)

    def arrive(k, carry):
        for c in range(pieces):
            arriving(c, k).wait_recv()
        receive((me - k + n) % n)
        return carry

    lax.fori_loop(1, n, arrive, 0)

    def gradient(k, carry):
        spot = pl.ds(pl.multiple_of(k * 8, 8), 8)
        for e in range(2):
            x = []
            for v in range(depth):
                j = 2 * v + e
                x.append(times((work_ref[j, 0, spot, :], work_ref[j, 1, spot, :]), turn_r_ref[j, 0:1, :], turn_r_ref[j, 1:2, :]))
            for b, value in enumerate(sixteen(x)):
                if e == 0:
                    real_ref[b] = value[0]
                    continue
                real = turn(value, 2 * math.pi * b / n)[0] if b else value[0]
                for c, total in ((b, real_ref[b] + real), (b + depth, real_ref[b] - real)):
                    lanes = slice(c * TILE, (c + 1) * TILE)
                    out_ref[spot, lanes] = total * scale
        return carry

    lax.fori_loop(0, TILE // 8, gradient, 0)

    def sent(k, carry):
        for c in range(pieces):
            sending(c, k).wait_send()
        return carry

    lax.fori_loop(1, n, sent, 0)


def row_weights(n, size):
    alpha = np.arange(TILE)
    i = np.arange(size // n // 2)
    turns = np.stack(trig(np.arange(n)[:, None] * alpha[None, :], size), axis=1).astype(np.float32)
    c, s = trig(alpha[:, None] * i[None, :], size // n)
    there, back = [], []
    for special in range(2):
        real = np.concatenate([c + s, c - s], axis=1)
        imag = np.concatenate([c - s, -c - s], axis=1)
        from_real = np.concatenate([c + s, c - s], axis=1)
        from_imag = np.concatenate([s - c, s + c], axis=1)
        if special:
            lane = len(i)
            real[:, lane] = from_real[:, lane] = 1.0 - 2.0 * (alpha % 2)
            imag[:, lane] = from_imag[:, lane] = 0.0
        for target, matrix in ((there, np.concatenate([real, imag], axis=0)), (back, np.concatenate([from_real.T, from_imag.T], axis=1))):
            target.append(np.concatenate(split_table(matrix), axis=0))
    return turns, np.stack(there), np.stack(back)


def column_tables(n, size):
    w = np.arange(size // n)
    t = np.arange(TILE)
    u = np.arange(n)
    r = 2 * np.arange(2 * TILE) + 1
    side = TILE // 2

    def lanes(c, s):
        out = np.zeros((c.shape[0], TILE))
        out[:, :n], out[:, side : side + n] = c, s
        return out.astype(np.float32)

    def matrix(x):
        return np.concatenate(split_table(x), axis=0)

    c, s = trig(t[:, None] * u[None, :], size)
    turns = lanes(c, -s)
    c, s = trig(w[:, None] * t[None, :], size // n)
    mat_h = matrix(np.concatenate([c, s], axis=1))
    mat_f = matrix(np.concatenate([c.T, -s.T], axis=0))
    c, s = trig(r[:, None] * u[None, :], 2 * G)
    turns_g = lanes(c, s)
    c, s = trig((w[:, None] * n + G // 4) * r[None, :], 2 * G)
    mat_g = matrix(np.concatenate([s, c], axis=1))
    c, s = trig(w * n + G // 4, 2 * G)
    slope = np.stack([s, c]) * (2.0 * G)
    slope = np.broadcast_to(slope[:, :, None], slope.shape + (TILE,)).astype(np.float32)
    c, s = trig(u, 2 * G)
    bend = np.stack([c, s], axis=1).astype(np.float32)
    return turns, mat_h, mat_f, turns_g, mat_g, slope, bend


def column_call(kernel, smems, args, out_shape, scratch, name, away=(), **params):
    smem = pl.BlockSpec(memory_space=pltpu.SMEM)
    vmem = pl.BlockSpec(memory_space=pltpu.VMEM)
    anywhere = pl.BlockSpec(memory_space=pltpu.HBM)
    return pl.pallas_call(
        kernel,
        out_shape=jax.ShapeDtypeStruct(out_shape, jnp.float32),
        in_specs=[smem] * len(smems) + [anywhere if k in away else vmem for k in range(len(args))],
        out_specs=vmem,
        scratch_shapes=scratch,
        compiler_params=pltpu.CompilerParams(**{"vmem_limit_bytes": 24 << 20, **params}),
        cost_estimate=pl.CostEstimate(flops=10**10, bytes_accessed=16 * 2**20, transcendentals=0),
        name=name,
    )(*smems, *args)


def shared(residual, position, owner, tile_local, xi, amplitude):
    n = lax.axis_size(parts)
    n_base = lax.axis_size("base")
    n_slab = lax.axis_size("half") * lax.axis_size("quad")
    quads = lax.axis_size("quad")
    base, parity, quad = (lax.axis_index(axis) for axis in parts)
    place = 2 * (base * quads + quad) + parity
    rows, size = xi.shape
    depth = size // n
    half = depth // 2
    tiles = G // TILE

    row_turns, there, back_again = (jnp.asarray(x) for x in row_weights(n, size))
    block = (n, rows, depth)
    work = pltpu.VMEM((n, 2, rows, depth), jnp.float32)
    blocks = residual.shape[0]
    room = 2 * n_base * (2 * blocks // n)
    sent = pack(owner, tile_local, residual, position, n_base, n_slab, room)
    got, spectrum = exchange(sent, n_slab, xi, amplitude, row_turns, there)
    field = lax.all_to_all(spectrum, parts, split_axis=0, concat_axis=0, tiled=True)

    sources = n_slab * n_base
    codes = got[:, :, room, 0, :].reshape(sources, TILE).astype(jnp.int32)

    turns, firsts, undos, weights = grid_row_weights(n, size)
    halves = grid_rows_two(
        room,
        codes,
        jnp.asarray(firsts),
        got.reshape(sources * (room + 1), 4, TILE),
        jnp.asarray(turns),
        jnp.asarray(undos),
        jnp.asarray(weights),
    )
    whole = lax.all_to_all(halves, ("base", "quad"), split_axis=0, concat_axis=0, tiled=True)

    turns, mat_h, mat_f, turns_g, mat_g, slope, bend = (jnp.asarray(x) for x in column_tables(n, size))
    me = jnp.reshape(place, (1,)).astype(jnp.int32)
    sky = column_call(
        functools.partial(field_kernel, 1.0 / size),
        [me, bend],
        [field, turns, mat_h, slope],
        block,
        [work],
        "field",
    )
    pieces = 2
    dma = pltpu.SemaphoreType.DMA
    return amplitude * column_call(
        functools.partial(image_kernel, 1.0 / size),
        [],
        [whole, sky, turns_g, mat_g, mat_f, turns, row_turns, back_again],
        (rows, size),
        [
            pltpu.VMEM((n, 2, 2 * rows, depth), jnp.float32), pltpu.VMEM((n // 2, 2, 8, depth), jnp.float32),
            pltpu.VMEM(block, jnp.float32), pltpu.VMEM(block, jnp.float32), pltpu.VMEM(block, jnp.float32),
            pltpu.VMEM((n // 2, 8, depth), jnp.float32), dma, dma((pieces, n)), dma((pieces, n)),
        ],
        "image",
        away=(1,),
        vmem_limit_bytes=36 << 20,
        collective_id=1,
        has_side_effects=True,
    )


def solution(mesh):
    n_base, n_slab = mesh.shape["base"], mesh.shape["slab"]
    body, axes = general, both
    if n_base == 4 and n_slab == 2 * n_base and 2 * n_base * n_slab == G // TILE:
        body, axes = shared, parts
        mesh = jax.sharding.Mesh(mesh.devices.reshape(n_base, 2, n_slab // 2), parts)
    placed = (
        P(axes, None, None),
        P(axes, None, None),
        P(axes, None),
        P(axes),
        P(axes, None),
        P(axes, None),
    )
    return jax.shard_map(body, mesh=mesh, in_specs=placed, out_specs=P(axes, None), check_vma=False)
```
